32 devices in a mesh: dp: 4 (over y, z), tp: 8 (over x, core).
Axes of the slice: x: 4, y: 2, z: 2, core: 2. Of those that a mesh axis runs over, the one named last changes fastest.
The devices are a block of a 4x4x8 slice.
Arguments:
- x: bfloat16 [4, 2048, 1024], P('dp', 'tp'), parts along dimension 0
- ln1_gamma: float32 [1024], replicated
- ln1_beta: float32 [1024], replicated
- w_qkv: bfloat16 [1024, 16, 3, 64], P(None, 'tp')
- b_qkv: float32 [16, 3, 64], P('tp')
- w_out: bfloat16 [1024, 1024], P('tp')
- b_out: float32 [1024], replicated
- ln2_gamma: float32 [1024], replicated
- ln2_beta: float32 [1024], replicated
- w_up: bfloat16 [1024, 4096], P(None, 'tp')
- b_up: float32 [4096], P('tp')
- w_down: bfloat16 [4096, 1024], P('tp')
- b_down: float32 [1024], replicated
- grad_y: bfloat16 [4, 2048, 1024], P('dp', 'tp'), parts along dimension 0
Outputs:
- output 1: bfloat16 [4, 2048, 1024], P('dp', 'tp'), parts along dimension 0
- output 2: bfloat16 [4, 2048, 1024], P('dp', 'tp'), parts along dimension 0
- output 3: float32 [4096], P('dp'), parts along dimension 0
- output 4: float32 [4096], P('dp'), parts along dimension 0
- output 5: bfloat16 [4096, 16, 3, 64], P('dp', 'tp'), parts along dimension 0
- output 6: float32 [64, 3, 64], P(('dp', 'tp')), parts along dimension 0
- output 7: bfloat16 [4096, 1024], P(('dp', 'tp')), parts along dimension 0
- output 8: float32 [4096], P('dp'), parts along dimension 0
- output 9: float32 [4096], P('dp'), parts along dimension 0
- output 10: float32 [4096], P('dp'), parts along dimension 0
- output 11: bfloat16 [4096, 4096], P('dp', 'tp'), parts along dimension 0
- output 12: float32 [16384], P(('dp', 'tp')), parts along dimension 0
- output 13: bfloat16 [16384, 1024], P(('dp', 'tp')), parts along dimension 0
- output 14: float32 [4096], P('dp'), parts along dimension 0
There are 4 independent parts. The reference program is written for one: setup_inputs(seed, part) draws one part's arguments, and reference() takes and returns one part's arrays. A program takes and returns all parts, laid end to end along the dimension named above; an argument that names none is the same for every part.
All inputs are finite; a program needn't handle non-finite values.
Results may differ from the reference program's by a relative error of at most 0.02.
Values are sent between devices in bfloat16 or wider.
A program may use at most 768 MiB of HBM per device.

```python
import math
import jax
import jax.numpy as jnp
from jax import lax

BATCH = 1
SEQ = 2048
D = 1024
HEADS = 16
HEAD = 64
FF = 4096
EPS = 1e-5
MASK_VALUE = -1e30


def alibi_slopes(n_heads):
    closest = 2 ** int(math.floor(math.log2(n_heads)))
    base_ratio = 2.0 ** (-8.0 / closest)
    extra_ratio = 2.0 ** (-4.0 / closest)
    remaining = min(closest, n_heads - closest)
    slopes = [base_ratio ** (i + 1) for i in range(closest)]
    slopes = slopes + [extra_ratio ** (2 * i + 1) for i in range(remaining)]
    return jnp.array(slopes, dtype=jnp.float32)


def layer_norm(values, ln_gain, ln_bias):
    row_mean = jnp.mean(values, axis=-1, keepdims=True)
    centered = values - row_mean
    variance = jnp.mean(centered * centered, axis=-1, keepdims=True)
    return centered * lax.rsqrt(variance + EPS) * ln_gain + ln_bias


def layer_forward(x, ln1_gamma, ln1_beta, w_qkv, b_qkv, w_out, b_out, ln2_gamma, ln2_beta, w_up, b_up, w_down, b_down):
    positions = jnp.arange(SEQ)
    causal = positions[None, :] <= positions[:, None]
    key_pos = positions.astype(jnp.float32)
    x_f = x.astype(jnp.float32)
    h_norm = layer_norm(x_f, ln1_gamma, ln1_beta).astype(jnp.bfloat16)
    qkv_vals = (jnp.einsum('bsd,dhte->bshte', h_norm.astype(jnp.float32), w_qkv.astype(jnp.float32)) + b_qkv).astype(jnp.bfloat16)
    per_head = jnp.moveaxis(qkv_vals, 2, 0)

    def head_attention(operands):
        head_qkv, head_slope = operands
        q_one = head_qkv[:, :, 0].astype(jnp.float32)
        k_one = head_qkv[:, :, 1].astype(jnp.float32)
        v_one = head_qkv[:, :, 2].astype(jnp.float32)
        scores = jnp.einsum('bie,bje->bij', q_one, k_one) * (HEAD ** -0.5) + head_slope * key_pos
        scores = jnp.where(causal, scores, MASK_VALUE)
        prob_bf = jax.nn.softmax(scores, axis=-1).astype(jnp.bfloat16)
        return jnp.einsum('bij,bje->bie', prob_bf.astype(jnp.float32), v_one).astype(jnp.bfloat16)

    context = lax.map(jax.checkpoint(head_attention), (per_head, alibi_slopes(HEADS)))
    context_flat = jnp.moveaxis(context, 0, 2).reshape(BATCH, SEQ, D)
    attn_out = jnp.einsum('bsc,cd->bsd', context_flat.astype(jnp.float32), w_out.astype(jnp.float32)).astype(jnp.bfloat16)
    x_mid = x_f + attn_out.astype(jnp.float32) + b_out
    g_norm = layer_norm(x_mid, ln2_gamma, ln2_beta).astype(jnp.bfloat16)
    pre_act = jnp.einsum('bsd,df->bsf', g_norm.astype(jnp.float32), w_up.astype(jnp.float32)) + b_up
    activated = jax.nn.gelu(pre_act, approximate=True).astype(jnp.bfloat16)
    mlp_out = jnp.einsum('bsf,fd->bsd', activated.astype(jnp.float32), w_down.astype(jnp.float32)).astype(jnp.bfloat16)
    return (x_mid + mlp_out.astype(jnp.float32) + b_down).astype(jnp.bfloat16)


def setup_inputs(seed: int = 0, part: int = 0) -> dict:
    key_list = jax.random.split(jax.random.key(seed), 14)

    def normal(rng_key, out_shape, std_dev):
        return std_dev * jax.random.normal(rng_key, out_shape, jnp.float32)

    return {
        'x': normal(jax.random.fold_in(key_list[0], part), (BATCH, SEQ, D), 1.0).astype(jnp.bfloat16),
        'ln1_gamma': 1.0 + normal(key_list[1], (D,), 0.2),
        'ln1_beta': normal(key_list[2], (D,), 0.2),
        'w_qkv': normal(key_list[3], (D, HEADS, 3, HEAD), D ** -0.5).astype(jnp.bfloat16),
        'b_qkv': normal(key_list[4], (HEADS, 3, HEAD), 0.5),
        'w_out': normal(key_list[5], (D, D), D ** -0.5).astype(jnp.bfloat16),
        'b_out': normal(key_list[6], (D,), 0.5),
        'ln2_gamma': 1.0 + normal(key_list[7], (D,), 0.2),
        'ln2_beta': normal(key_list[8], (D,), 0.2),
        'w_up': normal(key_list[9], (D, FF), D ** -0.5).astype(jnp.bfloat16),
        'b_up': normal(key_list[10], (FF,), 0.5),
        'w_down': normal(key_list[11], (FF, D), FF ** -0.5).astype(jnp.bfloat16),
        'b_down': normal(key_list[12], (D,), 0.5),
        'grad_y': normal(jax.random.fold_in(key_list[13], part), (BATCH, SEQ, D), 1.0).astype(jnp.bfloat16),
    }


def reference(x, ln1_gamma, ln1_beta, w_qkv, b_qkv, w_out, b_out, ln2_gamma, ln2_beta, w_up, b_up, w_down, b_down, grad_y):
    y, pullback = jax.vjp(layer_forward, x, ln1_gamma, ln1_beta, w_qkv, b_qkv, w_out, b_out, ln2_gamma, ln2_beta, w_up, b_up, w_down, b_down)
    (grad_x, grad_ln1_gamma, grad_ln1_beta, grad_w_qkv, grad_b_qkv, grad_w_out, grad_b_out,
     grad_ln2_gamma, grad_ln2_beta, grad_w_up, grad_b_up, grad_w_down, grad_b_down) = pullback(grad_y)
    return (y, grad_x, grad_ln1_gamma, grad_ln1_beta, grad_w_qkv, grad_b_qkv, grad_w_out, grad_b_out,
            grad_ln2_gamma, grad_ln2_beta, grad_w_up, grad_b_up, grad_w_down, grad_b_down)
```

```python
import functools
import math
import jax
import jax.numpy as jnp
import numpy as np
from jax import lax
from jax.experimental import pallas as pl
from jax.experimental.pallas import tpu as pltpu
from jax.sharding import PartitionSpec as P

EPS = 1e-5
MASK_VALUE = -1e30
BF, F32 = jnp.bfloat16, jnp.float32
VMEM = pltpu.VMEM
MESH = pl.DeviceIdType.MESH
VLIM = 62 * 1024 * 1024
GELU_C = math.sqrt(2.0 / math.pi)
PAIR = LOW, HIGH = (0, 1)
TRIPLE = (0, 1, 2)
NN = (((1,), (0,)), ((), ()))
T0 = (((0,), (0,)), ((), ()))
NT = (((1,), (1,)), ((), ()))


def alibi_slopes(n_heads):
    closest = 2 ** int(math.floor(math.log2(n_heads)))
    base_ratio = 2.0 ** (-8.0 / closest)
    extra_ratio = 2.0 ** (-4.0 / closest)
    remaining = min(closest, n_heads - closest)
    slopes = [base_ratio ** (i + 1) for i in range(closest)]
    slopes = slopes + [extra_ratio ** (2 * i + 1) for i in range(remaining)]
    return np.array(slopes, dtype=np.float32)


def mm(a, b, dims=NN):
    return lax.dot_general(a, b, dims, preferred_element_type=F32)


def loop(lo, hi, body, unroll=1):
    def step(i, carry):
        body(i)
        return carry
    lax.fori_loop(lo, hi, step, 0, unroll=unroll)


def rows_loop(total, rows, body, unroll=1):
    loop(0, total // rows, lambda r: body(pl.ds(pl.multiple_of(r * rows, rows), rows)), unroll)


def row_mean(z):
    return jnp.mean(z, axis=-1, keepdims=True)


def col_sum(z):
    return jnp.sum(z, axis=0, keepdims=True)


def norm_back(grad, hat, rstd):
    return rstd * (grad - row_mean(grad) - hat * row_mean(grad * hat))


def zero_fill(*refs):
    for ref in refs:
        ref[...] = jnp.zeros(ref.shape, ref.dtype)


def sort_weight(wp, wt):
    e = wp.shape[0] // 6
    for part_no in TRIPLE:
        for head in PAIR:
            dst = (part_no * 2 + head) * e
            src = (head * 3 + part_no) * e
            wp[dst:dst + e, :] = wt[src:src + e, :]


def norm_rows(z):
    cen = z - row_mean(z)
    rstd = lax.rsqrt(row_mean(cen * cen) + EPS)
    return cen * rstd, rstd


def fold8(v, op):
    out = v[0:8]
    for k in range(1, v.shape[0] // 8):
        out = op(out, v[8 * k:8 * k + 8])
    return out


class Ring:
    def __init__(self, n):
        self.n = n
        nx = n // 2
        self.me = lax.axis_index('tp')
        self.x = self.me // 2
        self.c = self.me % 2
        self.nx = nx
        self.xr = (self.x + 1) % nx
        self.xl = (self.x + nx - 1) % nx
        self.xf = (self.x + 2) % nx
        self.right = self.xr * 2 + self.c
        self.left = self.xl * 2 + self.c
        self.far = self.xf * 2 + self.c
        self.partner = self.x * 2 + (1 - self.c)

    def order(self, s):
        odd = s % 2
        dx = jnp.where(s < 2, 0, jnp.where(s >= 6, 2, jnp.where(odd == 0, self.nx - 1, 1)))
        mid = jnp.where(s < 4, 0, 1)
        dc = jnp.where(s < 2, odd, jnp.where(s >= 6, odd, mid))
        return ((self.x + dx) % self.nx) * 2 + (self.c + dc) % 2

    def barrier(self, everyone=False):
        sem = pltpu.get_barrier_semaphore()
        if everyone:
            peers = [(self.me + k) % self.n for k in range(1, self.n)]
        else:
            peers = [self.right, self.left, self.partner]
        for peer in peers:
            pl.semaphore_signal(sem, inc=1, device_id={'tp': peer}, device_id_type=MESH)
        pl.semaphore_wait(sem, len(peers))


class Gather:
    SENDS = 14

    def __init__(self, ring, buf, ssem, rsem):
        self.ring, self.buf, self.ssem, self.rsem = ring, buf, ssem, rsem
        self.half = buf.shape[1] // 2

    def cp(self, blk, half, dev, k):
        ref = self.buf.at[blk, pl.ds(half * self.half, self.half)]
        return pltpu.make_async_remote_copy(
            src_ref=ref, dst_ref=ref, send_sem=self.ssem.at[k], recv_sem=self.rsem.at[blk, half],
            device_id={'tp': dev}, device_id_type=MESH)

    def start(self):
        r = self.ring
        self.cp(r.me, LOW, r.right, 0).start()
        self.cp(r.me, HIGH, r.left, 1).start()
        self.cp(r.me, HIGH, r.right, 2).start()
        self.cp(r.me, LOW, r.left, 3).start()
        self.cp(r.me, LOW, r.partner, 4).start()
        self.cp(r.me, HIGH, r.partner, 5).start()

    def wait(self, blk, half):
        self.cp(blk, half, self.ring.me, 0).wait_recv()

    def wait_block(self, blk):
        for half in PAIR:
            self.wait(blk, half)

    def near1(self):
        r = self.ring
        self.wait(r.left, LOW)
        self.cp(r.left, LOW, r.right, 6).start()
        self.cp(r.left, LOW, r.partner, 7).start()
        self.wait(r.right, HIGH)
        self.cp(r.right, HIGH, r.left, 8).start()
        self.cp(r.right, HIGH, r.partner, 9).start()

    def near2(self):
        r = self.ring
        self.wait(r.left, HIGH)
        self.cp(r.left, HIGH, r.partner, 10).start()
        self.wait(r.right, LOW)
        self.cp(r.right, LOW, r.partner, 11).start()

    def far(self):
        r = self.ring
        self.wait(r.far, LOW)
        self.cp(r.far, LOW, r.partner, 12).start()
        self.wait(r.far, HIGH)
        self.cp(r.far, HIGH, r.partner, 13).start()

    def finish(self):
        for k in range(self.SENDS):
            self.cp(self.ring.me, 0, self.ring.right, k).wait_send()

    def run(self, body, after_near=None):
        r = self.ring

        def step(s):
            blk = r.order(s)

            @pl.when(s == 1)
            def _():
                self.wait_block(blk)

            @pl.when(s == 2)
            def _():
                self.near1()
                if after_near is not None:
                    after_near()
                self.near2()

            @pl.when((s == 4) | (s == 5) | (s == 7))
            def _():
                self.wait_block(blk)

            @pl.when(s == 6)
            def _():
                self.far()

            body(blk)

        loop(0, r.n, step)


class Scatter:
    SENDS = 10

    def __init__(self, ring, part, pair, stage, land, ssem, rsem):
        self.ring, self.part, self.pair, self.stage, self.land = ring, part, pair, stage, land
        self.ssem, self.rsem = ssem, rsem
        self.rows = part.shape[1]
        self.half = self.rows // 2

    def cp_pair(self, xp, k):
        r = self.ring
        return pltpu.make_async_remote_copy(
            src_ref=self.part.at[xp * 2 + (1 - r.c)], dst_ref=self.pair.at[xp], send_sem=self.ssem.at[k],
            recv_sem=self.rsem.at[xp], device_id={'tp': r.partner}, device_id_type=MESH)

    def cp(self, slot, half, dst_slot, dev, k):
        rows = pl.ds(half * self.half, self.half)
        return pltpu.make_async_remote_copy(
            src_ref=self.stage.at[slot, rows], dst_ref=self.land.at[dst_slot, rows],
            send_sem=self.ssem.at[k], recv_sem=self.rsem.at[4 + 2 * dst_slot + half],
            device_id={'tp': dev}, device_id_type=MESH)

    def wait_land(self, dst_slot, half):
        self.cp(0, half, dst_slot, self.ring.me, 0).wait_recv()

    def wait_pair(self, xp):
        self.cp_pair(xp, 0).wait_recv()

    def send_pair(self, xp, k):
        self.cp_pair(xp, k).start()

    def mix(self, slot, xp, half, with_far=False):
        blk = xp * 2 + self.ring.c
        step = 16

        def body(i):
            rows = pl.ds(pl.multiple_of(half * self.half + i * step, step), step)
            total = self.part[blk, rows, :].astype(F32) + self.pair[xp, rows, :].astype(F32)
            if with_far:
                total = total + self.land[0, rows, :].astype(F32)
            self.stage[slot, rows, :] = total.astype(BF)
        loop(0, self.half // step, body)

    def far(self):
        r = self.ring
        self.wait_pair(r.xf)
        self.mix(0, r.xf, 0)
        self.cp(0, 0, 0, r.right, 4).start()
        self.mix(0, r.xf, 1)
        self.cp(0, 1, 0, r.left, 5).start()

    def near_own(self):
        r = self.ring
        self.wait_pair(r.xr)
        self.mix(1, r.xr, 1)
        self.cp(1, 1, 1, r.right, 6).start()
        self.wait_pair(r.xl)
        self.mix(2, r.xl, 0)
        self.cp(2, 0, 2, r.left, 7).start()

    def near_sum(self):
        r = self.ring
        self.wait_land(0, 0)
        self.mix(1, r.xr, 0, with_far=True)
        self.cp(1, 0, 1, r.right, 8).start()
        self.wait_land(0, 1)
        self.mix(2, r.xl, 1, with_far=True)
        self.cp(2, 1, 2, r.left, 9).start()

    def wait_final(self):
        self.wait_pair(self.ring.x)
        for slot in (1, 2):
            for half in PAIR:
                self.wait_land(slot, half)

    def total(self, rows):
        r = self.ring
        return (self.part[r.me, rows, :].astype(F32) + self.pair[r.x, rows, :].astype(F32)
                + self.land[1, rows, :].astype(F32) + self.land[2, rows, :].astype(F32))

    def finish(self):
        for k in range(4):
            self.cp_pair(self.ring.x, k).wait_send()
        for k in range(4, self.SENDS):
            self.cp(0, 0, 0, self.ring.right, k).wait_send()


def scatter_scratch(n, rows, d):
    return [VMEM((n // 2, rows, d), BF), VMEM((3, rows, d), BF), VMEM((3, rows, d), BF),
            pltpu.SemaphoreType.DMA((Scatter.SENDS,)), pltpu.SemaphoreType.DMA((4 + 6,))]


def gather_scratch(n):
    return [pltpu.SemaphoreType.DMA((Gather.SENDS,)), pltpu.SemaphoreType.DMA((n, 2))]


def lane_mask(rows, h):
    lane = lax.broadcasted_iota(jnp.int32, (rows, 128), 1)
    return (lane < 64) if h == 0 else (lane >= 64)


def attend_block(i, q_ref, k_ref, v_ref, o_ref, lse_ref, s_ref, m_ref, l_ref, acc_ref, slopes, scale):
    t = q_ref.shape[2]
    key = lax.broadcasted_iota(jnp.int32, (t, t), 0)
    qry = lax.broadcasted_iota(jnp.int32, (t, t), 1)
    for h in PAIR:
        m_ref[h] = jnp.full((8, t), MASK_VALUE, F32)
        l_ref[h] = jnp.zeros((8, t), F32)
    zero_fill(acc_ref)

    def score(j, diag):
        pos = (key + j * t).astype(F32)
        for h in PAIR:
            s = mm(k_ref[j], q_ref[h, i], NT) * scale + slopes[h] * pos
            if diag:
                s = jnp.where(key <= qry, s, MASK_VALUE)
            s_ref[h, j] = s
            m_ref[h] = jnp.maximum(m_ref[h], fold8(s, jnp.maximum))

    loop(0, i, lambda j: score(j, False))
    score(i, True)
    top = [jnp.max(m_ref[h], axis=0, keepdims=True) for h in (0, 1)]

    def denom(j):
        for h in PAIR:
            l_ref[h] = l_ref[h] + fold8(jnp.exp(s_ref[h, j] - top[h]), jnp.add)

    loop(0, i + 1, denom)
    for h in PAIR:
        lse_ref[h, i] = top[h] + jnp.log(col_sum(l_ref[h]))

    def values(j):
        total = acc_ref[...]
        for h in PAIR:
            p = jnp.exp(s_ref[h, j] - lse_ref[h, i]).astype(BF)
            total = total + mm(p, v_ref[h, j], T0)
        acc_ref[...] = total

    loop(0, i + 1, values)
    o_ref[i] = acc_ref[...].astype(BF)


def kernel_a(n, scale, x_hbm, dy_hbm, g1, b1, wt, bqkv, wo, bo, g2, b2, slopes_ref,
             h, dy, q, k, v, o, lse, x1, g,
             xg, wp, s_ref, m_ref, l_ref, acc, part, pair, stage, land, rs_s, rs_r,
             ax_s, ax_r, ay_s, ay_r, local):
    ring = Ring(n)
    me = ring.me
    t = xg.shape[1]
    in_x = pltpu.make_async_copy(x_hbm, xg.at[me], local.at[0])
    in_y = pltpu.make_async_copy(dy_hbm, dy.at[me], local.at[1])
    in_x.start()
    in_y.start()
    ring.barrier()
    in_x.wait()
    gx = Gather(ring, xg, ax_s, ax_r)
    gy = Gather(ring, dy, ay_s, ay_r)
    gx.start()
    in_y.wait()
    sort_weight(wp, wt)

    def project(blk):
        def norm(rows):
            hat, _ = norm_rows(xg[blk, rows, :].astype(F32))
            h[blk, rows, :] = (hat * g1[...] + b1[...]).astype(BF)
        rows_loop(t, 32, norm)
        out = mm(h[blk], wp[...], NT) + bqkv[...]
        out = out.astype(BF)
        zero = jnp.zeros((t, 128), BF)
        for head in PAIR:
            q[head, blk] = jnp.where(lane_mask(t, head), out[:, 0:128], zero)
            v[head, blk] = jnp.where(lane_mask(t, head), out[:, 256:384], zero)
        k[blk] = out[:, 128:256]

    gx.run(project, after_near=gy.start)

    slopes = [slopes_ref[me * 2 + head] for head in PAIR]

    def attend(i):
        attend_block(i, q, k, v, o, lse, s_ref, m_ref, l_ref, acc, slopes, scale)

    def all_blocks(i):
        @pl.when(i == n // 2 + 1)
        def _():
            gy.near1()

        @pl.when(i == n - 1)
        def _():
            gy.near2()
        attend(i)

    loop(0, n, all_blocks)

    rs = Scatter(ring, part, pair, stage, land, rs_s, rs_r)

    def partial(xp, slot):
        for cc in PAIR:
            part[xp * 2 + cc] = mm(o[xp * 2 + cc], wo[...]).astype(BF)
        rs.send_pair(xp, slot)

    partial(ring.xf, 0)
    rs.far()
    partial(ring.xr, 1)
    partial(ring.xl, 2)
    rs.near_own()
    partial(ring.x, 3)
    gy.far()
    rs.near_sum()
    for dx in (ring.x, ring.xl, ring.xr, ring.xf):
        gy.wait_block(dx * 2 + (1 - ring.c))
    rs.wait_final()

    def last(rows):
        a = rs.total(rows).astype(BF).astype(F32)
        mid = xg[me, rows, :].astype(F32) + a + bo[...]
        x1[rows, :] = mid
        hat, _ = norm_rows(mid)
        g[rows, :] = (hat * g2[...] + b2[...]).astype(BF)
    rows_loop(t, 32, last)
    rs.finish()
    gx.finish()
    gy.finish()


def kernel_b(n, g_hbm, x1, dyo, dy, wu, bu, wd, g2,
             part_m, gwu, gbu, gwd, mid, da, small,
             gg, act, dpre, part, pair, stage, land, rs_s, rs_r, ag_s, ag_r, local):
    ring = Ring(n)
    me = ring.me
    t, d, f = gg.shape[1], gg.shape[2], wu.shape[1]
    in_g = pltpu.make_async_copy(g_hbm, gg.at[me], local.at[0])
    in_g.start()
    ring.barrier()
    in_g.wait()
    ag = Gather(ring, gg, ag_s, ag_r)
    ag.start()
    zero_fill(gbu)

    def mlp(blk):
        pre = mm(gg[blk], wu[...]) + bu[...]
        cot = mm(dy[blk], wd[...], NT).astype(BF).astype(F32)
        sq = pre * pre
        th = jnp.tanh(GELU_C * (pre + 0.044715 * sq * pre))
        cdf = 0.5 * (1.0 + th)
        act[blk] = (pre * cdf).astype(BF)
        slope = cdf + pre * (0.5 * (1.0 - th * th)) * (GELU_C * (1.0 + 3 * 0.044715 * sq))
        dp = cot * slope
        gbu[...] = gbu[...] + fold8(dp, jnp.add)
        dpre[blk] = dp.astype(BF)
        part[blk] = mm(dpre[blk], wu[...], NT).astype(BF)

    ag.run(mlp)
    rs = Scatter(ring, part, pair, stage, land, rs_s, rs_r)
    rs.send_pair(ring.xf, 0)
    rs.send_pair(ring.xr, 1)
    rs.send_pair(ring.xl, 2)
    rs.send_pair(ring.x, 3)
    rs.far()
    rs.near_own()

    def weight_down(i):
        cols = pl.ds(pl.multiple_of(i * 256, 256), 256)
        left = act[:, :, cols].reshape(n * t, 256)
        gwd[cols, :] = mm(left, dy[...].reshape(n * t, d), T0).astype(BF)

    def weight_up(i):
        cols = pl.ds(pl.multiple_of(i * 256, 256), 256)
        left = gg[:, :, cols].reshape(n * t, 256)
        gwu[cols, :] = mm(left, dpre[...].reshape(n * t, f), T0).astype(BF)

    loop(0, f // 256, weight_down)
    loop(0, d // 256, weight_up)
    rs.near_sum()

    def down(blk):
        part_m[blk] = mm(act[blk], wd[...]).astype(BF)
    loop(0, n, down)
    rs.wait_final()
    zero_fill(small)

    def last(rows):
        dg = rs.total(rows).astype(BF).astype(F32)
        hat, rstd = norm_rows(x1[rows, :])
        small[0] = small[0] + fold8(dg * hat, jnp.add)
        small[1] = small[1] + fold8(dg, jnp.add)
        dh = dg * g2[...]
        dz = norm_back(dh, hat, rstd)
        dyf = dyo[rows, :].astype(F32)
        dm = dyf + dz
        small[2] = small[2] + fold8(dm, jnp.add)
        small[3] = small[3] + fold8(dyf, jnp.add)
        mid[rows, :] = dm
        da[rows, :] = dm.astype(BF)
    rows_loop(t, 16, last)
    rs.finish()
    ag.finish()


def kernel_c(n, scale, da_hbm, mid, part_m, x_own, x1, h, q, k, v, o, lse, wt, wo, g1, bd, small_b, slopes_ref,
             y, gx, sums, gwt, gbq, gwo,
             dag, wp, km, dom, dlt, dq, dk_acc, dv_acc, d3, gwo_acc, small, every,
             part, pair, stage, land, rs_s, rs_r,
             pair_m, stage_m, land_m, rm_s, rm_r, ag_s, ag_r, ar_s, ar_r, local):
    ring = Ring(n)
    me = ring.me
    t, d = dag.shape[1], dag.shape[2]
    in_d = pltpu.make_async_copy(da_hbm, dag.at[me], local.at[0])
    in_d.start()
    ring.barrier(everyone=True)
    in_d.wait()
    ag = Gather(ring, dag, ag_s, ag_r)
    ag.start()
    rm = Scatter(ring, part_m, pair_m, stage_m, land_m, rm_s, rm_r)
    for slot, xp in enumerate((ring.xf, ring.xr, ring.xl, ring.x)):
        rm.send_pair(xp, slot)
    sort_weight(wp, wt)
    zero_fill(gwo_acc)

    def back_out(blk):
        dc = mm(dag[blk], wo[...], NT).astype(BF)
        zero = jnp.zeros((t, 128), BF)
        for head in PAIR:
            mask = lane_mask(t, head)
            dom[head, blk] = jnp.where(mask, dc, zero)
            km[head, blk] = jnp.where(mask, k[blk], zero)
        prod = (dc.astype(F32) * o[blk].astype(F32)).T
        dlt[LOW, blk] = col_sum(prod[:64])
        dlt[HIGH, blk] = col_sum(prod[64:])
        gwo_acc[...] = gwo_acc[...] + mm(o[blk], dag[blk], T0)
        dq[blk] = jnp.zeros((t, 128), F32)

    ag.run(back_out, after_near=rm.far)
    rm.near_own()
    gwo[...] = gwo_acc[...].astype(BF)
    slopes = [slopes_ref[me * 2 + head] for head in PAIR]
    key = lax.broadcasted_iota(jnp.int32, (t, t), 0)
    qry = lax.broadcasted_iota(jnp.int32, (t, t), 1)

    def kv_block(j):
        pos = (key + j * t).astype(F32)
        zero_fill(dk_acc, dv_acc)

        def pair_block(i, diag):
            tv, tk, tq = dv_acc[...], dk_acc[...], dq[i]
            for head in PAIR:
                s = mm(k[j], q[head, i], NT) * scale + slopes[head] * pos
                if diag:
                    s = jnp.where(key <= qry, s, MASK_VALUE)
                p = jnp.exp(s - lse[head, i])
                dp = mm(v[head, j], dom[head, i], NT).astype(BF).astype(F32)
                ds = (p * (dp - dlt[head, i])).astype(BF)
                tv = tv + mm(p.astype(BF), dom[head, i])
                tk = tk + mm(ds, q[head, i])
                tq = tq + mm(ds, km[head, j], T0)
            dv_acc[...] = tv
            dk_acc[...] = tk
            dq[i] = tq

        pair_block(j, True)
        loop(j + 1, n, lambda i: pair_block(i, False))
        d3[j, :, 128:256] = (dk_acc[...] * scale).astype(BF)
        d3[j, :, 256:384] = dv_acc[...].astype(BF)

        @pl.when(j == 1)
        def _():
            rm.near_sum()

    loop(0, n, kv_block)
    zero_fill(gbq)
    rs = Scatter(ring, part, pair, stage, land, rs_s, rs_r)

    def back_in(xp, slot):
        for cc in PAIR:
            blk = xp * 2 + cc
            d3[blk, :, 0:128] = (dq[blk] * scale).astype(BF)
            part[blk] = mm(d3[blk], wp[...]).astype(BF)
        rs.send_pair(xp, slot)

    back_in(ring.xf, 0)
    rs.far()
    back_in(ring.xr, 1)
    back_in(ring.xl, 2)
    rs.near_own()
    back_in(ring.x, 3)

    def weight_in(i):
        cols = pl.ds(pl.multiple_of(i * 128, 128), 128)
        left = d3[:, :, cols].reshape(n * t, 128)
        grad = mm(left, h[...].reshape(n * t, d), T0).astype(BF)
        for head in PAIR:
            gwt[head, i] = grad[head * 64:head * 64 + 64]
    loop(0, 3, weight_in)

    def bias_in(b):
        gbq[...] = gbq[...] + fold8(d3[b].astype(F32), jnp.add)
    loop(0, n, bias_in)
    rs.near_sum()
    rm.wait_final()

    def out_y(rows):
        m = rm.total(rows).astype(BF).astype(F32)
        y[rows, :] = (x1[rows, :] + m + bd[...]).astype(BF)
    rows_loop(t, 32, out_y)
    zero_fill(small)
    rs.wait_final()

    def last(rows):
        dh = rs.total(rows).astype(BF).astype(F32)
        hat, rstd = norm_rows(x_own[rows, :].astype(F32))
        small[0] = small[0] + fold8(dh * hat, jnp.add)
        small[1] = small[1] + fold8(dh, jnp.add)
        dn = dh * g1[...]
        dz = norm_back(dn, hat, rstd)
        gx[rows, :] = (mid[rows, :] + dz).astype(BF)
    rows_loop(t, 16, last)
    for i in range(2):
        every[me, i:i + 1, :] = col_sum(small[i])
    for i in range(4):
        every[me, 2 + i:3 + i, :] = col_sum(small_b[i])
    every[me, 6:8, :] = jnp.zeros((2, d), F32)

    def share(off):
        dev = (me + off) % n
        return pltpu.make_async_remote_copy(
            src_ref=every.at[me], dst_ref=every.at[me], send_sem=ar_s.at[off], recv_sem=ar_r.at[me],
            device_id={'tp': dev}, device_id_type=MESH)

    for off in range(1, n):
        share(off).start()
    for off in range(1, n):
        src = (me + off) % n
        pltpu.make_async_remote_copy(
            src_ref=every.at[src], dst_ref=every.at[src], send_sem=ar_s.at[0], recv_sem=ar_r.at[src],
            device_id={'tp': me}, device_id_type=MESH).wait_recv()
    total = every[0]
    for b in range(1, n):
        total = total + every[b]
    sums[...] = total
    for off in range(1, n):
        share(off).wait_send()
    rs.finish()
    rm.finish()
    ag.finish()


def whole():
    return pl.BlockSpec(memory_space=VMEM)


def anywhere():
    return pl.BlockSpec(memory_space=pl.ANY)


def smem():
    return pl.BlockSpec(memory_space=pltpu.SMEM)


def solution(mesh):
    n = mesh.shape['tp']

    def local_step(x, ln1_gamma, ln1_beta, w_qkv, b_qkv, w_out, b_out, ln2_gamma, ln2_beta, w_up, b_up, w_down, b_down, grad_y):
        t, d = x.shape[1], x.shape[2]
        heads, e = w_qkv.shape[1], w_qkv.shape[3]
        he = heads * e
        f = w_up.shape[1]
        scale = e ** -0.5
        slopes = jnp.asarray(alibi_slopes(heads * n))
        x2, dy2 = x[0], grad_y[0]
        row = lambda vec: vec.reshape(1, -1)
        wt = w_qkv.transpose(1, 2, 3, 0).reshape(heads * 3 * e, d)
        bq = b_qkv.transpose(1, 0, 2).reshape(1, 3 * he)
        sds = jax.ShapeDtypeStruct
        rows, full, half = (t, d), (n, t, d), (n, t, he)
        both, line = (len(PAIR),) + half, (len(PAIR), n, 1, t)
        packed = (len(TRIPLE) * he, d)
        params = lambda cid: pltpu.CompilerParams(collective_id=cid, has_side_effects=True, vmem_limit_bytes=VLIM)
        dma = pltpu.SemaphoreType.DMA

        h, dy, q, k, v, o, lse, x1, g = pl.pallas_call(
            functools.partial(kernel_a, n, scale),
            name='attend_forward',
            out_shape=[sds(full, BF), sds(full, BF), sds(both, BF), sds(half, BF),
                       sds(both, BF), sds(half, BF), sds(line, F32), sds(rows, F32),
                       sds(rows, BF)],
            in_specs=[anywhere(), anywhere()] + [whole()] * 8 + [smem()],
            out_specs=[whole()] * 9,
            scratch_shapes=[VMEM(full, BF), VMEM(packed, BF), VMEM((2, n, t, t), F32), VMEM((2, 8, t), F32),
                            VMEM((2, 8, t), F32), VMEM((t, he), F32), VMEM(full, BF)]
            + scatter_scratch(n, t, d) + gather_scratch(n) + gather_scratch(n) + [dma((2,))],
            compiler_params=params(0),
        )(x2, dy2, row(ln1_gamma), row(ln1_beta), wt, bq, w_out, row(b_out), row(ln2_gamma), row(ln2_beta), slopes)

        part_m, gwu, gbu, gwd, mid, da, small = pl.pallas_call(
            functools.partial(kernel_b, n),
            name='mlp_both',
            out_shape=[sds(full, BF), sds((d, f), BF), sds((8, f), F32), sds((f, d), BF), sds(rows, F32),
                       sds(rows, BF), sds((4, 8, d), F32)],
            in_specs=[anywhere()] + [whole()] * 7,
            out_specs=[whole()] * 7,
            scratch_shapes=[VMEM(full, BF), VMEM((n, t, f), BF), VMEM((n, t, f), BF), VMEM(full, BF)]
            + scatter_scratch(n, t, d) + gather_scratch(n) + [dma((1,))],
            compiler_params=params(1),
        )(g, x1, dy2, dy, w_up, row(b_up), w_down, row(ln2_gamma))

        y, gx, sums, gwt, gbq, gwo = pl.pallas_call(
            functools.partial(kernel_c, n, scale),
            name='attend_backward',
            out_shape=[sds(rows, BF), sds(rows, BF), sds((8, d), F32), sds((heads, 3, e, d), BF),
                       sds((8, 3 * he), F32), sds((he, d), BF)],
            in_specs=[anywhere()] + [whole()] * 15 + [smem()],
            out_specs=[whole()] * 6,
            scratch_shapes=[VMEM(full, BF), VMEM(packed, BF), VMEM(both, BF), VMEM(both, BF),
                            VMEM(line, F32), VMEM(half, F32), VMEM((t, he), F32), VMEM((t, he), F32),
                            VMEM((n, t, 3 * he), BF), VMEM((he, d), F32), VMEM((2, 8, d), F32), VMEM((n, 8, d), F32),
                            VMEM(full, BF)]
            + scatter_scratch(n, t, d) + scatter_scratch(n, t, d) + gather_scratch(n)
            + [dma((n,)), dma((n,)), dma((1,))],
            compiler_params=params(2),
        )(da, mid, part_m, x2, x1, h, q, k, v, o, lse, wt, w_out, row(ln1_gamma), row(b_down), small, slopes)

        s_g1, s_b1, s_g2, s_b2, s_bo, s_bd = list(sums)[:6]
        grad_w_qkv = gwt.transpose(3, 0, 1, 2)
        grad_b_qkv = jnp.sum(gbq, axis=0).reshape(3, heads, e).transpose(1, 0, 2)
        grad_b_up = jnp.sum(gbu, axis=0)
        return (y[None], gx[None], s_g1, s_b1, grad_w_qkv, grad_b_qkv, gwo, s_bo,
                s_g2, s_b2, gwu, grad_b_up, gwd, s_bd)

    row_spec = P('dp', 'tp', None)
    in_specs = (row_spec, P(), P(), P(None, 'tp', None, None), P('tp', None, None), P('tp', None), P(), P(), P(),
                P(None, 'tp'), P('tp'), P('tp', None), P(), row_spec)
    out_specs = (row_spec, row_spec, P('dp'), P('dp'), P('dp', 'tp', None, None), P(('dp', 'tp'), None, None),
                 P(('dp', 'tp'), None), P('dp'), P('dp'), P('dp'), P('dp', 'tp'), P(('dp', 'tp')), P(('dp', 'tp'), None), P('dp'))
    return jax.shard_map(local_step, mesh=mesh, in_specs=in_specs, out_specs=out_specs, check_vma=False)
```

```python
import functools
import math
import jax
import jax.numpy as jnp
import numpy as np
from jax import lax
from jax.experimental import pallas as pl
from jax.experimental.pallas import tpu as pltpu
from jax.sharding import PartitionSpec as P

EPS = 1e-5
MASK_VALUE = -1e30
BF, F32 = jnp.bfloat16, jnp.float32
VMEM = pltpu.VMEM
MESH = pl.DeviceIdType.MESH
scope = jax.named_scope
VLIM = 62 * 1024 * 1024
GELU_C = math.sqrt(2.0 / math.pi)
PAIR = LOW, HIGH = (0, 1)
TRIPLE = (0, 1, 2)
NN = (((1,), (0,)), ((), ()))
T0 = (((0,), (0,)), ((), ()))
NT = (((1,), (1,)), ((), ()))


def alibi_slopes(n_heads):
    closest = 2 ** int(math.floor(math.log2(n_heads)))
    base_ratio = 2.0 ** (-8.0 / closest)
    extra_ratio = 2.0 ** (-4.0 / closest)
    remaining = min(closest, n_heads - closest)
    slopes = [base_ratio ** (i + 1) for i in range(closest)]
    slopes = slopes + [extra_ratio ** (2 * i + 1) for i in range(remaining)]
    return np.array(slopes, dtype=np.float32)


def mm(a, b, dims=NN):
    return lax.dot_general(a, b, dims, preferred_element_type=F32)


def loop(lo, hi, body, unroll=1):
    def step(i, carry):
        body(i)
        return carry
    lax.fori_loop(lo, hi, step, 0, unroll=unroll)


def rows_loop(total, rows, body, unroll=1):
    loop(0, total // rows, lambda r: body(pl.ds(pl.multiple_of(r * rows, rows), rows)), unroll)


def row_mean(z):
    return jnp.mean(z, axis=-1, keepdims=True)


def col_sum(z):
    return jnp.sum(z, axis=0, keepdims=True)


def norm_back(grad, hat, rstd):
    return rstd * (grad - row_mean(grad) - hat * row_mean(grad * hat))


def zero_fill(*refs):
    for ref in refs:
        ref[...] = jnp.zeros(ref.shape, ref.dtype)


def sort_weight(wp, wt):
    e = wp.shape[0] // 6
    for part_no in TRIPLE:
        for head in PAIR:
            dst = (part_no * 2 + head) * e
            src = (head * 3 + part_no) * e
            wp[dst:dst + e, :] = wt[src:src + e, :]


def norm_rows(z):
    cen = z - row_mean(z)
    rstd = lax.rsqrt(row_mean(cen * cen) + EPS)
    return cen * rstd, rstd


def fold8(v, op):
    out = v[0:8]
    for k in range(1, v.shape[0] // 8):
        out = op(out, v[8 * k:8 * k + 8])
    return out


class Ring:
    def __init__(self, n):
        self.n = n
        nx = n // 2
        self.me = lax.axis_index('tp')
        self.x = self.me // 2
        self.c = self.me % 2
        self.nx = nx
        self.xr = (self.x + 1) % nx
        self.xl = (self.x + nx - 1) % nx
        self.xf = (self.x + 2) % nx
        self.right = self.xr * 2 + self.c
        self.left = self.xl * 2 + self.c
        self.far = self.xf * 2 + self.c
        self.partner = self.x * 2 + (1 - self.c)

    def order(self, s):
        odd = s % 2
        dx = jnp.where(s < 2, 0, jnp.where(s >= 6, 2, jnp.where(odd == 0, self.nx - 1, 1)))
        mid = jnp.where(s < 4, 0, 1)
        dc = jnp.where(s < 2, odd, jnp.where(s >= 6, odd, mid))
        return ((self.x + dx) % self.nx) * 2 + (self.c + dc) % 2

    def barrier(self, everyone=False):
        sem = pltpu.get_barrier_semaphore()
        if everyone:
            peers = [(self.me + k) % self.n for k in range(1, self.n)]
        else:
            peers = [self.right, self.left, self.partner]
        for peer in peers:
            pl.semaphore_signal(sem, inc=1, device_id={'tp': peer}, device_id_type=MESH)
        pl.semaphore_wait(sem, len(peers))


class Gather:
    SENDS = 14

    def __init__(self, ring, buf, ssem, rsem):
        self.ring, self.buf, self.ssem, self.rsem = ring, buf, ssem, rsem
        self.half = buf.shape[1] // 2

    def cp(self, blk, half, dev, k):
        ref = self.buf.at[blk, pl.ds(half * self.half, self.half)]
        return pltpu.make_async_remote_copy(
            src_ref=ref, dst_ref=ref, send_sem=self.ssem.at[k], recv_sem=self.rsem.at[blk, half],
            device_id={'tp': dev}, device_id_type=MESH)

    def start(self):
        r = self.ring
        self.cp(r.me, LOW, r.right, 0).start()
        self.cp(r.me, HIGH, r.left, 1).start()
        self.cp(r.me, HIGH, r.right, 2).start()
        self.cp(r.me, LOW, r.left, 3).start()
        self.cp(r.me, LOW, r.partner, 4).start()
        self.cp(r.me, HIGH, r.partner, 5).start()

    def wait(self, blk, half):
        self.cp(blk, half, self.ring.me, 0).wait_recv()

    def wait_block(self, blk):
        for half in PAIR:
            self.wait(blk, half)

    def near1(self):
        r = self.ring
        self.wait(r.left, LOW)
        self.cp(r.left, LOW, r.right, 6).start()
        self.cp(r.left, LOW, r.partner, 7).start()
        self.wait(r.right, HIGH)
        self.cp(r.right, HIGH, r.left, 8).start()
        self.cp(r.right, HIGH, r.partner, 9).start()

    def near2(self):
        r = self.ring
        self.wait(r.left, HIGH)
        self.cp(r.left, HIGH, r.partner, 10).start()
        self.wait(r.right, LOW)
        self.cp(r.right, LOW, r.partner, 11).start()

    def far(self):
        r = self.ring
        self.wait(r.far, LOW)
        self.cp(r.far, LOW, r.partner, 12).start()
        self.wait(r.far, HIGH)
        self.cp(r.far, HIGH, r.partner, 13).start()

    def finish(self):
        for k in range(self.SENDS):
            self.cp(self.ring.me, 0, self.ring.right, k).wait_send()

    def run(self, body, after_near=None):
        r = self.ring

        def step(s):
            blk = r.order(s)

            @pl.when(s == 1)
            def _():
                self.wait_block(blk)

            @pl.when(s == 2)
            def _():
                self.near1()
                if after_near is not None:
                    after_near()
                self.near2()

            @pl.when((s == 4) | (s == 5) | (s == 7))
            def _():
                self.wait_block(blk)

            @pl.when(s == 6)
            def _():
                self.far()

            body(blk)

        loop(0, r.n, step)


class Scatter:
    SENDS = 10

    def __init__(self, ring, part, pair, stage, land, ssem, rsem):
        self.ring, self.part, self.pair, self.stage, self.land = ring, part, pair, stage, land
        self.ssem, self.rsem = ssem, rsem
        self.rows = part.shape[1]
        self.half = self.rows // 2

    def cp_pair(self, xp, k):
        r = self.ring
        return pltpu.make_async_remote_copy(
            src_ref=self.part.at[xp * 2 + (1 - r.c)], dst_ref=self.pair.at[xp], send_sem=self.ssem.at[k],
            recv_sem=self.rsem.at[xp], device_id={'tp': r.partner}, device_id_type=MESH)

    def cp(self, slot, half, dst_slot, dev, k):
        rows = pl.ds(half * self.half, self.half)
        return pltpu.make_async_remote_copy(
            src_ref=self.stage.at[slot, rows], dst_ref=self.land.at[dst_slot, rows],
            send_sem=self.ssem.at[k], recv_sem=self.rsem.at[4 + 2 * dst_slot + half],
            device_id={'tp': dev}, device_id_type=MESH)

    def wait_land(self, dst_slot, half):
        self.cp(0, half, dst_slot, self.ring.me, 0).wait_recv()

    def wait_pair(self, xp):
        self.cp_pair(xp, 0).wait_recv()

    def send_pair(self, xp, k):
        self.cp_pair(xp, k).start()

    def mix(self, slot, xp, half, with_far=False):
        blk = xp * 2 + self.ring.c
        step = 16

        def body(i):
            rows = pl.ds(pl.multiple_of(half * self.half + i * step, step), step)
            total = self.part[blk, rows, :].astype(F32) + self.pair[xp, rows, :].astype(F32)
            if with_far:
                total = total + self.land[0, rows, :].astype(F32)
            self.stage[slot, rows, :] = total.astype(BF)
        loop(0, self.half // step, body)

    def far(self):
        r = self.ring
        self.wait_pair(r.xf)
        self.mix(0, r.xf, 0)
        self.cp(0, 0, 0, r.right, 4).start()
        self.mix(0, r.xf, 1)
        self.cp(0, 1, 0, r.left, 5).start()

    def near_own(self):
        r = self.ring
        self.wait_pair(r.xr)
        self.mix(1, r.xr, 1)
        self.cp(1, 1, 1, r.right, 6).start()
        self.wait_pair(r.xl)
        self.mix(2, r.xl, 0)
        self.cp(2, 0, 2, r.left, 7).start()

    def near_sum(self):
        r = self.ring
        self.wait_land(0, 0)
        self.mix(1, r.xr, 0, with_far=True)
        self.cp(1, 0, 1, r.right, 8).start()
        self.wait_land(0, 1)
        self.mix(2, r.xl, 1, with_far=True)
        self.cp(2, 1, 2, r.left, 9).start()

    def wait_final(self):
        self.wait_pair(self.ring.x)
        for slot in (1, 2):
            for half in PAIR:
                self.wait_land(slot, half)

    def total(self, rows):
        r = self.ring
        return (self.part[r.me, rows, :].astype(F32) + self.pair[r.x, rows, :].astype(F32)
                + self.land[1, rows, :].astype(F32) + self.land[2, rows, :].astype(F32))

    def finish(self):
        for k in range(4):
            self.cp_pair(self.ring.x, k).wait_send()
        for k in range(4, self.SENDS):
            self.cp(0, 0, 0, self.ring.right, k).wait_send()


def scatter_scratch(n, rows, d):
    return [VMEM((n // 2, rows, d), BF), VMEM((3, rows, d), BF), VMEM((3, rows, d), BF),
            pltpu.SemaphoreType.DMA((Scatter.SENDS,)), pltpu.SemaphoreType.DMA((4 + 6,))]


def gather_scratch(n):
    return [pltpu.SemaphoreType.DMA((Gather.SENDS,)), pltpu.SemaphoreType.DMA((n, 2))]


def lane_mask(rows, h):
    lane = lax.broadcasted_iota(jnp.int32, (rows, 128), 1)
    return (lane < 64) if h == 0 else (lane >= 64)


def attend_block(i, q_ref, k_ref, v_ref, o_ref, lse_ref, s_ref, m_ref, l_ref, acc_ref, slopes, scale):
    t = q_ref.shape[2]
    key = lax.broadcasted_iota(jnp.int32, (t, t), 0)
    qry = lax.broadcasted_iota(jnp.int32, (t, t), 1)
    for h in PAIR:
        m_ref[h] = jnp.full((8, t), MASK_VALUE, F32)
        l_ref[h] = jnp.zeros((8, t), F32)
    zero_fill(acc_ref)

    def score(j, diag):
        pos = (key + j * t).astype(F32)
        for h in PAIR:
            s = mm(k_ref[j], q_ref[h, i], NT) * scale + slopes[h] * pos
            if diag:
                s = jnp.where(key <= qry, s, MASK_VALUE)
            s_ref[h, j] = s
            m_ref[h] = jnp.maximum(m_ref[h], fold8(s, jnp.maximum))

    loop(0, i, lambda j: score(j, False))
    score(i, True)
    top = [jnp.max(m_ref[h], axis=0, keepdims=True) for h in (0, 1)]

    def denom(j):
        for h in PAIR:
            l_ref[h] = l_ref[h] + fold8(jnp.exp(s_ref[h, j] - top[h]), jnp.add)

    loop(0, i + 1, denom)
    for h in PAIR:
        lse_ref[h, i] = top[h] + jnp.log(col_sum(l_ref[h]))

    def values(j):
        total = acc_ref[...]
        for h in PAIR:
            p = jnp.exp(s_ref[h, j] - lse_ref[h, i]).astype(BF)
            total = total + mm(p, v_ref[h, j], T0)
        acc_ref[...] = total

    loop(0, i + 1, values)
    o_ref[i] = acc_ref[...].astype(BF)


def kernel_a(n, scale, x_hbm, dy_hbm, g1, b1, wt, bqkv, wo, bo, g2, b2, slopes_ref,
             h, dy, q, k, v, o, lse, x1, g,
             xg, wp, s_ref, m_ref, l_ref, acc, part, pair, stage, land, rs_s, rs_r,
             ax_s, ax_r, ay_s, ay_r, local):
    ring = Ring(n)
    me = ring.me
    t = xg.shape[1]
    in_x = pltpu.make_async_copy(x_hbm, xg.at[me], local.at[0])
    in_y = pltpu.make_async_copy(dy_hbm, dy.at[me], local.at[1])
    in_x.start()
    in_y.start()
    ring.barrier()
    in_x.wait()
    gx = Gather(ring, xg, ax_s, ax_r)
    gy = Gather(ring, dy, ay_s, ay_r)
    gx.start()
    in_y.wait()
    sort_weight(wp, wt)

    bias = jnp.concatenate([bqkv[part_no, head:head + 1, :] for part_no in TRIPLE for head in PAIR], axis=1)

    def project(blk):
        def norm(rows):
            hat, _ = norm_rows(xg[blk, rows, :].astype(F32))
            h[blk, rows, :] = (hat * g1[...] + b1[...]).astype(BF)
        rows_loop(t, 32, norm)
        out = mm(h[blk], wp[...], NT) + bias
        out = out.astype(BF)
        zero = jnp.zeros((t, 128), BF)
        for head in PAIR:
            q[head, blk] = jnp.where(lane_mask(t, head), out[:, 0:128], zero)
            v[head, blk] = jnp.where(lane_mask(t, head), out[:, 256:384], zero)
        k[blk] = out[:, 128:256]

    with scope('a_gather'):
        gx.run(project, after_near=gy.start)

    slopes = [slopes_ref[me * 2 + head] for head in PAIR]

    def attend(i):
        attend_block(i, q, k, v, o, lse, s_ref, m_ref, l_ref, acc, slopes, scale)

    def all_blocks(i):
        @pl.when(i == n // 2 + 1)
        def _():
            gy.near1()

        @pl.when(i == n - 1)
        def _():
            gy.near2()
        attend(i)

    with scope('a_attend'):
        loop(0, n, all_blocks)

    rs = Scatter(ring, part, pair, stage, land, rs_s, rs_r)

    def partial(xp, slot):
        for cc in PAIR:
            part[xp * 2 + cc] = mm(o[xp * 2 + cc], wo[...]).astype(BF)
        rs.send_pair(xp, slot)

    with scope('a_far'):
        partial(ring.xf, 0)
        rs.far()
    with scope('a_own'):
        partial(ring.xr, 1)
        partial(ring.xl, 2)
        rs.near_own()
        partial(ring.x, 3)
    with scope('a_gyfar'):
        gy.far()
    with scope('a_sum'):
        rs.near_sum()
    for dx in (ring.x, ring.xl, ring.xr, ring.xf):
        gy.wait_block(dx * 2 + (1 - ring.c))
    with scope('a_final'):
        rs.wait_final()

    def last(rows):
        a = rs.total(rows).astype(BF).astype(F32)
        mid = xg[me, rows, :].astype(F32) + a + bo[...]
        x1[rows, :] = mid
        hat, _ = norm_rows(mid)
        g[rows, :] = (hat * g2[...] + b2[...]).astype(BF)
    rows_loop(t, 32, last)
    rs.finish()
    gx.finish()
    gy.finish()


def kernel_b(n, g_hbm, x1, dyo, dy, wu, bu, wd, g2,
             part_m, gwu, gbu, gwd, mid, da, small,
             gg, act, dpre, part, pair, stage, land, rs_s, rs_r, ag_s, ag_r, local):
    ring = Ring(n)
    me = ring.me
    t, d, f = gg.shape[1], gg.shape[2], wu.shape[1]
    in_g = pltpu.make_async_copy(g_hbm, gg.at[me], local.at[0])
    in_g.start()
    ring.barrier()
    in_g.wait()
    ag = Gather(ring, gg, ag_s, ag_r)
    ag.start()
    zero_fill(gbu)

    def mlp(blk):
        pre = mm(gg[blk], wu[...]) + bu[...]
        cot = mm(dy[blk], wd[...], NT).astype(BF).astype(F32)
        sq = pre * pre
        th = jnp.tanh(GELU_C * (pre + 0.044715 * sq * pre))
        cdf = 0.5 * (1.0 + th)
        act[blk] = (pre * cdf).astype(BF)
        slope = cdf + pre * (0.5 * (1.0 - th * th)) * (GELU_C * (1.0 + 3 * 0.044715 * sq))
        dp = cot * slope
        gbu[...] = gbu[...] + fold8(dp, jnp.add)
        dpre[blk] = dp.astype(BF)
        part[blk] = mm(dpre[blk], wu[...], NT).astype(BF)

    with scope('b_gather'):
        ag.run(mlp)
    rs = Scatter(ring, part, pair, stage, land, rs_s, rs_r)
    rs.send_pair(ring.xf, 0)
    rs.send_pair(ring.xr, 1)
    rs.send_pair(ring.xl, 2)
    rs.send_pair(ring.x, 3)
    with scope('b_far'):
        rs.far()
    with scope('b_own'):
        rs.near_own()

    def weight_down(i):
        cols = pl.ds(pl.multiple_of(i * 256, 256), 256)
        left = act[:, :, cols].reshape(n * t, 256)
        gwd[cols, :] = mm(left, dy[...].reshape(n * t, d), T0).astype(BF)

    def weight_up(i):
        cols = pl.ds(pl.multiple_of(i * 256, 256), 256)
        left = gg[:, :, cols].reshape(n * t, 256)
        gwu[cols, :] = mm(left, dpre[...].reshape(n * t, f), T0).astype(BF)

    with scope('b_weights'):
        loop(0, f // 256, weight_down)
        loop(0, d // 256, weight_up)
    with scope('b_sum'):
        rs.near_sum()

    def down(blk):
        part_m[blk] = mm(act[blk], wd[...]).astype(BF)
    with scope('b_down'):
        loop(0, n, down)
    with scope('b_final'):
        rs.wait_final()
    zero_fill(small)

    def last(rows):
        dg = rs.total(rows).astype(BF).astype(F32)
        hat, rstd = norm_rows(x1[rows, :])
        small[0] = small[0] + fold8(dg * hat, jnp.add)
        small[1] = small[1] + fold8(dg, jnp.add)
        dh = dg * g2[...]
        dz = norm_back(dh, hat, rstd)
        dyf = dyo[rows, :].astype(F32)
        dm = dyf + dz
        small[2] = small[2] + fold8(dm, jnp.add)
        small[3] = small[3] + fold8(dyf, jnp.add)
        mid[rows, :] = dm
        da[rows, :] = dm.astype(BF)
    rows_loop(t, 16, last)
    rs.finish()
    ag.finish()


def kernel_c(n, scale, da_hbm, mid, part_m, x_own, x1, h, q, k, v, o, lse, wt, wo, g1, bd, small_b, slopes_ref,
             y, gx, sums, gwt, gbq, gwo,
             dag, wp, km, dom, dlt, dq, dk_acc, dv_acc, d3, gwo_acc, small, every,
             part, pair, stage, land, rs_s, rs_r,
             pair_m, stage_m, land_m, rm_s, rm_r, ag_s, ag_r, ar_s, ar_r, local):
    ring = Ring(n)
    me = ring.me
    t, d = dag.shape[1], dag.shape[2]
    in_d = pltpu.make_async_copy(da_hbm, dag.at[me], local.at[0])
    in_d.start()
    ring.barrier(everyone=True)
    in_d.wait()
    ag = Gather(ring, dag, ag_s, ag_r)
    ag.start()
    rm = Scatter(ring, part_m, pair_m, stage_m, land_m, rm_s, rm_r)
    for slot, xp in enumerate((ring.xf, ring.xr, ring.xl, ring.x)):
        rm.send_pair(xp, slot)
    sort_weight(wp, wt)
    zero_fill(gwo_acc)

    def back_out(blk):
        dc = mm(dag[blk], wo[...], NT).astype(BF)
        zero = jnp.zeros((t, 128), BF)
        for head in PAIR:
            mask = lane_mask(t, head)
            dom[head, blk] = jnp.where(mask, dc, zero)
            km[head, blk] = jnp.where(mask, k[blk], zero)
        prod = (dc.astype(F32) * o[blk].astype(F32)).T
        dlt[LOW, blk] = col_sum(prod[:64])
        dlt[HIGH, blk] = col_sum(prod[64:])
        gwo_acc[...] = gwo_acc[...] + mm(o[blk], dag[blk], T0)
        dq[blk] = jnp.zeros((t, 128), F32)

    with scope('c_gather'):
        ag.run(back_out, after_near=rm.far)
    with scope('c_mown'):
        rm.near_own()
    gwo[...] = gwo_acc[...].astype(BF)
    slopes = [slopes_ref[me * 2 + head] for head in PAIR]
    key = lax.broadcasted_iota(jnp.int32, (t, t), 0)
    qry = lax.broadcasted_iota(jnp.int32, (t, t), 1)

    def kv_block(j):
        pos = (key + j * t).astype(F32)
        zero_fill(dk_acc, dv_acc)

        def pair_block(i, diag):
            tv, tk, tq = dv_acc[...], dk_acc[...], dq[i]
            for head in PAIR:
                s = mm(k[j], q[head, i], NT) * scale + slopes[head] * pos
                if diag:
                    s = jnp.where(key <= qry, s, MASK_VALUE)
                p = jnp.exp(s - lse[head, i])
                dp = mm(v[head, j], dom[head, i], NT).astype(BF).astype(F32)
                ds = (p * (dp - dlt[head, i])).astype(BF)
                tv = tv + mm(p.astype(BF), dom[head, i])
                tk = tk + mm(ds, q[head, i])
                tq = tq + mm(ds, km[head, j], T0)
            dv_acc[...] = tv
            dk_acc[...] = tk
            dq[i] = tq

        pair_block(j, True)
        loop(j + 1, n, lambda i: pair_block(i, False))
        d3[j, :, 128:256] = (dk_acc[...] * scale).astype(BF)
        d3[j, :, 256:384] = dv_acc[...].astype(BF)

        @pl.when(j == 1)
        def _():
            rm.near_sum()

    with scope('c_attend'):
        loop(0, n, kv_block)
    zero_fill(gbq)
    rs = Scatter(ring, part, pair, stage, land, rs_s, rs_r)

    def back_in(xp, slot):
        for cc in PAIR:
            blk = xp * 2 + cc
            d3[blk, :, 0:128] = (dq[blk] * scale).astype(BF)
            part[blk] = mm(d3[blk], wp[...]).astype(BF)
        rs.send_pair(xp, slot)

    with scope('c_far'):
        back_in(ring.xf, 0)
        rs.far()
    with scope('c_own'):
        back_in(ring.xr, 1)
        back_in(ring.xl, 2)
        rs.near_own()
        back_in(ring.x, 3)

    def weight_in(i):
        cols = pl.ds(pl.multiple_of(i * 128, 128), 128)
        left = d3[:, :, cols].reshape(n * t, 128)
        grad = mm(left, h[...].reshape(n * t, d), T0).astype(BF)
        for head in PAIR:
            gwt[head, i] = grad[head * 64:head * 64 + 64]
    with scope('c_weights'):
        loop(0, len(TRIPLE), weight_in)

    def bias_in(b):
        gbq[...] = gbq[...] + fold8(d3[b].astype(F32), jnp.add)
    loop(0, n, bias_in)
    with scope('c_sum'):
        rs.near_sum()
    with scope('c_mfinal'):
        rm.wait_final()

    def out_y(rows):
        m = rm.total(rows).astype(BF).astype(F32)
        y[rows, :] = (x1[rows, :] + m + bd[...]).astype(BF)
    rows_loop(t, 32, out_y)
    zero_fill(small)
    with scope('c_final'):
        rs.wait_final()

    def last(rows):
        dh = rs.total(rows).astype(BF).astype(F32)
        hat, rstd = norm_rows(x_own[rows, :].astype(F32))
        small[0] = small[0] + fold8(dh * hat, jnp.add)
        small[1] = small[1] + fold8(dh, jnp.add)
        dn = dh * g1[...]
        dz = norm_back(dn, hat, rstd)
        gx[rows, :] = (mid[rows, :] + dz).astype(BF)
    rows_loop(t, 16, last)
    for i in range(2):
        every[me, i:i + 1, :] = col_sum(small[i])
    for i in range(4):
        every[me, 2 + i:3 + i, :] = col_sum(small_b[i])
    every[me, 6:8, :] = jnp.zeros((2, d), F32)

    def share(off):
        dev = (me + off) % n
        return pltpu.make_async_remote_copy(
            src_ref=every.at[me], dst_ref=every.at[me], send_sem=ar_s.at[off], recv_sem=ar_r.at[me],
            device_id={'tp': dev}, device_id_type=MESH)

    with scope('c_share'):
        for off in range(1, n):
            share(off).start()
    for off in range(1, n):
        src = (me + off) % n
        pltpu.make_async_remote_copy(
            src_ref=every.at[src], dst_ref=every.at[src], send_sem=ar_s.at[0], recv_sem=ar_r.at[src],
            device_id={'tp': me}, device_id_type=MESH).wait_recv()
    total = every[0]
    for b in range(1, n):
        total = total + every[b]
    sums[...] = total
    for off in range(1, n):
        share(off).wait_send()
    rs.finish()
    rm.finish()
    ag.finish()


def kernel_out(n_big, *refs):
    srcs, (gbq, gbu, sums), refs = refs[:n_big], refs[n_big:n_big + 3], refs[n_big + 3:]
    outs, (o_bq, o_bu), refs = refs[:n_big], refs[n_big:n_big + 2], refs[n_big + 2:]
    o_sums, refs = refs[:6], refs[6:]
    bufs, (sem_in, sem_out) = refs[:n_big], refs[n_big:]
    ins = [pltpu.make_async_copy(a, b, sem_in.at[i]) for i, (a, b) in enumerate(zip(srcs, bufs))]
    backs = [pltpu.make_async_copy(b, a, sem_out.at[i]) for i, (a, b) in enumerate(zip(outs, bufs))]
    for cp in ins:
        cp.start()
    o_bu[...] = col_sum(gbu[...])
    row = col_sum(gbq[...])
    e = o_bq.shape[2]
    for part_no in TRIPLE:
        for head in PAIR:
            at = (part_no * 2 + head) * e
            o_bq[part_no, head:head + 1, :] = row[:, at:at + e]
    for i, ref in enumerate(o_sums):
        ref[...] = sums[i:i + 1, :]
    for cp, back in zip(ins, backs):
        cp.wait()
        back.start()
    for back in backs:
        back.wait()


def whole():
    return pl.BlockSpec(memory_space=VMEM)


def anywhere():
    return pl.BlockSpec(memory_space=pl.ANY)


def smem():
    return pl.BlockSpec(memory_space=pltpu.SMEM)


def solution(mesh):
    n = mesh.shape['tp']

    def local_step(x, ln1_gamma, ln1_beta, w_qkv, b_qkv, w_out, b_out, ln2_gamma, ln2_beta, w_up, b_up, w_down, b_down, grad_y):
        t, d = x.shape[1], x.shape[2]
        heads, e = w_qkv.shape[1], w_qkv.shape[3]
        he = heads * e
        f = w_up.shape[1]
        scale = e ** -0.5
        slopes = jnp.asarray(alibi_slopes(heads * n))
        x2, dy2 = x[0], grad_y[0]
        row = lambda vec: vec.reshape(1, -1)
        wt = w_qkv.transpose(1, 2, 3, 0).reshape(heads * 3 * e, d)
        bq = b_qkv.transpose(1, 0, 2)
        sds = jax.ShapeDtypeStruct
        rows, full, half = (t, d), (n, t, d), (n, t, he)
        both, line = (len(PAIR),) + half, (len(PAIR), n, 1, t)
        packed = (len(TRIPLE) * he, d)
        params = lambda cid: pltpu.CompilerParams(collective_id=cid, has_side_effects=True, vmem_limit_bytes=VLIM)
        dma = pltpu.SemaphoreType.DMA

        h, dy, q, k, v, o, lse, x1, g = pl.pallas_call(
            functools.partial(kernel_a, n, scale),
            name='attend_forward',
            out_shape=[sds(full, BF), sds(full, BF), sds(both, BF), sds(half, BF),
                       sds(both, BF), sds(half, BF), sds(line, F32), sds(rows, F32),
                       sds(rows, BF)],
            in_specs=[anywhere(), anywhere()] + [whole()] * 8 + [smem()],
            out_specs=[whole()] * 9,
            scratch_shapes=[VMEM(full, BF), VMEM(packed, BF), VMEM((2, n, t, t), F32), VMEM((2, 8, t), F32),
                            VMEM((2, 8, t), F32), VMEM((t, he), F32), VMEM(full, BF)]
            + scatter_scratch(n, t, d) + gather_scratch(n) + gather_scratch(n) + [dma((2,))],
            compiler_params=params(0),
        )(x2, dy2, row(ln1_gamma), row(ln1_beta), wt, bq, w_out, row(b_out), row(ln2_gamma), row(ln2_beta), slopes)

        part_m, gwu, gbu, gwd, mid, da, small = pl.pallas_call(
            functools.partial(kernel_b, n),
            name='mlp_both',
            out_shape=[sds(full, BF), sds((d, f), BF), sds((8, f), F32), sds((f, d), BF), sds(rows, F32),
                       sds(rows, BF), sds((4, 8, d), F32)],
            in_specs=[anywhere()] + [whole()] * 7,
            out_specs=[whole()] * 7,
            scratch_shapes=[VMEM(full, BF), VMEM((n, t, f), BF), VMEM((n, t, f), BF), VMEM(full, BF)]
            + scatter_scratch(n, t, d) + gather_scratch(n) + [dma((1,))],
            compiler_params=params(1),
        )(g, x1, dy2, dy, w_up, row(b_up), w_down, row(ln2_gamma))

        y, gx, sums, gwt, gbq, gwo = pl.pallas_call(
            functools.partial(kernel_c, n, scale),
            name='attend_backward',
            out_shape=[sds(rows, BF), sds(rows, BF), sds((8, d), F32), sds((heads, 3, e, d), BF),
                       sds((8, 3 * he), F32), sds((he, d), BF)],
            in_specs=[anywhere()] + [whole()] * 15 + [smem()],
            out_specs=[whole()] * 6,
            scratch_shapes=[VMEM(full, BF), VMEM(packed, BF), VMEM(both, BF), VMEM(both, BF),
                            VMEM(line, F32), VMEM(half, F32), VMEM((t, he), F32), VMEM((t, he), F32),
                            VMEM((n, t, 3 * he), BF), VMEM((he, d), F32), VMEM((2, 8, d), F32), VMEM((n, 8, d), F32),
                            VMEM(full, BF)]
            + scatter_scratch(n, t, d) + scatter_scratch(n, t, d) + gather_scratch(n)
            + [dma((n,)), dma((n,)), dma((1,))],
            compiler_params=params(2),
        )(da, mid, part_m, x2, x1, h, q, k, v, o, lse, wt, w_out, row(ln1_gamma), row(b_down), small, slopes)

        big = (y, gx, gwt, gwo, gwu, gwd)
        res = pl.pallas_call(
            functools.partial(kernel_out, len(big)),
            name='results',
            out_shape=[sds(b.shape, b.dtype) for b in big] + [sds((len(TRIPLE), heads, e), F32), sds((1, f), F32)]
            + [sds((1, d), F32)] * 6,
            in_specs=[anywhere()] * len(big) + [whole()] * 3,
            out_specs=[anywhere()] * len(big) + [whole()] * 8,
            scratch_shapes=[VMEM(b.shape, b.dtype) for b in big] + [dma((len(big),))] * 2,
        )(*big, gbq, gbu, sums)
        y, gx, gwt, gwo, gwu, gwd, gbq, gbu, s_g1, s_b1, s_g2, s_b2, s_bo, s_bd = res
        vec = lambda a: a.reshape(-1)
        return (y[None], gx[None], vec(s_g1), vec(s_b1), gwt.transpose(3, 0, 1, 2), gbq.transpose(1, 0, 2), gwo, vec(s_bo),
                vec(s_g2), vec(s_b2), gwu, vec(gbu), gwd, vec(s_bd))

    row_spec = P('dp', 'tp', None)
    in_specs = (row_spec, P(), P(), P(None, 'tp', None, None), P('tp', None, None), P('tp', None), P(), P(), P(),
                P(None, 'tp'), P('tp'), P('tp', None), P(), row_spec)
    out_specs = (row_spec, row_spec, P('dp'), P('dp'), P('dp', 'tp', None, None), P(('dp', 'tp'), None, None),
                 P(('dp', 'tp'), None), P('dp'), P('dp'), P('dp'), P('dp', 'tp'), P(('dp', 'tp')), P(('dp', 'tp'), None), P('dp'))
    return jax.shard_map(local_step, mesh=mesh, in_specs=in_specs, out_specs=out_specs, check_vma=False)
```

```python
import functools
import math
import jax
import jax.numpy as jnp
import numpy as np
from jax import lax
from jax.experimental import pallas as pl
from jax.experimental.pallas import tpu as pltpu
from jax.sharding import PartitionSpec as P

EPS = 1e-5
MASK_VALUE = -1e30
BF, F32 = jnp.bfloat16, jnp.float32
VMEM = pltpu.VMEM
MESH = pl.DeviceIdType.MESH
scope = jax.named_scope
VLIM = 62 * 1024 * 1024
GELU_C = math.sqrt(2.0 / math.pi)
PAIR = LOW, HIGH = (0, 1)
TRIPLE = (0, 1, 2)
NN = (((1,), (0,)), ((), ()))
T0 = (((0,), (0,)), ((), ()))
NT = (((1,), (1,)), ((), ()))


def alibi_slopes(n_heads):
    closest = 2 ** int(math.floor(math.log2(n_heads)))
    base_ratio = 2.0 ** (-8.0 / closest)
    extra_ratio = 2.0 ** (-4.0 / closest)
    remaining = min(closest, n_heads - closest)
    slopes = [base_ratio ** (i + 1) for i in range(closest)]
    slopes = slopes + [extra_ratio ** (2 * i + 1) for i in range(remaining)]
    return np.array(slopes, dtype=np.float32)


def mm(a, b, dims=NN):
    return lax.dot_general(a, b, dims, preferred_element_type=F32)


def loop(lo, hi, body, unroll=1):
    def step(i, carry):
        body(i)
        return carry
    lax.fori_loop(lo, hi, step, 0, unroll=unroll)


def rows_loop(total, rows, body, unroll=1):
    loop(0, total // rows, lambda r: body(pl.ds(pl.multiple_of(r * rows, rows), rows)), unroll)


def row_mean(z):
    return jnp.mean(z, axis=-1, keepdims=True)


def col_sum(z):
    return jnp.sum(z, axis=0, keepdims=True)


def norm_back(grad, hat, rstd):
    return rstd * (grad - row_mean(grad) - hat * row_mean(grad * hat))


def zero_fill(*refs):
    for ref in refs:
        ref[...] = jnp.zeros(ref.shape, ref.dtype)


def sort_weight(wp, wt):
    e = wp.shape[0] // 6
    for part_no in TRIPLE:
        for head in PAIR:
            dst = (part_no * 2 + head) * e
            src = (head * 3 + part_no) * e
            wp[dst:dst + e, :] = wt[src:src + e, :]


def norm_rows(z):
    cen = z - row_mean(z)
    rstd = lax.rsqrt(row_mean(cen * cen) + EPS)
    return cen * rstd, rstd


def fold8(v, op):
    out = v[0:8]
    for k in range(1, v.shape[0] // 8):
        out = op(out, v[8 * k:8 * k + 8])
    return out


class Ring:
    def __init__(self, n):
        self.n = n
        nx = n // 2
        self.me = lax.axis_index('tp')
        self.x = self.me // 2
        self.c = self.me % 2
        self.nx = nx
        self.xr = (self.x + 1) % nx
        self.xl = (self.x + nx - 1) % nx
        self.xf = (self.x + 2) % nx
        self.right = self.xr * 2 + self.c
        self.left = self.xl * 2 + self.c
        self.far = self.xf * 2 + self.c
        self.partner = self.x * 2 + (1 - self.c)

    def order(self, s):
        odd = s % 2
        dx = jnp.where(s < 2, 0, jnp.where(s >= 6, 2, jnp.where(odd == 0, self.nx - 1, 1)))
        mid = jnp.where(s < 4, 0, 1)
        dc = jnp.where(s < 2, odd, jnp.where(s >= 6, odd, mid))
        return ((self.x + dx) % self.nx) * 2 + (self.c + dc) % 2

    def barrier(self, everyone=False):
        sem = pltpu.get_barrier_semaphore()
        if everyone:
            peers = [(self.me + k) % self.n for k in range(1, self.n)]
        else:
            peers = [self.right, self.left, self.partner]
        for peer in peers:
            pl.semaphore_signal(sem, inc=1, device_id={'tp': peer}, device_id_type=MESH)
        pl.semaphore_wait(sem, len(peers))


class Gather:
    SENDS = 14

    def __init__(self, ring, buf, ssem, rsem):
        self.ring, self.buf, self.ssem, self.rsem = ring, buf, ssem, rsem
        self.half = buf.shape[1] // 2

    def cp(self, blk, half, dev, k):
        ref = self.buf.at[blk, pl.ds(half * self.half, self.half)]
        return pltpu.make_async_remote_copy(
            src_ref=ref, dst_ref=ref, send_sem=self.ssem.at[k], recv_sem=self.rsem.at[blk, half],
            device_id={'tp': dev}, device_id_type=MESH)

    def start(self):
        r = self.ring
        self.cp(r.me, LOW, r.right, 0).start()
        self.cp(r.me, HIGH, r.left, 1).start()
        self.cp(r.me, HIGH, r.right, 2).start()
        self.cp(r.me, LOW, r.left, 3).start()
        self.cp(r.me, LOW, r.partner, 4).start()
        self.cp(r.me, HIGH, r.partner, 5).start()

    def wait(self, blk, half):
        self.cp(blk, half, self.ring.me, 0).wait_recv()

    def wait_block(self, blk):
        for half in PAIR:
            self.wait(blk, half)

    def near1(self):
        r = self.ring
        self.wait(r.left, LOW)
        self.cp(r.left, LOW, r.right, 6).start()
        self.cp(r.left, LOW, r.partner, 7).start()
        self.wait(r.right, HIGH)
        self.cp(r.right, HIGH, r.left, 8).start()
        self.cp(r.right, HIGH, r.partner, 9).start()

    def near2(self):
        r = self.ring
        self.wait(r.left, HIGH)
        self.cp(r.left, HIGH, r.partner, 10).start()
        self.wait(r.right, LOW)
        self.cp(r.right, LOW, r.partner, 11).start()

    def far(self):
        r = self.ring
        self.wait(r.far, LOW)
        self.cp(r.far, LOW, r.partner, 12).start()
        self.wait(r.far, HIGH)
        self.cp(r.far, HIGH, r.partner, 13).start()

    def finish(self):
        for k in range(self.SENDS):
            self.cp(self.ring.me, 0, self.ring.right, k).wait_send()

    def run(self, body, after_near=None):
        r = self.ring

        def step(s):
            blk = r.order(s)

            @pl.when(s == 1)
            def _():
                self.wait_block(blk)

            @pl.when(s == 2)
            def _():
                self.near1()
                if after_near is not None:
                    after_near()
                self.near2()

            @pl.when((s == 4) | (s == 5) | (s == 7))
            def _():
                self.wait_block(blk)

            @pl.when(s == 6)
            def _():
                self.far()

            body(blk)

        loop(0, r.n, step)


class Scatter:
    SENDS = 10

    def __init__(self, ring, part, pair, stage, land, ssem, rsem):
        self.ring, self.part, self.pair, self.stage, self.land = ring, part, pair, stage, land
        self.ssem, self.rsem = ssem, rsem
        self.rows = part.shape[1]
        self.half = self.rows // 2

    def cp_pair(self, xp, k):
        r = self.ring
        return pltpu.make_async_remote_copy(
            src_ref=self.part.at[xp * 2 + (1 - r.c)], dst_ref=self.pair.at[xp], send_sem=self.ssem.at[k],
            recv_sem=self.rsem.at[xp], device_id={'tp': r.partner}, device_id_type=MESH)

    def cp(self, slot, half, dst_slot, dev, k):
        rows = pl.ds(half * self.half, self.half)
        return pltpu.make_async_remote_copy(
            src_ref=self.stage.at[slot, rows], dst_ref=self.land.at[dst_slot, rows],
            send_sem=self.ssem.at[k], recv_sem=self.rsem.at[4 + 2 * dst_slot + half],
            device_id={'tp': dev}, device_id_type=MESH)

    def wait_land(self, dst_slot, half):
        self.cp(0, half, dst_slot, self.ring.me, 0).wait_recv()

    def wait_pair(self, xp):
        self.cp_pair(xp, 0).wait_recv()

    def send_pair(self, xp, k):
        self.cp_pair(xp, k).start()

    def mix(self, slot, xp, half, with_far=False):
        blk = xp * 2 + self.ring.c
        step = 16

        def body(i):
            rows = pl.ds(pl.multiple_of(half * self.half + i * step, step), step)
            total = self.part[blk, rows, :].astype(F32) + self.pair[xp, rows, :].astype(F32)
            if with_far:
                total = total + self.land[0, rows, :].astype(F32)
            self.stage[slot, rows, :] = total.astype(BF)
        loop(0, self.half // step, body)

    def far(self):
        r = self.ring
        self.wait_pair(r.xf)
        self.mix(0, r.xf, 0)
        self.cp(0, 0, 0, r.right, 4).start()
        self.mix(0, r.xf, 1)
        self.cp(0, 1, 0, r.left, 5).start()

    def near_own(self):
        r = self.ring
        self.wait_pair(r.xr)
        self.mix(1, r.xr, 1)
        self.cp(1, 1, 1, r.right, 6).start()
        self.wait_pair(r.xl)
        self.mix(2, r.xl, 0)
        self.cp(2, 0, 2, r.left, 7).start()

    def near_sum(self):
        r = self.ring
        self.wait_land(0, 0)
        self.mix(1, r.xr, 0, with_far=True)
        self.cp(1, 0, 1, r.right, 8).start()
        self.wait_land(0, 1)
        self.mix(2, r.xl, 1, with_far=True)
        self.cp(2, 1, 2, r.left, 9).start()

    def wait_final(self):
        self.wait_pair(self.ring.x)
        for slot in (1, 2):
            for half in PAIR:
                self.wait_land(slot, half)

    def total(self, rows):
        r = self.ring
        return (self.part[r.me, rows, :].astype(F32) + self.pair[r.x, rows, :].astype(F32)
                + self.land[1, rows, :].astype(F32) + self.land[2, rows, :].astype(F32))

    def finish(self):
        for k in range(4):
            self.cp_pair(self.ring.x, k).wait_send()
        for k in range(4, self.SENDS):
            self.cp(0, 0, 0, self.ring.right, k).wait_send()


def scatter_scratch(n, rows, d):
    return [VMEM((n // 2, rows, d), BF), VMEM((3, rows, d), BF), VMEM((3, rows, d), BF),
            pltpu.SemaphoreType.DMA((Scatter.SENDS,)), pltpu.SemaphoreType.DMA((4 + 6,))]


def gather_scratch(n):
    return [pltpu.SemaphoreType.DMA((Gather.SENDS,)), pltpu.SemaphoreType.DMA((n, 2))]


def lane_mask(rows, h):
    lane = lax.broadcasted_iota(jnp.int32, (rows, 128), 1)
    return (lane < 64) if h == 0 else (lane >= 64)


def attend_block(i, q_ref, k_ref, v_ref, o_ref, lse_ref, s_ref, m_ref, l_ref, acc_ref, slopes, scale):
    t = q_ref.shape[2]
    key = lax.broadcasted_iota(jnp.int32, (t, t), 0)
    qry = lax.broadcasted_iota(jnp.int32, (t, t), 1)
    for h in PAIR:
        m_ref[h] = jnp.full((8, t), MASK_VALUE, F32)
        l_ref[h] = jnp.zeros((8, t), F32)
    zero_fill(acc_ref)

    def score(j, diag):
        pos = (key + j * t).astype(F32)
        for h in PAIR:
            s = mm(k_ref[j], q_ref[h, i], NT) * scale + slopes[h] * pos
            if diag:
                s = jnp.where(key <= qry, s, MASK_VALUE)
            s_ref[h, j] = s
            m_ref[h] = jnp.maximum(m_ref[h], fold8(s, jnp.maximum))

    loop(0, i, lambda j: score(j, False))
    score(i, True)
    top = [jnp.max(m_ref[h], axis=0, keepdims=True) for h in (0, 1)]

    def denom(j):
        for h in PAIR:
            l_ref[h] = l_ref[h] + fold8(jnp.exp(s_ref[h, j] - top[h]), jnp.add)

    loop(0, i + 1, denom)
    for h in PAIR:
        lse_ref[h, i] = top[h] + jnp.log(col_sum(l_ref[h]))

    def values(j):
        total = acc_ref[...]
        for h in PAIR:
            p = jnp.exp(s_ref[h, j] - lse_ref[h, i]).astype(BF)
            total = total + mm(p, v_ref[h, j], T0)
        acc_ref[...] = total

    loop(0, i + 1, values)
    o_ref[i] = acc_ref[...].astype(BF)


def kernel_main(n, scale, x_hbm, dy_hbm, wt_hbm, wo_hbm, wu_hbm, wd_hbm, g1, b1, bqkv, bo, g2, b2, bu, bd, slopes_ref,
                y, gx, sums, gwt, gbq, gwo, gwu, gbu, gwd, h_hbm,
                xg, xo, dyo, dy, hg, wt, wp, wof, wu, wd, q, k, v, o, lse, orow, s_ref, m_ref, l_ref, acc,
                x1, act, dpre, mid, dcs, dcr, km, dom, dlt, dq, dk_acc, dv_acc, d3, small, every, part,
                *rest):
    rest = list(rest)

    def take(count):
        head = rest[:count]
        del rest[:count]
        return head

    ring = Ring(n)
    me = ring.me
    t, d, f = xg.shape[1], xg.shape[2], wu.shape[1]
    rs_refs, rm_refs = take(5), take(5)
    ax, ay, aw, ag, ad = [Gather(ring, buf, *take(2)) for buf in (xg, dy, wof, hg, xg)]
    o_send, o_recv, c_send, c_recv, ar_s, ar_r, local = take(7)

    def fetch(i, src, dst):
        cp = pltpu.make_async_copy(src, dst, local.at[i])
        cp.start()
        return cp

    in_x, in_wo, in_dy, in_wt = (fetch(0, x_hbm, xg.at[me]), fetch(1, wo_hbm, wof.at[me]),
                                 fetch(2, dy_hbm, dy.at[me]), fetch(3, wt_hbm, wt))
    later = [fetch(4, wu_hbm, wu), fetch(5, wd_hbm, wd), fetch(6, x_hbm, xo), fetch(7, dy_hbm, dyo)]
    ring.barrier(everyone=True)
    in_x.wait()
    ax.start()
    in_wt.wait()
    sort_weight(wp, wt)
    in_wo.wait()
    in_dy.wait()
    bias = jnp.concatenate([bqkv[kind, head:head + 1, :] for kind in TRIPLE for head in PAIR], axis=1)

    def project(blk):
        def norm(rows):
            hat, _ = norm_rows(xg[blk, rows, :].astype(F32))
            hg[blk, rows, :] = (hat * g1[...] + b1[...]).astype(BF)
        rows_loop(t, 32, norm)
        out = mm(hg[blk], wp[...], NT) + bias
        out = out.astype(BF)
        zero = jnp.zeros((t, 128), BF)
        for head in PAIR:
            q[head, blk] = jnp.where(lane_mask(t, head), out[:, :128], zero)
            v[head, blk] = jnp.where(lane_mask(t, head), out[:, 256:], zero)
        k[blk] = out[:, 128:256]
        fetch(0, hg.at[blk], h_hbm.at[blk])

    with scope('a_gather'):
        ax.run(project, after_near=aw.start)
    slopes = [slopes_ref[me * 2 + head] for head in PAIR]

    def send_o(i):
        cols = pl.ds(pl.multiple_of(me * 128, 128), 128)
        return pltpu.make_async_remote_copy(
            src_ref=o.at[i], dst_ref=orow.at[:, cols], send_sem=o_send.at[i], recv_sem=o_recv.at[me],
            device_id={'tp': i}, device_id_type=MESH)

    def all_blocks(i):
        for at, act_now in ((2, aw.near2), (3, aw.far), (n - 2, ay.near1), (n - 1, ay.near2)):
            pl.when(i == at)(act_now)
        attend_block(i, q, k, v, o, lse, s_ref, m_ref, l_ref, acc, slopes, scale)

        @pl.when(i != me)
        def _():
            send_o(i).start()

    with scope('a_attend'):
        aw.near1()
        ay.start()
        ax.finish()
        pltpu.make_async_copy(hg, h_hbm, local.at[0]).wait()
        loop(0, n, all_blocks)
    with scope('a_wait'):
        orow[:, pl.ds(pl.multiple_of(me * 128, 128), 128)] = o[me]
        for off in range(1, n):
            src = (me + off) % n
            cols = pl.ds(pl.multiple_of(src * 128, 128), 128)
            pltpu.make_async_remote_copy(
                src_ref=o.at[0], dst_ref=orow.at[:, cols], send_sem=o_send.at[0], recv_sem=o_recv.at[src],
                device_id={'tp': me}, device_id_type=MESH).wait_recv()
        for dx in (ring.x, ring.xl, ring.xr, ring.xf):
            aw.wait_block(dx * 2 + (1 - ring.c))
        later[2].wait()
    with scope('a_out'):
        x1[...] = mm(orow[...], wof[...].reshape(n * 128, d)).astype(BF).astype(F32)

        def enter(rows):
            row = xo[rows, :].astype(F32) + x1[rows, :] + bo[...]
            x1[rows, :] = row
            hat, _ = norm_rows(row)
            hg[me, rows, :] = (hat * g2[...] + b2[...]).astype(BF)
        rows_loop(t, 32, enter)
        ag.start()
    with scope('a_rest'):
        ay.far()
        for dx in (ring.x, ring.xl, ring.xr, ring.xf):
            ay.wait_block(dx * 2 + (1 - ring.c))
        for cp in (later[0], later[1], later[3]):
            cp.wait()
        zero_fill(gbu)

    def mlp(blk):
        pre = mm(hg[blk], wu[...]) + bu[...]
        cot = mm(dy[blk], wd[...], NT).astype(BF).astype(F32)
        sq = pre * pre
        th = jnp.tanh(GELU_C * (pre + 0.044715 * sq * pre))
        cdf = 0.5 * (1.0 + th)
        act[blk] = (pre * cdf).astype(BF)
        slope = cdf + pre * (0.5 * (1.0 - th * th)) * (GELU_C * (1.0 + 3 * 0.044715 * sq))
        dp = cot * slope
        gbu[...] = gbu[...] + fold8(dp, jnp.add)
        dpre[blk] = dp.astype(BF)
        part[blk] = mm(dpre[blk], wu[...], NT).astype(BF)

    with scope('b_gather'):
        ag.run(mlp)
    rs = Scatter(ring, part, *rs_refs)
    chips = (ring.xf, ring.xr, ring.xl, ring.x)
    for slot, xp in enumerate(chips):
        rs.send_pair(xp, slot)
    with scope('b_far'):
        rs.far()
    with scope('b_own'):
        rs.near_own()
    ay.finish()

    def weight_down(i):
        cols = pl.ds(pl.multiple_of(i * 256, 256), 256)
        left = act[:, :, cols].reshape(n * t, 256)
        gwd[cols, :] = mm(left, dy[...].reshape(n * t, d), T0).astype(BF)

    def weight_up(i):
        cols = pl.ds(pl.multiple_of(i * 256, 256), 256)
        left = hg[:, :, cols].reshape(n * t, 256)
        gwu[cols, :] = mm(left, dpre[...].reshape(n * t, f), T0).astype(BF)

    with scope('b_weights'):
        loop(0, f // 256, weight_down)
        loop(0, d // 256, weight_up)
    with scope('b_sum'):
        rs.near_sum()
    zero_fill(small)

    def down(blk):
        dy[blk] = mm(act[blk], wd[...]).astype(BF)
    with scope('b_down'):
        loop(0, n, down)
    with scope('b_final'):
        rs.wait_final()

    def leave(rows):
        dg = rs.total(rows).astype(BF).astype(F32)
        hat, rstd = norm_rows(x1[rows, :])
        small[2] = small[2] + fold8(dg * hat, jnp.add)
        small[3] = small[3] + fold8(dg, jnp.add)
        dz = norm_back(dg * g2[...], hat, rstd)
        dyf = dyo[rows, :].astype(F32)
        dm = dyf + dz
        small[4] = small[4] + fold8(dm, jnp.add)
        small[5] = small[5] + fold8(dyf, jnp.add)
        mid[rows, :] = dm
        xg[me, rows, :] = dm.astype(BF)

    def send_c(dev):
        return pltpu.make_async_remote_copy(
            src_ref=dcs.at[dev], dst_ref=dcr.at[me], send_sem=c_send.at[dev], recv_sem=c_recv.at[me],
            device_id={'tp': dev}, device_id_type=MESH)

    with scope('b_leave'):
        rows_loop(t, 16, leave)
        rs.finish()
        ag.finish()
    with scope('c_send'):
        def back_out(step):
            dev = ring.order(n - 1 - step)
            dcs[dev] = mm(xg[me], wof[dev], NT).astype(BF)

            @pl.when(step < n - 1)
            def _():
                send_c(dev).start()
        loop(0, n, back_out)
        ad.start()
        reload = fetch(0, h_hbm, hg)
    rm = Scatter(ring, dy, *rm_refs)
    for slot, xp in enumerate(chips):
        rm.send_pair(xp, slot)
    dcr[me] = dcs[me]

    def prepare(step):
        blk = ring.order(step)

        @pl.when(step > 0)
        def _():
            pltpu.make_async_remote_copy(
                src_ref=dcs.at[0], dst_ref=dcr.at[blk], send_sem=c_send.at[0], recv_sem=c_recv.at[blk],
                device_id={'tp': me}, device_id_type=MESH).wait_recv()
        dc = dcr[blk]
        zero = jnp.zeros((t, 128), BF)
        for head in PAIR:
            mask = lane_mask(t, head)
            dom[head, blk] = jnp.where(mask, dc, zero)
            km[head, blk] = jnp.where(mask, k[blk], zero)
        prod = (dc.astype(F32) * o[blk].astype(F32)).T
        dlt[LOW, blk] = col_sum(prod[:64])
        dlt[HIGH, blk] = col_sum(prod[64:])
        dq[blk] = jnp.zeros((t, 128), F32)

    with scope('c_prepare'):
        rm.far()
        loop(0, n, prepare)
    key = lax.broadcasted_iota(jnp.int32, (t, t), 0)
    qry = lax.broadcasted_iota(jnp.int32, (t, t), 1)

    def kv_block(j):
        pos = (key + j * t).astype(F32)
        zero_fill(dk_acc, dv_acc)

        def pair_block(i, diag):
            tv, tk, tq = dv_acc[...], dk_acc[...], dq[i]
            for head in PAIR:
                s = mm(k[j], q[head, i], NT) * scale + slopes[head] * pos
                if diag:
                    s = jnp.where(key <= qry, s, MASK_VALUE)
                p = jnp.exp(s - lse[head, i])
                dp = mm(v[head, j], dom[head, i], NT).astype(BF).astype(F32)
                ds = (p * (dp - dlt[head, i])).astype(BF)
                tv = tv + mm(p.astype(BF), dom[head, i])
                tk = tk + mm(ds, q[head, i])
                tq = tq + mm(ds, km[head, j], T0)
            dv_acc[...] = tv
            dk_acc[...] = tk
            dq[i] = tq

        for at, act_now in ((2, ad.near1), (2, rm.near_own), (3, ad.near2), (n - 3, rm.near_sum)):
            pl.when(j == at)(act_now)
        pair_block(j, True)
        loop(j + 1, n, lambda i: pair_block(i, False))
        d3[j, :, 128:256] = (dk_acc[...] * scale).astype(BF)
        d3[j, :, 256:] = dv_acc[...].astype(BF)

    with scope('c_attend'):
        loop(0, n, kv_block)
    zero_fill(gbq)

    def back_in(xp, slot):
        for cc in PAIR:
            blk = xp * 2 + cc
            d3[blk, :, :128] = (dq[blk] * scale).astype(BF)
            part[blk] = mm(d3[blk], wp[...]).astype(BF)
        rs.send_pair(xp, slot)

    with scope('c_far'):
        back_in(ring.xf, 0)
        rs.far()
    with scope('c_own'):
        back_in(ring.xr, 1)
        back_in(ring.xl, 2)
        rs.near_own()
        back_in(ring.x, 3)
    with scope('c_da'):
        ad.far()
        reload.wait()

    def weight_in(i):
        cols = pl.ds(pl.multiple_of(i * 128, 128), 128)
        left = d3[:, :, cols].reshape(n * t, 128)
        grad = mm(left, hg[...].reshape(n * t, d), T0).astype(BF)
        for head in PAIR:
            gwt[head, i] = grad[head * 64:head * 64 + 64]

    def bias_in(b):
        gbq[...] = gbq[...] + fold8(d3[b].astype(F32), jnp.add)

    with scope('c_weights'):
        loop(0, len(TRIPLE), weight_in)
        loop(0, n, bias_in)
    with scope('c_sum'):
        rs.near_sum()
    with scope('c_gwo'):
        for dx in (ring.x, ring.xl, ring.xr, ring.xf):
            ad.wait_block(dx * 2 + (1 - ring.c))
        gwo[...] = mm(o[...].reshape(n * t, 128), xg[...].reshape(n * t, d), T0).astype(BF)
    with scope('c_mfinal'):
        rm.wait_final()

    def out_y(rows):
        m = rm.total(rows).astype(BF).astype(F32)
        y[rows, :] = (x1[rows, :] + m + bd[...]).astype(BF)
    rows_loop(t, 32, out_y)
    with scope('c_final'):
        rs.wait_final()

    def last(rows):
        dh = rs.total(rows).astype(BF).astype(F32)
        hat, rstd = norm_rows(xo[rows, :].astype(F32))
        small[0] = small[0] + fold8(dh * hat, jnp.add)
        small[1] = small[1] + fold8(dh, jnp.add)
        gx[rows, :] = (mid[rows, :] + norm_back(dh * g1[...], hat, rstd)).astype(BF)
    with scope('c_last'):
        rows_loop(t, 16, last)
    for i in range(6):
        every[me, i:i + 1, :] = col_sum(small[i])
    every[me, 6:, :] = jnp.zeros((2, d), F32)

    def share(off):
        return pltpu.make_async_remote_copy(
            src_ref=every.at[me], dst_ref=every.at[me], send_sem=ar_s.at[off], recv_sem=ar_r.at[me],
            device_id={'tp': (me + off) % n}, device_id_type=MESH)

    with scope('c_share'):
        for off in range(1, n):
            share(off).start()
        for off in range(1, n):
            src = (me + off) % n
            pltpu.make_async_remote_copy(
                src_ref=every.at[src], dst_ref=every.at[src], send_sem=ar_s.at[0], recv_sem=ar_r.at[src],
                device_id={'tp': me}, device_id_type=MESH).wait_recv()
        total = every[0]
        for b in range(1, n):
            total = total + every[b]
        sums[...] = total
    for off in range(1, n):
        share(off).wait_send()
        send_o((me + off) % n).wait_send()
        send_c((me + off) % n).wait_send()
    for job in (rs, rm, aw, ad):
        job.finish()


def kernel_out(n_big, *refs):
    srcs, (gbq, gbu, sums), refs = refs[:n_big], refs[n_big:n_big + 3], refs[n_big + 3:]
    outs, (o_bq, o_bu), refs = refs[:n_big], refs[n_big:n_big + 2], refs[n_big + 2:]
    o_sums, refs = refs[:6], refs[6:]
    bufs, (sem_in, sem_out) = refs[:n_big], refs[n_big:]
    ins = [pltpu.make_async_copy(a, b, sem_in.at[i]) for i, (a, b) in enumerate(zip(srcs, bufs))]
    backs = [pltpu.make_async_copy(b, a, sem_out.at[i]) for i, (a, b) in enumerate(zip(outs, bufs))]
    for cp in ins:
        cp.start()
    o_bu[...] = col_sum(gbu[...])
    row = col_sum(gbq[...])
    e = o_bq.shape[2]
    for part_no in TRIPLE:
        for head in PAIR:
            at = (part_no * 2 + head) * e
            o_bq[part_no, head:head + 1, :] = row[:, at:at + e]
    for i, ref in enumerate(o_sums):
        ref[...] = sums[i:i + 1, :]
    for cp, back in zip(ins, backs):
        cp.wait()
        back.start()
    for back in backs:
        back.wait()


def whole():
    return pl.BlockSpec(memory_space=VMEM)


def anywhere():
    return pl.BlockSpec(memory_space=pl.ANY)


def smem():
    return pl.BlockSpec(memory_space=pltpu.SMEM)


def solution(mesh):
    n = mesh.shape['tp']

    def local_step(x, ln1_gamma, ln1_beta, w_qkv, b_qkv, w_out, b_out, ln2_gamma, ln2_beta, w_up, b_up, w_down, b_down, grad_y):
        t, d = x.shape[1], x.shape[2]
        heads, e = w_qkv.shape[1], w_qkv.shape[3]
        he = heads * e
        f = w_up.shape[1]
        scale = e ** -0.5
        slopes = jnp.asarray(alibi_slopes(heads * n))
        x2, dy2 = x[0], grad_y[0]
        row = lambda vec: vec.reshape(1, -1)
        wt = w_qkv.transpose(1, 2, 3, 0).reshape(heads * 3 * e, d)
        bq = b_qkv.transpose(1, 0, 2)
        sds = jax.ShapeDtypeStruct
        rows, full, half = (t, d), (n, t, d), (n, t, he)
        both, line = (len(PAIR),) + half, (len(PAIR), n, 1, t)
        packed = (len(TRIPLE) * he, d)
        params = lambda cid: pltpu.CompilerParams(collective_id=cid, has_side_effects=True, vmem_limit_bytes=VLIM)
        dma = pltpu.SemaphoreType.DMA

        vm = lambda dims, kind=BF: VMEM(dims, kind)
        stat, square = (len(PAIR), 8, t), (t, he)
        y, gx, sums, gwt, gbq, gwo, gwu, gbu, gwd, _ = pl.pallas_call(
            functools.partial(kernel_main, n, scale),
            name='layer',
            out_shape=[sds(rows, BF), sds(rows, BF), sds((8, d), F32), sds((heads, len(TRIPLE), e, d), BF),
                       sds((8, len(TRIPLE) * he), F32), sds((he, d), BF), sds((d, f), BF), sds((8, f), F32),
                       sds((f, d), BF), sds(full, BF)],
            in_specs=[anywhere()] * 6 + [whole()] * 8 + [smem()],
            out_specs=[whole()] * 9 + [anywhere()],
            scratch_shapes=[vm(full), vm(rows), vm(rows), vm(full), vm(full), vm(packed), vm(packed), vm((n, he, d)), vm((d, f)),
                            vm((f, d)), vm(both), vm(half), vm(both), vm(half), vm(line, F32), vm(rows),
                            vm((len(PAIR), n, t, t), F32), vm(stat, F32), vm(stat, F32), vm(square, F32),
                            vm(rows, F32), vm((n, t, f)), vm((n, t, f)), vm(rows, F32), vm(half), vm(half),
                            vm(both), vm(both), vm(line, F32), vm(half, F32), vm(square, F32), vm(square, F32),
                            vm((n, t, len(TRIPLE) * he)), vm((6, 8, d), F32), vm((n, 8, d), F32), vm(full)]
            + scatter_scratch(n, t, d) * 2 + gather_scratch(n) * 5 + [dma((n,))] * 7,
            compiler_params=params(0),
        )(x2, dy2, wt, w_out, w_up, w_down, row(ln1_gamma), row(ln1_beta), bq, row(b_out), row(ln2_gamma), row(ln2_beta),
          row(b_up), row(b_down), slopes)

        big = (y, gx, gwt, gwo, gwu, gwd)
        res = pl.pallas_call(
            functools.partial(kernel_out, len(big)),
            name='results',
            out_shape=[sds(b.shape, b.dtype) for b in big] + [sds((len(TRIPLE), heads, e), F32), sds((1, f), F32)]
            + [sds((1, d), F32)] * 6,
            in_specs=[anywhere()] * len(big) + [whole()] * 3,
            out_specs=[anywhere()] * len(big) + [whole()] * 8,
            scratch_shapes=[VMEM(b.shape, b.dtype) for b in big] + [dma((len(big),))] * 2,
        )(*big, gbq, gbu, sums)
        y, gx, gwt, gwo, gwu, gwd, gbq, gbu, s_g1, s_b1, s_g2, s_b2, s_bo, s_bd = res
        vec = lambda a: a.reshape(-1)
        return (y[None], gx[None], vec(s_g1), vec(s_b1), gwt.transpose(3, 0, 1, 2), gbq.transpose(1, 0, 2), gwo, vec(s_bo),
                vec(s_g2), vec(s_b2), gwu, vec(gbu), gwd, vec(s_bd))

    row_spec = P('dp', 'tp', None)
    in_specs = (row_spec, P(), P(), P(None, 'tp', None, None), P('tp', None, None), P('tp', None), P(), P(), P(),
                P(None, 'tp'), P('tp'), P('tp', None), P(), row_spec)
    out_specs = (row_spec, row_spec, P('dp'), P('dp'), P('dp', 'tp', None, None), P(('dp', 'tp'), None, None),
                 P(('dp', 'tp'), None), P('dp'), P('dp'), P('dp'), P('dp', 'tp'), P(('dp', 'tp')), P(('dp', 'tp'), None), P('dp'))
    return jax.shard_map(local_step, mesh=mesh, in_specs=in_specs, out_specs=out_specs, check_vma=False)
```

```python
import functools
import math
import jax
import jax.numpy as jnp
import numpy as np
from jax import lax
from jax.experimental import pallas as pl
from jax.experimental.pallas import tpu as pltpu
from jax.sharding import PartitionSpec as P

EPS = 1e-5
MASK_VALUE = -1e30
BF, F32 = jnp.bfloat16, jnp.float32
VMEM = pltpu.VMEM
MESH = pl.DeviceIdType.MESH
scope = jax.named_scope
VLIM = 62 * 1024 * 1024
GELU_C = math.sqrt(2.0 / math.pi)
PAIR = LOW, HIGH = (0, 1)
TRIPLE = (0, 1, 2)
NN = (((1,), (0,)), ((), ()))
T0 = (((0,), (0,)), ((), ()))
NT = (((1,), (1,)), ((), ()))


def alibi_slopes(n_heads):
    closest = 2 ** int(math.floor(math.log2(n_heads)))
    base_ratio = 2.0 ** (-8.0 / closest)
    extra_ratio = 2.0 ** (-4.0 / closest)
    remaining = min(closest, n_heads - closest)
    slopes = [base_ratio ** (i + 1) for i in range(closest)]
    slopes = slopes + [extra_ratio ** (2 * i + 1) for i in range(remaining)]
    return np.array(slopes, dtype=np.float32)


def mm(a, b, dims=NN):
    return lax.dot_general(a, b, dims, preferred_element_type=F32)


def loop(lo, hi, body, unroll=1):
    def step(i, carry):
        body(i)
        return carry
    lax.fori_loop(lo, hi, step, 0, unroll=unroll)


def rows_loop(total, rows, body, unroll=1):
    loop(0, total // rows, lambda r: body(pl.ds(pl.multiple_of(r * rows, rows), rows)), unroll)


def row_mean(z):
    return jnp.mean(z, axis=-1, keepdims=True)


def col_sum(z):
    return jnp.sum(z, axis=0, keepdims=True)


def norm_back(grad, hat, rstd):
    return rstd * (grad - row_mean(grad) - hat * row_mean(grad * hat))


def zero_fill(*refs):
    for ref in refs:
        ref[...] = jnp.zeros(ref.shape, ref.dtype)


def sort_weight(wp, wt):
    e = wp.shape[0] // 6
    for part_no in TRIPLE:
        for head in PAIR:
            dst = (part_no * 2 + head) * e
            src = (head * 3 + part_no) * e
            wp[dst:dst + e, :] = wt[src:src + e, :]


def norm_rows(z):
    cen = z - row_mean(z)
    rstd = lax.rsqrt(row_mean(cen * cen) + EPS)
    return cen * rstd, rstd


def fold8(v, op):
    out = v[0:8]
    for k in range(1, v.shape[0] // 8):
        out = op(out, v[8 * k:8 * k + 8])
    return out


class Ring:
    def __init__(self, n):
        self.n = n
        nx = n // 2
        self.me = lax.axis_index('tp')
        self.x = self.me // 2
        self.c = self.me % 2
        self.nx = nx
        self.xr = (self.x + 1) % nx
        self.xl = (self.x + nx - 1) % nx
        self.xf = (self.x + 2) % nx
        self.right = self.xr * 2 + self.c
        self.left = self.xl * 2 + self.c
        self.far = self.xf * 2 + self.c
        self.partner = self.x * 2 + (1 - self.c)

    def order(self, s):
        odd = s % 2
        dx = jnp.where(s < 2, 0, jnp.where(s >= 6, 2, jnp.where(odd == 0, self.nx - 1, 1)))
        mid = jnp.where(s < 4, 0, 1)
        dc = jnp.where(s < 2, odd, jnp.where(s >= 6, odd, mid))
        return ((self.x + dx) % self.nx) * 2 + (self.c + dc) % 2

    def barrier(self, everyone=False):
        sem = pltpu.get_barrier_semaphore()
        if everyone:
            peers = [(self.me + k) % self.n for k in range(1, self.n)]
        else:
            peers = [self.right, self.left, self.partner]
        for peer in peers:
            pl.semaphore_signal(sem, inc=1, device_id={'tp': peer}, device_id_type=MESH)
        pl.semaphore_wait(sem, len(peers))


class Gather:
    SENDS = 14

    def __init__(self, ring, buf, ssem, rsem):
        self.ring, self.buf, self.ssem, self.rsem = ring, buf, ssem, rsem
        self.half = buf.shape[1] // 2

    def cp(self, blk, half, dev, k):
        ref = self.buf.at[blk, pl.ds(half * self.half, self.half)]
        return pltpu.make_async_remote_copy(
            src_ref=ref, dst_ref=ref, send_sem=self.ssem.at[k], recv_sem=self.rsem.at[blk, half],
            device_id={'tp': dev}, device_id_type=MESH)

    def start(self):
        r = self.ring
        self.cp(r.me, LOW, r.right, 0).start()
        self.cp(r.me, HIGH, r.left, 1).start()
        self.cp(r.me, HIGH, r.right, 2).start()
        self.cp(r.me, LOW, r.left, 3).start()
        self.cp(r.me, LOW, r.partner, 4).start()
        self.cp(r.me, HIGH, r.partner, 5).start()

    def wait(self, blk, half):
        self.cp(blk, half, self.ring.me, 0).wait_recv()

    def wait_block(self, blk):
        for half in PAIR:
            self.wait(blk, half)

    def near1(self):
        r = self.ring
        self.wait(r.left, LOW)
        self.cp(r.left, LOW, r.right, 6).start()
        self.cp(r.left, LOW, r.partner, 7).start()
        self.wait(r.right, HIGH)
        self.cp(r.right, HIGH, r.left, 8).start()
        self.cp(r.right, HIGH, r.partner, 9).start()

    def near2(self):
        r = self.ring
        self.wait(r.left, HIGH)
        self.cp(r.left, HIGH, r.partner, 10).start()
        self.wait(r.right, LOW)
        self.cp(r.right, LOW, r.partner, 11).start()

    def far(self):
        r = self.ring
        self.wait(r.far, LOW)
        self.cp(r.far, LOW, r.partner, 12).start()
        self.wait(r.far, HIGH)
        self.cp(r.far, HIGH, r.partner, 13).start()

    def finish(self):
        for k in range(self.SENDS):
            self.cp(self.ring.me, 0, self.ring.right, k).wait_send()

    def run(self, body, before_near=None, after_far=None):
        r = self.ring

        def step(s):
            blk = r.order(s)

            @pl.when(s == 1)
            def _():
                self.wait_block(blk)

            @pl.when(s == 2)
            def _():
                if before_near is not None:
                    before_near()
                self.near1()
                self.near2()

            @pl.when((s == 4) | (s == 5) | (s == 7))
            def _():
                self.wait_block(blk)

            @pl.when(s == 6)
            def _():
                self.far()
                if after_far is not None:
                    after_far()

            body(blk)

        loop(0, r.n, step)


class Scatter:
    SENDS = 10

    def __init__(self, ring, part, pair, stage, land, ssem, rsem):
        self.ring, self.part, self.pair, self.stage, self.land = ring, part, pair, stage, land
        self.ssem, self.rsem = ssem, rsem
        self.rows = part.shape[1]
        self.half = self.rows // 2

    def cp_pair(self, xp, k):
        r = self.ring
        return pltpu.make_async_remote_copy(
            src_ref=self.part.at[xp * 2 + (1 - r.c)], dst_ref=self.pair.at[xp], send_sem=self.ssem.at[k],
            recv_sem=self.rsem.at[xp], device_id={'tp': r.partner}, device_id_type=MESH)

    def cp(self, slot, half, dst_slot, dev, k):
        rows = pl.ds(half * self.half, self.half)
        return pltpu.make_async_remote_copy(
            src_ref=self.stage.at[slot, rows], dst_ref=self.land.at[dst_slot, rows],
            send_sem=self.ssem.at[k], recv_sem=self.rsem.at[4 + 2 * dst_slot + half],
            device_id={'tp': dev}, device_id_type=MESH)

    def wait_land(self, dst_slot, half):
        self.cp(0, half, dst_slot, self.ring.me, 0).wait_recv()

    def wait_pair(self, xp):
        self.cp_pair(xp, 0).wait_recv()

    def send_pair(self, xp, k):
        self.cp_pair(xp, k).start()

    def mix(self, slot, xp, half, with_far=False):
        blk = xp * 2 + self.ring.c
        step = 16

        def body(i):
            rows = pl.ds(pl.multiple_of(half * self.half + i * step, step), step)
            total = self.part[blk, rows, :].astype(F32) + self.pair[xp, rows, :].astype(F32)
            if with_far:
                total = total + self.land[0, rows, :].astype(F32)
            self.stage[slot, rows, :] = total.astype(BF)
        loop(0, self.half // step, body)

    def far(self):
        r = self.ring
        self.wait_pair(r.xf)
        self.mix(0, r.xf, 0)
        self.cp(0, 0, 0, r.right, 4).start()
        self.mix(0, r.xf, 1)
        self.cp(0, 1, 0, r.left, 5).start()

    def near_own(self):
        r = self.ring
        self.wait_pair(r.xr)
        self.mix(1, r.xr, 1)
        self.cp(1, 1, 1, r.right, 6).start()
        self.wait_pair(r.xl)
        self.mix(2, r.xl, 0)
        self.cp(2, 0, 2, r.left, 7).start()

    def near_sum(self):
        r = self.ring
        self.wait_land(0, 0)
        self.mix(1, r.xr, 0, with_far=True)
        self.cp(1, 0, 1, r.right, 8).start()
        self.wait_land(0, 1)
        self.mix(2, r.xl, 1, with_far=True)
        self.cp(2, 1, 2, r.left, 9).start()

    def wait_final(self):
        self.wait_pair(self.ring.x)
        for slot in (1, 2):
            for half in PAIR:
                self.wait_land(slot, half)

    def total(self, rows):
        r = self.ring
        return (self.part[r.me, rows, :].astype(F32) + self.pair[r.x, rows, :].astype(F32)
                + self.land[1, rows, :].astype(F32) + self.land[2, rows, :].astype(F32))

    def finish(self):
        for k in range(4):
            self.cp_pair(self.ring.x, k).wait_send()
        for k in range(4, self.SENDS):
            self.cp(0, 0, 0, self.ring.right, k).wait_send()


def scatter_scratch(n, rows, d):
    return [VMEM((n // 2, rows, d), BF), VMEM((3, rows, d), BF), VMEM((3, rows, d), BF),
            pltpu.SemaphoreType.DMA((Scatter.SENDS,)), pltpu.SemaphoreType.DMA((4 + 6,))]


def gather_scratch(n):
    return [pltpu.SemaphoreType.DMA((Gather.SENDS,)), pltpu.SemaphoreType.DMA((n, 2))]


def lane_mask(rows, h):
    lane = lax.broadcasted_iota(jnp.int32, (rows, 128), 1)
    return (lane < 64) if h == 0 else (lane >= 64)


def attend_block(i, q_ref, k_ref, v_ref, o_ref, lse_ref, s_ref, m_ref, l_ref, acc_ref, slopes, scale):
    t = q_ref.shape[2]
    key = lax.broadcasted_iota(jnp.int32, (t, t), 0)
    qry = lax.broadcasted_iota(jnp.int32, (t, t), 1)
    for h in PAIR:
        m_ref[h] = jnp.full((8, t), MASK_VALUE, F32)
        l_ref[h] = jnp.zeros((8, t), F32)
    zero_fill(acc_ref)

    def score(j, diag):
        pos = (key + j * t).astype(F32)
        for h in PAIR:
            s = mm(k_ref[j], q_ref[h, i], NT) * scale + slopes[h] * pos
            if diag:
                s = jnp.where(key <= qry, s, MASK_VALUE)
            s_ref[h, j] = s
            m_ref[h] = jnp.maximum(m_ref[h], fold8(s, jnp.maximum))

    loop(0, i, lambda j: score(j, False))
    score(i, True)
    top = [jnp.max(m_ref[h], axis=0, keepdims=True) for h in (0, 1)]

    def denom(j):
        for h in PAIR:
            l_ref[h] = l_ref[h] + fold8(jnp.exp(s_ref[h, j] - top[h]), jnp.add)

    loop(0, i + 1, denom)
    for h in PAIR:
        lse_ref[h, i] = top[h] + jnp.log(col_sum(l_ref[h]))

    def values(j):
        total = acc_ref[...]
        for h in PAIR:
            p = jnp.exp(s_ref[h, j] - lse_ref[h, i]).astype(BF)
            total = total + mm(p, v_ref[h, j], T0)
        acc_ref[...] = total

    loop(0, i + 1, values)
    o_ref[i] = acc_ref[...].astype(BF)


def kernel_main(n, scale, x_hbm, dy_hbm, wt_hbm, wo_hbm, wu_hbm, wd_hbm, g1, b1, bqkv, bo, g2, b2, bu, bd, slopes_ref,
                y, gx, sums, gwt, gbq, gwo, gwu, gbu, gwd, h_hbm,
                xg, xo, dyo, dy, hg, wt, wp, wof, wu, wd, q, k, v, o, lse, orow, s_ref, m_ref, l_ref, acc,
                x1, act, dpre, mid, dcs, dcr, km, dom, dlt, dq, dk_acc, dv_acc, d3, small, every, part,
                *rest):
    rest = list(rest)

    def take(count):
        head = rest[:count]
        del rest[:count]
        return head

    ring = Ring(n)
    me = ring.me
    t, d, f = xg.shape[1], xg.shape[2], wu.shape[1]
    rs_refs, rm_refs = take(5), take(5)
    ax, ay, aw, ag, ad = [Gather(ring, buf, *take(2)) for buf in (xg, dy, wof, hg, xg)]
    o_send, o_recv, c_send, c_recv, ar_s, ar_r, local = take(7)

    def fetch(i, src, dst):
        cp = pltpu.make_async_copy(src, dst, local.at[i])
        cp.start()
        return cp

    in_x, in_wo, in_dy, in_wt = (fetch(0, x_hbm, xg.at[me]), fetch(1, wo_hbm, wof.at[me]),
                                 fetch(2, dy_hbm, dy.at[me]), fetch(3, wt_hbm, wt))
    later = [fetch(4, wu_hbm, wu), fetch(5, wd_hbm, wd), fetch(6, x_hbm, xo), fetch(7, dy_hbm, dyo)]
    ring.barrier(everyone=True)
    in_x.wait()
    ax.start()
    in_wt.wait()
    sort_weight(wp, wt)
    in_wo.wait()
    in_dy.wait()
    bias = jnp.concatenate([bqkv[kind, head:head + 1, :] for kind in TRIPLE for head in PAIR], axis=1)

    def project(blk):
        def norm(rows):
            hat, _ = norm_rows(xg[blk, rows, :].astype(F32))
            hg[blk, rows, :] = (hat * g1[...] + b1[...]).astype(BF)
        rows_loop(t, 64, norm)
        out = mm(hg[blk], wp[...], NT) + bias
        out = out.astype(BF)
        zero = jnp.zeros((t, 128), BF)
        for head in PAIR:
            q[head, blk] = jnp.where(lane_mask(t, head), out[:, :128], zero)
            v[head, blk] = jnp.where(lane_mask(t, head), out[:, 256:], zero)
        k[blk] = out[:, 128:256]
        fetch(0, hg.at[blk], h_hbm.at[blk])

    def background():
        aw.start()
        ay.start()

    with scope('a_gather'):
        ax.run(project, after_far=background)
    slopes = [slopes_ref[me * 2 + head] for head in PAIR]

    def send_o(i):
        cols = pl.ds(pl.multiple_of(me * 128, 128), 128)
        return pltpu.make_async_remote_copy(
            src_ref=o.at[i], dst_ref=orow.at[:, cols], send_sem=o_send.at[i], recv_sem=o_recv.at[me],
            device_id={'tp': i}, device_id_type=MESH)

    def all_blocks(i):
        for at, act_now in ((4, aw.near1), (5, aw.near2), (n - 2, ay.near1), (n - 1, aw.far), (n - 1, ay.near2)):
            pl.when(i == at)(act_now)
        attend_block(i, q, k, v, o, lse, s_ref, m_ref, l_ref, acc, slopes, scale)

        @pl.when(i != me)
        def _():
            send_o(i).start()

    with scope('a_attend'):
        ax.finish()
        pltpu.make_async_copy(hg, h_hbm, local.at[0]).wait()
        loop(0, n, all_blocks)
    with scope('a_wait'):
        orow[:, pl.ds(pl.multiple_of(me * 128, 128), 128)] = o[me]
        for off in range(1, n):
            src = (me + off) % n
            cols = pl.ds(pl.multiple_of(src * 128, 128), 128)
            pltpu.make_async_remote_copy(
                src_ref=o.at[0], dst_ref=orow.at[:, cols], send_sem=o_send.at[0], recv_sem=o_recv.at[src],
                device_id={'tp': me}, device_id_type=MESH).wait_recv()
        for dx in (ring.x, ring.xl, ring.xr, ring.xf):
            aw.wait_block(dx * 2 + (1 - ring.c))
        later[2].wait()
    with scope('a_out'):
        x1[...] = mm(orow[...], wof[...].reshape(n * 128, d)).astype(BF).astype(F32)

        def enter(rows):
            row = xo[rows, :].astype(F32) + x1[rows, :] + bo[...]
            x1[rows, :] = row
            hat, _ = norm_rows(row)
            hg[me, rows, :] = (hat * g2[...] + b2[...]).astype(BF)
        rows_loop(t, 64, enter)
        ag.start()
    for cp in (later[0], later[1], later[3]):
        cp.wait()
    zero_fill(gbu)
    ay.wait_block(ring.partner)

    def rest():
        ay.far()
        for dx in (ring.xl, ring.xr, ring.xf):
            ay.wait_block(dx * 2 + (1 - ring.c))

    def mlp(blk):
        pre = mm(hg[blk], wu[...]) + bu[...]
        cot = mm(dy[blk], wd[...], NT).astype(BF).astype(F32)
        sq = pre * pre
        th = jnp.tanh(GELU_C * (pre + 0.044715 * sq * pre))
        cdf = 0.5 * (1.0 + th)
        act[blk] = (pre * cdf).astype(BF)
        slope = cdf + pre * (0.5 * (1.0 - th * th)) * (GELU_C * (1.0 + 3 * 0.044715 * sq))
        dp = cot * slope
        gbu[...] = gbu[...] + fold8(dp, jnp.add)
        dpre[blk] = dp.astype(BF)
        part[blk] = mm(dpre[blk], wu[...], NT).astype(BF)

    with scope('b_gather'):
        ag.run(mlp, before_near=rest)
    rs = Scatter(ring, part, *rs_refs)
    chips = (ring.xf, ring.xr, ring.xl, ring.x)
    for slot, xp in enumerate(chips):
        rs.send_pair(xp, slot)
    with scope('b_far'):
        rs.far()
    with scope('b_own'):
        rs.near_own()
    ay.finish()

    def weight_down(i):
        cols = pl.ds(pl.multiple_of(i * 256, 256), 256)
        left = act[:, :, cols].reshape(n * t, 256)
        gwd[cols, :] = mm(left, dy[...].reshape(n * t, d), T0).astype(BF)

    def weight_up(i):
        cols = pl.ds(pl.multiple_of(i * 256, 256), 256)
        left = hg[:, :, cols].reshape(n * t, 256)
        gwu[cols, :] = mm(left, dpre[...].reshape(n * t, f), T0).astype(BF)

    with scope('b_weights'):
        loop(0, f // 256, weight_down)
        loop(0, d // 256, weight_up)
    with scope('b_sum'):
        rs.near_sum()
    zero_fill(small)

    def down(blk):
        dy[blk] = mm(act[blk], wd[...]).astype(BF)
    with scope('b_down'):
        loop(0, n, down)
    with scope('b_final'):
        rs.wait_final()

    def leave(rows):
        dg = rs.total(rows).astype(BF).astype(F32)
        hat, rstd = norm_rows(x1[rows, :])
        small[2] = small[2] + fold8(dg * hat, jnp.add)
        small[3] = small[3] + fold8(dg, jnp.add)
        dz = norm_back(dg * g2[...], hat, rstd)
        dyf = dyo[rows, :].astype(F32)
        dm = dyf + dz
        small[4] = small[4] + fold8(dm, jnp.add)
        small[5] = small[5] + fold8(dyf, jnp.add)
        mid[rows, :] = dm
        xg[me, rows, :] = dm.astype(BF)

    def send_c(dev):
        return pltpu.make_async_remote_copy(
            src_ref=dcs.at[dev], dst_ref=dcr.at[me], send_sem=c_send.at[dev], recv_sem=c_recv.at[me],
            device_id={'tp': dev}, device_id_type=MESH)

    with scope('b_leave'):
        rows_loop(t, 64, leave)
        rs.finish()
        ag.finish()
    with scope('c_send'):
        def back_out(step):
            dev = ring.order(n - 1 - step)
            dcs[dev] = mm(xg[me], wof[dev], NT).astype(BF)

            @pl.when(step < n - 1)
            def _():
                send_c(dev).start()
        loop(0, n, back_out)
        ad.start()
        reload = fetch(0, h_hbm, hg)
    rm = Scatter(ring, dy, *rm_refs)
    for slot, xp in enumerate(chips):
        rm.send_pair(xp, slot)
    dcr[me] = dcs[me]

    def prepare(step):
        blk = ring.order(step)

        @pl.when(step > 0)
        def _():
            pltpu.make_async_remote_copy(
                src_ref=dcs.at[0], dst_ref=dcr.at[blk], send_sem=c_send.at[0], recv_sem=c_recv.at[blk],
                device_id={'tp': me}, device_id_type=MESH).wait_recv()
        dc = dcr[blk]
        zero = jnp.zeros((t, 128), BF)
        for head in PAIR:
            mask = lane_mask(t, head)
            dom[head, blk] = jnp.where(mask, dc, zero)
            km[head, blk] = jnp.where(mask, k[blk], zero)
        prod = (dc.astype(F32) * o[blk].astype(F32)).T
        dlt[LOW, blk] = col_sum(prod[:64])
        dlt[HIGH, blk] = col_sum(prod[64:])
        dq[blk] = jnp.zeros((t, 128), F32)

    with scope('c_prepare'):
        rm.far()
        loop(0, n, prepare)
    key = lax.broadcasted_iota(jnp.int32, (t, t), 0)
    qry = lax.broadcasted_iota(jnp.int32, (t, t), 1)

    def kv_block(j):
        pos = (key + j * t).astype(F32)
        zero_fill(dk_acc, dv_acc)

        def pair_block(i, diag):
            tv, tk, tq = dv_acc[...], dk_acc[...], dq[i]
            for head in PAIR:
                s = mm(k[j], q[head, i], NT) * scale + slopes[head] * pos
                if diag:
                    s = jnp.where(key <= qry, s, MASK_VALUE)
                p = jnp.exp(s - lse[head, i])
                dp = mm(v[head, j], dom[head, i], NT).astype(BF).astype(F32)
                ds = (p * (dp - dlt[head, i])).astype(BF)
                tv = tv + mm(p.astype(BF), dom[head, i])
                tk = tk + mm(ds, q[head, i])
                tq = tq + mm(ds, km[head, j], T0)
            dv_acc[...] = tv
            dk_acc[...] = tk
            dq[i] = tq

        for at, act_now in ((2, ad.near1), (2, rm.near_own), (3, ad.near2), (n - 3, rm.near_sum)):
            pl.when(j == at)(act_now)
        pair_block(j, True)
        loop(j + 1, n, lambda i: pair_block(i, False))
        d3[j, :, 128:256] = (dk_acc[...] * scale).astype(BF)
        d3[j, :, 256:] = dv_acc[...].astype(BF)

    with scope('c_attend'):
        loop(0, n, kv_block)
    zero_fill(gbq)

    def back_in(xp, slot):
        for cc in PAIR:
            blk = xp * 2 + cc
            d3[blk, :, :128] = (dq[blk] * scale).astype(BF)
            part[blk] = mm(d3[blk], wp[...]).astype(BF)
        rs.send_pair(xp, slot)

    with scope('c_far'):
        back_in(ring.xf, 0)
        rs.far()
    with scope('c_own'):
        back_in(ring.xr, 1)
        back_in(ring.xl, 2)
        rs.near_own()
        back_in(ring.x, 3)
    with scope('c_da'):
        ad.far()
        reload.wait()

    def weight_in(i):
        cols = pl.ds(pl.multiple_of(i * 128, 128), 128)
        left = d3[:, :, cols].reshape(n * t, 128)
        grad = mm(left, hg[...].reshape(n * t, d), T0).astype(BF)
        for head in PAIR:
            gwt[head, i] = grad[head * 64:head * 64 + 64]

    def bias_in(b):
        gbq[...] = gbq[...] + fold8(d3[b].astype(F32), jnp.add)

    with scope('c_weights'):
        loop(0, len(TRIPLE), weight_in)
        loop(0, n, bias_in)
    with scope('c_sum'):
        rs.near_sum()
    with scope('c_gwo'):
        for dx in (ring.x, ring.xl, ring.xr, ring.xf):
            ad.wait_block(dx * 2 + (1 - ring.c))
        gwo[...] = mm(o[...].reshape(n * t, 128), xg[...].reshape(n * t, d), T0).astype(BF)
    with scope('c_mfinal'):
        rm.wait_final()

    def out_y(rows):
        m = rm.total(rows).astype(BF).astype(F32)
        y[rows, :] = (x1[rows, :] + m + bd[...]).astype(BF)
    rows_loop(t, 64, out_y)
    with scope('c_final'):
        rs.wait_final()

    def sum_in(rows):
        dh = rs.total(rows).astype(BF).astype(F32)
        hat, _ = norm_rows(xo[rows, :].astype(F32))
        small[0] = small[0] + fold8(dh * hat, jnp.add)
        small[1] = small[1] + fold8(dh, jnp.add)

    def last(rows):
        dh = rs.total(rows).astype(BF).astype(F32)
        hat, rstd = norm_rows(xo[rows, :].astype(F32))
        gx[rows, :] = (mid[rows, :] + norm_back(dh * g1[...], hat, rstd)).astype(BF)

    with scope('c_sums'):
        rows_loop(t, 64, sum_in)
    for i in range(6):
        every[me, i:i + 1, :] = col_sum(small[i])
    every[me, 6:, :] = jnp.zeros((2, d), F32)

    def share(off):
        return pltpu.make_async_remote_copy(
            src_ref=every.at[me], dst_ref=every.at[me], send_sem=ar_s.at[off], recv_sem=ar_r.at[me],
            device_id={'tp': (me + off) % n}, device_id_type=MESH)

    with scope('c_share'):
        for off in range(1, n):
            share(off).start()
        rows_loop(t, 64, last)
        for off in range(1, n):
            src = (me + off) % n
            pltpu.make_async_remote_copy(
                src_ref=every.at[src], dst_ref=every.at[src], send_sem=ar_s.at[0], recv_sem=ar_r.at[src],
                device_id={'tp': me}, device_id_type=MESH).wait_recv()
        total = every[0]
        for b in range(1, n):
            total = total + every[b]
        sums[...] = total
    for off in range(1, n):
        share(off).wait_send()
        send_o((me + off) % n).wait_send()
        send_c((me + off) % n).wait_send()
    for job in (rs, rm, aw, ad):
        job.finish()


def kernel_out(n_big, *refs):
    srcs, (gbq, gbu, sums), refs = refs[:n_big], refs[n_big:n_big + 3], refs[n_big + 3:]
    outs, (o_bq, o_bu), refs = refs[:n_big], refs[n_big:n_big + 2], refs[n_big + 2:]
    o_sums, refs = refs[:6], refs[6:]
    bufs, (sem_in, sem_out) = refs[:n_big], refs[n_big:]
    ins = [pltpu.make_async_copy(a, b, sem_in.at[i]) for i, (a, b) in enumerate(zip(srcs, bufs))]
    backs = [pltpu.make_async_copy(b, a, sem_out.at[i]) for i, (a, b) in enumerate(zip(outs, bufs))]
    for cp in ins:
        cp.start()
    o_bu[...] = col_sum(gbu[...])
    row = col_sum(gbq[...])
    e = o_bq.shape[2]
    for part_no in TRIPLE:
        for head in PAIR:
            at = (part_no * 2 + head) * e
            o_bq[part_no, head:head + 1, :] = row[:, at:at + e]
    for i, ref in enumerate(o_sums):
        ref[...] = sums[i:i + 1, :]
    for cp, back in zip(ins, backs):
        cp.wait()
        back.start()
    for back in backs:
        back.wait()


def whole():
    return pl.BlockSpec(memory_space=VMEM)


def anywhere():
    return pl.BlockSpec(memory_space=pl.ANY)


def smem():
    return pl.BlockSpec(memory_space=pltpu.SMEM)


def solution(mesh):
    n = mesh.shape['tp']

    def local_step(x, ln1_gamma, ln1_beta, w_qkv, b_qkv, w_out, b_out, ln2_gamma, ln2_beta, w_up, b_up, w_down, b_down, grad_y):
        t, d = x.shape[1], x.shape[2]
        heads, e = w_qkv.shape[1], w_qkv.shape[3]
        he = heads * e
        f = w_up.shape[1]
        scale = e ** -0.5
        slopes = jnp.asarray(alibi_slopes(heads * n))
        x2, dy2 = x[0], grad_y[0]
        row = lambda vec: vec.reshape(1, -1)
        wt = w_qkv.transpose(1, 2, 3, 0).reshape(heads * 3 * e, d)
        bq = b_qkv.transpose(1, 0, 2)
        sds = jax.ShapeDtypeStruct
        rows, full, half = (t, d), (n, t, d), (n, t, he)
        both, line = (len(PAIR),) + half, (len(PAIR), n, 1, t)
        packed = (len(TRIPLE) * he, d)
        params = lambda cid: pltpu.CompilerParams(collective_id=cid, has_side_effects=True, vmem_limit_bytes=VLIM)
        dma = pltpu.SemaphoreType.DMA

        vm = lambda dims, kind=BF: VMEM(dims, kind)
        stat, square = (len(PAIR), 8, t), (t, he)
        y, gx, sums, gwt, gbq, gwo, gwu, gbu, gwd, _ = pl.pallas_call(
            functools.partial(kernel_main, n, scale),
            name='layer',
            out_shape=[sds(rows, BF), sds(rows, BF), sds((8, d), F32), sds((heads, len(TRIPLE), e, d), BF),
                       sds((8, len(TRIPLE) * he), F32), sds((he, d), BF), sds((d, f), BF), sds((8, f), F32),
                       sds((f, d), BF), sds(full, BF)],
            in_specs=[anywhere()] * 6 + [whole()] * 8 + [smem()],
            out_specs=[whole()] * 9 + [anywhere()],
            scratch_shapes=[vm(full), vm(rows), vm(rows), vm(full), vm(full), vm(packed), vm(packed), vm((n, he, d)), vm((d, f)),
                            vm((f, d)), vm(both), vm(half), vm(both), vm(half), vm(line, F32), vm(rows),
                            vm((len(PAIR), n, t, t), F32), vm(stat, F32), vm(stat, F32), vm(square, F32),
                            vm(rows, F32), vm((n, t, f)), vm((n, t, f)), vm(rows, F32), vm(half), vm(half),
                            vm(both), vm(both), vm(line, F32), vm(half, F32), vm(square, F32), vm(square, F32),
                            vm((n, t, len(TRIPLE) * he)), vm((6, 8, d), F32), vm((n, 8, d), F32), vm(full)]
            + scatter_scratch(n, t, d) * 2 + gather_scratch(n) * 5 + [dma((n,))] * 7,
            compiler_params=params(0),
        )(x2, dy2, wt, w_out, w_up, w_down, row(ln1_gamma), row(ln1_beta), bq, row(b_out), row(ln2_gamma), row(ln2_beta),
          row(b_up), row(b_down), slopes)

        big = (y, gx, gwt, gwo, gwu, gwd)
        res = pl.pallas_call(
            functools.partial(kernel_out, len(big)),
            name='results',
            out_shape=[sds(b.shape, b.dtype) for b in big] + [sds((len(TRIPLE), heads, e), F32), sds((1, f), F32)]
            + [sds((1, d), F32)] * 6,
            in_specs=[anywhere()] * len(big) + [whole()] * 3,
            out_specs=[anywhere()] * len(big) + [whole()] * 8,
            scratch_shapes=[VMEM(b.shape, b.dtype) for b in big] + [dma((len(big),))] * 2,
        )(*big, gbq, gbu, sums)
        y, gx, gwt, gwo, gwu, gwd, gbq, gbu, s_g1, s_b1, s_g2, s_b2, s_bo, s_bd = res
        vec = lambda a: a.reshape(-1)
        return (y[None], gx[None], vec(s_g1), vec(s_b1), gwt.transpose(3, 0, 1, 2), gbq.transpose(1, 0, 2), gwo, vec(s_bo),
                vec(s_g2), vec(s_b2), gwu, vec(gbu), gwd, vec(s_bd))

    row_spec = P('dp', 'tp', None)
    in_specs = (row_spec, P(), P(), P(None, 'tp', None, None), P('tp', None, None), P('tp', None), P(), P(), P(),
                P(None, 'tp'), P('tp'), P('tp', None), P(), row_spec)
    out_specs = (row_spec, row_spec, P('dp'), P('dp'), P('dp', 'tp', None, None), P(('dp', 'tp'), None, None),
                 P(('dp', 'tp'), None), P('dp'), P('dp'), P('dp'), P('dp', 'tp'), P(('dp', 'tp')), P(('dp', 'tp'), None), P('dp'))
    return jax.shard_map(local_step, mesh=mesh, in_specs=in_specs, out_specs=out_specs, check_vma=False)
```

```python
import functools
import math
import jax
import jax.numpy as jnp
import numpy as np
from jax import lax
from jax.experimental import pallas as pl
from jax.experimental.pallas import tpu as pltpu
from jax.sharding import PartitionSpec as P

EPS = 1e-5
MASK_VALUE = -1e30
BF, F32 = jnp.bfloat16, jnp.float32
VMEM = pltpu.VMEM
MESH = pl.DeviceIdType.MESH
scope = jax.named_scope
VLIM = 62 * 1024 * 1024
GELU_C = math.sqrt(2.0 / math.pi)
PAIR = LOW, HIGH = (0, 1)
TRIPLE = (0, 1, 2)
NN = (((1,), (0,)), ((), ()))
T0 = (((0,), (0,)), ((), ()))
NT = (((1,), (1,)), ((), ()))


def alibi_slopes(n_heads):
    closest = 2 ** int(math.floor(math.log2(n_heads)))
    base_ratio = 2.0 ** (-8.0 / closest)
    extra_ratio = 2.0 ** (-4.0 / closest)
    remaining = min(closest, n_heads - closest)
    slopes = [base_ratio ** (i + 1) for i in range(closest)]
    slopes = slopes + [extra_ratio ** (2 * i + 1) for i in range(remaining)]
    return np.array(slopes, dtype=np.float32)


def mm(a, b, dims=NN):
    return lax.dot_general(a, b, dims, preferred_element_type=F32)


def loop(lo, hi, body, unroll=1):
    def step(i, carry):
        body(i)
        return carry
    lax.fori_loop(lo, hi, step, 0, unroll=unroll)


def rows_loop(total, rows, body, unroll=1):
    loop(0, total // rows, lambda r: body(pl.ds(pl.multiple_of(r * rows, rows), rows)), unroll)


def row_mean(z):
    return jnp.mean(z, axis=-1, keepdims=True)


def col_sum(z):
    return jnp.sum(z, axis=0, keepdims=True)


def norm_back(grad, hat, rstd):
    return rstd * (grad - row_mean(grad) - hat * row_mean(grad * hat))


def zero_fill(*refs):
    for ref in refs:
        ref[...] = jnp.zeros(ref.shape, ref.dtype)


def sort_weight(wp, wt):
    e = wp.shape[0] // 6
    for part_no in TRIPLE:
        for head in PAIR:
            dst = (part_no * 2 + head) * e
            src = (head * 3 + part_no) * e
            wp[dst:dst + e, :] = wt[src:src + e, :]


def norm_rows(z):
    cen = z - row_mean(z)
    rstd = lax.rsqrt(row_mean(cen * cen) + EPS)
    return cen * rstd, rstd


def fold8(v, op):
    out = v[0:8]
    for k in range(1, v.shape[0] // 8):
        out = op(out, v[8 * k:8 * k + 8])
    return out


class Ring:
    def __init__(self, n):
        self.n = n
        nx = n // 2
        self.me = lax.axis_index('tp')
        self.x = self.me // 2
        self.c = self.me % 2
        self.nx = nx
        self.xr = (self.x + 1) % nx
        self.xl = (self.x + nx - 1) % nx
        self.xf = (self.x + 2) % nx
        self.right = self.xr * 2 + self.c
        self.left = self.xl * 2 + self.c
        self.far = self.xf * 2 + self.c
        self.partner = self.x * 2 + (1 - self.c)

    def order(self, s):
        odd = s % 2
        dx = jnp.where(s < 2, 0, jnp.where(s >= 6, 2, jnp.where(odd == 0, self.nx - 1, 1)))
        mid = jnp.where(s < 4, 0, 1)
        dc = jnp.where(s < 2, odd, jnp.where(s >= 6, odd, mid))
        return ((self.x + dx) % self.nx) * 2 + (self.c + dc) % 2

    def barrier(self, everyone=False):
        sem = pltpu.get_barrier_semaphore()
        if everyone:
            peers = [(self.me + k) % self.n for k in range(1, self.n)]
        else:
            peers = [self.right, self.left, self.partner]
        for peer in peers:
            pl.semaphore_signal(sem, inc=1, device_id={'tp': peer}, device_id_type=MESH)
        pl.semaphore_wait(sem, len(peers))


class Gather:
    SENDS = 14

    def __init__(self, ring, buf, ssem, rsem):
        self.ring, self.buf, self.ssem, self.rsem = ring, buf, ssem, rsem
        self.half = buf.shape[1] // 2

    def cp(self, blk, half, dev, k):
        ref = self.buf.at[blk, pl.ds(half * self.half, self.half)]
        return pltpu.make_async_remote_copy(
            src_ref=ref, dst_ref=ref, send_sem=self.ssem.at[k], recv_sem=self.rsem.at[blk, half],
            device_id={'tp': dev}, device_id_type=MESH)

    def start(self):
        r = self.ring
        self.cp(r.me, LOW, r.right, 0).start()
        self.cp(r.me, HIGH, r.left, 1).start()
        self.cp(r.me, HIGH, r.right, 2).start()
        self.cp(r.me, LOW, r.left, 3).start()
        self.cp(r.me, LOW, r.partner, 4).start()
        self.cp(r.me, HIGH, r.partner, 5).start()

    def wait(self, blk, half):
        self.cp(blk, half, self.ring.me, 0).wait_recv()

    def wait_block(self, blk):
        for half in PAIR:
            self.wait(blk, half)

    def near1(self):
        r = self.ring
        self.wait(r.left, LOW)
        self.cp(r.left, LOW, r.right, 6).start()
        self.cp(r.left, LOW, r.partner, 7).start()
        self.wait(r.right, HIGH)
        self.cp(r.right, HIGH, r.left, 8).start()
        self.cp(r.right, HIGH, r.partner, 9).start()

    def near2(self):
        r = self.ring
        self.wait(r.left, HIGH)
        self.cp(r.left, HIGH, r.partner, 10).start()
        self.wait(r.right, LOW)
        self.cp(r.right, LOW, r.partner, 11).start()

    def far(self):
        r = self.ring
        self.wait(r.far, LOW)
        self.cp(r.far, LOW, r.partner, 12).start()
        self.wait(r.far, HIGH)
        self.cp(r.far, HIGH, r.partner, 13).start()

    def finish(self):
        for k in range(self.SENDS):
            self.cp(self.ring.me, 0, self.ring.right, k).wait_send()

    def run(self, body, before_near=None, after_near=None, after_far=None):
        r = self.ring

        def step(s):
            blk = r.order(s)

            @pl.when(s == 1)
            def _():
                self.wait_block(blk)

            @pl.when(s == 2)
            def _():
                if before_near is not None:
                    before_near()
                self.near1()
                if after_near is not None:
                    after_near()
                self.near2()

            @pl.when((s == 4) | (s == 5) | (s == 7))
            def _():
                self.wait_block(blk)

            @pl.when(s == 6)
            def _():
                self.far()
                if after_far is not None:
                    after_far()

            body(blk)

        loop(0, r.n, step)


class Scatter:
    SENDS = 10

    def __init__(self, ring, part, pair, stage, land, ssem, rsem):
        self.ring, self.part, self.pair, self.stage, self.land = ring, part, pair, stage, land
        self.ssem, self.rsem = ssem, rsem
        self.rows = part.shape[1]
        self.half = self.rows // 2

    def cp_pair(self, xp, k):
        r = self.ring
        return pltpu.make_async_remote_copy(
            src_ref=self.part.at[xp * 2 + (1 - r.c)], dst_ref=self.pair.at[xp], send_sem=self.ssem.at[k],
            recv_sem=self.rsem.at[xp], device_id={'tp': r.partner}, device_id_type=MESH)

    def cp(self, slot, half, dst_slot, dev, k):
        rows = pl.ds(half * self.half, self.half)
        return pltpu.make_async_remote_copy(
            src_ref=self.stage.at[slot, rows], dst_ref=self.land.at[dst_slot, rows],
            send_sem=self.ssem.at[k], recv_sem=self.rsem.at[4 + 2 * dst_slot + half],
            device_id={'tp': dev}, device_id_type=MESH)

    def wait_land(self, dst_slot, half):
        self.cp(0, half, dst_slot, self.ring.me, 0).wait_recv()

    def wait_pair(self, xp):
        self.cp_pair(xp, 0).wait_recv()

    def send_pair(self, xp, k):
        self.cp_pair(xp, k).start()

    def mix(self, slot, xp, half, with_far=False):
        blk = xp * 2 + self.ring.c
        step = 16

        def body(i):
            rows = pl.ds(pl.multiple_of(half * self.half + i * step, step), step)
            total = self.part[blk, rows, :].astype(F32) + self.pair[xp, rows, :].astype(F32)
            if with_far:
                total = total + self.land[0, rows, :].astype(F32)
            self.stage[slot, rows, :] = total.astype(BF)
        loop(0, self.half // step, body)

    def far(self):
        r = self.ring
        self.wait_pair(r.xf)
        self.mix(0, r.xf, 0)
        self.cp(0, 0, 0, r.right, 4).start()
        self.mix(0, r.xf, 1)
        self.cp(0, 1, 0, r.left, 5).start()

    def near_own(self):
        r = self.ring
        self.wait_pair(r.xr)
        self.mix(1, r.xr, 1)
        self.cp(1, 1, 1, r.right, 6).start()
        self.wait_pair(r.xl)
        self.mix(2, r.xl, 0)
        self.cp(2, 0, 2, r.left, 7).start()

    def near_sum(self):
        r = self.ring
        self.wait_land(0, 0)
        self.mix(1, r.xr, 0, with_far=True)
        self.cp(1, 0, 1, r.right, 8).start()
        self.wait_land(0, 1)
        self.mix(2, r.xl, 1, with_far=True)
        self.cp(2, 1, 2, r.left, 9).start()

    def wait_final(self):
        self.wait_pair(self.ring.x)
        for slot in (1, 2):
            for half in PAIR:
                self.wait_land(slot, half)

    def total(self, rows):
        r = self.ring
        return (self.part[r.me, rows, :].astype(F32) + self.pair[r.x, rows, :].astype(F32)
                + self.land[1, rows, :].astype(F32) + self.land[2, rows, :].astype(F32))

    def finish(self):
        for k in range(4):
            self.cp_pair(self.ring.x, k).wait_send()
        for k in range(4, self.SENDS):
            self.cp(0, 0, 0, self.ring.right, k).wait_send()


def scatter_scratch(n, rows, d):
    return [VMEM((n // 2, rows, d), BF), VMEM((3, rows, d), BF), VMEM((3, rows, d), BF),
            pltpu.SemaphoreType.DMA((Scatter.SENDS,)), pltpu.SemaphoreType.DMA((4 + 6,))]


def gather_scratch(n):
    return [pltpu.SemaphoreType.DMA((Gather.SENDS,)), pltpu.SemaphoreType.DMA((n, 2))]


def lane_mask(rows, h):
    lane = lax.broadcasted_iota(jnp.int32, (rows, 128), 1)
    return (lane < 64) if h == 0 else (lane >= 64)


def attend_block(i, q_ref, k_ref, vt_ref, o_ref, lse_ref, s_ref, m_ref, l_ref, acc_ref, bt_ref, slopes):
    t = q_ref.shape[2]
    e = acc_ref.shape[0] // 2
    key = lax.broadcasted_iota(jnp.int32, (t, t), 0)
    qry = lax.broadcasted_iota(jnp.int32, (t, t), 1)
    for h in PAIR:
        m_ref[h] = jnp.full((8, t), MASK_VALUE, F32)
        l_ref[h] = jnp.zeros((8, t), F32)
    zero_fill(acc_ref)

    def shift(h, j):
        return slopes[h] * (j * t).astype(F32)

    def score(j, diag):
        for h in PAIR:
            s = mm(k_ref[j], q_ref[h, i], NT) + bt_ref[h]
            if diag:
                s = jnp.where(key <= qry, s, MASK_VALUE)
            s_ref[h, j] = s
            m_ref[h] = jnp.maximum(m_ref[h], fold8(s, jnp.maximum) + shift(h, j))

    loop(0, i, lambda j: score(j, False))
    score(i, True)
    top = [jnp.max(m_ref[h], axis=0, keepdims=True) for h in PAIR]

    def denom(j):
        for h in PAIR:
            l_ref[h] = l_ref[h] + fold8(jnp.exp(s_ref[h, j] + (shift(h, j) - top[h])), jnp.add)

    loop(0, i + 1, denom)
    for h in PAIR:
        lse_ref[h, i] = top[h] + jnp.log(col_sum(l_ref[h]))

    def values(j):
        for h in PAIR:
            p = jnp.exp(s_ref[h, j] + (shift(h, j) - lse_ref[h, i])).astype(BF)
            rows = pl.ds(h * e, e)
            acc_ref[rows, :] = acc_ref[rows, :] + mm(vt_ref[j, rows, :], p)

    loop(0, i + 1, values)
    o_ref[i] = acc_ref[...].T.astype(BF)


def kernel_main(n, scale, x_hbm, dy_hbm, wt_hbm, wo_hbm, wu_hbm, wd_hbm, g1, b1, bqkv, bo, g2, b2, bu, bd, slopes_ref,
                y, gx, sums, gwt, gbq, gwo, gwu, gbu, gwd, h_hbm,
                xg, xo, dyo, dy, hg, wt, wp, wof, wu, wd, q, k, v, kt, vt, o, lse, orow, s_ref, m_ref, l_ref, acc, bt,
                x1, act, dpre, mid, dom, dqt, dk, dv, d3, small, every, part,
                *rest):
    rest = list(rest)

    def take(count):
        head = rest[:count]
        del rest[:count]
        return head

    ring = Ring(n)
    me = ring.me
    t, d, f = xg.shape[1], xg.shape[2], wu.shape[1]
    rs_refs, rm_refs = take(5), take(5)
    ax, ay, aw, ag, ad = [Gather(ring, buf, *take(2)) for buf in (xg, dy, wof, hg, xg)]
    o_send, o_recv, ar_s, ar_r, local = take(5)

    def fetch(i, src, dst):
        cp = pltpu.make_async_copy(src, dst, local.at[i])
        cp.start()
        return cp

    in_x, in_wo, in_dy, in_wt = (fetch(0, x_hbm, xg.at[me]), fetch(1, wo_hbm, wof.at[me]),
                                 fetch(2, dy_hbm, dy.at[me]), fetch(3, wt_hbm, wt))
    later = [fetch(4, wu_hbm, wu), fetch(5, wd_hbm, wd), fetch(6, x_hbm, xo), fetch(7, dy_hbm, dyo)]
    ring.barrier(everyone=True)
    in_x.wait()
    ax.start()
    in_wt.wait()
    sort_weight(wp, wt)
    in_wo.wait()
    in_dy.wait()
    bias = jnp.concatenate([bqkv[kind, head:head + 1, :] for kind in TRIPLE for head in PAIR], axis=1)

    def project(blk):
        def norm(rows):
            hat, _ = norm_rows(xg[blk, rows, :].astype(F32))
            hg[blk, rows, :] = (hat * g1[...] + b1[...]).astype(BF)
        rows_loop(t, 64, norm)
        out = mm(hg[blk], wp[...], NT) + bias
        out = out.astype(BF)
        zero = jnp.zeros((t, 128), BF)
        qs = (out[:, :128].astype(F32) * scale).astype(BF)
        for head in PAIR:
            q[head, blk] = jnp.where(lane_mask(t, head), qs, zero)
        k[blk] = out[:, 128:256]
        v[blk] = out[:, 256:]
        kt[blk] = out[:, 128:256].T
        vt[blk] = out[:, 256:].T
        fetch(0, hg.at[blk], h_hbm.at[blk])

    def background():
        aw.start()
        ay.start()

    with scope('a_gather'):
        ax.run(project, after_far=background)
    slopes = [slopes_ref[me * 2 + head] for head in PAIR]
    key = lax.broadcasted_iota(jnp.int32, (t, t), 0)
    qry = lax.broadcasted_iota(jnp.int32, (t, t), 1)
    for head in PAIR:
        bt[head] = slopes[head] * key.astype(F32)

    def send_o(i):
        cols = pl.ds(pl.multiple_of(me * 128, 128), 128)
        return pltpu.make_async_remote_copy(
            src_ref=o.at[i], dst_ref=orow.at[:, cols], send_sem=o_send.at[i], recv_sem=o_recv.at[me],
            device_id={'tp': i}, device_id_type=MESH)

    def all_blocks(i):
        for at, act_now in ((4, aw.near1), (5, aw.near2), (n - 1, ay.near1)):
            pl.when(i == at)(act_now)
        attend_block(i, q, k, vt, o, lse, s_ref, m_ref, l_ref, acc, bt, slopes)

        @pl.when(i != me)
        def _():
            send_o(i).start()

    with scope('a_attend'):
        ax.finish()
        pltpu.make_async_copy(hg, h_hbm, local.at[0]).wait()
        loop(0, n, all_blocks)
    with scope('a_wait'):
        aw.far()
        ay.near2()
        orow[:, pl.ds(pl.multiple_of(me * 128, 128), 128)] = o[me]
        for off in range(1, n):
            src = (me + off) % n
            cols = pl.ds(pl.multiple_of(src * 128, 128), 128)
            pltpu.make_async_remote_copy(
                src_ref=o.at[0], dst_ref=orow.at[:, cols], send_sem=o_send.at[0], recv_sem=o_recv.at[src],
                device_id={'tp': me}, device_id_type=MESH).wait_recv()
        for dx in (ring.x, ring.xl, ring.xr, ring.xf):
            aw.wait_block(dx * 2 + (1 - ring.c))
        later[2].wait()
    with scope('a_out'):
        x1[...] = mm(orow[...], wof[...].reshape(n * 128, d)).astype(BF).astype(F32)

        def enter(rows):
            row = xo[rows, :].astype(F32) + x1[rows, :] + bo[...]
            x1[rows, :] = row
            hat, _ = norm_rows(row)
            hg[me, rows, :] = (hat * g2[...] + b2[...]).astype(BF)
        rows_loop(t, 64, enter)
        ag.start()
    for cp in (later[0], later[1], later[3]):
        cp.wait()
    zero_fill(gbu)
    ay.wait_block(ring.partner)

    def rest():
        ay.far()
        for dx in (ring.xl, ring.xr, ring.xf):
            ay.wait_block(dx * 2 + (1 - ring.c))

    def mlp(blk):
        pre = mm(hg[blk], wu[...]) + bu[...]
        cot = mm(dy[blk], wd[...], NT).astype(BF).astype(F32)
        sq = pre * pre
        th = jnp.tanh(GELU_C * (pre + 0.044715 * sq * pre))
        cdf = 0.5 * (1.0 + th)
        act[blk] = (pre * cdf).astype(BF)
        slope = cdf + pre * (0.5 * (1.0 - th * th)) * (GELU_C * (1.0 + 3 * 0.044715 * sq))
        dp = cot * slope
        gbu[...] = gbu[...] + fold8(dp, jnp.add)
        dpre[blk] = dp.astype(BF)
        part[blk] = mm(dpre[blk], wu[...], NT).astype(BF)

    with scope('b_gather'):
        ag.run(mlp, before_near=rest)
    rs = Scatter(ring, part, *rs_refs)
    chips = (ring.xf, ring.xr, ring.xl, ring.x)
    for slot, xp in enumerate(chips):
        rs.send_pair(xp, slot)
    with scope('b_far'):
        rs.far()
    with scope('b_own'):
        rs.near_own()
    ay.finish()

    def weight_down(i):
        cols = pl.ds(pl.multiple_of(i * 256, 256), 256)
        left = act[:, :, cols].reshape(n * t, 256)
        gwd[cols, :] = mm(left, dy[...].reshape(n * t, d), T0).astype(BF)

    def weight_up(i):
        cols = pl.ds(pl.multiple_of(i * 256, 256), 256)
        left = hg[:, :, cols].reshape(n * t, 256)
        gwu[cols, :] = mm(left, dpre[...].reshape(n * t, f), T0).astype(BF)

    with scope('b_weights'):
        loop(0, f // 256, weight_down)
        loop(0, d // 256, weight_up)
    with scope('b_sum'):
        rs.near_sum()
    zero_fill(small)

    def down(blk):
        dy[blk] = mm(act[blk], wd[...]).astype(BF)
    with scope('b_down'):
        loop(0, n, down)
    with scope('b_final'):
        rs.wait_final()

    def leave(rows):
        dg = rs.total(rows).astype(BF).astype(F32)
        hat, rstd = norm_rows(x1[rows, :])
        small[2] = small[2] + fold8(dg * hat, jnp.add)
        small[3] = small[3] + fold8(dg, jnp.add)
        dz = norm_back(dg * g2[...], hat, rstd)
        dyf = dyo[rows, :].astype(F32)
        dm = dyf + dz
        small[4] = small[4] + fold8(dm, jnp.add)
        small[5] = small[5] + fold8(dyf, jnp.add)
        mid[rows, :] = dm
        xg[me, rows, :] = dm.astype(BF)

    with scope('b_leave'):
        rows_loop(t, 64, leave)
        rs.finish()
        ag.finish()
    ad.start()
    reload = fetch(0, h_hbm, hg)
    rm = Scatter(ring, dy, *rm_refs)
    for slot, xp in enumerate(chips):
        rm.send_pair(xp, slot)
    zero_fill(dk, dv)

    def back_block(i):
        dc = mm(xg[i], wof[me], NT).astype(BF)
        zero = jnp.zeros((t, 128), BF)
        prod = (dc.astype(F32) * o[i].astype(F32)).T
        dlt = (col_sum(prod[:64]), col_sum(prod[64:]))
        for head in PAIR:
            dom[head] = jnp.where(lane_mask(t, head), dc, zero)
        zero_fill(dqt)

        def pair_block(j, diag):
            tv, tk = dv[j], dk[j]
            for head in PAIR:
                s = mm(k[j], q[head, i], NT) + bt[head]
                if diag:
                    s = jnp.where(key <= qry, s, MASK_VALUE)
                p = jnp.exp(s + (slopes[head] * (j * t).astype(F32) - lse[head, i]))
                dp = mm(v[j], dom[head], NT).astype(BF).astype(F32)
                ds = (p * (dp - dlt[head])).astype(BF)
                tv = tv + mm(p.astype(BF), dom[head])
                tk = tk + mm(ds, q[head, i])
                rows = pl.ds(head * 64, 64)
                dqt[rows, :] = dqt[rows, :] + mm(kt[j, rows, :], ds)
            dv[j] = tv
            dk[j] = tk

        loop(0, i, lambda j: pair_block(j, False))
        pair_block(i, True)
        d3[i, :, :128] = (dqt[...].T * scale).astype(BF)

    with scope('c_attend'):
        ad.run(back_block, before_near=rm.far, after_near=rm.near_own, after_far=rm.near_sum)
    zero_fill(gbq)

    def back_in(xp, slot):
        for cc in PAIR:
            blk = xp * 2 + cc
            d3[blk, :, 128:256] = dk[blk].astype(BF)
            d3[blk, :, 256:] = dv[blk].astype(BF)
            part[blk] = mm(d3[blk], wp[...]).astype(BF)
        rs.send_pair(xp, slot)

    with scope('c_far'):
        back_in(ring.xf, 0)
        rs.far()
    with scope('c_own'):
        back_in(ring.xr, 1)
        back_in(ring.xl, 2)
        rs.near_own()
        back_in(ring.x, 3)
    reload.wait()

    def weight_in(i):
        cols = pl.ds(pl.multiple_of(i * 128, 128), 128)
        left = d3[:, :, cols].reshape(n * t, 128)
        grad = mm(left, hg[...].reshape(n * t, d), T0).astype(BF)
        for head in PAIR:
            gwt[head, i] = grad[head * 64:head * 64 + 64]

    def bias_in(b):
        gbq[...] = gbq[...] + fold8(d3[b].astype(F32), jnp.add)

    with scope('c_weights'):
        loop(0, len(TRIPLE), weight_in)
        loop(0, n, bias_in)
    with scope('c_sum'):
        rs.near_sum()
    with scope('c_gwo'):
        gwo[...] = mm(o[...].reshape(n * t, 128), xg[...].reshape(n * t, d), T0).astype(BF)
    with scope('c_mfinal'):
        rm.wait_final()

    def out_y(rows):
        m = rm.total(rows).astype(BF).astype(F32)
        y[rows, :] = (x1[rows, :] + m + bd[...]).astype(BF)
    rows_loop(t, 64, out_y)
    with scope('c_final'):
        rs.wait_final()

    def sum_in(rows):
        dh = rs.total(rows).astype(BF).astype(F32)
        hat, _ = norm_rows(xo[rows, :].astype(F32))
        small[0] = small[0] + fold8(dh * hat, jnp.add)
        small[1] = small[1] + fold8(dh, jnp.add)

    def last(rows):
        dh = rs.total(rows).astype(BF).astype(F32)
        hat, rstd = norm_rows(xo[rows, :].astype(F32))
        gx[rows, :] = (mid[rows, :] + norm_back(dh * g1[...], hat, rstd)).astype(BF)

    with scope('c_sums'):
        rows_loop(t, 64, sum_in)
    for i in range(6):
        every[me, i:i + 1, :] = col_sum(small[i])
    every[me, 6:, :] = jnp.zeros((2, d), F32)

    def share(off):
        return pltpu.make_async_remote_copy(
            src_ref=every.at[me], dst_ref=every.at[me], send_sem=ar_s.at[off], recv_sem=ar_r.at[me],
            device_id={'tp': (me + off) % n}, device_id_type=MESH)

    with scope('c_share'):
        for off in range(1, n):
            share(off).start()
        rows_loop(t, 64, last)
        for off in range(1, n):
            src = (me + off) % n
            pltpu.make_async_remote_copy(
                src_ref=every.at[src], dst_ref=every.at[src], send_sem=ar_s.at[0], recv_sem=ar_r.at[src],
                device_id={'tp': me}, device_id_type=MESH).wait_recv()
        total = every[0]
        for b in range(1, n):
            total = total + every[b]
        sums[...] = total
    for off in range(1, n):
        share(off).wait_send()
        send_o((me + off) % n).wait_send()
    for job in (rs, rm, aw, ad):
        job.finish()


def kernel_out(n_big, *refs):
    srcs, (gbq, gbu, sums), refs = refs[:n_big], refs[n_big:n_big + 3], refs[n_big + 3:]
    outs, (o_bq, o_bu), refs = refs[:n_big], refs[n_big:n_big + 2], refs[n_big + 2:]
    o_sums, refs = refs[:6], refs[6:]
    bufs, (sem_in, sem_out) = refs[:n_big], refs[n_big:]
    ins = [pltpu.make_async_copy(a, b, sem_in.at[i]) for i, (a, b) in enumerate(zip(srcs, bufs))]
    backs = [pltpu.make_async_copy(b, a, sem_out.at[i]) for i, (a, b) in enumerate(zip(outs, bufs))]
    for cp in ins:
        cp.start()
    o_bu[...] = col_sum(gbu[...])
    row = col_sum(gbq[...])
    e = o_bq.shape[2]
    for part_no in TRIPLE:
        for head in PAIR:
            at = (part_no * 2 + head) * e
            o_bq[part_no, head:head + 1, :] = row[:, at:at + e]
    for i, ref in enumerate(o_sums):
        ref[...] = sums[i:i + 1, :]
    for cp, back in zip(ins, backs):
        cp.wait()
        back.start()
    for back in backs:
        back.wait()


def whole():
    return pl.BlockSpec(memory_space=VMEM)


def anywhere():
    return pl.BlockSpec(memory_space=pl.ANY)


def smem():
    return pl.BlockSpec(memory_space=pltpu.SMEM)


def solution(mesh):
    n = mesh.shape['tp']

    def local_step(x, ln1_gamma, ln1_beta, w_qkv, b_qkv, w_out, b_out, ln2_gamma, ln2_beta, w_up, b_up, w_down, b_down, grad_y):
        t, d = x.shape[1], x.shape[2]
        heads, e = w_qkv.shape[1], w_qkv.shape[3]
        he = heads * e
        f = w_up.shape[1]
        scale = e ** -0.5
        slopes = jnp.asarray(alibi_slopes(heads * n))
        x2, dy2 = x[0], grad_y[0]
        row = lambda vec: vec.reshape(1, -1)
        wt = w_qkv.transpose(1, 2, 3, 0).reshape(heads * 3 * e, d)
        bq = b_qkv.transpose(1, 0, 2)
        sds = jax.ShapeDtypeStruct
        rows, full, half = (t, d), (n, t, d), (n, t, he)
        both, line = (len(PAIR),) + half, (len(PAIR), n, 1, t)
        packed = (len(TRIPLE) * he, d)
        params = lambda cid: pltpu.CompilerParams(collective_id=cid, has_side_effects=True, vmem_limit_bytes=VLIM)
        dma = pltpu.SemaphoreType.DMA

        vm = lambda dims, kind=BF: VMEM(dims, kind)
        stat, turned = (len(PAIR), 8, t), (n, he, t)
        y, gx, sums, gwt, gbq, gwo, gwu, gbu, gwd, _ = pl.pallas_call(
            functools.partial(kernel_main, n, scale),
            name='layer',
            out_shape=[sds(rows, BF), sds(rows, BF), sds((8, d), F32), sds((heads, len(TRIPLE), e, d), BF),
                       sds((8, len(TRIPLE) * he), F32), sds((he, d), BF), sds((d, f), BF), sds((8, f), F32),
                       sds((f, d), BF), sds(full, BF)],
            in_specs=[anywhere()] * 6 + [whole()] * 8 + [smem()],
            out_specs=[whole()] * 9 + [anywhere()],
            scratch_shapes=[vm(full), vm(rows), vm(rows), vm(full), vm(full), vm(packed), vm(packed), vm((n, he, d)),
                            vm((d, f)), vm((f, d)), vm(both), vm(half), vm(half), vm(turned), vm(turned), vm(half),
                            vm(line, F32), vm(rows), vm((len(PAIR), n, t, t), F32), vm(stat, F32), vm(stat, F32),
                            vm((he, t), F32), vm((len(PAIR), t, t), F32), vm(rows, F32), vm((n, t, f)), vm((n, t, f)),
                            vm(rows, F32), vm((len(PAIR), t, he)), vm((he, t), F32), vm(half, F32), vm(half, F32),
                            vm((n, t, len(TRIPLE) * he)), vm((6, 8, d), F32), vm((n, 8, d), F32), vm(full)]
            + scatter_scratch(n, t, d) * 2 + gather_scratch(n) * 5 + [dma((n,))] * 5,
            compiler_params=params(0),
        )(x2, dy2, wt, w_out, w_up, w_down, row(ln1_gamma), row(ln1_beta), bq, row(b_out), row(ln2_gamma), row(ln2_beta),
          row(b_up), row(b_down), slopes)

        big = (y, gx, gwt, gwo, gwu, gwd)
        res = pl.pallas_call(
            functools.partial(kernel_out, len(big)),
            name='results',
            out_shape=[sds(b.shape, b.dtype) for b in big] + [sds((len(TRIPLE), heads, e), F32), sds((1, f), F32)]
            + [sds((1, d), F32)] * 6,
            in_specs=[anywhere()] * len(big) + [whole()] * 3,
            out_specs=[anywhere()] * len(big) + [whole()] * 8,
            scratch_shapes=[VMEM(b.shape, b.dtype) for b in big] + [dma((len(big),))] * 2,
        )(*big, gbq, gbu, sums)
        y, gx, gwt, gwo, gwu, gwd, gbq, gbu, s_g1, s_b1, s_g2, s_b2, s_bo, s_bd = res
        vec = lambda a: a.reshape(-1)
        return (y[None], gx[None], vec(s_g1), vec(s_b1), gwt.transpose(3, 0, 1, 2), gbq.transpose(1, 0, 2), gwo, vec(s_bo),
                vec(s_g2), vec(s_b2), gwu, vec(gbu), gwd, vec(s_bd))

    row_spec = P('dp', 'tp', None)
    in_specs = (row_spec, P(), P(), P(None, 'tp', None, None), P('tp', None, None), P('tp', None), P(), P(), P(),
                P(None, 'tp'), P('tp'), P('tp', None), P(), row_spec)
    out_specs = (row_spec, row_spec, P('dp'), P('dp'), P('dp', 'tp', None, None), P(('dp', 'tp'), None, None),
                 P(('dp', 'tp'), None), P('dp'), P('dp'), P('dp'), P('dp', 'tp'), P(('dp', 'tp')), P(('dp', 'tp'), None), P('dp'))
    return jax.shard_map(local_step, mesh=mesh, in_specs=in_specs, out_specs=out_specs, check_vma=False)
```

```python
import functools
import math
import jax
import jax.numpy as jnp
import numpy as np
from jax import lax
from jax.experimental import pallas as pl
from jax.experimental.pallas import tpu as pltpu
from jax.sharding import PartitionSpec as P

EPS = 1e-5
MASK_VALUE = -1e30
BF, F32 = jnp.bfloat16, jnp.float32
VMEM = pltpu.VMEM
MESH = pl.DeviceIdType.MESH
scope = jax.named_scope
VLIM = 62 * 1024 * 1024
GELU_C = math.sqrt(2.0 / math.pi)
PAIR = LOW, HIGH = (0, 1)
TRIPLE = (0, 1, 2)
NN = (((1,), (0,)), ((), ()))
T0 = (((0,), (0,)), ((), ()))
NT = (((1,), (1,)), ((), ()))


def alibi_slopes(n_heads):
    closest = 2 ** int(math.floor(math.log2(n_heads)))
    base_ratio = 2.0 ** (-8.0 / closest)
    extra_ratio = 2.0 ** (-4.0 / closest)
    remaining = min(closest, n_heads - closest)
    slopes = [base_ratio ** (i + 1) for i in range(closest)]
    slopes = slopes + [extra_ratio ** (2 * i + 1) for i in range(remaining)]
    return np.array(slopes, dtype=np.float32)


def mm(a, b, dims=NN):
    return lax.dot_general(a, b, dims, preferred_element_type=F32)


def loop(lo, hi, body, unroll=1):
    def step(i, carry):
        body(i)
        return carry
    lax.fori_loop(lo, hi, step, 0, unroll=unroll)


def twos(count, body):
    loop(0, count // 2, lambda i: body((2 * i, 2 * i + 1)))

    @pl.when(count % 2 == 1)
    def _():
        body((count - 1,))


def rows_loop(total, rows, body, unroll=1):
    loop(0, total // rows, lambda r: body(pl.ds(pl.multiple_of(r * rows, rows), rows)), unroll)


def row_mean(z):
    return jnp.mean(z, axis=-1, keepdims=True)


def col_sum(z):
    return jnp.sum(z, axis=0, keepdims=True)


def norm_back(grad, hat, rstd):
    return rstd * (grad - row_mean(grad) - hat * row_mean(grad * hat))


def zero_fill(*refs):
    for ref in refs:
        ref[...] = jnp.zeros(ref.shape, ref.dtype)


def sort_weight(wp, wt):
    e = wp.shape[0] // 6
    for part_no in TRIPLE:
        for head in PAIR:
            dst = (part_no * 2 + head) * e
            src = (head * 3 + part_no) * e
            wp[dst:dst + e, :] = wt[src:src + e, :]


def norm_rows(z):
    cen = z - row_mean(z)
    rstd = lax.rsqrt(row_mean(cen * cen) + EPS)
    return cen * rstd, rstd


def fold8(v, op):
    out = v[0:8]
    for k in range(1, v.shape[0] // 8):
        out = op(out, v[8 * k:8 * k + 8])
    return out


class Ring:
    def __init__(self, n):
        self.n = n
        nx = n // 2
        self.me = lax.axis_index('tp')
        self.x = self.me // 2
        self.c = self.me % 2
        self.nx = nx
        self.xr = (self.x + 1) % nx
        self.xl = (self.x + nx - 1) % nx
        self.xf = (self.x + 2) % nx
        self.right = self.xr * 2 + self.c
        self.left = self.xl * 2 + self.c
        self.far = self.xf * 2 + self.c
        self.partner = self.x * 2 + (1 - self.c)

    def order(self, s):
        odd = s % 2
        dx = jnp.where(s < 2, 0, jnp.where(s >= 6, 2, jnp.where(odd == 0, self.nx - 1, 1)))
        mid = jnp.where(s < 4, 0, 1)
        dc = jnp.where(s < 2, odd, jnp.where(s >= 6, odd, mid))
        return ((self.x + dx) % self.nx) * 2 + (self.c + dc) % 2

    def barrier(self, everyone=False):
        sem = pltpu.get_barrier_semaphore()
        if everyone:
            peers = [(self.me + k) % self.n for k in range(1, self.n)]
        else:
            peers = [self.right, self.left, self.partner]
        for peer in peers:
            pl.semaphore_signal(sem, inc=1, device_id={'tp': peer}, device_id_type=MESH)
        pl.semaphore_wait(sem, len(peers))


class Gather:
    SENDS = 14

    def __init__(self, ring, buf, ssem, rsem):
        self.ring, self.buf, self.ssem, self.rsem = ring, buf, ssem, rsem
        self.half = buf.shape[1] // 2
        self.open = list(range(self.SENDS))

    def cp(self, blk, half, dev, k):
        ref = self.buf.at[blk, pl.ds(half * self.half, self.half)]
        return pltpu.make_async_remote_copy(
            src_ref=ref, dst_ref=ref, send_sem=self.ssem.at[k], recv_sem=self.rsem.at[blk, half],
            device_id={'tp': dev}, device_id_type=MESH)

    def start(self):
        r = self.ring
        self.cp(r.me, LOW, r.right, 0).start()
        self.cp(r.me, HIGH, r.left, 1).start()
        self.cp(r.me, HIGH, r.right, 2).start()
        self.cp(r.me, LOW, r.left, 3).start()
        self.cp(r.me, LOW, r.partner, 4).start()
        self.cp(r.me, HIGH, r.partner, 5).start()

    def wait(self, blk, half):
        self.cp(blk, half, self.ring.me, 0).wait_recv()

    def wait_block(self, blk):
        for half in PAIR:
            self.wait(blk, half)

    def near1(self):
        r = self.ring
        self.wait(r.left, LOW)
        self.cp(r.left, LOW, r.right, 6).start()
        self.cp(r.left, LOW, r.partner, 7).start()
        self.wait(r.right, HIGH)
        self.cp(r.right, HIGH, r.left, 8).start()
        self.cp(r.right, HIGH, r.partner, 9).start()

    def near2(self):
        r = self.ring
        self.wait(r.left, HIGH)
        self.cp(r.left, HIGH, r.partner, 10).start()
        self.wait(r.right, LOW)
        self.cp(r.right, LOW, r.partner, 11).start()

    def far(self):
        r = self.ring
        self.wait(r.far, LOW)
        self.cp(r.far, LOW, r.partner, 12).start()
        self.wait(r.far, HIGH)
        self.cp(r.far, HIGH, r.partner, 13).start()

    def drain(self, *which):
        for k in which:
            self.open.remove(k)
            self.cp(self.ring.me, LOW, self.ring.right, k).wait_send()

    def finish(self):
        self.drain(*list(self.open))

    def run(self, body, before_near=None, after_near=None, before_far=None, after_far=None):
        r = self.ring

        def step(s):
            blk = r.order(s)

            @pl.when(s == 1)
            def _():
                self.wait_block(blk)

            @pl.when(s == 2)
            def _():
                if before_near is not None:
                    before_near()
                self.near1()
                if after_near is not None:
                    after_near()
                self.near2()

            @pl.when((s == 4) | (s == 5) | (s == 7))
            def _():
                self.wait_block(blk)

            @pl.when(s == 6)
            def _():
                if before_far is not None:
                    before_far()
                self.far()
                if after_far is not None:
                    after_far()

            body(blk)

        loop(0, r.n, step)


class Scatter:
    SENDS = 10

    def __init__(self, ring, part, pair, stage, land, ssem, rsem):
        self.ring, self.part, self.pair, self.stage, self.land = ring, part, pair, stage, land
        self.ssem, self.rsem = ssem, rsem
        self.rows = part.shape[1]
        self.half = self.rows // 2
        self.open = list(range(4, self.SENDS))

    def cp_pair(self, xp, k):
        r = self.ring
        return pltpu.make_async_remote_copy(
            src_ref=self.part.at[xp * 2 + (1 - r.c)], dst_ref=self.pair.at[xp], send_sem=self.ssem.at[k],
            recv_sem=self.rsem.at[xp], device_id={'tp': r.partner}, device_id_type=MESH)

    def cp(self, slot, half, dst_slot, dev, k):
        rows = pl.ds(half * self.half, self.half)
        return pltpu.make_async_remote_copy(
            src_ref=self.stage.at[slot, rows], dst_ref=self.land.at[dst_slot, rows],
            send_sem=self.ssem.at[k], recv_sem=self.rsem.at[4 + 2 * dst_slot + half],
            device_id={'tp': dev}, device_id_type=MESH)

    def wait_land(self, dst_slot, half):
        self.cp(0, half, dst_slot, self.ring.me, 0).wait_recv()

    def wait_pair(self, xp):
        self.cp_pair(xp, 0).wait_recv()

    def send_pair(self, xp, k):
        self.cp_pair(xp, k).start()

    def mix(self, slot, xp, half, with_far=False):
        blk = xp * 2 + self.ring.c
        step = 16

        def body(i):
            rows = pl.ds(pl.multiple_of(half * self.half + i * step, step), step)
            total = self.part[blk, rows, :].astype(F32) + self.pair[xp, rows, :].astype(F32)
            if with_far:
                total = total + self.land[0, rows, :].astype(F32)
            self.stage[slot, rows, :] = total.astype(BF)
        loop(0, self.half // step, body)

    def far(self):
        r = self.ring
        self.wait_pair(r.xf)
        self.mix(0, r.xf, 0)
        self.cp(0, 0, 0, r.right, 4).start()
        self.mix(0, r.xf, 1)
        self.cp(0, 1, 0, r.left, 5).start()

    def near_own(self):
        r = self.ring
        self.wait_pair(r.xr)
        self.mix(1, r.xr, 1)
        self.cp(1, 1, 1, r.right, 6).start()
        self.wait_pair(r.xl)
        self.mix(2, r.xl, 0)
        self.cp(2, 0, 2, r.left, 7).start()

    def near_sum(self):
        r = self.ring
        self.wait_land(0, 0)
        self.mix(1, r.xr, 0, with_far=True)
        self.cp(1, 0, 1, r.right, 8).start()
        self.wait_land(0, 1)
        self.mix(2, r.xl, 1, with_far=True)
        self.cp(2, 1, 2, r.left, 9).start()

    def wait_final(self):
        self.wait_pair(self.ring.x)
        for slot in (1, 2):
            for half in PAIR:
                self.wait_land(slot, half)

    def total(self, rows):
        r = self.ring
        return (self.part[r.me, rows, :].astype(F32) + self.pair[r.x, rows, :].astype(F32)
                + self.land[1, rows, :].astype(F32) + self.land[2, rows, :].astype(F32))

    def drain(self, *which):
        for k in which:
            self.open.remove(k)
            self.cp(LOW, LOW, LOW, self.ring.right, k).wait_send()

    def finish(self):
        for k in range(4):
            self.cp_pair(self.ring.x, k).wait_send()
        self.drain(*list(self.open))
        self.open = list(range(4, self.SENDS))


def scatter_scratch(n, rows, d):
    return [VMEM((n // 2, rows, d), BF), VMEM((3, rows, d), BF), VMEM((3, rows, d), BF),
            pltpu.SemaphoreType.DMA((Scatter.SENDS,)), pltpu.SemaphoreType.DMA((4 + 6,))]


def gather_scratch(n):
    return [pltpu.SemaphoreType.DMA((Gather.SENDS,)), pltpu.SemaphoreType.DMA((n, 2))]


def lane_mask(rows, h):
    lane = lax.broadcasted_iota(jnp.int32, (rows, 128), 1)
    return (lane < 64) if h == 0 else (lane >= 64)


def attend_block(i, q_ref, k_ref, vt_ref, o_ref, lse_ref, s_ref, m_ref, l_ref, acc_ref, bt_ref, slopes):
    t = q_ref.shape[2]
    e = acc_ref.shape[0] // 2
    key = lax.broadcasted_iota(jnp.int32, (t, t), 0)
    qry = lax.broadcasted_iota(jnp.int32, (t, t), 1)
    for h in PAIR:
        m_ref[h] = jnp.full((8, t), MASK_VALUE, F32)
        l_ref[h] = jnp.zeros((8, t), F32)
    zero_fill(acc_ref)

    def shift(h, j):
        return slopes[h] * (j * t).astype(F32)

    def score(blocks, diag):
        top = [m_ref[h] for h in PAIR]
        for j in blocks:
            for h in PAIR:
                s = mm(k_ref[j], q_ref[h, i], NT) + bt_ref[h]
                if diag:
                    s = jnp.where(key <= qry, s, MASK_VALUE)
                s_ref[h, j] = s
                top[h] = jnp.maximum(top[h], fold8(s, jnp.maximum) + shift(h, j))
        for h in PAIR:
            m_ref[h] = top[h]

    twos(i, lambda blocks: score(blocks, False))
    score((i,), True)
    top = [jnp.max(m_ref[h], axis=0, keepdims=True) for h in PAIR]

    def denom(j):
        for h in PAIR:
            l_ref[h] = l_ref[h] + fold8(jnp.exp(s_ref[h, j] + (shift(h, j) - top[h])), jnp.add)

    loop(0, i + 1, denom)
    for h in PAIR:
        lse_ref[h, i] = top[h] + jnp.log(col_sum(l_ref[h]))

    def values(blocks):
        for h in PAIR:
            rows = pl.ds(h * e, e)
            total = acc_ref[rows, :]
            for j in blocks:
                p = jnp.exp(s_ref[h, j] + (shift(h, j) - lse_ref[h, i])).astype(BF)
                total = total + mm(vt_ref[j, rows, :], p)
            acc_ref[rows, :] = total

    twos(i + 1, values)
    o_ref[i] = acc_ref[...].T.astype(BF)


def kernel_main(n, scale, x_hbm, dy_hbm, wt_hbm, wo_hbm, wu_hbm, wd_hbm, g1, b1, bqkv, bo, g2, b2, bu, bd, slopes_ref,
                y, gx, sums, gwt, gbq, gwo, gwu, gbu, gwd, h_hbm,
                xg, xo, dyo, dy, hg, wt, wp, wof, wu, wd, q, k, v, kt, vt, o, lse, orow, s_ref, m_ref, l_ref, acc, bt,
                x1, act, dpre, mid, dom, dqt, dk, dv, d3, small, every, part,
                *rest):
    rest = list(rest)

    def take(count):
        head = rest[:count]
        del rest[:count]
        return head

    ring = Ring(n)
    me = ring.me
    t, d, f = xg.shape[1], xg.shape[2], wu.shape[1]
    rs_refs, rm_refs = take(5), take(5)
    ax, ay, aw, ag, ad = [Gather(ring, buf, *take(2)) for buf in (xg, dy, wof, hg, xg)]
    o_send, o_recv, ar_s, ar_r, local = take(5)

    def fetch(i, src, dst):
        cp = pltpu.make_async_copy(src, dst, local.at[i])
        cp.start()
        return cp

    in_x, in_wo, in_dy, in_wt = (fetch(0, x_hbm, xg.at[me]), fetch(1, wo_hbm, wof.at[me]),
                                 fetch(2, dy_hbm, dy.at[me]), fetch(3, wt_hbm, wt))
    later = [fetch(4, wu_hbm, wu), fetch(5, wd_hbm, wd), fetch(6, x_hbm, xo), fetch(7, dy_hbm, dyo)]
    ring.barrier(everyone=True)
    in_x.wait()
    ax.start()
    in_wt.wait()
    sort_weight(wp, wt)
    in_wo.wait()
    in_dy.wait()
    bias = jnp.concatenate([bqkv[kind, head:head + 1, :] for kind in TRIPLE for head in PAIR], axis=1)

    def project(blk):
        def norm(rows):
            hat, _ = norm_rows(xg[blk, rows, :].astype(F32))
            hg[blk, rows, :] = (hat * g1[...] + b1[...]).astype(BF)
        rows_loop(t, 64, norm)
        out = mm(hg[blk], wp[...], NT) + bias
        out = out.astype(BF)
        zero = jnp.zeros((t, 128), BF)
        qs = (out[:, :128].astype(F32) * scale).astype(BF)
        for head in PAIR:
            q[head, blk] = jnp.where(lane_mask(t, head), qs, zero)
        k[blk] = out[:, 128:256]
        v[blk] = out[:, 256:]
        kt[blk] = out[:, 128:256].T
        vt[blk] = out[:, 256:].T
        fetch(0, hg.at[blk], h_hbm.at[blk])

    def background():
        ax.drain(6, 8)
        aw.start()

    with scope('a_gather'):
        ax.run(project, before_far=background, after_far=ay.start)
    slopes = [slopes_ref[me * 2 + head] for head in PAIR]
    key = lax.broadcasted_iota(jnp.int32, (t, t), 0)
    qry = lax.broadcasted_iota(jnp.int32, (t, t), 1)
    for head in PAIR:
        bt[head] = slopes[head] * key.astype(F32)

    def send_o(i):
        cols = pl.ds(pl.multiple_of(me * 128, 128), 128)
        return pltpu.make_async_remote_copy(
            src_ref=o.at[i], dst_ref=orow.at[:, cols], send_sem=o_send.at[i], recv_sem=o_recv.at[me],
            device_id={'tp': i}, device_id_type=MESH)

    def all_blocks(i):
        for at, act_now in ((4, aw.near1), (5, aw.near2), (n - 1, ay.near1)):
            pl.when(i == at)(act_now)
        attend_block(i, q, k, vt, o, lse, s_ref, m_ref, l_ref, acc, bt, slopes)

        @pl.when(i != me)
        def _():
            send_o(i).start()

    with scope('a_attend'):
        ax.finish()
        pltpu.make_async_copy(hg, h_hbm, local.at[0]).wait()
        loop(0, n, all_blocks)
    with scope('a_wait'):
        aw.far()
        ay.near2()
        orow[:, pl.ds(pl.multiple_of(me * 128, 128), 128)] = o[me]
        for off in range(1, n):
            src = (me + off) % n
            cols = pl.ds(pl.multiple_of(src * 128, 128), 128)
            pltpu.make_async_remote_copy(
                src_ref=o.at[0], dst_ref=orow.at[:, cols], send_sem=o_send.at[0], recv_sem=o_recv.at[src],
                device_id={'tp': me}, device_id_type=MESH).wait_recv()
        for dx in (ring.x, ring.xl, ring.xr, ring.xf):
            aw.wait_block(dx * 2 + (1 - ring.c))
        later[2].wait()
    with scope('a_out'):
        x1[...] = mm(orow[...], wof[...].reshape(n * 128, d)).astype(BF).astype(F32)

        def enter(rows):
            row = xo[rows, :].astype(F32) + x1[rows, :] + bo[...]
            x1[rows, :] = row
            hat, _ = norm_rows(row)
            hg[me, rows, :] = (hat * g2[...] + b2[...]).astype(BF)
        rows_loop(t, 64, enter)
        ag.start()
    for cp in (later[0], later[1], later[3]):
        cp.wait()
    zero_fill(gbu)
    ay.wait_block(ring.partner)

    def rest():
        ay.far()
        for dx in (ring.xl, ring.xr, ring.xf):
            ay.wait_block(dx * 2 + (1 - ring.c))

    def mlp(blk):
        pre = mm(hg[blk], wu[...]) + bu[...]
        cot = mm(dy[blk], wd[...], NT).astype(BF).astype(F32)
        sq = pre * pre
        th = jnp.tanh(GELU_C * (pre + 0.044715 * sq * pre))
        cdf = 0.5 * (1.0 + th)
        act[blk] = (pre * cdf).astype(BF)
        slope = cdf + pre * (0.5 * (1.0 - th * th)) * (GELU_C * (1.0 + 3 * 0.044715 * sq))
        dp = cot * slope
        gbu[...] = gbu[...] + fold8(dp, jnp.add)
        dpre[blk] = dp.astype(BF)
        part[blk] = mm(dpre[blk], wu[...], NT).astype(BF)

    with scope('b_gather'):
        ag.run(mlp, before_near=rest)
    rs = Scatter(ring, part, *rs_refs)
    chips = (ring.xf, ring.xr, ring.xl, ring.x)
    for slot, xp in enumerate(chips):
        rs.send_pair(xp, slot)
    with scope('b_far'):
        rs.far()
    with scope('b_own'):
        rs.near_own()
    ay.finish()

    def weight_down(i):
        cols = pl.ds(pl.multiple_of(i * 256, 256), 256)
        left = act[:, :, cols].reshape(n * t, 256)
        gwd[cols, :] = mm(left, dy[...].reshape(n * t, d), T0).astype(BF)

    def weight_up(i):
        cols = pl.ds(pl.multiple_of(i * 256, 256), 256)
        left = hg[:, :, cols].reshape(n * t, 256)
        gwu[cols, :] = mm(left, dpre[...].reshape(n * t, f), T0).astype(BF)

    with scope('b_weights'):
        loop(0, f // 256, weight_down)
        loop(0, d // 256, weight_up)
    with scope('b_sum'):
        rs.near_sum()
    zero_fill(small)

    def down(blk):
        dy[blk] = mm(act[blk], wd[...]).astype(BF)
    with scope('b_down'):
        loop(0, n, down)
        rm = Scatter(ring, dy, *rm_refs)
        for slot, xp in enumerate(chips):
            rm.send_pair(xp, slot)
        rs.drain(8, 9)
        rm.far()
    with scope('b_final'):
        rs.wait_final()

    def leave(rows):
        dg = rs.total(rows).astype(BF).astype(F32)
        hat, rstd = norm_rows(x1[rows, :])
        small[2] = small[2] + fold8(dg * hat, jnp.add)
        small[3] = small[3] + fold8(dg, jnp.add)
        dz = norm_back(dg * g2[...], hat, rstd)
        dyf = dyo[rows, :].astype(F32)
        dm = dyf + dz
        small[4] = small[4] + fold8(dm, jnp.add)
        small[5] = small[5] + fold8(dyf, jnp.add)
        mid[rows, :] = dm
        xg[me, rows, :] = dm.astype(BF)

    with scope('b_leave'):
        rows_loop(t, 64, leave)
        rs.finish()
        ag.finish()
    ad.start()
    reload = fetch(0, h_hbm, hg)
    zero_fill(dk, dv)

    def back_block(i):
        dc = mm(xg[i], wof[me], NT).astype(BF)
        zero = jnp.zeros((t, 128), BF)
        prod = (dc.astype(F32) * o[i].astype(F32)).T
        dlt = (col_sum(prod[:64]), col_sum(prod[64:]))
        for head in PAIR:
            dom[head] = jnp.where(lane_mask(t, head), dc, zero)
        zero_fill(dqt)

        def pair_block(blocks, diag):
            cases = [(j, head) for j in blocks for head in PAIR]
            ps, dss = [], []
            for j, head in cases:
                s = mm(k[j], q[head, i], NT) + bt[head]
                if diag:
                    s = jnp.where(key <= qry, s, MASK_VALUE)
                p = jnp.exp(s + (slopes[head] * (j * t).astype(F32) - lse[head, i]))
                dp = mm(v[j], dom[head], NT).astype(BF).astype(F32)
                dss.append((p * (dp - dlt[head])).astype(BF))
                ps.append(p.astype(BF))
            wide = list(zip(cases, ps, dss))
            for j in blocks:
                dv[j] = dv[j] + sum(mm(p, dom[head]) for (b, head), p, _ in wide if b is j)
                dk[j] = dk[j] + sum(mm(ds, q[head, i]) for (b, head), _, ds in wide if b is j)
            for head in PAIR:
                rows = pl.ds(head * 64, 64)
                dqt[rows, :] = dqt[rows, :] + sum(mm(kt[b, rows, :], ds) for (b, h), _, ds in wide if h == head)

        twos(i, lambda blocks: pair_block(blocks, False))
        pair_block((i,), True)
        d3[i, :, :128] = (dqt[...].T * scale).astype(BF)

    with scope('c_attend'):
        ad.run(back_block, after_near=rm.near_own, after_far=rm.near_sum)
    zero_fill(gbq)

    def back_in(xp, slot):
        for cc in PAIR:
            blk = xp * 2 + cc
            d3[blk, :, 128:256] = dk[blk].astype(BF)
            d3[blk, :, 256:] = dv[blk].astype(BF)
            part[blk] = mm(d3[blk], wp[...]).astype(BF)
        rs.send_pair(xp, slot)

    with scope('c_far'):
        back_in(ring.xf, 0)
        rs.far()
    with scope('c_own'):
        back_in(ring.xr, 1)
        back_in(ring.xl, 2)
        rs.near_own()
        back_in(ring.x, 3)
    reload.wait()

    def weight_in(i):
        cols = pl.ds(pl.multiple_of(i * 128, 128), 128)
        left = d3[:, :, cols].reshape(n * t, 128)
        grad = mm(left, hg[...].reshape(n * t, d), T0).astype(BF)
        for head in PAIR:
            gwt[head, i] = grad[head * 64:head * 64 + 64]

    def bias_in(b):
        gbq[...] = gbq[...] + fold8(d3[b].astype(F32), jnp.add)

    with scope('c_weights'):
        loop(0, len(TRIPLE), weight_in)
        loop(0, n, bias_in)
    with scope('c_sum'):
        rs.near_sum()
    with scope('c_gwo'):
        gwo[...] = mm(o[...].reshape(n * t, 128), xg[...].reshape(n * t, d), T0).astype(BF)
    with scope('c_mfinal'):
        rm.wait_final()

    def out_y(rows):
        m = rm.total(rows).astype(BF).astype(F32)
        y[rows, :] = (x1[rows, :] + m + bd[...]).astype(BF)
    rows_loop(t, 64, out_y)
    with scope('c_final'):
        rs.wait_final()

    def sum_in(rows):
        dh = rs.total(rows).astype(BF).astype(F32)
        hat, _ = norm_rows(xo[rows, :].astype(F32))
        small[0] = small[0] + fold8(dh * hat, jnp.add)
        small[1] = small[1] + fold8(dh, jnp.add)

    def last(rows):
        dh = rs.total(rows).astype(BF).astype(F32)
        hat, rstd = norm_rows(xo[rows, :].astype(F32))
        gx[rows, :] = (mid[rows, :] + norm_back(dh * g1[...], hat, rstd)).astype(BF)

    with scope('c_sums'):
        rows_loop(t, 64, sum_in)
    for i in range(6):
        every[me, i:i + 1, :] = col_sum(small[i])
    every[me, 6:, :] = jnp.zeros((2, d), F32)

    def share(off):
        return pltpu.make_async_remote_copy(
            src_ref=every.at[me], dst_ref=every.at[me], send_sem=ar_s.at[off], recv_sem=ar_r.at[me],
            device_id={'tp': (me + off) % n}, device_id_type=MESH)

    with scope('c_share'):
        for off in range(1, n):
            share(off).start()
        rows_loop(t, 64, last)
        for off in range(1, n):
            src = (me + off) % n
            pltpu.make_async_remote_copy(
                src_ref=every.at[src], dst_ref=every.at[src], send_sem=ar_s.at[0], recv_sem=ar_r.at[src],
                device_id={'tp': me}, device_id_type=MESH).wait_recv()
        total = every[0]
        for b in range(1, n):
            total = total + every[b]
        sums[...] = total
    for off in range(1, n):
        share(off).wait_send()
        send_o((me + off) % n).wait_send()
    for job in (rs, rm, aw, ad):
        job.finish()


def kernel_out(n_big, *refs):
    srcs, (gbq, gbu, sums), refs = refs[:n_big], refs[n_big:n_big + 3], refs[n_big + 3:]
    outs, (o_bq, o_bu), refs = refs[:n_big], refs[n_big:n_big + 2], refs[n_big + 2:]
    o_sums, refs = refs[:6], refs[6:]
    bufs, (sem_in, sem_out) = refs[:n_big], refs[n_big:]
    ins = [pltpu.make_async_copy(a, b, sem_in.at[i]) for i, (a, b) in enumerate(zip(srcs, bufs))]
    backs = [pltpu.make_async_copy(b, a, sem_out.at[i]) for i, (a, b) in enumerate(zip(outs, bufs))]
    for cp in ins:
        cp.start()
    o_bu[...] = col_sum(gbu[...])
    row = col_sum(gbq[...])
    e = o_bq.shape[2]
    for part_no in TRIPLE:
        for head in PAIR:
            at = (part_no * 2 + head) * e
            o_bq[part_no, head:head + 1, :] = row[:, at:at + e]
    for i, ref in enumerate(o_sums):
        ref[...] = sums[i:i + 1, :]
    for cp, back in zip(ins, backs):
        cp.wait()
        back.start()
    for back in backs:
        back.wait()


def whole():
    return pl.BlockSpec(memory_space=VMEM)


def anywhere():
    return pl.BlockSpec(memory_space=pl.ANY)


def smem():
    return pl.BlockSpec(memory_space=pltpu.SMEM)


def solution(mesh):
    n = mesh.shape['tp']

    def local_step(x, ln1_gamma, ln1_beta, w_qkv, b_qkv, w_out, b_out, ln2_gamma, ln2_beta, w_up, b_up, w_down, b_down, grad_y):
        t, d = x.shape[1], x.shape[2]
        heads, e = w_qkv.shape[1], w_qkv.shape[3]
        he = heads * e
        f = w_up.shape[1]
        scale = e ** -0.5
        slopes = jnp.asarray(alibi_slopes(heads * n))
        x2, dy2 = x[0], grad_y[0]
        row = lambda vec: vec.reshape(1, -1)
        wt = w_qkv.transpose(1, 2, 3, 0).reshape(heads * 3 * e, d)
        bq = b_qkv.transpose(1, 0, 2)
        sds = jax.ShapeDtypeStruct
        rows, full, half = (t, d), (n, t, d), (n, t, he)
        both, line = (len(PAIR),) + half, (len(PAIR), n, 1, t)
        packed = (len(TRIPLE) * he, d)
        params = lambda cid: pltpu.CompilerParams(collective_id=cid, has_side_effects=True, vmem_limit_bytes=VLIM)
        dma = pltpu.SemaphoreType.DMA

        vm = lambda dims, kind=BF: VMEM(dims, kind)
        stat, turned = (len(PAIR), 8, t), (n, he, t)
        y, gx, sums, gwt, gbq, gwo, gwu, gbu, gwd, _ = pl.pallas_call(
            functools.partial(kernel_main, n, scale),
            name='layer',
            out_shape=[sds(rows, BF), sds(rows, BF), sds((8, d), F32), sds((heads, len(TRIPLE), e, d), BF),
                       sds((8, len(TRIPLE) * he), F32), sds((he, d), BF), sds((d, f), BF), sds((8, f), F32),
                       sds((f, d), BF), sds(full, BF)],
            in_specs=[anywhere()] * 6 + [whole()] * 8 + [smem()],
            out_specs=[whole()] * 9 + [anywhere()],
            scratch_shapes=[vm(full), vm(rows), vm(rows), vm(full), vm(full), vm(packed), vm(packed), vm((n, he, d)),
                            vm((d, f)), vm((f, d)), vm(both), vm(half), vm(half), vm(turned), vm(turned), vm(half),
                            vm(line, F32), vm(rows), vm((len(PAIR), n, t, t), F32), vm(stat, F32), vm(stat, F32),
                            vm((he, t), F32), vm((len(PAIR), t, t), F32), vm(rows, F32), vm((n, t, f)), vm((n, t, f)),
                            vm(rows, F32), vm((len(PAIR), t, he)), vm((he, t), F32), vm(half, F32), vm(half, F32),
                            vm((n, t, len(TRIPLE) * he)), vm((6, 8, d), F32), vm((n, 8, d), F32), vm(full)]
            + scatter_scratch(n, t, d) * 2 + gather_scratch(n) * 5 + [dma((n,))] * 5,
            compiler_params=params(0),
        )(x2, dy2, wt, w_out, w_up, w_down, row(ln1_gamma), row(ln1_beta), bq, row(b_out), row(ln2_gamma), row(ln2_beta),
          row(b_up), row(b_down), slopes)

        big = (y, gx, gwt, gwo, gwu, gwd)
        res = pl.pallas_call(
            functools.partial(kernel_out, len(big)),
            name='results',
            out_shape=[sds(b.shape, b.dtype) for b in big] + [sds((len(TRIPLE), heads, e), F32), sds((1, f), F32)]
            + [sds((1, d), F32)] * 6,
            in_specs=[anywhere()] * len(big) + [whole()] * 3,
            out_specs=[anywhere()] * len(big) + [whole()] * 8,
            scratch_shapes=[VMEM(b.shape, b.dtype) for b in big] + [dma((len(big),))] * 2,
        )(*big, gbq, gbu, sums)
        y, gx, gwt, gwo, gwu, gwd, gbq, gbu, s_g1, s_b1, s_g2, s_b2, s_bo, s_bd = res
        vec = lambda a: a.reshape(-1)
        return (y[None], gx[None], vec(s_g1), vec(s_b1), gwt.transpose(3, 0, 1, 2), gbq.transpose(1, 0, 2), gwo, vec(s_bo),
                vec(s_g2), vec(s_b2), gwu, vec(gbu), gwd, vec(s_bd))

    row_spec = P('dp', 'tp', None)
    in_specs = (row_spec, P(), P(), P(None, 'tp', None, None), P('tp', None, None), P('tp', None), P(), P(), P(),
                P(None, 'tp'), P('tp'), P('tp', None), P(), row_spec)
    out_specs = (row_spec, row_spec, P('dp'), P('dp'), P('dp', 'tp', None, None), P(('dp', 'tp'), None, None),
                 P(('dp', 'tp'), None), P('dp'), P('dp'), P('dp'), P('dp', 'tp'), P(('dp', 'tp')), P(('dp', 'tp'), None), P('dp'))
    return jax.shard_map(local_step, mesh=mesh, in_specs=in_specs, out_specs=out_specs, check_vma=False)
```

```python
import functools
import math
import jax
import jax.numpy as jnp
import numpy as np
from jax import lax
from jax.experimental import pallas as pl
from jax.experimental.pallas import tpu as pltpu
from jax.sharding import PartitionSpec as P

EPS = 1e-5
MASK_VALUE = -1e30
BF, F32 = jnp.bfloat16, jnp.float32
VMEM = pltpu.VMEM
MESH = pl.DeviceIdType.MESH
scope = jax.named_scope
VLIM = 62 * 1024 * 1024
GELU_C = math.sqrt(2.0 / math.pi)
PAIR = LOW, HIGH = (0, 1)
TRIPLE = (0, 1, 2)
NN = (((1,), (0,)), ((), ()))
T0 = (((0,), (0,)), ((), ()))
NT = (((1,), (1,)), ((), ()))


def alibi_slopes(n_heads):
    closest = 2 ** int(math.floor(math.log2(n_heads)))
    base_ratio = 2.0 ** (-8.0 / closest)
    extra_ratio = 2.0 ** (-4.0 / closest)
    remaining = min(closest, n_heads - closest)
    slopes = [base_ratio ** (i + 1) for i in range(closest)]
    slopes = slopes + [extra_ratio ** (2 * i + 1) for i in range(remaining)]
    return np.array(slopes, dtype=np.float32)


def mm(a, b, dims=NN):
    return lax.dot_general(a, b, dims, preferred_element_type=F32)


def loop(lo, hi, body, unroll=1):
    def step(i, carry):
        body(i)
        return carry
    lax.fori_loop(lo, hi, step, 0, unroll=unroll)


def twos(count, body):
    loop(0, count // 2, lambda i: body((2 * i, 2 * i + 1)))

    @pl.when(count % 2 == 1)
    def _():
        body((count - 1,))


def rows_loop(total, rows, body, unroll=1):
    loop(0, total // rows, lambda r: body(pl.ds(pl.multiple_of(r * rows, rows), rows)), unroll)


def row_mean(z):
    return jnp.mean(z, axis=-1, keepdims=True)


def col_sum(z):
    return jnp.sum(z, axis=0, keepdims=True)


def norm_back(grad, hat, rstd):
    return rstd * (grad - row_mean(grad) - hat * row_mean(grad * hat))


def zero_fill(*refs):
    for ref in refs:
        ref[...] = jnp.zeros(ref.shape, ref.dtype)


def sort_weight(wp, wt):
    e = wp.shape[0] // 6
    for part_no in TRIPLE:
        for head in PAIR:
            dst = (part_no * 2 + head) * e
            src = (head * 3 + part_no) * e
            wp[dst:dst + e, :] = wt[src:src + e, :]


def norm_rows(z):
    cen = z - row_mean(z)
    rstd = lax.rsqrt(row_mean(cen * cen) + EPS)
    return cen * rstd, rstd


def fold8(v, op):
    out = v[0:8]
    for k in range(1, v.shape[0] // 8):
        out = op(out, v[8 * k:8 * k + 8])
    return out


class Ring:
    def __init__(self, n):
        self.n = n
        nx = n // 2
        self.me = lax.axis_index('tp')
        self.x = self.me // 2
        self.c = self.me % 2
        self.nx = nx
        self.xr = (self.x + 1) % nx
        self.xl = (self.x + nx - 1) % nx
        self.xf = (self.x + 2) % nx
        self.right = self.xr * 2 + self.c
        self.left = self.xl * 2 + self.c
        self.far = self.xf * 2 + self.c
        self.partner = self.x * 2 + (1 - self.c)

    def order(self, s):
        odd = s % 2
        dx = jnp.where(s < 2, 0, jnp.where(s >= 6, 2, jnp.where(odd == 0, self.nx - 1, 1)))
        mid = jnp.where(s < 4, 0, 1)
        dc = jnp.where(s < 2, odd, jnp.where(s >= 6, odd, mid))
        return ((self.x + dx) % self.nx) * 2 + (self.c + dc) % 2

    def barrier(self, everyone=False):
        sem = pltpu.get_barrier_semaphore()
        if everyone:
            peers = [(self.me + k) % self.n for k in range(1, self.n)]
        else:
            peers = [self.right, self.left, self.partner]
        for peer in peers:
            pl.semaphore_signal(sem, inc=1, device_id={'tp': peer}, device_id_type=MESH)
        pl.semaphore_wait(sem, len(peers))


class Gather:
    SENDS = 14

    def __init__(self, ring, buf, ssem, rsem):
        self.ring, self.buf, self.ssem, self.rsem = ring, buf, ssem, rsem
        self.half = buf.shape[1] // 2
        self.open = list(range(self.SENDS))

    def cp(self, blk, half, dev, k):
        ref = self.buf.at[blk, pl.ds(half * self.half, self.half)]
        return pltpu.make_async_remote_copy(
            src_ref=ref, dst_ref=ref, send_sem=self.ssem.at[k], recv_sem=self.rsem.at[blk, half],
            device_id={'tp': dev}, device_id_type=MESH)

    def start(self):
        r = self.ring
        self.cp(r.me, LOW, r.right, 0).start()
        self.cp(r.me, HIGH, r.left, 1).start()
        self.cp(r.me, HIGH, r.right, 2).start()
        self.cp(r.me, LOW, r.left, 3).start()
        self.cp(r.me, LOW, r.partner, 4).start()
        self.cp(r.me, HIGH, r.partner, 5).start()

    def wait(self, blk, half):
        self.cp(blk, half, self.ring.me, 0).wait_recv()

    def wait_block(self, blk):
        for half in PAIR:
            self.wait(blk, half)

    def near1(self):
        r = self.ring
        self.wait(r.left, LOW)
        self.cp(r.left, LOW, r.right, 6).start()
        self.cp(r.left, LOW, r.partner, 7).start()
        self.wait(r.right, HIGH)
        self.cp(r.right, HIGH, r.left, 8).start()
        self.cp(r.right, HIGH, r.partner, 9).start()

    def near2(self):
        r = self.ring
        self.wait(r.left, HIGH)
        self.cp(r.left, HIGH, r.partner, 10).start()
        self.wait(r.right, LOW)
        self.cp(r.right, LOW, r.partner, 11).start()

    def far(self):
        r = self.ring
        self.wait(r.far, LOW)
        self.cp(r.far, LOW, r.partner, 12).start()
        self.wait(r.far, HIGH)
        self.cp(r.far, HIGH, r.partner, 13).start()

    def drain(self, *which):
        for k in which:
            self.open.remove(k)
            self.cp(self.ring.me, LOW, self.ring.right, k).wait_send()

    def finish(self):
        self.drain(*list(self.open))

    def run(self, body, before_near=None, after_near=None, before_far=None, after_far=None):
        r = self.ring

        def step(s):
            blk = r.order(s)

            @pl.when(s == 1)
            def _():
                self.wait_block(blk)

            @pl.when(s == 2)
            def _():
                if before_near is not None:
                    before_near()
                self.near1()
                if after_near is not None:
                    after_near()
                self.near2()

            @pl.when((s == 4) | (s == 5) | (s == 7))
            def _():
                self.wait_block(blk)

            @pl.when(s == 6)
            def _():
                if before_far is not None:
                    before_far()
                self.far()
                if after_far is not None:
                    after_far()

            body(blk)

        loop(0, r.n, step)


class Scatter:
    SENDS = 10

    def __init__(self, ring, part, pair, stage, land, ssem, rsem):
        self.ring, self.part, self.pair, self.stage, self.land = ring, part, pair, stage, land
        self.ssem, self.rsem = ssem, rsem
        self.rows = part.shape[1]
        self.half = self.rows // 2
        self.open = list(range(4, self.SENDS))

    def cp_pair(self, xp, k):
        r = self.ring
        return pltpu.make_async_remote_copy(
            src_ref=self.part.at[xp * 2 + (1 - r.c)], dst_ref=self.pair.at[xp], send_sem=self.ssem.at[k],
            recv_sem=self.rsem.at[xp], device_id={'tp': r.partner}, device_id_type=MESH)

    def cp(self, slot, half, dst_slot, dev, k):
        rows = pl.ds(half * self.half, self.half)
        return pltpu.make_async_remote_copy(
            src_ref=self.stage.at[slot, rows], dst_ref=self.land.at[dst_slot, rows],
            send_sem=self.ssem.at[k], recv_sem=self.rsem.at[4 + 2 * dst_slot + half],
            device_id={'tp': dev}, device_id_type=MESH)

    def wait_land(self, dst_slot, half):
        self.cp(0, half, dst_slot, self.ring.me, 0).wait_recv()

    def wait_pair(self, xp):
        self.cp_pair(xp, 0).wait_recv()

    def send_pair(self, xp, k):
        self.cp_pair(xp, k).start()

    def mix(self, slot, xp, half, with_far=False):
        blk = xp * 2 + self.ring.c
        step = 16

        def body(i):
            rows = pl.ds(pl.multiple_of(half * self.half + i * step, step), step)
            total = self.part[blk, rows, :].astype(F32) + self.pair[xp, rows, :].astype(F32)
            if with_far:
                total = total + self.land[0, rows, :].astype(F32)
            self.stage[slot, rows, :] = total.astype(BF)
        loop(0, self.half // step, body)

    def far(self):
        r = self.ring
        self.wait_pair(r.xf)
        self.mix(0, r.xf, 0)
        self.cp(0, 0, 0, r.right, 4).start()
        self.mix(0, r.xf, 1)
        self.cp(0, 1, 0, r.left, 5).start()

    def near_own(self):
        r = self.ring
        self.wait_pair(r.xr)
        self.mix(1, r.xr, 1)
        self.cp(1, 1, 1, r.right, 6).start()
        self.wait_pair(r.xl)
        self.mix(2, r.xl, 0)
        self.cp(2, 0, 2, r.left, 7).start()

    def near_sum(self):
        r = self.ring
        self.wait_land(0, 0)
        self.mix(1, r.xr, 0, with_far=True)
        self.cp(1, 0, 1, r.right, 8).start()
        self.wait_land(0, 1)
        self.mix(2, r.xl, 1, with_far=True)
        self.cp(2, 1, 2, r.left, 9).start()

    def wait_final(self):
        self.wait_pair(self.ring.x)
        for slot in (1, 2):
            for half in PAIR:
                self.wait_land(slot, half)

    def total(self, rows):
        r = self.ring
        return (self.part[r.me, rows, :].astype(F32) + self.pair[r.x, rows, :].astype(F32)
                + self.land[1, rows, :].astype(F32) + self.land[2, rows, :].astype(F32))

    def drain(self, *which):
        for k in which:
            self.open.remove(k)
            self.cp(LOW, LOW, LOW, self.ring.right, k).wait_send()

    def finish(self):
        for k in range(4):
            self.cp_pair(self.ring.x, k).wait_send()
        self.drain(*list(self.open))
        self.open = list(range(4, self.SENDS))


def scatter_scratch(n, rows, d):
    return [VMEM((n // 2, rows, d), BF), VMEM((3, rows, d), BF), VMEM((3, rows, d), BF),
            pltpu.SemaphoreType.DMA((Scatter.SENDS,)), pltpu.SemaphoreType.DMA((4 + 6,))]


def gather_scratch(n):
    return [pltpu.SemaphoreType.DMA((Gather.SENDS,)), pltpu.SemaphoreType.DMA((n, 2))]


def lane_mask(rows, h):
    lane = lax.broadcasted_iota(jnp.int32, (rows, 128), 1)
    return (lane < 64) if h == 0 else (lane >= 64)


def attend_block(i, q_ref, k_ref, vt_ref, o_ref, lse_ref, s_ref, m_ref, l_ref, acc_ref, bt_ref, slopes):
    t = q_ref.shape[2]
    e = acc_ref.shape[0] // 2
    key = lax.broadcasted_iota(jnp.int32, (t, t), 0)
    qry = lax.broadcasted_iota(jnp.int32, (t, t), 1)
    for h in PAIR:
        m_ref[h] = jnp.full((8, t), MASK_VALUE, F32)
        l_ref[h] = jnp.zeros((8, t), F32)
    zero_fill(acc_ref)

    def shift(h, j):
        return slopes[h] * (j * t).astype(F32)

    def score(blocks, diag):
        top = [m_ref[h] for h in PAIR]
        for j in blocks:
            for h in PAIR:
                s = mm(k_ref[j], q_ref[h, i], NT) + bt_ref[h]
                if diag:
                    s = jnp.where(key <= qry, s, MASK_VALUE)
                s_ref[h, j] = s
                top[h] = jnp.maximum(top[h], fold8(s, jnp.maximum) + shift(h, j))
        for h in PAIR:
            m_ref[h] = top[h]

    twos(i, lambda blocks: score(blocks, False))
    score((i,), True)
    top = [jnp.max(m_ref[h], axis=0, keepdims=True) for h in PAIR]

    def denom(j):
        for h in PAIR:
            l_ref[h] = l_ref[h] + fold8(jnp.exp(s_ref[h, j] + (shift(h, j) - top[h])), jnp.add)

    loop(0, i + 1, denom)
    for h in PAIR:
        lse_ref[h, i] = top[h] + jnp.log(col_sum(l_ref[h]))

    def values(blocks):
        for h in PAIR:
            rows = pl.ds(h * e, e)
            total = acc_ref[rows, :]
            for j in blocks:
                p = jnp.exp(s_ref[h, j] + (shift(h, j) - lse_ref[h, i])).astype(BF)
                total = total + mm(vt_ref[j, rows, :], p)
            acc_ref[rows, :] = total

    twos(i + 1, values)
    o_ref[i] = acc_ref[...].T.astype(BF)


def kernel_main(n, scale, x_hbm, dy_hbm, wt_hbm, wo_hbm, wu_hbm, wd_hbm, g1, b1, bqkv, bo, g2, b2, bu, bd, slopes_ref,
                y, gx, sums, gwt, gbq, gwo, gwu, gbu, gwd, h_hbm,
                xg, xo, dyo, dy, hg, wt, wp, wof, wu, wd, q, k, v, kt, vt, o, lse, orow, s_ref, m_ref, l_ref, acc, bt,
                x1, act, dpre, mid, dom, dqt, dk, dv, d3, small, every, part,
                *rest):
    rest = list(rest)

    def take(count):
        head = rest[:count]
        del rest[:count]
        return head

    ring = Ring(n)
    me = ring.me
    t, d, f = xg.shape[1], xg.shape[2], wu.shape[1]
    rs_refs, rm_refs = take(5), take(5)
    ax, ay, aw, ag, ad = [Gather(ring, buf, *take(2)) for buf in (xg, dy, wof, hg, xg)]
    o_send, o_recv, ar_s, ar_r, local = take(5)

    def fetch(i, src, dst):
        cp = pltpu.make_async_copy(src, dst, local.at[i])
        cp.start()
        return cp

    in_x, in_wo, in_dy, in_wt = (fetch(0, x_hbm, xg.at[me]), fetch(1, wo_hbm, wof.at[me]),
                                 fetch(2, dy_hbm, dy.at[me]), fetch(3, wt_hbm, wt))
    later = [fetch(4, wu_hbm, wu), fetch(5, wd_hbm, wd), fetch(6, x_hbm, xo), fetch(7, dy_hbm, dyo)]
    ring.barrier(everyone=True)
    in_x.wait()
    ax.start()
    in_wt.wait()
    sort_weight(wp, wt)
    in_wo.wait()
    in_dy.wait()
    bias = jnp.concatenate([bqkv[kind, head:head + 1, :] for kind in TRIPLE for head in PAIR], axis=1)

    def project(blk):
        def norm(rows):
            hat, _ = norm_rows(xg[blk, rows, :].astype(F32))
            hg[blk, rows, :] = (hat * g1[...] + b1[...]).astype(BF)
        rows_loop(t, 64, norm)
        out = mm(hg[blk], wp[...], NT) + bias
        out = out.astype(BF)
        zero = jnp.zeros((t, 128), BF)
        qs = (out[:, :128].astype(F32) * scale).astype(BF)
        for head in PAIR:
            q[head, blk] = jnp.where(lane_mask(t, head), qs, zero)
        k[blk] = out[:, 128:256]
        v[blk] = out[:, 256:]
        kt[blk] = out[:, 128:256].T
        vt[blk] = out[:, 256:].T
        fetch(0, hg.at[blk], h_hbm.at[blk])

    def background():
        ax.drain(6, 8)
        aw.start()

    with scope('a_gather'):
        ax.run(project, before_far=background, after_far=ay.start)
    slopes = [slopes_ref[me * 2 + head] for head in PAIR]
    key = lax.broadcasted_iota(jnp.int32, (t, t), 0)
    qry = lax.broadcasted_iota(jnp.int32, (t, t), 1)
    for head in PAIR:
        bt[head] = slopes[head] * key.astype(F32)

    def send_o(i):
        cols = pl.ds(pl.multiple_of(me * 128, 128), 128)
        return pltpu.make_async_remote_copy(
            src_ref=o.at[i], dst_ref=orow.at[:, cols], send_sem=o_send.at[i], recv_sem=o_recv.at[me],
            device_id={'tp': i}, device_id_type=MESH)

    def all_blocks(step):
        i = ring.order(n - 1 - step)
        for at, act_now in ((4, aw.near1), (5, aw.near2), (n - 1, ay.near1)):
            pl.when(step == at)(act_now)
        attend_block(i, q, k, vt, o, lse, s_ref, m_ref, l_ref, acc, bt, slopes)

        @pl.when(step < n - 1)
        def _():
            send_o(i).start()

    with scope('a_attend'):
        ax.finish()
        pltpu.make_async_copy(hg, h_hbm, local.at[0]).wait()
        loop(0, n, all_blocks)
    with scope('a_wait'):
        aw.far()
        ay.near2()
        orow[:, pl.ds(pl.multiple_of(me * 128, 128), 128)] = o[me]
        for off in range(1, n):
            src = (me + off) % n
            cols = pl.ds(pl.multiple_of(src * 128, 128), 128)
            pltpu.make_async_remote_copy(
                src_ref=o.at[0], dst_ref=orow.at[:, cols], send_sem=o_send.at[0], recv_sem=o_recv.at[src],
                device_id={'tp': me}, device_id_type=MESH).wait_recv()
        for dx in (ring.x, ring.xl, ring.xr, ring.xf):
            aw.wait_block(dx * 2 + (1 - ring.c))
        later[2].wait()
    with scope('a_out'):
        x1[...] = mm(orow[...], wof[...].reshape(n * 128, d)).astype(BF).astype(F32)

        def enter(rows):
            row = xo[rows, :].astype(F32) + x1[rows, :] + bo[...]
            x1[rows, :] = row
            hat, _ = norm_rows(row)
            hg[me, rows, :] = (hat * g2[...] + b2[...]).astype(BF)
        rows_loop(t, 64, enter)
        ag.start()
    for cp in (later[0], later[1], later[3]):
        cp.wait()
    zero_fill(gbu)
    ay.wait_block(ring.partner)

    def rest():
        ay.far()
        for dx in (ring.xl, ring.xr, ring.xf):
            ay.wait_block(dx * 2 + (1 - ring.c))

    def mlp(blk):
        pre = mm(hg[blk], wu[...]) + bu[...]
        cot = mm(dy[blk], wd[...], NT).astype(BF).astype(F32)
        sq = pre * pre
        th = jnp.tanh(GELU_C * (pre + 0.044715 * sq * pre))
        cdf = 0.5 * (1.0 + th)
        act[blk] = (pre * cdf).astype(BF)
        slope = cdf + pre * (0.5 * (1.0 - th * th)) * (GELU_C * (1.0 + 3 * 0.044715 * sq))
        dp = cot * slope
        gbu[...] = gbu[...] + fold8(dp, jnp.add)
        dpre[blk] = dp.astype(BF)
        part[blk] = mm(dpre[blk], wu[...], NT).astype(BF)

    with scope('b_gather'):
        ag.run(mlp, before_near=rest)
    rs = Scatter(ring, part, *rs_refs)
    chips = (ring.xf, ring.xr, ring.xl, ring.x)
    for slot, xp in enumerate(chips):
        rs.send_pair(xp, slot)
    with scope('b_far'):
        rs.far()
    with scope('b_own'):
        rs.near_own()
    ay.finish()

    def weight_down(i):
        cols = pl.ds(pl.multiple_of(i * 256, 256), 256)
        left = act[:, :, cols].reshape(n * t, 256)
        gwd[cols, :] = mm(left, dy[...].reshape(n * t, d), T0).astype(BF)

    def weight_up(i):
        cols = pl.ds(pl.multiple_of(i * 256, 256), 256)
        left = hg[:, :, cols].reshape(n * t, 256)
        gwu[cols, :] = mm(left, dpre[...].reshape(n * t, f), T0).astype(BF)

    with scope('b_weights'):
        loop(0, f // 256, weight_down)
        loop(0, d // 256, weight_up)
    with scope('b_sum'):
        rs.near_sum()
    zero_fill(small)

    def down(blk):
        dy[blk] = mm(act[blk], wd[...]).astype(BF)
    with scope('b_down'):
        loop(0, n, down)
        rm = Scatter(ring, dy, *rm_refs)
        for slot, xp in enumerate(chips):
            rm.send_pair(xp, slot)
        rs.drain(8, 9)
        rm.far()
    with scope('b_final'):
        rs.wait_final()

    def leave(rows):
        dg = rs.total(rows).astype(BF).astype(F32)
        hat, rstd = norm_rows(x1[rows, :])
        small[2] = small[2] + fold8(dg * hat, jnp.add)
        small[3] = small[3] + fold8(dg, jnp.add)
        dz = norm_back(dg * g2[...], hat, rstd)
        dyf = dyo[rows, :].astype(F32)
        dm = dyf + dz
        small[4] = small[4] + fold8(dm, jnp.add)
        small[5] = small[5] + fold8(dyf, jnp.add)
        mid[rows, :] = dm
        xg[me, rows, :] = dm.astype(BF)

    with scope('b_leave'):
        rows_loop(t, 64, leave)
        rs.finish()
        ag.finish()
    ad.start()
    reload = fetch(0, h_hbm, hg)
    zero_fill(dk, dv)

    def back_block(i):
        dc = mm(xg[i], wof[me], NT).astype(BF)
        zero = jnp.zeros((t, 128), BF)
        prod = (dc.astype(F32) * o[i].astype(F32)).T
        dlt = (col_sum(prod[:64]), col_sum(prod[64:]))
        for head in PAIR:
            dom[head] = jnp.where(lane_mask(t, head), dc, zero)
        zero_fill(dqt)

        def pair_block(blocks, diag):
            cases = [(j, head) for j in blocks for head in PAIR]
            ps, dss = [], []
            for j, head in cases:
                s = mm(k[j], q[head, i], NT) + bt[head]
                if diag:
                    s = jnp.where(key <= qry, s, MASK_VALUE)
                p = jnp.exp(s + (slopes[head] * (j * t).astype(F32) - lse[head, i]))
                dp = mm(v[j], dom[head], NT).astype(BF).astype(F32)
                dss.append((p * (dp - dlt[head])).astype(BF))
                ps.append(p.astype(BF))
            wide = list(zip(cases, ps, dss))
            for j in blocks:
                dv[j] = dv[j] + sum(mm(p, dom[head]) for (b, head), p, _ in wide if b is j)
                dk[j] = dk[j] + sum(mm(ds, q[head, i]) for (b, head), _, ds in wide if b is j)
            for head in PAIR:
                rows = pl.ds(head * 64, 64)
                dqt[rows, :] = dqt[rows, :] + sum(mm(kt[b, rows, :], ds) for (b, h), _, ds in wide if h == head)

        twos(i, lambda blocks: pair_block(blocks, False))
        pair_block((i,), True)
        d3[i, :, :128] = (dqt[...].T * scale).astype(BF)

    with scope('c_attend'):
        ad.run(back_block, after_near=rm.near_own, after_far=rm.near_sum)
    zero_fill(gbq)

    def back_in(xp, slot):
        for cc in PAIR:
            blk = xp * 2 + cc
            d3[blk, :, 128:256] = dk[blk].astype(BF)
            d3[blk, :, 256:] = dv[blk].astype(BF)
            part[blk] = mm(d3[blk], wp[...]).astype(BF)
        rs.send_pair(xp, slot)

    with scope('c_far'):
        back_in(ring.xf, 0)
        rs.far()
    with scope('c_own'):
        back_in(ring.xr, 1)
        back_in(ring.xl, 2)
        rs.near_own()
        back_in(ring.x, 3)
    reload.wait()

    def weight_in(i):
        cols = pl.ds(pl.multiple_of(i * 128, 128), 128)
        left = d3[:, :, cols].reshape(n * t, 128)
        grad = mm(left, hg[...].reshape(n * t, d), T0).astype(BF)
        for head in PAIR:
            gwt[head, i] = grad[head * 64:head * 64 + 64]

    def bias_in(b):
        gbq[...] = gbq[...] + fold8(d3[b].astype(F32), jnp.add)

    with scope('c_weights'):
        loop(0, len(TRIPLE), weight_in)
        loop(0, n, bias_in)
    with scope('c_sum'):
        rs.near_sum()
    with scope('c_gwo'):
        gwo[...] = mm(o[...].reshape(n * t, 128), xg[...].reshape(n * t, d), T0).astype(BF)
    with scope('c_mfinal'):
        rm.wait_final()

    def out_y(rows):
        m = rm.total(rows).astype(BF).astype(F32)
        y[rows, :] = (x1[rows, :] + m + bd[...]).astype(BF)
    rows_loop(t, 64, out_y)
    with scope('c_final'):
        rs.wait_final()

    def sum_in(rows):
        dh = rs.total(rows).astype(BF).astype(F32)
        hat, _ = norm_rows(xo[rows, :].astype(F32))
        small[0] = small[0] + fold8(dh * hat, jnp.add)
        small[1] = small[1] + fold8(dh, jnp.add)

    def last(rows):
        dh = rs.total(rows).astype(BF).astype(F32)
        hat, rstd = norm_rows(xo[rows, :].astype(F32))
        gx[rows, :] = (mid[rows, :] + norm_back(dh * g1[...], hat, rstd)).astype(BF)

    with scope('c_sums'):
        rows_loop(t, 64, sum_in)
    for i in range(6):
        every[me, i:i + 1, :] = col_sum(small[i])
    every[me, 6:, :] = jnp.zeros((2, d), F32)

    def share(off):
        return pltpu.make_async_remote_copy(
            src_ref=every.at[me], dst_ref=every.at[me], send_sem=ar_s.at[off], recv_sem=ar_r.at[me],
            device_id={'tp': (me + off) % n}, device_id_type=MESH)

    with scope('c_share'):
        for off in range(1, n):
            share(off).start()
        rows_loop(t, 64, last)
        for off in range(1, n):
            src = (me + off) % n
            pltpu.make_async_remote_copy(
                src_ref=every.at[src], dst_ref=every.at[src], send_sem=ar_s.at[0], recv_sem=ar_r.at[src],
                device_id={'tp': me}, device_id_type=MESH).wait_recv()
        total = every[0]
        for b in range(1, n):
            total = total + every[b]
        sums[...] = total
    for off in range(1, n):
        share(off).wait_send()
        send_o((me + off) % n).wait_send()
    for job in (rs, rm, aw, ad):
        job.finish()


def kernel_out(n_big, *refs):
    srcs, (gbq, gbu, sums), refs = refs[:n_big], refs[n_big:n_big + 3], refs[n_big + 3:]
    outs, (o_bq, o_bu), refs = refs[:n_big], refs[n_big:n_big + 2], refs[n_big + 2:]
    o_sums, refs = refs[:6], refs[6:]
    bufs, (sem_in, sem_out) = refs[:n_big], refs[n_big:]
    ins = [pltpu.make_async_copy(a, b, sem_in.at[i]) for i, (a, b) in enumerate(zip(srcs, bufs))]
    backs = [pltpu.make_async_copy(b, a, sem_out.at[i]) for i, (a, b) in enumerate(zip(outs, bufs))]
    for cp in ins:
        cp.start()
    o_bu[...] = col_sum(gbu[...])
    row = col_sum(gbq[...])
    e = o_bq.shape[2]
    for part_no in TRIPLE:
        for head in PAIR:
            at = (part_no * 2 + head) * e
            o_bq[part_no, head:head + 1, :] = row[:, at:at + e]
    for i, ref in enumerate(o_sums):
        ref[...] = sums[i:i + 1, :]
    for cp, back in zip(ins, backs):
        cp.wait()
        back.start()
    for back in backs:
        back.wait()


def whole():
    return pl.BlockSpec(memory_space=VMEM)


def anywhere():
    return pl.BlockSpec(memory_space=pl.ANY)


def smem():
    return pl.BlockSpec(memory_space=pltpu.SMEM)


def solution(mesh):
    n = mesh.shape['tp']

    def local_step(x, ln1_gamma, ln1_beta, w_qkv, b_qkv, w_out, b_out, ln2_gamma, ln2_beta, w_up, b_up, w_down, b_down, grad_y):
        t, d = x.shape[1], x.shape[2]
        heads, e = w_qkv.shape[1], w_qkv.shape[3]
        he = heads * e
        f = w_up.shape[1]
        scale = e ** -0.5
        slopes = jnp.asarray(alibi_slopes(heads * n))
        x2, dy2 = x[0], grad_y[0]
        row = lambda vec: vec.reshape(1, -1)
        wt = w_qkv.transpose(1, 2, 3, 0).reshape(heads * 3 * e, d)
        bq = b_qkv.transpose(1, 0, 2)
        sds = jax.ShapeDtypeStruct
        rows, full, half = (t, d), (n, t, d), (n, t, he)
        both, line = (len(PAIR),) + half, (len(PAIR), n, 1, t)
        packed = (len(TRIPLE) * he, d)
        params = lambda cid: pltpu.CompilerParams(collective_id=cid, has_side_effects=True, vmem_limit_bytes=VLIM)
        dma = pltpu.SemaphoreType.DMA

        vm = lambda dims, kind=BF: VMEM(dims, kind)
        stat, turned = (len(PAIR), 8, t), (n, he, t)
        y, gx, sums, gwt, gbq, gwo, gwu, gbu, gwd, _ = pl.pallas_call(
            functools.partial(kernel_main, n, scale),
            name='layer',
            out_shape=[sds(rows, BF), sds(rows, BF), sds((8, d), F32), sds((heads, len(TRIPLE), e, d), BF),
                       sds((8, len(TRIPLE) * he), F32), sds((he, d), BF), sds((d, f), BF), sds((8, f), F32),
                       sds((f, d), BF), sds(full, BF)],
            in_specs=[anywhere()] * 6 + [whole()] * 8 + [smem()],
            out_specs=[whole()] * 9 + [anywhere()],
            scratch_shapes=[vm(full), vm(rows), vm(rows), vm(full), vm(full), vm(packed), vm(packed), vm((n, he, d)),
                            vm((d, f)), vm((f, d)), vm(both), vm(half), vm(half), vm(turned), vm(turned), vm(half),
                            vm(line, F32), vm(rows), vm((len(PAIR), n, t, t), F32), vm(stat, F32), vm(stat, F32),
                            vm((he, t), F32), vm((len(PAIR), t, t), F32), vm(rows, F32), vm((n, t, f)), vm((n, t, f)),
                            vm(rows, F32), vm((len(PAIR), t, he)), vm((he, t), F32), vm(half, F32), vm(half, F32),
                            vm((n, t, len(TRIPLE) * he)), vm((6, 8, d), F32), vm((n, 8, d), F32), vm(full)]
            + scatter_scratch(n, t, d) * 2 + gather_scratch(n) * 5 + [dma((n,))] * 5,
            compiler_params=params(0),
        )(x2, dy2, wt, w_out, w_up, w_down, row(ln1_gamma), row(ln1_beta), bq, row(b_out), row(ln2_gamma), row(ln2_beta),
          row(b_up), row(b_down), slopes)

        big = (y, gx, gwt, gwo, gwu, gwd)
        res = pl.pallas_call(
            functools.partial(kernel_out, len(big)),
            name='results',
            out_shape=[sds(b.shape, b.dtype) for b in big] + [sds((len(TRIPLE), heads, e), F32), sds((1, f), F32)]
            + [sds((1, d), F32)] * 6,
            in_specs=[anywhere()] * len(big) + [whole()] * 3,
            out_specs=[anywhere()] * len(big) + [whole()] * 8,
            scratch_shapes=[VMEM(b.shape, b.dtype) for b in big] + [dma((len(big),))] * 2,
        )(*big, gbq, gbu, sums)
        y, gx, gwt, gwo, gwu, gwd, gbq, gbu, s_g1, s_b1, s_g2, s_b2, s_bo, s_bd = res
        vec = lambda a: a.reshape(-1)
        return (y[None], gx[None], vec(s_g1), vec(s_b1), gwt.transpose(3, 0, 1, 2), gbq.transpose(1, 0, 2), gwo, vec(s_bo),
                vec(s_g2), vec(s_b2), gwu, vec(gbu), gwd, vec(s_bd))

    row_spec = P('dp', 'tp', None)
    in_specs = (row_spec, P(), P(), P(None, 'tp', None, None), P('tp', None, None), P('tp', None), P(), P(), P(),
                P(None, 'tp'), P('tp'), P('tp', None), P(), row_spec)
    out_specs = (row_spec, row_spec, P('dp'), P('dp'), P('dp', 'tp', None, None), P(('dp', 'tp'), None, None),
                 P(('dp', 'tp'), None), P('dp'), P('dp'), P('dp'), P('dp', 'tp'), P(('dp', 'tp')), P(('dp', 'tp'), None), P('dp'))
    return jax.shard_map(local_step, mesh=mesh, in_specs=in_specs, out_specs=out_specs, check_vma=False)
```

```python
import functools
import math
import jax
import jax.numpy as jnp
import numpy as np
from jax import lax
from jax.experimental import pallas as pl
from jax.experimental.pallas import tpu as pltpu
from jax.sharding import PartitionSpec as P

EPS = 1e-5
MASK_VALUE = -1e30
BF, F32 = jnp.bfloat16, jnp.float32
VMEM = pltpu.VMEM
MESH = pl.DeviceIdType.MESH
scope = jax.named_scope
VLIM = 62 * 1024 * 1024
GELU_C = math.sqrt(2.0 / math.pi)
PAIR = LOW, HIGH = (0, 1)
TRIPLE = (0, 1, 2)
NN = (((1,), (0,)), ((), ()))
T0 = (((0,), (0,)), ((), ()))
NT = (((1,), (1,)), ((), ()))


def alibi_slopes(n_heads):
    closest = 2 ** int(math.floor(math.log2(n_heads)))
    base_ratio = 2.0 ** (-8.0 / closest)
    extra_ratio = 2.0 ** (-4.0 / closest)
    remaining = min(closest, n_heads - closest)
    slopes = [base_ratio ** (i + 1) for i in range(closest)]
    slopes = slopes + [extra_ratio ** (2 * i + 1) for i in range(remaining)]
    return np.array(slopes, dtype=np.float32)


def mm(a, b, dims=NN):
    return lax.dot_general(a, b, dims, preferred_element_type=F32)


def loop(lo, hi, body, unroll=1):
    def step(i, carry):
        body(i)
        return carry
    lax.fori_loop(lo, hi, step, 0, unroll=unroll)


def twos(count, body):
    loop(0, count // 2, lambda i: body((2 * i, 2 * i + 1)))

    @pl.when(count % 2 == 1)
    def _():
        body((count - 1,))


def rows_loop(total, rows, body, unroll=1):
    loop(0, total // rows, lambda r: body(pl.ds(pl.multiple_of(r * rows, rows), rows)), unroll)


def row_mean(z):
    return jnp.mean(z, axis=-1, keepdims=True)


def col_sum(z):
    return jnp.sum(z, axis=0, keepdims=True)


def norm_back(grad, hat, rstd):
    return rstd * (grad - row_mean(grad) - hat * row_mean(grad * hat))


def zero_fill(*refs):
    for ref in refs:
        ref[...] = jnp.zeros(ref.shape, ref.dtype)


def sort_weight(wp, wt):
    e = wp.shape[0] // 6
    for part_no in TRIPLE:
        for head in PAIR:
            dst = (part_no * 2 + head) * e
            src = (head * 3 + part_no) * e
            wp[dst:dst + e, :] = wt[src:src + e, :]


def norm_rows(z):
    cen = z - row_mean(z)
    rstd = lax.rsqrt(row_mean(cen * cen) + EPS)
    return cen * rstd, rstd


def fold8(v, op):
    out = v[0:8]
    for k in range(1, v.shape[0] // 8):
        out = op(out, v[8 * k:8 * k + 8])
    return out


class Ring:
    def __init__(self, n):
        self.n = n
        nx = n // 2
        self.me = lax.axis_index('tp')
        self.x = self.me // 2
        self.c = self.me % 2
        self.nx = nx
        self.xr = (self.x + 1) % nx
        self.xl = (self.x + nx - 1) % nx
        self.xf = (self.x + 2) % nx
        self.right = self.xr * 2 + self.c
        self.left = self.xl * 2 + self.c
        self.far = self.xf * 2 + self.c
        self.partner = self.x * 2 + (1 - self.c)

    def order(self, s):
        odd = s % 2
        dx = jnp.where(s < 2, 0, jnp.where(s >= 6, 2, jnp.where(odd == 0, self.nx - 1, 1)))
        mid = jnp.where(s < 4, 0, 1)
        dc = jnp.where(s < 2, odd, jnp.where(s >= 6, odd, mid))
        return ((self.x + dx) % self.nx) * 2 + (self.c + dc) % 2

    def barrier(self, everyone=False):
        sem = pltpu.get_barrier_semaphore()
        if everyone:
            peers = [(self.me + k) % self.n for k in range(1, self.n)]
        else:
            peers = [self.right, self.left, self.partner]
        for peer in peers:
            pl.semaphore_signal(sem, inc=1, device_id={'tp': peer}, device_id_type=MESH)
        pl.semaphore_wait(sem, len(peers))


class Gather:
    SENDS = 14

    def __init__(self, ring, buf, ssem, rsem):
        self.ring, self.buf, self.ssem, self.rsem = ring, buf, ssem, rsem
        self.half = buf.shape[1] // 2
        self.open = list(range(self.SENDS))

    def cp(self, blk, half, dev, k):
        ref = self.buf.at[blk, pl.ds(half * self.half, self.half)]
        return pltpu.make_async_remote_copy(
            src_ref=ref, dst_ref=ref, send_sem=self.ssem.at[k], recv_sem=self.rsem.at[blk, half],
            device_id={'tp': dev}, device_id_type=MESH)

    def start(self):
        r = self.ring
        self.cp(r.me, LOW, r.right, 0).start()
        self.cp(r.me, HIGH, r.left, 1).start()
        self.cp(r.me, HIGH, r.right, 2).start()
        self.cp(r.me, LOW, r.left, 3).start()
        self.cp(r.me, LOW, r.partner, 4).start()
        self.cp(r.me, HIGH, r.partner, 5).start()

    def wait(self, blk, half):
        self.cp(blk, half, self.ring.me, 0).wait_recv()

    def wait_block(self, blk):
        for half in PAIR:
            self.wait(blk, half)

    def near1(self):
        r = self.ring
        self.wait(r.left, LOW)
        self.cp(r.left, LOW, r.right, 6).start()
        self.cp(r.left, LOW, r.partner, 7).start()
        self.wait(r.right, HIGH)
        self.cp(r.right, HIGH, r.left, 8).start()
        self.cp(r.right, HIGH, r.partner, 9).start()

    def near2(self):
        r = self.ring
        self.wait(r.left, HIGH)
        self.cp(r.left, HIGH, r.partner, 10).start()
        self.wait(r.right, LOW)
        self.cp(r.right, LOW, r.partner, 11).start()

    def far(self):
        r = self.ring
        self.wait(r.far, LOW)
        self.cp(r.far, LOW, r.partner, 12).start()
        self.wait(r.far, HIGH)
        self.cp(r.far, HIGH, r.partner, 13).start()

    def drain(self, *which):
        for k in which:
            self.open.remove(k)
            self.cp(self.ring.me, LOW, self.ring.right, k).wait_send()

    def finish(self):
        self.drain(*list(self.open))

    def run(self, body, before_near=None, after_near=None, before_far=None, after_far=None):
        r = self.ring

        def step(s):
            blk = r.order(s)

            @pl.when(s == 1)
            def _():
                self.wait_block(blk)

            @pl.when(s == 2)
            def _():
                if before_near is not None:
                    before_near()
                self.near1()
                if after_near is not None:
                    after_near()
                self.near2()

            @pl.when((s == 4) | (s == 5) | (s == 7))
            def _():
                self.wait_block(blk)

            @pl.when(s == 6)
            def _():
                if before_far is not None:
                    before_far()
                self.far()
                if after_far is not None:
                    after_far()

            body(blk)

        loop(0, r.n, step)


class Scatter:
    SENDS = 10

    def __init__(self, ring, part, pair, stage, land, ssem, rsem):
        self.ring, self.part, self.pair, self.stage, self.land = ring, part, pair, stage, land
        self.ssem, self.rsem = ssem, rsem
        self.rows = part.shape[1]
        self.half = self.rows // 2
        self.open = list(range(4, self.SENDS))

    def cp_pair(self, xp, k):
        r = self.ring
        return pltpu.make_async_remote_copy(
            src_ref=self.part.at[xp * 2 + (1 - r.c)], dst_ref=self.pair.at[xp], send_sem=self.ssem.at[k],
            recv_sem=self.rsem.at[xp], device_id={'tp': r.partner}, device_id_type=MESH)

    def cp(self, slot, half, dst_slot, dev, k):
        rows = pl.ds(half * self.half, self.half)
        return pltpu.make_async_remote_copy(
            src_ref=self.stage.at[slot, rows], dst_ref=self.land.at[dst_slot, rows],
            send_sem=self.ssem.at[k], recv_sem=self.rsem.at[4 + 2 * dst_slot + half],
            device_id={'tp': dev}, device_id_type=MESH)

    def wait_land(self, dst_slot, half):
        self.cp(0, half, dst_slot, self.ring.me, 0).wait_recv()

    def wait_pair(self, xp):
        self.cp_pair(xp, 0).wait_recv()

    def send_pair(self, xp, k):
        self.cp_pair(xp, k).start()

    def mix(self, slot, xp, half, with_far=False):
        blk = xp * 2 + self.ring.c
        step = 16

        def body(i):
            rows = pl.ds(pl.multiple_of(half * self.half + i * step, step), step)
            total = self.part[blk, rows, :].astype(F32) + self.pair[xp, rows, :].astype(F32)
            if with_far:
                total = total + self.land[0, rows, :].astype(F32)
            self.stage[slot, rows, :] = total.astype(BF)
        loop(0, self.half // step, body)

    def far(self):
        r = self.ring
        self.wait_pair(r.xf)
        self.mix(0, r.xf, 0)
        self.cp(0, 0, 0, r.right, 4).start()
        self.mix(0, r.xf, 1)
        self.cp(0, 1, 0, r.left, 5).start()

    def near_own(self):
        r = self.ring
        self.wait_pair(r.xr)
        self.mix(1, r.xr, 1)
        self.cp(1, 1, 1, r.right, 6).start()
        self.wait_pair(r.xl)
        self.mix(2, r.xl, 0)
        self.cp(2, 0, 2, r.left, 7).start()

    def near_sum(self):
        r = self.ring
        self.wait_land(0, 0)
        self.mix(1, r.xr, 0, with_far=True)
        self.cp(1, 0, 1, r.right, 8).start()
        self.wait_land(0, 1)
        self.mix(2, r.xl, 1, with_far=True)
        self.cp(2, 1, 2, r.left, 9).start()

    def wait_final(self):
        self.wait_pair(self.ring.x)
        for slot in (1, 2):
            for half in PAIR:
                self.wait_land(slot, half)

    def total(self, rows):
        r = self.ring
        return (self.part[r.me, rows, :].astype(F32) + self.pair[r.x, rows, :].astype(F32)
                + self.land[1, rows, :].astype(F32) + self.land[2, rows, :].astype(F32))

    def drain(self, *which):
        for k in which:
            self.open.remove(k)
            self.cp(LOW, LOW, LOW, self.ring.right, k).wait_send()

    def finish(self):
        for k in range(4):
            self.cp_pair(self.ring.x, k).wait_send()
        self.drain(*list(self.open))
        self.open = list(range(4, self.SENDS))


def scatter_scratch(n, rows, d):
    return [VMEM((n // 2, rows, d), BF), VMEM((3, rows, d), BF), VMEM((3, rows, d), BF),
            pltpu.SemaphoreType.DMA((Scatter.SENDS,)), pltpu.SemaphoreType.DMA((4 + 6,))]


def gather_scratch(n):
    return [pltpu.SemaphoreType.DMA((Gather.SENDS,)), pltpu.SemaphoreType.DMA((n, 2))]


def lane_mask(rows, h):
    lane = lax.broadcasted_iota(jnp.int32, (rows, 128), 1)
    return (lane < 64) if h == 0 else (lane >= 64)


def attend_block(i, q_ref, k_ref, vt_ref, o_ref, lse_ref, s_ref, m_ref, l_ref, acc_ref, bt_ref, slopes):
    t = q_ref.shape[2]
    e = acc_ref.shape[0] // 2
    key = lax.broadcasted_iota(jnp.int32, (t, t), 0)
    qry = lax.broadcasted_iota(jnp.int32, (t, t), 1)
    for h in PAIR:
        m_ref[h] = jnp.full((8, t), MASK_VALUE, F32)
        l_ref[h] = jnp.zeros((8, t), F32)
    zero_fill(acc_ref)

    def shift(h, j):
        return slopes[h] * (j * t).astype(F32)

    def score(blocks, diag):
        top = [m_ref[h] for h in PAIR]
        for j in blocks:
            for h in PAIR:
                s = mm(k_ref[j], q_ref[h, i], NT) + bt_ref[h]
                if diag:
                    s = jnp.where(key <= qry, s, MASK_VALUE)
                s_ref[h, j] = s
                top[h] = jnp.maximum(top[h], fold8(s, jnp.maximum) + shift(h, j))
        for h in PAIR:
            m_ref[h] = top[h]

    twos(i, lambda blocks: score(blocks, False))
    score((i,), True)
    top = [jnp.max(m_ref[h], axis=0, keepdims=True) for h in PAIR]

    def denom(j):
        for h in PAIR:
            l_ref[h] = l_ref[h] + fold8(jnp.exp(s_ref[h, j] + (shift(h, j) - top[h])), jnp.add)

    loop(0, i + 1, denom)
    for h in PAIR:
        lse_ref[h, i] = top[h] + jnp.log(col_sum(l_ref[h]))

    def values(blocks):
        for h in PAIR:
            rows = pl.ds(h * e, e)
            total = acc_ref[rows, :]
            for j in blocks:
                p = jnp.exp(s_ref[h, j] + (shift(h, j) - lse_ref[h, i])).astype(BF)
                total = total + mm(vt_ref[j, rows, :], p)
            acc_ref[rows, :] = total

    twos(i + 1, values)
    o_ref[i] = acc_ref[...].T.astype(BF)


def kernel_main(n, scale, n_vec, n_out, x_hbm, dy_hbm, wt_hbm, wo_hbm, wu_hbm, wd_hbm, *refs):
    vec_hbm, (slopes_ref,), refs = refs[:n_vec], refs[n_vec:n_vec + 1], refs[n_vec + 1:]
    out_hbm, (h_hbm,), refs = refs[:n_out], refs[n_out:n_out + 1], refs[n_out + 1:]
    vecs, results, refs = refs[:n_vec], refs[n_vec:n_vec + n_out], refs[n_vec + n_out:]
    run_layer(n, scale, vec_hbm, vecs, out_hbm, results, x_hbm, dy_hbm, wt_hbm, wo_hbm, wu_hbm, wd_hbm, slopes_ref, h_hbm, *refs)


def run_layer(n, scale, vec_hbm, vecs, out_hbm, results, x_hbm, dy_hbm, wt_hbm, wo_hbm, wu_hbm, wd_hbm, slopes_ref, h_hbm,
                xg, xo, dyo, dy, hg, wt, wp, wof, wu, wd, q, k, v, kt, vt, o, lse, orow, s_ref, m_ref, l_ref, acc, bt,
                x1, act, dpre, mid, dom, dqt, dk, dv, d3, small, every, part,
                *rest):
    g1, b1, bqkv, bo, g2, b2, bu, bd = vecs
    y, gx, sums, gwt, gbq, gwo, gwu, gbu, gwd = results
    rest = list(rest)

    def take(count):
        head = rest[:count]
        del rest[:count]
        return head

    ring = Ring(n)
    me = ring.me
    t, d, f = xg.shape[1], xg.shape[2], wu.shape[1]
    rs_refs, rm_refs = take(5), take(5)
    ax, ay, aw, ag, ad = [Gather(ring, buf, *take(2)) for buf in (xg, dy, wof, hg, xg)]
    o_send, o_recv, ar_s, ar_r, local, vec_sem, out_sem = take(7)
    outs = [pltpu.make_async_copy(b, a, out_sem.at[i]) for i, (a, b) in enumerate(zip(out_hbm, results))]
    out_y, out_gx, out_sums, out_gwt, out_gbq, out_gwo, out_gwu, out_gbu, out_gwd = outs

    def fetch(i, src, dst):
        cp = pltpu.make_async_copy(src, dst, local.at[i])
        cp.start()
        return cp

    in_x, in_wo, in_dy, in_wt = (fetch(0, x_hbm, xg.at[me]), fetch(1, wo_hbm, wof.at[me]),
                                 fetch(2, dy_hbm, dy.at[me]), fetch(3, wt_hbm, wt))
    later = [fetch(4, wu_hbm, wu), fetch(5, wd_hbm, wd), fetch(6, x_hbm, xo), fetch(7, dy_hbm, dyo)]
    vec_in = [pltpu.make_async_copy(a, b, vec_sem.at[i]) for i, (a, b) in enumerate(zip(vec_hbm, vecs))]
    for cp in vec_in:
        cp.start()
    ring.barrier(everyone=True)
    in_x.wait()
    ax.start()
    for cp in vec_in:
        cp.wait()
    in_wt.wait()
    sort_weight(wp, wt)
    in_wo.wait()
    in_dy.wait()
    bias = jnp.concatenate([bqkv[kind, head:head + 1, :] for kind in TRIPLE for head in PAIR], axis=1)

    def project(blk):
        def norm(rows):
            hat, _ = norm_rows(xg[blk, rows, :].astype(F32))
            hg[blk, rows, :] = (hat * g1[...] + b1[...]).astype(BF)
        rows_loop(t, 64, norm)
        out = mm(hg[blk], wp[...], NT) + bias
        out = out.astype(BF)
        zero = jnp.zeros((t, 128), BF)
        qs = (out[:, :128].astype(F32) * scale).astype(BF)
        for head in PAIR:
            q[head, blk] = jnp.where(lane_mask(t, head), qs, zero)
        k[blk] = out[:, 128:256]
        v[blk] = out[:, 256:]
        kt[blk] = out[:, 128:256].T
        vt[blk] = out[:, 256:].T
        fetch(0, hg.at[blk], h_hbm.at[blk])

    def background():
        ax.drain(6, 8)
        aw.start()

    with scope('a_gather'):
        ax.run(project, before_far=background, after_far=ay.start)
    slopes = [slopes_ref[me * 2 + head] for head in PAIR]
    key = lax.broadcasted_iota(jnp.int32, (t, t), 0)
    qry = lax.broadcasted_iota(jnp.int32, (t, t), 1)
    for head in PAIR:
        bt[head] = slopes[head] * key.astype(F32)

    def send_o(i):
        cols = pl.ds(pl.multiple_of(me * 128, 128), 128)
        return pltpu.make_async_remote_copy(
            src_ref=o.at[i], dst_ref=orow.at[:, cols], send_sem=o_send.at[i], recv_sem=o_recv.at[me],
            device_id={'tp': i}, device_id_type=MESH)

    def all_blocks(step):
        i = ring.order(n - 1 - step)
        for at, act_now in ((4, aw.near1), (5, aw.near2), (n - 1, ay.near1)):
            pl.when(step == at)(act_now)
        attend_block(i, q, k, vt, o, lse, s_ref, m_ref, l_ref, acc, bt, slopes)

        @pl.when(step < n - 1)
        def _():
            send_o(i).start()

    with scope('a_attend'):
        ax.finish()
        pltpu.make_async_copy(hg, h_hbm, local.at[0]).wait()
        loop(0, n, all_blocks)
    with scope('a_wait'):
        aw.far()
        ay.near2()
        orow[:, pl.ds(pl.multiple_of(me * 128, 128), 128)] = o[me]
        for off in range(1, n):
            src = (me + off) % n
            cols = pl.ds(pl.multiple_of(src * 128, 128), 128)
            pltpu.make_async_remote_copy(
                src_ref=o.at[0], dst_ref=orow.at[:, cols], send_sem=o_send.at[0], recv_sem=o_recv.at[src],
                device_id={'tp': me}, device_id_type=MESH).wait_recv()
        for dx in (ring.x, ring.xl, ring.xr, ring.xf):
            aw.wait_block(dx * 2 + (1 - ring.c))
        later[2].wait()
    with scope('a_out'):
        x1[...] = mm(orow[...], wof[...].reshape(n * 128, d)).astype(BF).astype(F32)

        def enter(rows):
            row = xo[rows, :].astype(F32) + x1[rows, :] + bo[...]
            x1[rows, :] = row
            hat, _ = norm_rows(row)
            hg[me, rows, :] = (hat * g2[...] + b2[...]).astype(BF)
        rows_loop(t, 64, enter)
        ag.start()
    for cp in (later[0], later[1], later[3]):
        cp.wait()
    zero_fill(gbu)
    ay.wait_block(ring.partner)

    def rest():
        ay.far()
        for dx in (ring.xl, ring.xr, ring.xf):
            ay.wait_block(dx * 2 + (1 - ring.c))

    def mlp(blk):
        pre = mm(hg[blk], wu[...]) + bu[...]
        cot = mm(dy[blk], wd[...], NT).astype(BF).astype(F32)
        sq = pre * pre
        th = jnp.tanh(GELU_C * (pre + 0.044715 * sq * pre))
        cdf = 0.5 * (1.0 + th)
        act[blk] = (pre * cdf).astype(BF)
        slope = cdf + pre * (0.5 * (1.0 - th * th)) * (GELU_C * (1.0 + 3 * 0.044715 * sq))
        dp = cot * slope
        gbu[...] = gbu[...] + fold8(dp, jnp.add)
        dpre[blk] = dp.astype(BF)
        part[blk] = mm(dpre[blk], wu[...], NT).astype(BF)

    with scope('b_gather'):
        ag.run(mlp, before_near=rest)
    rs = Scatter(ring, part, *rs_refs)
    chips = (ring.xf, ring.xr, ring.xl, ring.x)
    for slot, xp in enumerate(chips):
        rs.send_pair(xp, slot)
    with scope('b_far'):
        rs.far()
    with scope('b_own'):
        rs.near_own()
    ay.finish()

    def weight_down(i):
        cols = pl.ds(pl.multiple_of(i * 256, 256), 256)
        left = act[:, :, cols].reshape(n * t, 256)
        gwd[cols, :] = mm(left, dy[...].reshape(n * t, d), T0).astype(BF)

    def weight_up(i):
        cols = pl.ds(pl.multiple_of(i * 256, 256), 256)
        left = hg[:, :, cols].reshape(n * t, 256)
        gwu[cols, :] = mm(left, dpre[...].reshape(n * t, f), T0).astype(BF)

    with scope('b_weights'):
        loop(0, f // 256, weight_down)
        loop(0, d // 256, weight_up)
        for cp in (out_gwd, out_gwu, out_gbu):
            cp.start()
    with scope('b_sum'):
        rs.near_sum()
    zero_fill(small)

    def down(blk):
        dy[blk] = mm(act[blk], wd[...]).astype(BF)
    with scope('b_down'):
        loop(0, n, down)
        rm = Scatter(ring, dy, *rm_refs)
        for slot, xp in enumerate(chips):
            rm.send_pair(xp, slot)
        rs.drain(8, 9)
        rm.far()
    with scope('b_final'):
        rs.wait_final()

    def leave(rows):
        dg = rs.total(rows).astype(BF).astype(F32)
        hat, rstd = norm_rows(x1[rows, :])
        small[2] = small[2] + fold8(dg * hat, jnp.add)
        small[3] = small[3] + fold8(dg, jnp.add)
        dz = norm_back(dg * g2[...], hat, rstd)
        dyf = dyo[rows, :].astype(F32)
        dm = dyf + dz
        small[4] = small[4] + fold8(dm, jnp.add)
        small[5] = small[5] + fold8(dyf, jnp.add)
        mid[rows, :] = dm
        xg[me, rows, :] = dm.astype(BF)

    with scope('b_leave'):
        rows_loop(t, 64, leave)
        rs.finish()
        ag.finish()
    ad.start()
    reload = fetch(0, h_hbm, hg)
    zero_fill(dk, dv)

    def back_block(i):
        dc = mm(xg[i], wof[me], NT).astype(BF)
        zero = jnp.zeros((t, 128), BF)
        prod = (dc.astype(F32) * o[i].astype(F32)).T
        dlt = (col_sum(prod[:64]), col_sum(prod[64:]))
        for head in PAIR:
            dom[head] = jnp.where(lane_mask(t, head), dc, zero)
        zero_fill(dqt)

        def pair_block(blocks, diag):
            cases = [(j, head) for j in blocks for head in PAIR]
            ps, dss = [], []
            for j, head in cases:
                s = mm(k[j], q[head, i], NT) + bt[head]
                if diag:
                    s = jnp.where(key <= qry, s, MASK_VALUE)
                p = jnp.exp(s + (slopes[head] * (j * t).astype(F32) - lse[head, i]))
                dp = mm(v[j], dom[head], NT).astype(BF).astype(F32)
                dss.append((p * (dp - dlt[head])).astype(BF))
                ps.append(p.astype(BF))
            wide = list(zip(cases, ps, dss))
            for j in blocks:
                dv[j] = dv[j] + sum(mm(p, dom[head]) for (b, head), p, _ in wide if b is j)
                dk[j] = dk[j] + sum(mm(ds, q[head, i]) for (b, head), _, ds in wide if b is j)
            for head in PAIR:
                rows = pl.ds(head * 64, 64)
                dqt[rows, :] = dqt[rows, :] + sum(mm(kt[b, rows, :], ds) for (b, h), _, ds in wide if h == head)

        twos(i, lambda blocks: pair_block(blocks, False))
        pair_block((i,), True)
        d3[i, :, :128] = (dqt[...].T * scale).astype(BF)

    with scope('c_attend'):
        ad.run(back_block, after_near=rm.near_own, after_far=rm.near_sum)
    zero_fill(gbq)

    def back_in(xp, slot):
        for cc in PAIR:
            blk = xp * 2 + cc
            d3[blk, :, 128:256] = dk[blk].astype(BF)
            d3[blk, :, 256:] = dv[blk].astype(BF)
            part[blk] = mm(d3[blk], wp[...]).astype(BF)
        rs.send_pair(xp, slot)

    with scope('c_far'):
        back_in(ring.xf, 0)
        rs.far()
    with scope('c_own'):
        back_in(ring.xr, 1)
        back_in(ring.xl, 2)
        rs.near_own()
        back_in(ring.x, 3)
    reload.wait()

    def weight_in(i):
        cols = pl.ds(pl.multiple_of(i * 128, 128), 128)
        left = d3[:, :, cols].reshape(n * t, 128)
        grad = mm(left, hg[...].reshape(n * t, d), T0).astype(BF)
        for head in PAIR:
            gwt[head, i] = grad[head * 64:head * 64 + 64]

    def bias_in(b):
        gbq[...] = gbq[...] + fold8(d3[b].astype(F32), jnp.add)

    with scope('c_weights'):
        loop(0, len(TRIPLE), weight_in)
        loop(0, n, bias_in)
        for cp in (out_gwt, out_gbq):
            cp.start()
    with scope('c_sum'):
        rs.near_sum()
    with scope('c_gwo'):
        gwo[...] = mm(o[...].reshape(n * t, 128), xg[...].reshape(n * t, d), T0).astype(BF)
        out_gwo.start()
    with scope('c_mfinal'):
        rm.wait_final()

    def finish_y(rows):
        m = rm.total(rows).astype(BF).astype(F32)
        y[rows, :] = (x1[rows, :] + m + bd[...]).astype(BF)
    rows_loop(t, 64, finish_y)
    out_y.start()
    with scope('c_final'):
        rs.wait_final()

    def sum_in(rows):
        dh = rs.total(rows).astype(BF).astype(F32)
        hat, _ = norm_rows(xo[rows, :].astype(F32))
        small[0] = small[0] + fold8(dh * hat, jnp.add)
        small[1] = small[1] + fold8(dh, jnp.add)

    def last(rows):
        dh = rs.total(rows).astype(BF).astype(F32)
        hat, rstd = norm_rows(xo[rows, :].astype(F32))
        gx[rows, :] = (mid[rows, :] + norm_back(dh * g1[...], hat, rstd)).astype(BF)

    with scope('c_sums'):
        rows_loop(t, 64, sum_in)
    for i in range(6):
        every[me, i:i + 1, :] = col_sum(small[i])
    every[me, 6:, :] = jnp.zeros((2, d), F32)

    def share(off):
        return pltpu.make_async_remote_copy(
            src_ref=every.at[me], dst_ref=every.at[me], send_sem=ar_s.at[off], recv_sem=ar_r.at[me],
            device_id={'tp': (me + off) % n}, device_id_type=MESH)

    with scope('c_share'):
        for off in range(1, n):
            share(off).start()
        rows_loop(t, 64, last)
        out_gx.start()
        for off in range(1, n):
            src = (me + off) % n
            pltpu.make_async_remote_copy(
                src_ref=every.at[src], dst_ref=every.at[src], send_sem=ar_s.at[0], recv_sem=ar_r.at[src],
                device_id={'tp': me}, device_id_type=MESH).wait_recv()
        total = every[0]
        for b in range(1, n):
            total = total + every[b]
        sums[...] = total
        out_sums.start()
    for off in range(1, n):
        share(off).wait_send()
        send_o((me + off) % n).wait_send()
    for job in (rs, rm, aw, ad):
        job.finish()
    for cp in outs:
        cp.wait()


def kernel_out(n_big, *refs):
    count = n_big + 3
    srcs, refs = refs[:count], refs[count:]
    outs, refs = refs[:n_big + 8], refs[n_big + 8:]
    bufs, tail, (sem_in, sem_out) = refs[:count], refs[count:-2], refs[-2:]
    gbq, gbu, sums = bufs[n_big:]
    o_bq, o_bu, o_sums = tail
    ins = [pltpu.make_async_copy(a, b, sem_in.at[i]) for i, (a, b) in enumerate(zip(srcs, bufs))]
    kept = list(bufs[:n_big]) + [o_bq, o_bu] + [o_sums.at[i:i + 1] for i in range(6)]
    backs = [pltpu.make_async_copy(b, a, sem_out.at[i]) for i, (a, b) in enumerate(zip(outs, kept))]
    for cp in ins[n_big:] + ins[:n_big]:
        cp.start()
    for cp in ins[n_big:]:
        cp.wait()
    o_bu[...] = col_sum(gbu[...])
    row = col_sum(gbq[...])
    e = o_bq.shape[2]
    for part_no in TRIPLE:
        for head in PAIR:
            at = (part_no * 2 + head) * e
            o_bq[part_no, head:head + 1, :] = row[:, at:at + e]
    o_sums[...] = sums[...]
    for back in backs[n_big:]:
        back.start()
    for cp, back in zip(ins[:n_big], backs):
        cp.wait()
        back.start()
    for back in backs:
        back.wait()


def anywhere():
    return pl.BlockSpec(memory_space=pl.ANY)


def smem():
    return pl.BlockSpec(memory_space=pltpu.SMEM)


def solution(mesh):
    n = mesh.shape['tp']

    def local_step(x, ln1_gamma, ln1_beta, w_qkv, b_qkv, w_out, b_out, ln2_gamma, ln2_beta, w_up, b_up, w_down, b_down, grad_y):
        t, d = x.shape[1], x.shape[2]
        heads, e = w_qkv.shape[1], w_qkv.shape[3]
        he = heads * e
        f = w_up.shape[1]
        scale = e ** -0.5
        slopes = jnp.asarray(alibi_slopes(heads * n))
        x2, dy2 = x[0], grad_y[0]
        row = lambda vec: vec.reshape(1, -1)
        wt = w_qkv.transpose(1, 2, 3, 0).reshape(heads * 3 * e, d)
        bq = b_qkv.transpose(1, 0, 2)
        sds = jax.ShapeDtypeStruct
        rows, full, half = (t, d), (n, t, d), (n, t, he)
        both, line = (len(PAIR),) + half, (len(PAIR), n, 1, t)
        packed = (len(TRIPLE) * he, d)
        params = lambda cid: pltpu.CompilerParams(collective_id=cid, has_side_effects=True, vmem_limit_bytes=VLIM)
        dma = pltpu.SemaphoreType.DMA

        vm = lambda dims, kind=BF: VMEM(dims, kind)
        stat, turned = (len(PAIR), 8, t), (n, he, t)
        vecs = (row(ln1_gamma), row(ln1_beta), bq, row(b_out), row(ln2_gamma), row(ln2_beta), row(b_up), row(b_down))
        results = [sds(rows, BF), sds(rows, BF), sds((8, d), F32), sds((heads, len(TRIPLE), e, d), BF),
                   sds((8, len(TRIPLE) * he), F32), sds((he, d), BF), sds((d, f), BF), sds((8, f), F32), sds((f, d), BF)]
        y, gx, sums, gwt, gbq, gwo, gwu, gbu, gwd, _ = pl.pallas_call(
            functools.partial(kernel_main, n, scale, len(vecs), len(results)),
            name='layer',
            out_shape=results + [sds(full, BF)],
            in_specs=[anywhere()] * (6 + len(vecs)) + [smem()],
            out_specs=[anywhere()] * (len(results) + 1),
            scratch_shapes=[vm(b.shape, b.dtype) for b in list(vecs) + results] + [vm(full), vm(rows), vm(rows), vm(full), vm(full), vm(packed), vm(packed), vm((n, he, d)),
                            vm((d, f)), vm((f, d)), vm(both), vm(half), vm(half), vm(turned), vm(turned), vm(half),
                            vm(line, F32), vm(rows), vm((len(PAIR), n, t, t), F32), vm(stat, F32), vm(stat, F32),
                            vm((he, t), F32), vm((len(PAIR), t, t), F32), vm(rows, F32), vm((n, t, f)), vm((n, t, f)),
                            vm(rows, F32), vm((len(PAIR), t, he)), vm((he, t), F32), vm(half, F32), vm(half, F32),
                            vm((n, t, len(TRIPLE) * he)), vm((6, 8, d), F32), vm((n, 8, d), F32), vm(full)]
            + scatter_scratch(n, t, d) * 2 + gather_scratch(n) * 5 + [dma((n,))] * 5 + [dma((len(vecs),)), dma((len(results),))],
            compiler_params=params(0),
        )(x2, dy2, wt, w_out, w_up, w_down, *vecs, slopes)

        big = (y, gx, gwt, gwo, gwu, gwd)
        little = (gbq, gbu, sums)
        bias_dims, up_dims = (len(TRIPLE), heads, e), (1, f)
        res = pl.pallas_call(
            functools.partial(kernel_out, len(big)),
            name='results',
            out_shape=[sds(b.shape, b.dtype) for b in big] + [sds(bias_dims, F32), sds(up_dims, F32)] + [sds((1, d), F32)] * 6,
            in_specs=[anywhere()] * (len(big) + 3),
            out_specs=[anywhere()] * (len(big) + 8),
            scratch_shapes=[VMEM(b.shape, b.dtype) for b in big + little]
            + [vm(bias_dims, F32), vm(up_dims, F32), vm((8, d), F32)] + [dma((len(big) + 8,))] * 2,
        )(*big, *little)
        y, gx, gwt, gwo, gwu, gwd, gbq, gbu, s_g1, s_b1, s_g2, s_b2, s_bo, s_bd = res
        vec = lambda a: a.reshape(-1)
        return (y[None], gx[None], vec(s_g1), vec(s_b1), gwt.transpose(3, 0, 1, 2), gbq.transpose(1, 0, 2), gwo, vec(s_bo),
                vec(s_g2), vec(s_b2), gwu, vec(gbu), gwd, vec(s_bd))

    row_spec = P('dp', 'tp', None)
    in_specs = (row_spec, P(), P(), P(None, 'tp', None, None), P('tp', None, None), P('tp', None), P(), P(), P(),
                P(None, 'tp'), P('tp'), P('tp', None), P(), row_spec)
    out_specs = (row_spec, row_spec, P('dp'), P('dp'), P('dp', 'tp', None, None), P(('dp', 'tp'), None, None),
                 P(('dp', 'tp'), None), P('dp'), P('dp'), P('dp'), P('dp', 'tp'), P(('dp', 'tp')), P(('dp', 'tp'), None), P('dp'))
    return jax.shard_map(local_step, mesh=mesh, in_specs=in_specs, out_specs=out_specs, check_vma=False)
```

```python
import functools
import math
import jax
import jax.numpy as jnp
import numpy as np
from jax import lax
from jax.experimental import pallas as pl
from jax.experimental.pallas import tpu as pltpu
from jax.sharding import PartitionSpec as P

EPS = 1e-5
MASK_VALUE = -1e30
BF, F32 = jnp.bfloat16, jnp.float32
VMEM = pltpu.VMEM
MESH = pl.DeviceIdType.MESH
scope = jax.named_scope
VLIM = 62 * 1024 * 1024
GELU_C = math.sqrt(2.0 / math.pi)
PAIR = LOW, HIGH = (0, 1)
TRIPLE = (0, 1, 2)
NN = (((1,), (0,)), ((), ()))
T0 = (((0,), (0,)), ((), ()))
NT = (((1,), (1,)), ((), ()))


def alibi_slopes(n_heads):
    closest = 2 ** int(math.floor(math.log2(n_heads)))
    base_ratio = 2.0 ** (-8.0 / closest)
    extra_ratio = 2.0 ** (-4.0 / closest)
    remaining = min(closest, n_heads - closest)
    slopes = [base_ratio ** (i + 1) for i in range(closest)]
    slopes = slopes + [extra_ratio ** (2 * i + 1) for i in range(remaining)]
    return np.array(slopes, dtype=np.float32)


def mm(a, b, dims=NN):
    return lax.dot_general(a, b, dims, preferred_element_type=F32)


def loop(lo, hi, body, unroll=1):
    def step(i, carry):
        body(i)
        return carry
    lax.fori_loop(lo, hi, step, 0, unroll=unroll)


def twos(count, body):
    loop(0, count // 2, lambda i: body((2 * i, 2 * i + 1)))

    @pl.when(count % 2 == 1)
    def _():
        body((count - 1,))


def rows_loop(total, rows, body, base=0):
    loop(0, total // rows, lambda r: body(pl.ds(pl.multiple_of(base + r * rows, rows), rows)))


def row_mean(z):
    return jnp.mean(z, axis=-1, keepdims=True)


def col_sum(z):
    return jnp.sum(z, axis=0, keepdims=True)


def norm_back(grad, hat, rstd):
    return rstd * (grad - row_mean(grad) - hat * row_mean(grad * hat))


def zero_fill(*refs):
    for ref in refs:
        ref[...] = jnp.zeros(ref.shape, ref.dtype)


def sort_weight(wp, wt):
    e = wp.shape[0] // 6
    for part_no in TRIPLE:
        for head in PAIR:
            dst = (part_no * 2 + head) * e
            src = (head * 3 + part_no) * e
            wp[dst:dst + e, :] = wt[src:src + e, :]


def norm_rows(z):
    cen = z - row_mean(z)
    rstd = lax.rsqrt(row_mean(cen * cen) + EPS)
    return cen * rstd, rstd


def fold8(v, op):
    out = v[0:8]
    for k in range(1, v.shape[0] // 8):
        out = op(out, v[8 * k:8 * k + 8])
    return out


class Ring:
    def __init__(self, n):
        self.n = n
        nx = n // 2
        self.me = lax.axis_index('tp')
        self.x = self.me // 2
        self.c = self.me % 2
        self.nx = nx
        self.xr = (self.x + 1) % nx
        self.xl = (self.x + nx - 1) % nx
        self.xf = (self.x + 2) % nx
        self.right = self.xr * 2 + self.c
        self.left = self.xl * 2 + self.c
        self.far = self.xf * 2 + self.c
        self.partner = self.x * 2 + (1 - self.c)

    def order(self, s):
        odd = s % 2
        dx = jnp.where(s < 2, 0, jnp.where(s >= 6, 2, jnp.where(odd == 0, self.nx - 1, 1)))
        mid = jnp.where(s < 4, 0, 1)
        dc = jnp.where(s < 2, odd, jnp.where(s >= 6, odd, mid))
        return ((self.x + dx) % self.nx) * 2 + (self.c + dc) % 2

    def barrier(self, everyone=False):
        sem = pltpu.get_barrier_semaphore()
        if everyone:
            peers = [(self.me + k) % self.n for k in range(1, self.n)]
        else:
            peers = [self.right, self.left, self.partner]
        for peer in peers:
            pl.semaphore_signal(sem, inc=1, device_id={'tp': peer}, device_id_type=MESH)
        pl.semaphore_wait(sem, len(peers))


class Gather:
    SENDS = 14

    def __init__(self, ring, buf, ssem, rsem, base=0, size=None):
        self.ring, self.buf, self.ssem, self.rsem = ring, buf, ssem, rsem
        self.base = base
        self.half = (size or buf.shape[1]) // 2
        self.open = list(range(self.SENDS))

    def cp(self, blk, half, dev, k):
        ref = self.buf.at[blk, pl.ds(self.base + half * self.half, self.half)]
        return pltpu.make_async_remote_copy(
            src_ref=ref, dst_ref=ref, send_sem=self.ssem.at[k], recv_sem=self.rsem.at[blk, half],
            device_id={'tp': dev}, device_id_type=MESH)

    def start(self):
        r = self.ring
        self.cp(r.me, LOW, r.right, 0).start()
        self.cp(r.me, HIGH, r.left, 1).start()
        self.cp(r.me, HIGH, r.right, 2).start()
        self.cp(r.me, LOW, r.left, 3).start()
        self.cp(r.me, LOW, r.partner, 4).start()
        self.cp(r.me, HIGH, r.partner, 5).start()

    def wait(self, blk, half):
        self.cp(blk, half, self.ring.me, 0).wait_recv()

    def wait_block(self, blk):
        for half in PAIR:
            self.wait(blk, half)

    def near1(self):
        r = self.ring
        self.wait(r.left, LOW)
        self.cp(r.left, LOW, r.right, 6).start()
        self.cp(r.left, LOW, r.partner, 7).start()
        self.wait(r.right, HIGH)
        self.cp(r.right, HIGH, r.left, 8).start()
        self.cp(r.right, HIGH, r.partner, 9).start()

    def near2(self):
        r = self.ring
        self.wait(r.left, HIGH)
        self.cp(r.left, HIGH, r.partner, 10).start()
        self.wait(r.right, LOW)
        self.cp(r.right, LOW, r.partner, 11).start()

    def far(self):
        r = self.ring
        self.wait(r.far, LOW)
        self.cp(r.far, LOW, r.partner, 12).start()
        self.wait(r.far, HIGH)
        self.cp(r.far, HIGH, r.partner, 13).start()

    def drain(self, *which):
        for k in which:
            self.open.remove(k)
            self.cp(self.ring.me, LOW, self.ring.right, k).wait_send()

    def finish(self):
        self.drain(*list(self.open))

    def run(self, body, before_near=None, after_near=None, before_far=None, after_far=None):
        r = self.ring

        def step(s):
            blk = r.order(s)

            @pl.when(s == 1)
            def _():
                self.wait_block(blk)

            @pl.when(s == 2)
            def _():
                if before_near is not None:
                    before_near()
                self.near1()
                if after_near is not None:
                    after_near()
                self.near2()

            @pl.when((s == 4) | (s == 5) | (s == 7))
            def _():
                self.wait_block(blk)

            @pl.when(s == 6)
            def _():
                if before_far is not None:
                    before_far()
                self.far()
                if after_far is not None:
                    after_far()

            body(blk)

        loop(0, r.n, step)


class Scatter:
    SENDS = 10

    def __init__(self, ring, part, pair, stage, land, ssem, rsem, base=0, size=None):
        self.ring, self.part, self.pair, self.stage, self.land = ring, part, pair, stage, land
        self.ssem, self.rsem = ssem, rsem
        self.base = base
        self.size = size or part.shape[1]
        self.half = self.size // 2
        self.open = list(range(4, self.SENDS))

    def cp_pair(self, xp, k):
        r = self.ring
        rows = pl.ds(self.base, self.size)
        return pltpu.make_async_remote_copy(
            src_ref=self.part.at[xp * 2 + (1 - r.c), rows], dst_ref=self.pair.at[xp, rows], send_sem=self.ssem.at[k],
            recv_sem=self.rsem.at[xp], device_id={'tp': r.partner}, device_id_type=MESH)

    def cp(self, slot, half, dst_slot, dev, k):
        rows = pl.ds(self.base + half * self.half, self.half)
        return pltpu.make_async_remote_copy(
            src_ref=self.stage.at[slot, rows], dst_ref=self.land.at[dst_slot, rows],
            send_sem=self.ssem.at[k], recv_sem=self.rsem.at[4 + 2 * dst_slot + half],
            device_id={'tp': dev}, device_id_type=MESH)

    def wait_land(self, dst_slot, half):
        self.cp(0, half, dst_slot, self.ring.me, 0).wait_recv()

    def wait_pair(self, xp):
        self.cp_pair(xp, 0).wait_recv()

    def send_pair(self, xp, k):
        self.cp_pair(xp, k).start()

    def mix(self, slot, xp, half, with_far=False):
        blk = xp * 2 + self.ring.c
        step = 32

        def body(i):
            rows = pl.ds(pl.multiple_of(self.base + half * self.half + i * step, step), step)
            total = self.part[blk, rows, :].astype(F32) + self.pair[xp, rows, :].astype(F32)
            if with_far:
                total = total + self.land[0, rows, :].astype(F32)
            self.stage[slot, rows, :] = total.astype(BF)
        loop(0, self.half // step, body)

    def far(self):
        r = self.ring
        self.wait_pair(r.xf)
        self.mix(0, r.xf, 0)
        self.cp(0, 0, 0, r.right, 4).start()
        self.mix(0, r.xf, 1)
        self.cp(0, 1, 0, r.left, 5).start()

    def near_own(self):
        r = self.ring
        self.wait_pair(r.xr)
        self.mix(1, r.xr, 1)
        self.cp(1, 1, 1, r.right, 6).start()
        self.wait_pair(r.xl)
        self.mix(2, r.xl, 0)
        self.cp(2, 0, 2, r.left, 7).start()

    def near_sum(self):
        r = self.ring
        self.wait_land(0, 0)
        self.mix(1, r.xr, 0, with_far=True)
        self.cp(1, 0, 1, r.right, 8).start()
        self.wait_land(0, 1)
        self.mix(2, r.xl, 1, with_far=True)
        self.cp(2, 1, 2, r.left, 9).start()

    def wait_final(self):
        self.wait_pair(self.ring.x)
        for slot in (1, 2):
            for half in PAIR:
                self.wait_land(slot, half)

    def total(self, rows):
        r = self.ring
        return (self.part[r.me, rows, :].astype(F32) + self.pair[r.x, rows, :].astype(F32)
                + self.land[1, rows, :].astype(F32) + self.land[2, rows, :].astype(F32))

    def drain(self, *which):
        for k in which:
            self.open.remove(k)
            self.cp(LOW, LOW, LOW, self.ring.right, k).wait_send()

    def finish(self):
        for k in range(4):
            self.cp_pair(self.ring.x, k).wait_send()
        self.drain(*list(self.open))
        self.open = list(range(4, self.SENDS))


def scatter_buffers(n, rows, d):
    return [VMEM((n // 2, rows, d), BF), VMEM((3, rows, d), BF), VMEM((3, rows, d), BF)]


def scatter_sems():
    return [pltpu.SemaphoreType.DMA((Scatter.SENDS,))] * 2


def hooked(count, body, hooks):
    def step(i):
        for at, actions in hooks.items():
            @pl.when(i == at)
            def _():
                for act in actions:
                    act()
        body(i)
    loop(0, count, step)


def gather_scratch(n):
    return [pltpu.SemaphoreType.DMA((Gather.SENDS,)), pltpu.SemaphoreType.DMA((n, 2))]


def lane_mask(rows, h):
    lane = lax.broadcasted_iota(jnp.int32, (rows, 128), 1)
    return (lane < 64) if h == 0 else (lane >= 64)


def attend_block(i, q_ref, k_ref, vt_ref, o_ref, lse_ref, s_ref, m_ref, l_ref, acc_ref, bt_ref, slopes):
    t = q_ref.shape[2]
    e = acc_ref.shape[0] // 2
    key = lax.broadcasted_iota(jnp.int32, (t, t), 0)
    qry = lax.broadcasted_iota(jnp.int32, (t, t), 1)
    for h in PAIR:
        m_ref[h] = jnp.full((8, t), MASK_VALUE, F32)
        l_ref[h] = jnp.zeros((8, t), F32)
    zero_fill(acc_ref)

    def shift(h, j):
        return slopes[h] * (j * t).astype(F32)

    def score(blocks, diag):
        top = [m_ref[h] for h in PAIR]
        for j in blocks:
            for h in PAIR:
                s = mm(k_ref[j], q_ref[h, i], NT) + bt_ref[h]
                if diag:
                    s = jnp.where(key <= qry, s, MASK_VALUE)
                s_ref[h, j] = s
                top[h] = jnp.maximum(top[h], fold8(s, jnp.maximum) + shift(h, j))
        for h in PAIR:
            m_ref[h] = top[h]

    twos(i, lambda blocks: score(blocks, False))
    score((i,), True)
    top = [jnp.max(m_ref[h], axis=0, keepdims=True) for h in PAIR]

    def denom(j):
        for h in PAIR:
            l_ref[h] = l_ref[h] + fold8(jnp.exp(s_ref[h, j] + (shift(h, j) - top[h])), jnp.add)

    loop(0, i + 1, denom)
    for h in PAIR:
        lse_ref[h, i] = top[h] + jnp.log(col_sum(l_ref[h]))

    def values(blocks):
        for h in PAIR:
            rows = pl.ds(h * e, e)
            total = acc_ref[rows, :]
            for j in blocks:
                p = jnp.exp(s_ref[h, j] + (shift(h, j) - lse_ref[h, i])).astype(BF)
                total = total + mm(vt_ref[j, rows, :], p)
            acc_ref[rows, :] = total

    twos(i + 1, values)
    o_ref[i] = acc_ref[...].T.astype(BF)


def kernel_main(n, scale, n_vec, n_out, x_hbm, dy_hbm, wt_hbm, wo_hbm, wu_hbm, wd_hbm, *refs):
    vec_hbm, (slopes_ref,), refs = refs[:n_vec], refs[n_vec:n_vec + 1], refs[n_vec + 1:]
    out_hbm, (h_hbm,), refs = refs[:n_out], refs[n_out:n_out + 1], refs[n_out + 1:]
    vecs, results, refs = refs[:n_vec], refs[n_vec:n_vec + n_out], refs[n_vec + n_out:]
    run_layer(n, scale, vec_hbm, vecs, out_hbm, results, x_hbm, dy_hbm, wt_hbm, wo_hbm, wu_hbm, wd_hbm, slopes_ref, h_hbm, *refs)


def run_layer(n, scale, vec_hbm, vecs, out_hbm, results, x_hbm, dy_hbm, wt_hbm, wo_hbm, wu_hbm, wd_hbm, slopes_ref, h_hbm,
                xg, xo, dyo, dy, hg, wt, wp, wof, wu, wd, q, k, v, kt, vt, o, lse, orow, s_ref, m_ref, l_ref, acc, bt,
                x1, act, dpre, mid, dom, dqt, dk, dv, d3, small, every, part,
                *rest):
    g1, b1, bqkv, bo, g2, b2, bu, bd = vecs
    y, gx, sums, gwt, gbq, gwo, gwu, gbu, gwd = results
    rest = list(rest)

    def take(count):
        head = rest[:count]
        del rest[:count]
        return head

    ring = Ring(n)
    me = ring.me
    t, d, f = xg.shape[1], xg.shape[2], wu.shape[1]
    rs_bufs, rm_bufs = take(3), take(3)
    st = t // 2
    streams = (0, st)
    r0, r1 = [Scatter(ring, part, *rs_bufs, *take(2), base=base, size=st) for base in streams]
    rs = Scatter(ring, part, *rs_bufs, *take(2))
    rm = Scatter(ring, dy, *rm_bufs, *take(2))
    ax, ay, aw = [Gather(ring, buf, *take(2)) for buf in (xg, dy, wof)]
    g0, g1s = [Gather(ring, hg, *take(2), base=base, size=st) for base in streams]
    d0, d1 = [Gather(ring, xg, *take(2), base=base, size=st) for base in streams]
    o_send, o_recv, ar_s, ar_r, local, vec_sem, out_sem = take(7)
    outs = [pltpu.make_async_copy(b, a, out_sem.at[i]) for i, (a, b) in enumerate(zip(out_hbm, results))]
    out_y, out_gx, out_sums, out_gwt, out_gbq, out_gwo, out_gwu, out_gbu, out_gwd = outs

    def fetch(i, src, dst):
        cp = pltpu.make_async_copy(src, dst, local.at[i])
        cp.start()
        return cp

    in_x, in_wo, in_dy, in_wt = (fetch(0, x_hbm, xg.at[me]), fetch(1, wo_hbm, wof.at[me]),
                                 fetch(2, dy_hbm, dy.at[me]), fetch(3, wt_hbm, wt))
    later = [fetch(4, wu_hbm, wu), fetch(5, wd_hbm, wd), fetch(6, x_hbm, xo), fetch(7, dy_hbm, dyo)]
    vec_in = [pltpu.make_async_copy(a, b, vec_sem.at[i]) for i, (a, b) in enumerate(zip(vec_hbm, vecs))]
    for cp in vec_in:
        cp.start()
    ring.barrier(everyone=True)
    in_x.wait()
    ax.start()
    for cp in vec_in:
        cp.wait()
    in_wt.wait()
    sort_weight(wp, wt)
    in_wo.wait()
    in_dy.wait()
    bias = jnp.concatenate([bqkv[kind, head:head + 1, :] for kind in TRIPLE for head in PAIR], axis=1)

    def project(blk):
        def norm(rows):
            hat, _ = norm_rows(xg[blk, rows, :].astype(F32))
            hg[blk, rows, :] = (hat * g1[...] + b1[...]).astype(BF)
        rows_loop(t, 64, norm)
        out = mm(hg[blk], wp[...], NT) + bias
        out = out.astype(BF)
        zero = jnp.zeros((t, 128), BF)
        qs = (out[:, :128].astype(F32) * scale).astype(BF)
        for head in PAIR:
            q[head, blk] = jnp.where(lane_mask(t, head), qs, zero)
        k[blk] = out[:, 128:256]
        v[blk] = out[:, 256:]
        kt[blk] = out[:, 128:256].T
        vt[blk] = out[:, 256:].T
        fetch(0, hg.at[blk], h_hbm.at[blk])

    def background():
        ax.drain(6, 8)
        aw.start()

    with scope('a_gather'):
        ax.run(project, before_far=background, after_far=ay.start)
    slopes = [slopes_ref[me * 2 + head] for head in PAIR]
    key = lax.broadcasted_iota(jnp.int32, (t, t), 0)
    qry = lax.broadcasted_iota(jnp.int32, (t, t), 1)
    for head in PAIR:
        bt[head] = slopes[head] * key.astype(F32)

    def send_o(i):
        cols = pl.ds(pl.multiple_of(me * 128, 128), 128)
        return pltpu.make_async_remote_copy(
            src_ref=o.at[i], dst_ref=orow.at[:, cols], send_sem=o_send.at[i], recv_sem=o_recv.at[me],
            device_id={'tp': i}, device_id_type=MESH)

    def all_blocks(step):
        i = ring.order(n - 1 - step)
        for at, act_now in ((4, aw.near1), (5, aw.near2), (n - 1, ay.near1)):
            pl.when(step == at)(act_now)
        attend_block(i, q, k, vt, o, lse, s_ref, m_ref, l_ref, acc, bt, slopes)

        @pl.when(step < n - 1)
        def _():
            send_o(i).start()

    with scope('a_attend'):
        ax.finish()
        pltpu.make_async_copy(hg, h_hbm, local.at[0]).wait()
        loop(0, n, all_blocks)
    with scope('a_wait'):
        aw.far()
        ay.near2()
        orow[:, pl.ds(pl.multiple_of(me * 128, 128), 128)] = o[me]
        for off in range(1, n):
            src = (me + off) % n
            cols = pl.ds(pl.multiple_of(src * 128, 128), 128)
            pltpu.make_async_remote_copy(
                src_ref=o.at[0], dst_ref=orow.at[:, cols], send_sem=o_send.at[0], recv_sem=o_recv.at[src],
                device_id={'tp': me}, device_id_type=MESH).wait_recv()
        for dx in (ring.x, ring.xl, ring.xr, ring.xf):
            aw.wait_block(dx * 2 + (1 - ring.c))
        later[2].wait()
    with scope('a_out'):
        x1[...] = mm(orow[...], wof[...].reshape(n * 128, d)).astype(BF).astype(F32)

        def enter(rows):
            row = xo[rows, :].astype(F32) + x1[rows, :] + bo[...]
            x1[rows, :] = row
            hat, _ = norm_rows(row)
            hg[me, rows, :] = (hat * g2[...] + b2[...]).astype(BF)
        rows_loop(st, 64, enter)
        g0.start()
        rows_loop(st, 64, enter, base=st)
    for cp in (later[0], later[1], later[3]):
        cp.wait()
    zero_fill(gbu)
    ay.wait_block(ring.partner)

    def rest():
        ay.far()
        for dx in (ring.xl, ring.xr, ring.xf):
            ay.wait_block(dx * 2 + (1 - ring.c))

    def mlp(blk, stream):
        rows = pl.ds(pl.multiple_of(stream * st, st), st)
        pre = mm(hg[blk, rows, :], wu[...]) + bu[...]
        cot = mm(dy[blk, rows, :], wd[...], NT).astype(BF).astype(F32)
        sq = pre * pre
        th = jnp.tanh(GELU_C * (pre + 0.044715 * sq * pre))
        cdf = 0.5 * (1.0 + th)
        act[blk, rows, :] = (pre * cdf).astype(BF)
        slope = cdf + pre * (0.5 * (1.0 - th * th)) * (GELU_C * (1.0 + 3 * 0.044715 * sq))
        dp = cot * slope
        gbu[...] = gbu[...] + fold8(dp, jnp.add)
        dpb = dp.astype(BF)
        dpre[blk, rows, :] = dpb
        part[blk, rows, :] = mm(dpb, wu[...], NT).astype(BF)

    chips = (ring.xf, ring.xr, ring.xl, ring.x)
    other = 1 - ring.c
    pleft, pright, pfar = [xp * 2 + other for xp in (ring.xl, ring.xr, ring.xf)]

    def pairs(job):
        for slot, xp in enumerate(chips):
            job.send_pair(xp, slot)

    def item(step):
        late = (step == 4) | (step == 5) | (step >= 10)
        pos = jnp.where(step < 4, step, jnp.where(step < 6, step - 4, jnp.where(step < 10, step - 2, step - 8)))
        mlp(ring.order(pos), jnp.where(late, 1, 0))

    arrive = functools.partial
    with scope('b_gather'):
        hooked(2 * n, item, {
            1: [arrive(g0.wait_block, ring.partner)],
            2: [rest, g0.near1, g1s.start, g0.near2],
            5: [arrive(g1s.wait_block, ring.partner)],
            6: [arrive(g0.wait_block, pleft)],
            7: [arrive(g0.wait_block, pright)],
            8: [g0.far],
            9: [arrive(g0.wait_block, pfar)],
            10: [arrive(pairs, r0), g1s.near1, r0.far, g1s.near2],
            12: [r0.near_own, arrive(g1s.wait_block, pleft)],
            13: [arrive(g1s.wait_block, pright)],
            14: [g1s.far],
            15: [arrive(g1s.wait_block, pfar)]})
    with scope('b_far'):
        pairs(r1)
        r0.near_sum()
        r1.far()
    with scope('b_own'):
        r1.near_own()
    ay.finish()

    def weight_down(i):
        cols = pl.ds(pl.multiple_of(i * 256, 256), 256)
        left = act[:, :, cols].reshape(n * t, 256)
        gwd[cols, :] = mm(left, dy[...].reshape(n * t, d), T0).astype(BF)

    def weight_up(i):
        cols = pl.ds(pl.multiple_of(i * 256, 256), 256)
        left = hg[:, :, cols].reshape(n * t, 256)
        gwu[cols, :] = mm(left, dpre[...].reshape(n * t, f), T0).astype(BF)

    with scope('b_weights'):
        loop(0, f // 256, weight_down)
        loop(0, d // 256, weight_up)
        for cp in (out_gwd, out_gwu, out_gbu):
            cp.start()
    zero_fill(small)

    def down(blk):
        dy[blk] = mm(act[blk], wd[...]).astype(BF)

    def leave(rows):
        dg = rs.total(rows).astype(BF).astype(F32)
        hat, rstd = norm_rows(x1[rows, :])
        small[2] = small[2] + fold8(dg * hat, jnp.add)
        small[3] = small[3] + fold8(dg, jnp.add)
        dz = norm_back(dg * g2[...], hat, rstd)
        dyf = dyo[rows, :].astype(F32)
        dm = dyf + dz
        small[4] = small[4] + fold8(dm, jnp.add)
        small[5] = small[5] + fold8(dyf, jnp.add)
        mid[rows, :] = dm
        xg[me, rows, :] = dm.astype(BF)

    with scope('b_sum'):
        r1.near_sum()
    with scope('b_final'):
        r0.wait_final()
    with scope('b_leave'):
        rows_loop(st, 64, leave)
        d0.start()
    with scope('b_down'):
        loop(0, n, down)
        pairs(rm)
    with scope('b_final1'):
        r1.wait_final()
    with scope('b_leave1'):
        rows_loop(st, 64, leave, base=st)
        d1.start()
    with scope('b_finish'):
        for job in (r0, r1, g0, g1s):
            job.finish()
    reload = fetch(0, h_hbm, hg)
    zero_fill(dk, dv)

    def back_block(i):
        dc = mm(xg[i], wof[me], NT).astype(BF)
        zero = jnp.zeros((t, 128), BF)
        prod = (dc.astype(F32) * o[i].astype(F32)).T
        dlt = (col_sum(prod[:64]), col_sum(prod[64:]))
        for head in PAIR:
            dom[head] = jnp.where(lane_mask(t, head), dc, zero)
        zero_fill(dqt)

        def pair_block(blocks, diag):
            cases = [(j, head) for j in blocks for head in PAIR]
            ps, dss = [], []
            for j, head in cases:
                s = mm(k[j], q[head, i], NT) + bt[head]
                if diag:
                    s = jnp.where(key <= qry, s, MASK_VALUE)
                p = jnp.exp(s + (slopes[head] * (j * t).astype(F32) - lse[head, i]))
                dp = mm(v[j], dom[head], NT).astype(BF).astype(F32)
                dss.append((p * (dp - dlt[head])).astype(BF))
                ps.append(p.astype(BF))
            wide = list(zip(cases, ps, dss))
            for j in blocks:
                dv[j] = dv[j] + sum(mm(p, dom[head]) for (b, head), p, _ in wide if b is j)
                dk[j] = dk[j] + sum(mm(ds, q[head, i]) for (b, head), _, ds in wide if b is j)
            for head in PAIR:
                rows = pl.ds(head * 64, 64)
                dqt[rows, :] = dqt[rows, :] + sum(mm(kt[b, rows, :], ds) for (b, h), _, ds in wide if h == head)

        twos(i, lambda blocks: pair_block(blocks, False))
        pair_block((i,), True)
        d3[i, :, :128] = (dqt[...].T * scale).astype(BF)

    def both_in(blk):
        for job in (d0, d1):
            job.wait_block(blk)

    with scope('c_attend'):
        hooked(n, lambda step: back_block(ring.order(step)), {
            1: [arrive(both_in, ring.partner), d0.near1, d0.near2],
            2: [d1.near1, rm.far, rm.near_own, d1.near2],
            4: [arrive(both_in, pleft)],
            5: [arrive(both_in, pright)],
            6: [d0.far, d1.far, rm.near_sum],
            7: [arrive(both_in, pfar)]})
    zero_fill(gbq)

    def back_in(xp, slot):
        for cc in PAIR:
            blk = xp * 2 + cc
            d3[blk, :, 128:256] = dk[blk].astype(BF)
            d3[blk, :, 256:] = dv[blk].astype(BF)
            part[blk] = mm(d3[blk], wp[...]).astype(BF)
        rs.send_pair(xp, slot)

    with scope('c_far'):
        back_in(ring.xf, 0)
        rs.far()
    with scope('c_own'):
        back_in(ring.xr, 1)
        back_in(ring.xl, 2)
        rs.near_own()
        back_in(ring.x, 3)
    reload.wait()

    def weight_in(i):
        cols = pl.ds(pl.multiple_of(i * 128, 128), 128)
        left = d3[:, :, cols].reshape(n * t, 128)
        grad = mm(left, hg[...].reshape(n * t, d), T0).astype(BF)
        for head in PAIR:
            gwt[head, i] = grad[head * 64:head * 64 + 64]

    def bias_in(b):
        gbq[...] = gbq[...] + fold8(d3[b].astype(F32), jnp.add)

    with scope('c_weights'):
        loop(0, len(TRIPLE), weight_in)
        loop(0, n, bias_in)
        for cp in (out_gwt, out_gbq):
            cp.start()
    with scope('c_sum'):
        rs.near_sum()
    with scope('c_gwo'):
        gwo[...] = mm(o[...].reshape(n * t, 128), xg[...].reshape(n * t, d), T0).astype(BF)
        out_gwo.start()
    with scope('c_mfinal'):
        rm.wait_final()

    def finish_y(rows):
        m = rm.total(rows).astype(BF).astype(F32)
        y[rows, :] = (x1[rows, :] + m + bd[...]).astype(BF)
    rows_loop(t, 64, finish_y)
    out_y.start()
    with scope('c_final'):
        rs.wait_final()

    def sum_in(rows):
        dh = rs.total(rows).astype(BF).astype(F32)
        hat, _ = norm_rows(xo[rows, :].astype(F32))
        small[0] = small[0] + fold8(dh * hat, jnp.add)
        small[1] = small[1] + fold8(dh, jnp.add)

    def last(rows):
        dh = rs.total(rows).astype(BF).astype(F32)
        hat, rstd = norm_rows(xo[rows, :].astype(F32))
        gx[rows, :] = (mid[rows, :] + norm_back(dh * g1[...], hat, rstd)).astype(BF)

    with scope('c_sums'):
        rows_loop(t, 64, sum_in)
    for i in range(6):
        every[me, i:i + 1, :] = col_sum(small[i])
    every[me, 6:, :] = jnp.zeros((2, d), F32)

    def share(off):
        return pltpu.make_async_remote_copy(
            src_ref=every.at[me], dst_ref=every.at[me], send_sem=ar_s.at[off], recv_sem=ar_r.at[me],
            device_id={'tp': (me + off) % n}, device_id_type=MESH)

    with scope('c_share'):
        for off in range(1, n):
            share(off).start()
        rows_loop(t, 64, last)
        out_gx.start()
        for off in range(1, n):
            src = (me + off) % n
            pltpu.make_async_remote_copy(
                src_ref=every.at[src], dst_ref=every.at[src], send_sem=ar_s.at[0], recv_sem=ar_r.at[src],
                device_id={'tp': me}, device_id_type=MESH).wait_recv()
        total = every[0]
        for b in range(1, n):
            total = total + every[b]
        sums[...] = total
        out_sums.start()
    for off in range(1, n):
        share(off).wait_send()
        send_o((me + off) % n).wait_send()
    with scope('d_finish'):
        for job in (rs, rm, aw, d0, d1):
            job.finish()
    with scope('d_outs'):
        for cp in outs:
            cp.wait()


def kernel_out(n_big, *refs):
    count = n_big + 3
    srcs, refs = refs[:count], refs[count:]
    outs, refs = refs[:n_big + 8], refs[n_big + 8:]
    bufs, tail, (sem_in, sem_out) = refs[:count], refs[count:-2], refs[-2:]
    gbq, gbu, sums = bufs[n_big:]
    o_bq, o_bu, o_sums = tail
    ins = [pltpu.make_async_copy(a, b, sem_in.at[i]) for i, (a, b) in enumerate(zip(srcs, bufs))]
    kept = list(bufs[:n_big]) + [o_bq, o_bu] + [o_sums.at[i:i + 1] for i in range(6)]
    backs = [pltpu.make_async_copy(b, a, sem_out.at[i]) for i, (a, b) in enumerate(zip(outs, kept))]
    for cp in ins[n_big:] + ins[:n_big]:
        cp.start()
    for cp in ins[n_big:]:
        cp.wait()
    o_bu[...] = col_sum(gbu[...])
    row = col_sum(gbq[...])
    e = o_bq.shape[2]
    for part_no in TRIPLE:
        for head in PAIR:
            at = (part_no * 2 + head) * e
            o_bq[part_no, head:head + 1, :] = row[:, at:at + e]
    o_sums[...] = sums[...]
    for back in backs[n_big:]:
        back.start()
    for cp, back in zip(ins[:n_big], backs):
        cp.wait()
        back.start()
    for back in backs:
        back.wait()


def anywhere():
    return pl.BlockSpec(memory_space=pl.ANY)


def smem():
    return pl.BlockSpec(memory_space=pltpu.SMEM)


def solution(mesh):
    n = mesh.shape['tp']

    def local_step(x, ln1_gamma, ln1_beta, w_qkv, b_qkv, w_out, b_out, ln2_gamma, ln2_beta, w_up, b_up, w_down, b_down, grad_y):
        t, d = x.shape[1], x.shape[2]
        heads, e = w_qkv.shape[1], w_qkv.shape[3]
        he = heads * e
        f = w_up.shape[1]
        scale = e ** -0.5
        slopes = jnp.asarray(alibi_slopes(heads * n))
        x2, dy2 = x[0], grad_y[0]
        row = lambda vec: vec.reshape(1, -1)
        wt = w_qkv.transpose(1, 2, 3, 0).reshape(heads * 3 * e, d)
        bq = b_qkv.transpose(1, 0, 2)
        sds = jax.ShapeDtypeStruct
        rows, full, half = (t, d), (n, t, d), (n, t, he)
        both, line = (len(PAIR),) + half, (len(PAIR), n, 1, t)
        packed = (len(TRIPLE) * he, d)
        params = lambda cid: pltpu.CompilerParams(collective_id=cid, has_side_effects=True, vmem_limit_bytes=VLIM)
        dma = pltpu.SemaphoreType.DMA

        vm = lambda dims, kind=BF: VMEM(dims, kind)
        stat, turned = (len(PAIR), 8, t), (n, he, t)
        vecs = (row(ln1_gamma), row(ln1_beta), bq, row(b_out), row(ln2_gamma), row(ln2_beta), row(b_up), row(b_down))
        results = [sds(rows, BF), sds(rows, BF), sds((8, d), F32), sds((heads, len(TRIPLE), e, d), BF),
                   sds((8, len(TRIPLE) * he), F32), sds((he, d), BF), sds((d, f), BF), sds((8, f), F32), sds((f, d), BF)]
        y, gx, sums, gwt, gbq, gwo, gwu, gbu, gwd, _ = pl.pallas_call(
            functools.partial(kernel_main, n, scale, len(vecs), len(results)),
            name='layer',
            out_shape=results + [sds(full, BF)],
            in_specs=[anywhere()] * (6 + len(vecs)) + [smem()],
            out_specs=[anywhere()] * (len(results) + 1),
            scratch_shapes=[vm(b.shape, b.dtype) for b in list(vecs) + results] + [vm(full), vm(rows), vm(rows), vm(full), vm(full), vm(packed), vm(packed), vm((n, he, d)),
                            vm((d, f)), vm((f, d)), vm(both), vm(half), vm(half), vm(turned), vm(turned), vm(half),
                            vm(line, F32), vm(rows), vm((len(PAIR), n, t, t), F32), vm(stat, F32), vm(stat, F32),
                            vm((he, t), F32), vm((len(PAIR), t, t), F32), vm(rows, F32), vm((n, t, f)), vm((n, t, f)),
                            vm(rows, F32), vm((len(PAIR), t, he)), vm((he, t), F32), vm(half, F32), vm(half, F32),
                            vm((n, t, len(TRIPLE) * he)), vm((6, 8, d), F32), vm((n, 8, d), F32), vm(full)]
            + scatter_buffers(n, t, d) * 2 + scatter_sems() * 4 + gather_scratch(n) * 7 + [dma((n,))] * 5 + [dma((len(vecs),)), dma((len(results),))],
            compiler_params=params(0),
        )(x2, dy2, wt, w_out, w_up, w_down, *vecs, slopes)

        big = (y, gx, gwt, gwo, gwu, gwd)
        little = (gbq, gbu, sums)
        bias_dims, up_dims = (len(TRIPLE), heads, e), (1, f)
        res = pl.pallas_call(
            functools.partial(kernel_out, len(big)),
            name='results',
            out_shape=[sds(b.shape, b.dtype) for b in big] + [sds(bias_dims, F32), sds(up_dims, F32)] + [sds((1, d), F32)] * 6,
            in_specs=[anywhere()] * (len(big) + 3),
            out_specs=[anywhere()] * (len(big) + 8),
            scratch_shapes=[VMEM(b.shape, b.dtype) for b in big + little]
            + [vm(bias_dims, F32), vm(up_dims, F32), vm((8, d), F32)] + [dma((len(big) + 8,))] * 2,
        )(*big, *little)
        y, gx, gwt, gwo, gwu, gwd, gbq, gbu, s_g1, s_b1, s_g2, s_b2, s_bo, s_bd = res
        vec = lambda a: a.reshape(-1)
        return (y[None], gx[None], vec(s_g1), vec(s_b1), gwt.transpose(3, 0, 1, 2), gbq.transpose(1, 0, 2), gwo, vec(s_bo),
                vec(s_g2), vec(s_b2), gwu, vec(gbu), gwd, vec(s_bd))

    row_spec = P('dp', 'tp', None)
    in_specs = (row_spec, P(), P(), P(None, 'tp', None, None), P('tp', None, None), P('tp', None), P(), P(), P(),
                P(None, 'tp'), P('tp'), P('tp', None), P(), row_spec)
    out_specs = (row_spec, row_spec, P('dp'), P('dp'), P('dp', 'tp', None, None), P(('dp', 'tp'), None, None),
                 P(('dp', 'tp'), None), P('dp'), P('dp'), P('dp'), P('dp', 'tp'), P(('dp', 'tp')), P(('dp', 'tp'), None), P('dp'))
    return jax.shard_map(local_step, mesh=mesh, in_specs=in_specs, out_specs=out_specs, check_vma=False)
```

```python
import functools
import math
import jax
import jax.numpy as jnp
import numpy as np
from jax import lax
from jax.experimental import pallas as pl
from jax.experimental.pallas import tpu as pltpu
from jax.sharding import PartitionSpec as P

EPS = 1e-5
MASK_VALUE = -1e30
BF, F32 = jnp.bfloat16, jnp.float32
VMEM = pltpu.VMEM
MESH = pl.DeviceIdType.MESH
scope = jax.named_scope
VLIM = 62 * 1024 * 1024
GELU_C = math.sqrt(2.0 / math.pi)
PAIR = LOW, HIGH = (0, 1)
TRIPLE = (0, 1, 2)
NN = (((1,), (0,)), ((), ()))
T0 = (((0,), (0,)), ((), ()))
NT = (((1,), (1,)), ((), ()))


def alibi_slopes(n_heads):
    closest = 2 ** int(math.floor(math.log2(n_heads)))
    base_ratio = 2.0 ** (-8.0 / closest)
    extra_ratio = 2.0 ** (-4.0 / closest)
    remaining = min(closest, n_heads - closest)
    slopes = [base_ratio ** (i + 1) for i in range(closest)]
    slopes = slopes + [extra_ratio ** (2 * i + 1) for i in range(remaining)]
    return np.array(slopes, dtype=np.float32)


def mm(a, b, dims=NN):
    return lax.dot_general(a, b, dims, preferred_element_type=F32)


def loop(lo, hi, body, unroll=1):
    def step(i, carry):
        body(i)
        return carry
    lax.fori_loop(lo, hi, step, 0, unroll=unroll)


def twos(count, body):
    loop(0, count // 2, lambda i: body((2 * i, 2 * i + 1)))

    @pl.when(count % 2 == 1)
    def _():
        body((count - 1,))


def rows_loop(total, rows, body, base=0):
    loop(0, total // rows, lambda r: body(pl.ds(pl.multiple_of(base + r * rows, rows), rows)))


def row_mean(z):
    return jnp.mean(z, axis=-1, keepdims=True)


def col_sum(z):
    return jnp.sum(z, axis=0, keepdims=True)


def norm_back(grad, hat, rstd):
    return rstd * (grad - row_mean(grad) - hat * row_mean(grad * hat))


def zero_fill(*refs):
    for ref in refs:
        ref[...] = jnp.zeros(ref.shape, ref.dtype)


def sort_weight(wp, wt):
    e = wp.shape[0] // 6
    for part_no in TRIPLE:
        for head in PAIR:
            dst = (part_no * 2 + head) * e
            src = (head * 3 + part_no) * e
            wp[dst:dst + e, :] = wt[src:src + e, :]


def norm_rows(z):
    cen = z - row_mean(z)
    rstd = lax.rsqrt(row_mean(cen * cen) + EPS)
    return cen * rstd, rstd


def fold8(v, op):
    out = v[0:8]
    for k in range(1, v.shape[0] // 8):
        out = op(out, v[8 * k:8 * k + 8])
    return out


class Ring:
    def __init__(self, n):
        self.n = n
        nx = n // 2
        self.me = lax.axis_index('tp')
        self.x = self.me // 2
        self.c = self.me % 2
        self.nx = nx
        self.xr = (self.x + 1) % nx
        self.xl = (self.x + nx - 1) % nx
        self.xf = (self.x + 2) % nx
        self.right = self.xr * 2 + self.c
        self.left = self.xl * 2 + self.c
        self.far = self.xf * 2 + self.c
        other = 1 - self.c
        self.partner = self.x * 2 + other
        self.others = [xp * 2 + other for xp in (self.x, self.xl, self.xr, self.xf)]

    def order(self, s):
        odd = s % 2
        dx = jnp.where(s < 2, 0, jnp.where(s >= 6, 2, jnp.where(odd == 0, self.nx - 1, 1)))
        mid = jnp.where(s < 4, 0, 1)
        dc = jnp.where(s < 2, odd, jnp.where(s >= 6, odd, mid))
        return ((self.x + dx) % self.nx) * 2 + (self.c + dc) % 2

    def barrier(self, everyone=False):
        sem = pltpu.get_barrier_semaphore()
        if everyone:
            peers = [(self.me + k) % self.n for k in range(1, self.n)]
        else:
            peers = [self.right, self.left, self.partner]
        for peer in peers:
            pl.semaphore_signal(sem, inc=1, device_id={'tp': peer}, device_id_type=MESH)
        pl.semaphore_wait(sem, len(peers))


class Gather:
    LEFT, RIGHT, FAR, SIDE = 0, 2, 4, 6
    SLOTS = 10

    def __init__(self, ring, buf, ssem, rsem, base=0, size=None, cut=None):
        self.ring, self.buf, self.ssem, self.rsem = ring, buf, ssem, rsem
        self.base = base
        self.size = size or buf.shape[1]
        self.cut = cut or self.size // 2
        self.drained = False

    def rows(self, half):
        if half == LOW:
            return pl.ds(self.base, self.cut)
        return pl.ds(self.base + self.cut, self.size - self.cut)

    def copy(self, ref, dev, slot, onward):
        return pltpu.make_async_remote_copy(
            src_ref=ref, dst_ref=ref, send_sem=self.ssem.at[onward], recv_sem=self.rsem.at[slot],
            device_id={'tp': dev}, device_id_type=MESH)

    def send(self, blk, half, dev, slot, onward=LOW):
        self.copy(self.buf.at[blk, self.rows(half)], dev, slot, onward).start()

    def wait(self, blk, half, slot):
        self.copy(self.buf.at[blk, self.rows(half)], self.ring.me, slot, LOW).wait_recv()

    def side(self, which):
        ref = self.buf.at[self.ring.others[which], pl.ds(self.base, self.size)]
        self.copy(ref, self.ring.me, self.SIDE + which, LOW).wait_recv()

    def start(self):
        r = self.ring
        for half in PAIR:
            self.send(r.me, half, r.right, self.LEFT + half)
            self.send(r.me, HIGH - half, r.left, self.RIGHT + HIGH - half)
        for half in PAIR:
            self.send(r.me, half, r.partner, self.SIDE)

    def near1(self):
        r = self.ring
        self.wait(r.left, LOW, self.LEFT)
        self.send(r.left, LOW, r.right, self.FAR, HIGH)
        self.send(r.left, LOW, r.partner, self.SIDE + 1)
        self.wait(r.right, HIGH, self.RIGHT + HIGH)
        self.send(r.right, HIGH, r.left, self.FAR + HIGH, HIGH)
        self.send(r.right, HIGH, r.partner, self.SIDE + 2)

    def near2(self):
        r = self.ring
        self.wait(r.left, HIGH, self.LEFT + HIGH)
        self.send(r.left, HIGH, r.partner, self.SIDE + 1)
        self.wait(r.right, LOW, self.RIGHT)
        self.send(r.right, LOW, r.partner, self.SIDE + 2)

    def far(self):
        r = self.ring
        for half in PAIR:
            self.wait(r.far, half, self.FAR + half)
            self.send(r.far, half, r.partner, self.SIDE + 3)

    def gone(self, blocks, onward):
        ref = self.buf.at[pl.ds(0, blocks), pl.ds(self.base, self.size)]
        self.copy(ref, self.ring.right, LOW, onward).wait_send()

    def drain(self):
        self.gone(1, HIGH)
        self.drained = True

    def finish(self):
        self.gone(6, LOW)
        if not self.drained:
            self.gone(1, HIGH)


class Scatter:
    def __init__(self, ring, part, pair, stage, land, ssem, rsem, base=0, size=None):
        self.ring, self.part, self.pair, self.stage, self.land = ring, part, pair, stage, land
        self.ssem, self.rsem = ssem, rsem
        self.base = base
        self.size = size or part.shape[1]
        self.half = self.size // 2

    def cp_pair(self, xp):
        r = self.ring
        rows = pl.ds(self.base, self.size)
        return pltpu.make_async_remote_copy(
            src_ref=self.part.at[xp * 2 + (1 - r.c), rows], dst_ref=self.pair.at[xp, rows], send_sem=self.ssem.at[LOW],
            recv_sem=self.rsem.at[xp], device_id={'tp': r.partner}, device_id_type=MESH)

    def cp(self, slot, half, dst_slot, dev):
        rows = pl.ds(self.base + half * self.half, self.half)
        return pltpu.make_async_remote_copy(
            src_ref=self.stage.at[slot, rows], dst_ref=self.land.at[dst_slot, rows],
            send_sem=self.ssem.at[HIGH], recv_sem=self.rsem.at[4 + 2 * dst_slot + half],
            device_id={'tp': dev}, device_id_type=MESH)

    def wait_land(self, dst_slot, half):
        self.cp(0, half, dst_slot, self.ring.me).wait_recv()

    def wait_pair(self, xp):
        self.cp_pair(xp).wait_recv()

    def send_pair(self, xp):
        self.cp_pair(xp).start()

    def mix(self, slot, xp, half, with_far=False):
        blk = xp * 2 + self.ring.c
        step = 32

        def body(i):
            rows = pl.ds(pl.multiple_of(self.base + half * self.half + i * step, step), step)
            total = self.part[blk, rows, :].astype(F32) + self.pair[xp, rows, :].astype(F32)
            if with_far:
                total = total + self.land[0, rows, :].astype(F32)
            self.stage[slot, rows, :] = total.astype(BF)
        loop(0, self.half // step, body)

    def far(self):
        r = self.ring
        self.wait_pair(r.xf)
        self.mix(0, r.xf, 0)
        self.cp(0, 0, 0, r.right).start()
        self.mix(0, r.xf, 1)
        self.cp(0, 1, 0, r.left).start()

    def near_own(self):
        r = self.ring
        self.wait_pair(r.xr)
        self.mix(1, r.xr, 1)
        self.cp(1, 1, 1, r.right).start()
        self.wait_pair(r.xl)
        self.mix(2, r.xl, 0)
        self.cp(2, 0, 2, r.left).start()

    def near_sum(self):
        r = self.ring
        self.wait_land(0, 0)
        self.mix(1, r.xr, 0, with_far=True)
        self.cp(1, 0, 1, r.right).start()
        self.wait_land(0, 1)
        self.mix(2, r.xl, 1, with_far=True)
        self.cp(2, 1, 2, r.left).start()

    def wait_final(self):
        self.wait_pair(self.ring.x)
        for slot in (1, 2):
            for half in PAIR:
                self.wait_land(slot, half)

    def total(self, rows):
        r = self.ring
        return (self.part[r.me, rows, :].astype(F32) + self.pair[r.x, rows, :].astype(F32)
                + self.land[1, rows, :].astype(F32) + self.land[2, rows, :].astype(F32))

    def finish(self):
        r = self.ring
        rows = pl.ds(self.base, self.size)
        for ref, which in ((self.pair.at[:, rows], LOW), (self.stage.at[:, rows], HIGH)):
            pltpu.make_async_remote_copy(
                src_ref=ref, dst_ref=ref, send_sem=self.ssem.at[which], recv_sem=self.rsem.at[0],
                device_id={'tp': r.partner}, device_id_type=MESH).wait_send()


def scatter_buffers(n, rows, d):
    return [VMEM((n // 2, rows, d), BF), VMEM((3, rows, d), BF), VMEM((3, rows, d), BF)]


def scatter_sems():
    return [pltpu.SemaphoreType.DMA((2,)), pltpu.SemaphoreType.DMA((4 + 6,))]


def hooked(count, body, hooks):
    def step(i):
        for at, actions in hooks.items():
            @pl.when(i == at)
            def _():
                for act in actions:
                    act()
        body(i)
    loop(0, count, step)


def gather_sems():
    return [pltpu.SemaphoreType.DMA((2,)), pltpu.SemaphoreType.DMA((Gather.SLOTS,))]


def lane_mask(rows, h):
    lane = lax.broadcasted_iota(jnp.int32, (rows, 128), 1)
    return (lane < 64) if h == 0 else (lane >= 64)


def attend_block(i, q_ref, k_ref, vt_ref, o_ref, lse_ref, s_ref, m_ref, l_ref, acc_ref, bt_ref, slopes):
    t = q_ref.shape[2]
    e = acc_ref.shape[0] // 2
    key = lax.broadcasted_iota(jnp.int32, (t, t), 0)
    qry = lax.broadcasted_iota(jnp.int32, (t, t), 1)
    for h in PAIR:
        m_ref[h] = jnp.full((8, t), MASK_VALUE, F32)
        l_ref[h] = jnp.zeros((8, t), F32)
    zero_fill(acc_ref)

    def shift(h, j):
        return slopes[h] * (j * t).astype(F32)

    def score(blocks, diag):
        top = [m_ref[h] for h in PAIR]
        for j in blocks:
            for h in PAIR:
                s = mm(k_ref[j], q_ref[h, i], NT) + bt_ref[h]
                if diag:
                    s = jnp.where(key <= qry, s, MASK_VALUE)
                s_ref[h, j] = s
                top[h] = jnp.maximum(top[h], fold8(s, jnp.maximum) + shift(h, j))
        for h in PAIR:
            m_ref[h] = top[h]

    twos(i, lambda blocks: score(blocks, False))
    score((i,), True)
    top = [jnp.max(m_ref[h], axis=0, keepdims=True) for h in PAIR]

    def denom(j):
        for h in PAIR:
            l_ref[h] = l_ref[h] + fold8(jnp.exp(s_ref[h, j] + (shift(h, j) - top[h])), jnp.add)

    loop(0, i + 1, denom)
    for h in PAIR:
        lse_ref[h, i] = top[h] + jnp.log(col_sum(l_ref[h]))

    def values(blocks):
        for h in PAIR:
            rows = pl.ds(h * e, e)
            total = acc_ref[rows, :]
            for j in blocks:
                p = jnp.exp(s_ref[h, j] + (shift(h, j) - lse_ref[h, i])).astype(BF)
                total = total + mm(vt_ref[j, rows, :], p)
            acc_ref[rows, :] = total

    twos(i + 1, values)
    o_ref[i] = acc_ref[...].T.astype(BF)


def kernel_main(n, scale, n_vec, n_out, x_hbm, dy_hbm, wt_hbm, wo_hbm, wu_hbm, wd_hbm, *refs):
    vec_hbm, (slopes_ref,), refs = refs[:n_vec], refs[n_vec:n_vec + 1], refs[n_vec + 1:]
    out_hbm, (h_hbm,), refs = refs[:n_out], refs[n_out:n_out + 1], refs[n_out + 1:]
    vecs, results, refs = refs[:n_vec], refs[n_vec:n_vec + n_out], refs[n_vec + n_out:]
    run_layer(n, scale, vec_hbm, vecs, out_hbm, results, x_hbm, dy_hbm, wt_hbm, wo_hbm, wu_hbm, wd_hbm, slopes_ref, h_hbm, *refs)


def run_layer(n, scale, vec_hbm, vecs, out_hbm, results, x_hbm, dy_hbm, wt_hbm, wo_hbm, wu_hbm, wd_hbm, slopes_ref, h_hbm,
                xg, xo, dyo, dy, hg, wt, wp, wof, wu, wd, q, k, v, kt, vt, o, lse, orow, s_ref, m_ref, l_ref, acc, bt,
                x1, act, dpre, mid, dom, dqt, dk, dv, d3, small, early, late, part,
                *rest):
    g1, b1, bqkv, bo, g2, b2, bu, bd = vecs
    y, gx, sums, gwt, gbq, gwo, gwu, gbu, gwd = results
    rest = list(rest)

    def take(count):
        head = rest[:count]
        del rest[:count]
        return head

    ring = Ring(n)
    me = ring.me
    t, d, f = xg.shape[1], xg.shape[2], wu.shape[1]
    rs_bufs, rm_bufs = take(3), take(3)
    st = t // 2
    streams = (0, st)
    r_sems = [take(2) for _ in PAIR]
    r0, r1 = [Scatter(ring, part, *rs_bufs, *sems, base=base, size=st) for base, sems in zip(streams, r_sems)]
    rs = Scatter(ring, part, *rs_bufs, *r_sems[0])
    rm = Scatter(ring, dy, *rm_bufs, *take(2))
    g_sems = [take(2) for _ in PAIR]
    ax, aw = [Gather(ring, buf, *sems) for buf, sems in zip((xg, wof), g_sems)]
    ay = Gather(ring, dy, *take(2))
    g0, g1s = [Gather(ring, hg, *sems, base=base, size=st) for base, sems in zip(streams, g_sems)]
    d0, d1 = [Gather(ring, xg, *sems, base=base, size=st) for base, sems in zip(streams, g_sems)]
    few, local, vec_sem, out_sem = take(4)
    o_send, o_recv, e_send, e_recv, l_send, l_recv = [few.at[i] for i in range(6)]
    outs = [pltpu.make_async_copy(b, a, out_sem.at[i]) for i, (a, b) in enumerate(zip(out_hbm, results))]
    out_y, out_gx, out_sums, out_gwt, out_gbq, out_gwo, out_gwu, out_gbu, out_gwd = outs

    def fetch(i, src, dst):
        cp = pltpu.make_async_copy(src, dst, local.at[i])
        cp.start()
        return cp

    in_x, in_wo, in_dy, in_wt = (fetch(0, x_hbm, xg.at[me]), fetch(1, wo_hbm, wof.at[me]),
                                 fetch(2, dy_hbm, dy.at[me]), fetch(3, wt_hbm, wt))
    later = [fetch(4, wu_hbm, wu), fetch(5, wd_hbm, wd), fetch(6, x_hbm, xo), fetch(7, dy_hbm, dyo)]
    vec_in = [pltpu.make_async_copy(a, b, vec_sem.at[i]) for i, (a, b) in enumerate(zip(vec_hbm, vecs))]
    for cp in vec_in:
        cp.start()
    ring.barrier(everyone=True)
    in_x.wait()
    ax.start()
    for cp in vec_in:
        cp.wait()
    in_wt.wait()
    sort_weight(wp, wt)
    in_wo.wait()
    in_dy.wait()
    bias = jnp.concatenate([bqkv[kind, head:head + 1, :] for kind in TRIPLE for head in PAIR], axis=1)

    def project(blk):
        def norm(rows):
            hat, _ = norm_rows(xg[blk, rows, :].astype(F32))
            hg[blk, rows, :] = (hat * g1[...] + b1[...]).astype(BF)
        rows_loop(t, 64, norm)
        out = mm(hg[blk], wp[...], NT) + bias
        out = out.astype(BF)
        zero = jnp.zeros((t, 128), BF)
        qs = (out[:, :128].astype(F32) * scale).astype(BF)
        for head in PAIR:
            q[head, blk] = jnp.where(lane_mask(t, head), qs, zero)
        k[blk] = out[:, 128:256]
        v[blk] = out[:, 256:]
        kt[blk] = out[:, 128:256].T
        vt[blk] = out[:, 256:].T
        fetch(0, hg.at[blk], h_hbm.at[blk])

    arrive = functools.partial
    with scope('a_gather'):
        hooked(n, lambda step: project(ring.order(step)), {
            1: [arrive(ax.side, 0)],
            2: [ax.near1, ax.near2],
            4: [arrive(ax.side, 1)],
            5: [arrive(ax.side, 2)],
            6: [ax.drain, aw.start, ax.far, ay.start],
            7: [arrive(ax.side, 3)]})
    slopes = [slopes_ref[me * 2 + head] for head in PAIR]
    key = lax.broadcasted_iota(jnp.int32, (t, t), 0)
    qry = lax.broadcasted_iota(jnp.int32, (t, t), 1)
    for head in PAIR:
        bt[head] = slopes[head] * key.astype(F32)

    def send_o(i):
        cols = pl.ds(pl.multiple_of(me * 128, 128), 128)
        return pltpu.make_async_remote_copy(
            src_ref=o.at[i], dst_ref=orow.at[:, cols], send_sem=o_send, recv_sem=o_recv,
            device_id={'tp': i}, device_id_type=MESH)

    def one_block(step):
        i = ring.order(n - 1 - step)
        attend_block(i, q, k, vt, o, lse, s_ref, m_ref, l_ref, acc, bt, slopes)

        @pl.when(step < n - 1)
        def _():
            send_o(i).start()

    with scope('a_attend'):
        ax.finish()
        pltpu.make_async_copy(hg, h_hbm, local.at[0]).wait()
        hooked(n, one_block, {4: [aw.near1], 5: [aw.near2]})
    most = pl.ds(0, n - 1)
    with scope('a_wait'):
        aw.far()
        ay.near1()
        orow[:, pl.ds(pl.multiple_of(me * 128, 128), 128)] = o[me]
        wide = orow.at[:, pl.ds(0, (n - 1) * 128)]
        pltpu.make_async_remote_copy(
            src_ref=wide, dst_ref=wide, send_sem=o_send, recv_sem=o_recv,
            device_id={'tp': me}, device_id_type=MESH).wait_recv()
        for which in range(4):
            aw.side(which)
        aw.finish()
        later[2].wait()
    with scope('a_out'):
        x1[...] = mm(orow[...], wof[...].reshape(n * 128, d)).astype(BF).astype(F32)

        def enter(rows):
            row = xo[rows, :].astype(F32) + x1[rows, :] + bo[...]
            x1[rows, :] = row
            hat, _ = norm_rows(row)
            hg[me, rows, :] = (hat * g2[...] + b2[...]).astype(BF)
        rows_loop(st, 64, enter)
        g0.start()
        rows_loop(st, 64, enter, base=st)
    for cp in (later[0], later[1], later[3]):
        cp.wait()
    zero_fill(gbu)
    ay.side(0)

    def rest():
        ay.near2()
        ay.far()
        for which in range(1, 4):
            ay.side(which)

    def mlp(blk, stream):
        rows = pl.ds(pl.multiple_of(stream * st, st), st)
        pre = mm(hg[blk, rows, :], wu[...]) + bu[...]
        cot = mm(dy[blk, rows, :], wd[...], NT).astype(BF).astype(F32)
        sq = pre * pre
        th = jnp.tanh(GELU_C * (pre + 0.044715 * sq * pre))
        cdf = 0.5 * (1.0 + th)
        act[blk, rows, :] = (pre * cdf).astype(BF)
        slope = cdf + pre * (0.5 * (1.0 - th * th)) * (GELU_C * (1.0 + 3 * 0.044715 * sq))
        dp = cot * slope
        gbu[...] = gbu[...] + fold8(dp, jnp.add)
        dpb = dp.astype(BF)
        dpre[blk, rows, :] = dpb
        part[blk, rows, :] = mm(dpb, wu[...], NT).astype(BF)

    chips = (ring.xf, ring.xr, ring.xl, ring.x)
    def pairs(job):
        for xp in chips:
            job.send_pair(xp)

    def item(step):
        late = (step == 4) | (step == 5) | (step >= 10)
        pos = jnp.where(step < 4, step, jnp.where(step < 6, step - 4, jnp.where(step < 10, step - 2, step - 8)))
        mlp(ring.order(pos), jnp.where(late, 1, 0))

    with scope('b_gather'):
        hooked(2 * n, item, {
            1: [arrive(g0.side, 0)],
            2: [rest, g0.near1, g1s.start, g0.near2],
            5: [arrive(g1s.side, 0)],
            6: [arrive(g0.side, 1)],
            7: [arrive(g0.side, 2)],
            8: [g0.far],
            9: [arrive(g0.side, 3)],
            10: [arrive(pairs, r0), g1s.near1, r0.far, g1s.near2],
            12: [r0.near_own, arrive(g1s.side, 1)],
            13: [arrive(g1s.side, 2)],
            14: [g1s.far],
            15: [arrive(g1s.side, 3)]})
    with scope('b_far'):
        pairs(r1)
        r0.near_sum()
        r1.far()
    with scope('b_own'):
        r1.near_own()
    ay.finish()

    def weight_down(i):
        cols = pl.ds(pl.multiple_of(i * 256, 256), 256)
        left = act[:, :, cols].reshape(n * t, 256)
        gwd[cols, :] = mm(left, dy[...].reshape(n * t, d), T0).astype(BF)

    def weight_up(i):
        cols = pl.ds(pl.multiple_of(i * 256, 256), 256)
        left = hg[:, :, cols].reshape(n * t, 256)
        gwu[cols, :] = mm(left, dpre[...].reshape(n * t, f), T0).astype(BF)

    with scope('b_weights'):
        loop(0, f // 256, weight_down)
        loop(0, d // 256, weight_up)
        for cp in (out_gwd, out_gwu, out_gbu):
            cp.start()
    zero_fill(small)

    def down(blk):
        dy[blk] = mm(act[blk], wd[...]).astype(BF)

    def leave(rows):
        dg = rs.total(rows).astype(BF).astype(F32)
        hat, rstd = norm_rows(x1[rows, :])
        small[2] = small[2] + fold8(dg * hat, jnp.add)
        small[3] = small[3] + fold8(dg, jnp.add)
        dz = norm_back(dg * g2[...], hat, rstd)
        dyf = dyo[rows, :].astype(F32)
        dm = dyf + dz
        small[4] = small[4] + fold8(dm, jnp.add)
        small[5] = small[5] + fold8(dyf, jnp.add)
        mid[rows, :] = dm
        xg[me, rows, :] = dm.astype(BF)

    with scope('b_sum'):
        r1.near_sum()
    with scope('b_final'):
        r0.wait_final()
    with scope('b_leave'):
        rows_loop(st, 64, leave)
        g0.finish()
        d0.start()
    with scope('b_down'):
        loop(0, n, down)
        pairs(rm)
    with scope('b_final1'):
        r1.wait_final()
    with scope('b_leave1'):
        rows_loop(st, 64, leave, base=st)
        g1s.finish()
        d1.start()
    with scope('b_finish'):
        for job in (r0, r1):
            job.finish()
    reload = fetch(0, h_hbm, hg)

    def share(buf, off, send_sem, recv_sem):
        return pltpu.make_async_remote_copy(
            src_ref=buf.at[me], dst_ref=buf.at[me], send_sem=send_sem, recv_sem=recv_sem,
            device_id={'tp': (me + off) % n}, device_id_type=MESH)

    def all_in(buf, send_sem, recv_sem):
        return pltpu.make_async_remote_copy(
            src_ref=buf.at[most], dst_ref=buf.at[most], send_sem=send_sem, recv_sem=recv_sem,
            device_id={'tp': me}, device_id_type=MESH)

    def early_out():
        for i in range(4):
            early[me, i:i + 1, :] = col_sum(small[2 + i])
        for off in range(1, n):
            share(early, off, e_send, e_recv).start()

    def add_up(buf):
        total = buf[0]
        for b in range(1, n):
            total = total + buf[b]
        return total
    zero_fill(dk, dv)

    def back_block(i):
        dc = mm(xg[i], wof[me], NT).astype(BF)
        zero = jnp.zeros((t, 128), BF)
        prod = (dc.astype(F32) * o[i].astype(F32)).T
        dlt = (col_sum(prod[:64]), col_sum(prod[64:]))
        for head in PAIR:
            dom[head] = jnp.where(lane_mask(t, head), dc, zero)
        zero_fill(dqt)

        def pair_block(blocks, diag):
            cases = [(j, head) for j in blocks for head in PAIR]
            ps, dss = [], []
            for j, head in cases:
                s = mm(k[j], q[head, i], NT) + bt[head]
                if diag:
                    s = jnp.where(key <= qry, s, MASK_VALUE)
                p = jnp.exp(s + (slopes[head] * (j * t).astype(F32) - lse[head, i]))
                dp = mm(v[j], dom[head], NT).astype(BF).astype(F32)
                dss.append((p * (dp - dlt[head])).astype(BF))
                ps.append(p.astype(BF))
            wide = list(zip(cases, ps, dss))
            for j in blocks:
                dv[j] = dv[j] + sum(mm(p, dom[head]) for (b, head), p, _ in wide if b is j)
                dk[j] = dk[j] + sum(mm(ds, q[head, i]) for (b, head), _, ds in wide if b is j)
            for head in PAIR:
                rows = pl.ds(head * 64, 64)
                dqt[rows, :] = dqt[rows, :] + sum(mm(kt[b, rows, :], ds) for (b, h), _, ds in wide if h == head)

        twos(i, lambda blocks: pair_block(blocks, False))
        pair_block((i,), True)
        d3[i, :, :128] = (dqt[...].T * scale).astype(BF)

    def both_in(which):
        for job in (d0, d1):
            job.side(which)

    with scope('c_attend'):
        hooked(n, lambda step: back_block(ring.order(step)), {
            1: [arrive(both_in, 0), d0.near1, d0.near2],
            2: [d1.near1, rm.far, rm.near_own, d1.near2],
            4: [arrive(both_in, 1)],
            5: [arrive(both_in, 2)],
            6: [d0.far, d1.far, rm.near_sum, early_out],
            7: [arrive(both_in, 3)]})
    zero_fill(gbq)

    def back_in(xp):
        for cc in PAIR:
            blk = xp * 2 + cc
            d3[blk, :, 128:256] = dk[blk].astype(BF)
            d3[blk, :, 256:] = dv[blk].astype(BF)
            part[blk] = mm(d3[blk], wp[...]).astype(BF)
        rs.send_pair(xp)

    with scope('c_far'):
        back_in(ring.xf)
        rs.far()
    with scope('c_own'):
        back_in(ring.xr)
        back_in(ring.xl)
        rs.near_own()
        back_in(ring.x)
    reload.wait()

    def weight_in(i):
        cols = pl.ds(pl.multiple_of(i * 128, 128), 128)
        left = d3[:, :, cols].reshape(n * t, 128)
        grad = mm(left, hg[...].reshape(n * t, d), T0).astype(BF)
        for head in PAIR:
            gwt[head, i] = grad[head * 64:head * 64 + 64]

    def bias_in(b):
        gbq[...] = gbq[...] + fold8(d3[b].astype(F32), jnp.add)

    with scope('c_weights'):
        loop(0, len(TRIPLE), weight_in)
        loop(0, n, bias_in)
        for cp in (out_gwt, out_gbq):
            cp.start()
    with scope('c_sum'):
        rs.near_sum()
    with scope('c_gwo'):
        gwo[...] = mm(o[...].reshape(n * t, 128), xg[...].reshape(n * t, d), T0).astype(BF)
        out_gwo.start()
    with scope('c_mfinal'):
        rm.wait_final()

    def finish_y(rows):
        m = rm.total(rows).astype(BF).astype(F32)
        y[rows, :] = (x1[rows, :] + m + bd[...]).astype(BF)
    rows_loop(t, 64, finish_y)
    out_y.start()
    with scope('c_final'):
        rs.wait_final()

    def sum_in(rows):
        dh = rs.total(rows).astype(BF).astype(F32)
        hat, _ = norm_rows(xo[rows, :].astype(F32))
        small[0] = small[0] + fold8(dh * hat, jnp.add)
        small[1] = small[1] + fold8(dh, jnp.add)

    def last(rows):
        dh = rs.total(rows).astype(BF).astype(F32)
        hat, rstd = norm_rows(xo[rows, :].astype(F32))
        gx[rows, :] = (mid[rows, :] + norm_back(dh * g1[...], hat, rstd)).astype(BF)

    with scope('c_sums'):
        rows_loop(t, 64, sum_in)
    for i in PAIR:
        late[me, i:i + 1, :] = col_sum(small[i])
    with scope('c_share'):
        for off in range(1, n):
            share(late, off, l_send, l_recv).start()
        rows_loop(t, 64, last)
        out_gx.start()
        all_in(early, e_send, e_recv).wait_recv()
        sums[2:6, :] = add_up(early)
        all_in(late, l_send, l_recv).wait_recv()
        sums[0:2, :] = add_up(late)
        out_sums.start()
        all_in(early, e_send, e_recv).wait_send()
        all_in(late, l_send, l_recv).wait_send()
        all_in(o, o_send, o_recv).wait_send()
    with scope('d_finish'):
        for job in (rs, rm, d0, d1):
            job.finish()
    with scope('d_outs'):
        for cp in outs:
            cp.wait()


def kernel_out(n_big, *refs):
    count = n_big + 3
    srcs, refs = refs[:count], refs[count:]
    outs, refs = refs[:n_big + 8], refs[n_big + 8:]
    bufs, tail, (sem_in, sem_out) = refs[:count], refs[count:-2], refs[-2:]
    gbq, gbu, sums = bufs[n_big:]
    o_bq, o_bu, o_sums = tail
    ins = [pltpu.make_async_copy(a, b, sem_in.at[i]) for i, (a, b) in enumerate(zip(srcs, bufs))]
    kept = list(bufs[:n_big]) + [o_bq, o_bu] + [o_sums.at[i:i + 1] for i in range(6)]
    backs = [pltpu.make_async_copy(b, a, sem_out.at[i]) for i, (a, b) in enumerate(zip(outs, kept))]
    for cp in ins[n_big:] + ins[:n_big]:
        cp.start()
    for cp in ins[n_big:]:
        cp.wait()
    o_bu[...] = col_sum(gbu[...])
    row = col_sum(gbq[...])
    e = o_bq.shape[2]
    for part_no in TRIPLE:
        for head in PAIR:
            at = (part_no * 2 + head) * e
            o_bq[part_no, head:head + 1, :] = row[:, at:at + e]
    o_sums[...] = sums[...]
    for back in backs[n_big:]:
        back.start()
    for cp, back in zip(ins[:n_big], backs):
        cp.wait()
        back.start()
    for back in backs:
        back.wait()


def anywhere():
    return pl.BlockSpec(memory_space=pl.ANY)


def smem():
    return pl.BlockSpec(memory_space=pltpu.SMEM)


def solution(mesh):
    n = mesh.shape['tp']

    def local_step(x, ln1_gamma, ln1_beta, w_qkv, b_qkv, w_out, b_out, ln2_gamma, ln2_beta, w_up, b_up, w_down, b_down, grad_y):
        t, d = x.shape[1], x.shape[2]
        heads, e = w_qkv.shape[1], w_qkv.shape[3]
        he = heads * e
        f = w_up.shape[1]
        scale = e ** -0.5
        slopes = jnp.asarray(alibi_slopes(heads * n))
        x2, dy2 = x[0], grad_y[0]
        row = lambda vec: vec.reshape(1, -1)
        wt = w_qkv.transpose(1, 2, 3, 0).reshape(heads * 3 * e, d)
        bq = b_qkv.transpose(1, 0, 2)
        sds = jax.ShapeDtypeStruct
        rows, full, half = (t, d), (n, t, d), (n, t, he)
        both, line = (len(PAIR),) + half, (len(PAIR), n, 1, t)
        packed = (len(TRIPLE) * he, d)
        params = lambda cid: pltpu.CompilerParams(collective_id=cid, has_side_effects=True, vmem_limit_bytes=VLIM)
        dma = pltpu.SemaphoreType.DMA

        vm = lambda dims, kind=BF: VMEM(dims, kind)
        stat, turned = (len(PAIR), 8, t), (n, he, t)
        vecs = (row(ln1_gamma), row(ln1_beta), bq, row(b_out), row(ln2_gamma), row(ln2_beta), row(b_up), row(b_down))
        results = [sds(rows, BF), sds(rows, BF), sds((8, d), F32), sds((heads, len(TRIPLE), e, d), BF),
                   sds((8, len(TRIPLE) * he), F32), sds((he, d), BF), sds((d, f), BF), sds((8, f), F32), sds((f, d), BF)]
        y, gx, sums, gwt, gbq, gwo, gwu, gbu, gwd, _ = pl.pallas_call(
            functools.partial(kernel_main, n, scale, len(vecs), len(results)),
            name='layer',
            out_shape=results + [sds(full, BF)],
            in_specs=[anywhere()] * (6 + len(vecs)) + [smem()],
            out_specs=[anywhere()] * (len(results) + 1),
            scratch_shapes=[vm(b.shape, b.dtype) for b in list(vecs) + results] + [vm(full), vm(rows), vm(rows), vm(full), vm(full), vm(packed), vm(packed), vm((n, he, d)),
                            vm((d, f)), vm((f, d)), vm(both), vm(half), vm(half), vm(turned), vm(turned), vm(half),
                            vm(line, F32), vm(rows), vm((len(PAIR), n, t, t), F32), vm(stat, F32), vm(stat, F32),
                            vm((he, t), F32), vm((len(PAIR), t, t), F32), vm(rows, F32), vm((n, t, f)), vm((n, t, f)),
                            vm(rows, F32), vm((len(PAIR), t, he)), vm((he, t), F32), vm(half, F32), vm(half, F32),
                            vm((n, t, len(TRIPLE) * he)), vm((6, 8, d), F32), vm((n, 4, d), F32), vm((n, 2, d), F32), vm(full)]
            + scatter_buffers(n, t, d) * 2 + scatter_sems() * 3 + gather_sems() * 3 + [dma((n,))] * 2 + [dma((len(vecs),)), dma((len(results),))],
            compiler_params=params(0),
        )(x2, dy2, wt, w_out, w_up, w_down, *vecs, slopes)

        big = (y, gx, gwt, gwo, gwu, gwd)
        little = (gbq, gbu, sums)
        bias_dims, up_dims = (len(TRIPLE), heads, e), (1, f)
        res = pl.pallas_call(
            functools.partial(kernel_out, len(big)),
            name='results',
            out_shape=[sds(b.shape, b.dtype) for b in big] + [sds(bias_dims, F32), sds(up_dims, F32)] + [sds((1, d), F32)] * 6,
            in_specs=[anywhere()] * (len(big) + 3),
            out_specs=[anywhere()] * (len(big) + 8),
            scratch_shapes=[VMEM(b.shape, b.dtype) for b in big + little]
            + [vm(bias_dims, F32), vm(up_dims, F32), vm((8, d), F32)] + [dma((len(big) + 8,))] * 2,
        )(*big, *little)
        y, gx, gwt, gwo, gwu, gwd, gbq, gbu, s_g1, s_b1, s_g2, s_b2, s_bo, s_bd = res
        vec = lambda a: a.reshape(-1)
        return (y[None], gx[None], vec(s_g1), vec(s_b1), gwt.transpose(3, 0, 1, 2), gbq.transpose(1, 0, 2), gwo, vec(s_bo),
                vec(s_g2), vec(s_b2), gwu, vec(gbu), gwd, vec(s_bd))

    row_spec = P('dp', 'tp', None)
    in_specs = (row_spec, P(), P(), P(None, 'tp', None, None), P('tp', None, None), P('tp', None), P(), P(), P(),
                P(None, 'tp'), P('tp'), P('tp', None), P(), row_spec)
    out_specs = (row_spec, row_spec, P('dp'), P('dp'), P('dp', 'tp', None, None), P(('dp', 'tp'), None, None),
                 P(('dp', 'tp'), None), P('dp'), P('dp'), P('dp'), P('dp', 'tp'), P(('dp', 'tp')), P(('dp', 'tp'), None), P('dp'))
    return jax.shard_map(local_step, mesh=mesh, in_specs=in_specs, out_specs=out_specs, check_vma=False)
```

```python
import functools
import math
import jax
import jax.numpy as jnp
import numpy as np
from jax import lax
from jax.experimental import pallas as pl
from jax.experimental.pallas import tpu as pltpu
from jax.sharding import PartitionSpec as P

EPS = 1e-5
MASK_VALUE = -1e30
BF, F32 = jnp.bfloat16, jnp.float32
VMEM = pltpu.VMEM
MESH = pl.DeviceIdType.MESH
scope = jax.named_scope
VLIM = 58 * 1024 * 1024
GELU_C = math.sqrt(2.0 / math.pi)
PAIR = LOW, HIGH = (0, 1)
TRIPLE = (0, 1, 2)
NN = (((1,), (0,)), ((), ()))
T0 = (((0,), (0,)), ((), ()))
NT = (((1,), (1,)), ((), ()))


def alibi_slopes(n_heads):
    closest = 2 ** int(math.floor(math.log2(n_heads)))
    base_ratio = 2.0 ** (-8.0 / closest)
    extra_ratio = 2.0 ** (-4.0 / closest)
    remaining = min(closest, n_heads - closest)
    slopes = [base_ratio ** (i + 1) for i in range(closest)]
    slopes = slopes + [extra_ratio ** (2 * i + 1) for i in range(remaining)]
    return np.array(slopes, dtype=np.float32)


def mm(a, b, dims=NN):
    return lax.dot_general(a, b, dims, preferred_element_type=F32)


def loop(lo, hi, body, unroll=1):
    def step(i, carry):
        body(i)
        return carry
    lax.fori_loop(lo, hi, step, 0, unroll=unroll)


def twos(count, body):
    loop(0, count // 2, lambda i: body((2 * i, 2 * i + 1)))

    @pl.when(count % 2 == 1)
    def _():
        body((count - 1,))


def rows_loop(total, rows, body, base=0):
    loop(0, total // rows, lambda r: body(pl.ds(pl.multiple_of(base + r * rows, rows), rows)))


def row_mean(z):
    return jnp.mean(z, axis=-1, keepdims=True)


def col_sum(z):
    return jnp.sum(z, axis=0, keepdims=True)


def norm_back(grad, hat, rstd):
    return rstd * (grad - row_mean(grad) - hat * row_mean(grad * hat))


def zero_fill(*refs):
    for ref in refs:
        ref[...] = jnp.zeros(ref.shape, ref.dtype)


def sort_weight(wp, wt):
    e = wp.shape[0] // 6
    for part_no in TRIPLE:
        for head in PAIR:
            dst = (part_no * 2 + head) * e
            src = (head * 3 + part_no) * e
            wp[dst:dst + e, :] = wt[src:src + e, :]


def norm_rows(z):
    cen = z - row_mean(z)
    rstd = lax.rsqrt(row_mean(cen * cen) + EPS)
    return cen * rstd, rstd


def fold8(v, op):
    out = v[0:8]
    for k in range(1, v.shape[0] // 8):
        out = op(out, v[8 * k:8 * k + 8])
    return out


class Ring:
    def __init__(self, n):
        self.n = n
        nx = n // 2
        self.me = lax.axis_index('tp')
        self.x = self.me // 2
        self.c = self.me % 2
        self.nx = nx
        self.xr = (self.x + 1) % nx
        self.xl = (self.x + nx - 1) % nx
        self.xf = (self.x + 2) % nx
        self.right = self.xr * 2 + self.c
        self.left = self.xl * 2 + self.c
        self.far = self.xf * 2 + self.c
        other = 1 - self.c
        self.partner = self.x * 2 + other
        self.others = [xp * 2 + other for xp in (self.x, self.xl, self.xr, self.xf)]

    def order(self, s):
        odd = s % 2
        dx = jnp.where(s < 2, 0, jnp.where(s >= 6, 2, jnp.where(odd == 0, self.nx - 1, 1)))
        mid = jnp.where(s < 4, 0, 1)
        dc = jnp.where(s < 2, odd, jnp.where(s >= 6, odd, mid))
        return ((self.x + dx) % self.nx) * 2 + (self.c + dc) % 2

    def barrier(self):
        sem = pltpu.get_barrier_semaphore()
        peers = [self.right, self.left, self.partner]
        for peer in peers:
            pl.semaphore_signal(sem, inc=1, device_id={'tp': peer}, device_id_type=MESH)
        pl.semaphore_wait(sem, len(peers))


class Gather:
    LEFT, RIGHT, FAR, SIDE = 0, 2, 4, 6
    SLOTS = 10

    def __init__(self, ring, buf, ssem, rsem, base=0, size=None, cut=None):
        self.ring, self.buf, self.ssem, self.rsem = ring, buf, ssem, rsem
        self.base = base
        self.size = size or buf.shape[1]
        self.cut = cut or self.size // 2
        self.drained = False

    def rows(self, half):
        if half == LOW:
            return pl.ds(self.base, self.cut)
        return pl.ds(self.base + self.cut, self.size - self.cut)

    def copy(self, ref, dev, slot, onward):
        return pltpu.make_async_remote_copy(
            src_ref=ref, dst_ref=ref, send_sem=self.ssem.at[onward], recv_sem=self.rsem.at[slot],
            device_id={'tp': dev}, device_id_type=MESH)

    def send(self, blk, half, dev, slot, onward=LOW):
        self.copy(self.buf.at[blk, self.rows(half)], dev, slot, onward).start()

    def wait(self, blk, half, slot):
        self.copy(self.buf.at[blk, self.rows(half)], self.ring.me, slot, LOW).wait_recv()

    def side(self, which):
        ref = self.buf.at[self.ring.others[which], pl.ds(self.base, self.size)]
        self.copy(ref, self.ring.me, self.SIDE + which, LOW).wait_recv()

    def start(self):
        r = self.ring
        for half in PAIR:
            self.send(r.me, half, r.right, self.LEFT + half)
            self.send(r.me, HIGH - half, r.left, self.RIGHT + HIGH - half)
        for half in PAIR:
            self.send(r.me, half, r.partner, self.SIDE)

    def near1(self):
        r = self.ring
        self.wait(r.left, LOW, self.LEFT)
        self.send(r.left, LOW, r.right, self.FAR, HIGH)
        self.send(r.left, LOW, r.partner, self.SIDE + 1)
        self.wait(r.right, HIGH, self.RIGHT + HIGH)
        self.send(r.right, HIGH, r.left, self.FAR + HIGH, HIGH)
        self.send(r.right, HIGH, r.partner, self.SIDE + 2)

    def near2(self):
        r = self.ring
        self.wait(r.left, HIGH, self.LEFT + HIGH)
        self.send(r.left, HIGH, r.partner, self.SIDE + 1)
        self.wait(r.right, LOW, self.RIGHT)
        self.send(r.right, LOW, r.partner, self.SIDE + 2)

    def far(self):
        r = self.ring
        for half in PAIR:
            self.wait(r.far, half, self.FAR + half)
            self.send(r.far, half, r.partner, self.SIDE + 3)

    def gone(self, blocks, onward):
        ref = self.buf.at[pl.ds(0, blocks), pl.ds(self.base, self.size)]
        self.copy(ref, self.ring.right, LOW, onward).wait_send()

    def drain(self):
        self.gone(1, HIGH)
        self.drained = True

    def finish(self):
        self.gone(6, LOW)
        if not self.drained:
            self.gone(1, HIGH)


class Scatter:
    def __init__(self, ring, part, pair, stage, land, ssem, rsem, base=0, size=None):
        self.ring, self.part, self.pair, self.stage, self.land = ring, part, pair, stage, land
        self.ssem, self.rsem = ssem, rsem
        self.base = base
        self.size = size or part.shape[1]
        self.half = self.size // 2

    def cp_pair(self, xp):
        r = self.ring
        rows = pl.ds(self.base, self.size)
        return pltpu.make_async_remote_copy(
            src_ref=self.part.at[xp * 2 + (1 - r.c), rows], dst_ref=self.pair.at[xp, rows], send_sem=self.ssem.at[LOW],
            recv_sem=self.rsem.at[xp], device_id={'tp': r.partner}, device_id_type=MESH)

    def cp(self, slot, half, dst_slot, dev):
        rows = pl.ds(self.base + half * self.half, self.half)
        return pltpu.make_async_remote_copy(
            src_ref=self.stage.at[slot, rows], dst_ref=self.land.at[dst_slot, rows],
            send_sem=self.ssem.at[HIGH], recv_sem=self.rsem.at[4 + 2 * dst_slot + half],
            device_id={'tp': dev}, device_id_type=MESH)

    def wait_land(self, dst_slot, half):
        self.cp(0, half, dst_slot, self.ring.me).wait_recv()

    def wait_pair(self, xp):
        self.cp_pair(xp).wait_recv()

    def send_pair(self, xp):
        self.cp_pair(xp).start()

    def mix(self, slot, xp, half, with_far=False):
        blk = xp * 2 + self.ring.c
        step = 32

        def body(i):
            rows = pl.ds(pl.multiple_of(self.base + half * self.half + i * step, step), step)
            total = self.part[blk, rows, :].astype(F32) + self.pair[xp, rows, :].astype(F32)
            if with_far:
                total = total + self.land[0, rows, :].astype(F32)
            self.stage[slot, rows, :] = total.astype(BF)
        loop(0, self.half // step, body)

    def far(self):
        r = self.ring
        self.wait_pair(r.xf)
        self.mix(0, r.xf, 0)
        self.cp(0, 0, 0, r.right).start()
        self.mix(0, r.xf, 1)
        self.cp(0, 1, 0, r.left).start()

    def near_own(self):
        r = self.ring
        self.wait_pair(r.xr)
        self.mix(1, r.xr, 1)
        self.cp(1, 1, 1, r.right).start()
        self.wait_pair(r.xl)
        self.mix(2, r.xl, 0)
        self.cp(2, 0, 2, r.left).start()

    def near_sum(self):
        r = self.ring
        self.wait_land(0, 0)
        self.mix(1, r.xr, 0, with_far=True)
        self.cp(1, 0, 1, r.right).start()
        self.wait_land(0, 1)
        self.mix(2, r.xl, 1, with_far=True)
        self.cp(2, 1, 2, r.left).start()

    def wait_final(self):
        self.wait_pair(self.ring.x)
        for slot in (1, 2):
            for half in PAIR:
                self.wait_land(slot, half)

    def total(self, rows):
        r = self.ring
        return (self.part[r.me, rows, :].astype(F32) + self.pair[r.x, rows, :].astype(F32)
                + self.land[1, rows, :].astype(F32) + self.land[2, rows, :].astype(F32))

    def finish(self):
        r = self.ring
        rows = pl.ds(self.base, self.size)
        for ref, which in ((self.pair.at[:, rows], LOW), (self.stage.at[:, rows], HIGH)):
            pltpu.make_async_remote_copy(
                src_ref=ref, dst_ref=ref, send_sem=self.ssem.at[which], recv_sem=self.rsem.at[0],
                device_id={'tp': r.partner}, device_id_type=MESH).wait_send()


def scatter_buffers(n, rows, d):
    return [VMEM((n // 2, rows, d), BF), VMEM((3, rows, d), BF), VMEM((3, rows, d), BF)]


def scatter_sems():
    return [pltpu.SemaphoreType.DMA((2,)), pltpu.SemaphoreType.DMA((4 + 6,))]


def hooked(count, body, hooks):
    def step(i):
        for at, actions in hooks.items():
            @pl.when(i == at)
            def _():
                for act in actions:
                    act()
        body(i)
    loop(0, count, step)


def gather_sems():
    return [pltpu.SemaphoreType.DMA((2,)), pltpu.SemaphoreType.DMA((Gather.SLOTS,))]


def lane_mask(rows, h):
    lane = lax.broadcasted_iota(jnp.int32, (rows, 128), 1)
    return (lane < 64) if h == 0 else (lane >= 64)


def attend_block(i, q_ref, k_ref, vt_ref, o_ref, lse_ref, s_ref, m_ref, l_ref, acc_ref, bt_ref, slopes):
    t = q_ref.shape[2]
    e = acc_ref.shape[0] // 2
    key = lax.broadcasted_iota(jnp.int32, (t, t), 0)
    qry = lax.broadcasted_iota(jnp.int32, (t, t), 1)
    for h in PAIR:
        m_ref[h] = jnp.full((8, t), MASK_VALUE, F32)
        l_ref[h] = jnp.zeros((8, t), F32)
    zero_fill(acc_ref)

    def shift(h, j):
        return slopes[h] * (j * t).astype(F32)

    def score(blocks, diag):
        top = [m_ref[h] for h in PAIR]
        for j in blocks:
            for h in PAIR:
                s = mm(k_ref[j], q_ref[h, i], NT) + bt_ref[h]
                if diag:
                    s = jnp.where(key <= qry, s, MASK_VALUE)
                s_ref[h, j] = s
                top[h] = jnp.maximum(top[h], fold8(s, jnp.maximum) + shift(h, j))
        for h in PAIR:
            m_ref[h] = top[h]

    twos(i, lambda blocks: score(blocks, False))
    score((i,), True)
    top = [jnp.max(m_ref[h], axis=0, keepdims=True) for h in PAIR]

    def denom(j):
        for h in PAIR:
            l_ref[h] = l_ref[h] + fold8(jnp.exp(s_ref[h, j] + (shift(h, j) - top[h])), jnp.add)

    loop(0, i + 1, denom)
    for h in PAIR:
        lse_ref[h, i] = top[h] + jnp.log(col_sum(l_ref[h]))

    def values(blocks):
        for h in PAIR:
            rows = pl.ds(h * e, e)
            total = acc_ref[rows, :]
            for j in blocks:
                p = jnp.exp(s_ref[h, j] + (shift(h, j) - lse_ref[h, i])).astype(BF)
                total = total + mm(vt_ref[j, rows, :], p)
            acc_ref[rows, :] = total

    twos(i + 1, values)
    o_ref[i] = acc_ref[...].T.astype(BF)


def kernel_main(n, scale, n_vec, n_out, x_hbm, dy_hbm, wt_hbm, wo_hbm, wu_hbm, wd_hbm, *refs):
    vec_hbm, (slopes_ref,), refs = refs[:n_vec], refs[n_vec:n_vec + 1], refs[n_vec + 1:]
    results, (h_hbm,), refs = refs[:n_out], refs[n_out:n_out + 1], refs[n_out + 1:]
    vecs, refs = refs[:n_vec], refs[n_vec:]
    run_layer(n, scale, vec_hbm, vecs, results, x_hbm, dy_hbm, wt_hbm, wo_hbm, wu_hbm, wd_hbm, slopes_ref, h_hbm, *refs)


def run_layer(n, scale, vec_hbm, vecs, results, x_hbm, dy_hbm, wt_hbm, wo_hbm, wu_hbm, wd_hbm, slopes_ref, h_hbm,
                xg, xo, dyo, dy, hg, wt, wp, wof, wu, wd, q, k, v, kt, vt, o, lse, orow, s_ref, m_ref, l_ref, acc, bt,
                x1, act, dpre, mid, dom, dqt, dk, dv, d3, small, early, late, part,
                *rest):
    g1, b1, bqkv, bo, g2, b2, bu, bd = vecs
    y, gx, sums, gwt, gbq, gwo, gwu, gbu, gwd = results
    rest = list(rest)

    def take(count):
        head = rest[:count]
        del rest[:count]
        return head

    ring = Ring(n)
    me = ring.me
    t, d, f = xg.shape[1], xg.shape[2], wu.shape[1]
    rs_bufs, rm_bufs = take(3), take(3)
    st = t // 2
    streams = (0, st)
    r_sems = [take(2) for _ in PAIR]
    r0, r1 = [Scatter(ring, part, *rs_bufs, *sems, base=base, size=st) for base, sems in zip(streams, r_sems)]
    rs = Scatter(ring, part, *rs_bufs, *r_sems[0])
    rm = Scatter(ring, dy, *rm_bufs, *take(2))
    g_sems = [take(2) for _ in PAIR]
    ax, aw = [Gather(ring, buf, *sems) for buf, sems in zip((xg, wof), g_sems)]
    ay = Gather(ring, dy, *take(2))
    g0, g1s = [Gather(ring, hg, *sems, base=base, size=st) for base, sems in zip(streams, g_sems)]
    d0, d1 = [Gather(ring, xg, *sems, base=base, size=st) for base, sems in zip(streams, g_sems)]
    few, local, vec_sem = take(3)
    o_send, o_recv, e_send, e_recv, l_send, l_recv = [few.at[i] for i in range(6)]

    def fetch(i, src, dst):
        cp = pltpu.make_async_copy(src, dst, local.at[i])
        cp.start()
        return cp

    in_x, in_wo, in_dy, in_wt = (fetch(0, x_hbm, xg.at[me]), fetch(1, wo_hbm, wof.at[me]),
                                 fetch(2, dy_hbm, dy.at[me]), fetch(3, wt_hbm, wt))
    later = [fetch(4, wu_hbm, wu), fetch(5, wd_hbm, wd), fetch(6, x_hbm, xo), fetch(7, dy_hbm, dyo)]
    vec_in = [pltpu.make_async_copy(a, b, vec_sem.at[i]) for i, (a, b) in enumerate(zip(vec_hbm, vecs))]
    for cp in vec_in:
        cp.start()
    ring.barrier()
    in_x.wait()
    ax.start()
    for cp in vec_in:
        cp.wait()
    in_wt.wait()
    sort_weight(wp, wt)
    in_wo.wait()
    in_dy.wait()
    bias = jnp.concatenate([bqkv[kind, head:head + 1, :] for kind in TRIPLE for head in PAIR], axis=1)

    def project(blk):
        def norm(rows):
            hat, _ = norm_rows(xg[blk, rows, :].astype(F32))
            hg[blk, rows, :] = (hat * g1[...] + b1[...]).astype(BF)
        rows_loop(t, 64, norm)
        out = mm(hg[blk], wp[...], NT) + bias
        out = out.astype(BF)
        zero = jnp.zeros((t, 128), BF)
        qs = (out[:, :128].astype(F32) * scale).astype(BF)
        for head in PAIR:
            q[head, blk] = jnp.where(lane_mask(t, head), qs, zero)
        k[blk] = out[:, 128:256]
        v[blk] = out[:, 256:]
        kt[blk] = out[:, 128:256].T
        vt[blk] = out[:, 256:].T
        fetch(0, hg.at[blk], h_hbm.at[blk])

    arrive = functools.partial
    with scope('a_gather'):
        hooked(n, lambda step: project(ring.order(step)), {
            1: [arrive(ax.side, 0)],
            2: [ax.near1, ax.near2],
            4: [arrive(ax.side, 1)],
            5: [arrive(ax.side, 2)],
            6: [ax.drain, aw.start, ax.far, ay.start],
            7: [arrive(ax.side, 3)]})
    slopes = [slopes_ref[me * 2 + head] for head in PAIR]
    key = lax.broadcasted_iota(jnp.int32, (t, t), 0)
    qry = lax.broadcasted_iota(jnp.int32, (t, t), 1)
    for head in PAIR:
        bt[head] = slopes[head] * key.astype(F32)

    def send_o(i):
        cols = pl.ds(pl.multiple_of(me * 128, 128), 128)
        return pltpu.make_async_remote_copy(
            src_ref=o.at[i], dst_ref=orow.at[:, cols], send_sem=o_send, recv_sem=o_recv,
            device_id={'tp': i}, device_id_type=MESH)

    def one_block(step):
        i = ring.order(n - 1 - step)
        attend_block(i, q, k, vt, o, lse, s_ref, m_ref, l_ref, acc, bt, slopes)

        @pl.when(step < n - 1)
        def _():
            send_o(i).start()

    with scope('a_attend'):
        ax.finish()
        pltpu.make_async_copy(hg, h_hbm, local.at[0]).wait()
        hooked(n, one_block, {4: [aw.near1], 5: [aw.near2]})
    most = pl.ds(0, n - 1)
    with scope('a_wait'):
        aw.far()
        ay.near1()
        orow[:, pl.ds(pl.multiple_of(me * 128, 128), 128)] = o[me]
        wide = orow.at[:, pl.ds(0, (n - 1) * 128)]
        pltpu.make_async_remote_copy(
            src_ref=wide, dst_ref=wide, send_sem=o_send, recv_sem=o_recv,
            device_id={'tp': me}, device_id_type=MESH).wait_recv()
        for which in range(4):
            aw.side(which)
        aw.finish()
        later[2].wait()
    with scope('a_out'):
        x1[...] = mm(orow[...], wof[...].reshape(n * 128, d)).astype(BF).astype(F32)

        def enter(rows):
            row = xo[rows, :].astype(F32) + x1[rows, :] + bo[...]
            x1[rows, :] = row
            hat, _ = norm_rows(row)
            hg[me, rows, :] = (hat * g2[...] + b2[...]).astype(BF)
        rows_loop(st, 64, enter)
        g0.start()
        rows_loop(st, 64, enter, base=st)
    for cp in (later[0], later[1], later[3]):
        cp.wait()
    zero_fill(gbu)
    ay.side(0)

    def rest():
        ay.near2()
        ay.far()
        for which in range(1, 4):
            ay.side(which)

    def mlp(blk, stream):
        rows = pl.ds(pl.multiple_of(stream * st, st), st)
        pre = mm(hg[blk, rows, :], wu[...]) + bu[...]
        cot = mm(dy[blk, rows, :], wd[...], NT).astype(BF).astype(F32)
        sq = pre * pre
        th = jnp.tanh(GELU_C * (pre + 0.044715 * sq * pre))
        cdf = 0.5 * (1.0 + th)
        act[blk, rows, :] = (pre * cdf).astype(BF)
        slope = cdf + pre * (0.5 * (1.0 - th * th)) * (GELU_C * (1.0 + 3 * 0.044715 * sq))
        dp = cot * slope
        gbu[...] = gbu[...] + fold8(dp, jnp.add)
        dpb = dp.astype(BF)
        dpre[blk, rows, :] = dpb
        part[blk, rows, :] = mm(dpb, wu[...], NT).astype(BF)

    chips = (ring.xf, ring.xr, ring.xl, ring.x)
    def pairs(job):
        for xp in chips:
            job.send_pair(xp)

    def item(step):
        late = (step == 4) | (step == 5) | (step >= 10)
        pos = jnp.where(step < 4, step, jnp.where(step < 6, step - 4, jnp.where(step < 10, step - 2, step - 8)))
        mlp(ring.order(pos), jnp.where(late, 1, 0))

    with scope('b_gather'):
        hooked(2 * n, item, {
            1: [arrive(g0.side, 0)],
            2: [rest, g0.near1, g1s.start, g0.near2],
            5: [arrive(g1s.side, 0)],
            6: [arrive(g0.side, 1)],
            7: [arrive(g0.side, 2)],
            8: [g0.far],
            9: [arrive(g0.side, 3)],
            10: [arrive(pairs, r0), g1s.near1, r0.far, g1s.near2],
            12: [r0.near_own, arrive(g1s.side, 1)],
            13: [arrive(g1s.side, 2)],
            14: [g1s.far],
            15: [arrive(g1s.side, 3)]})
    with scope('b_far'):
        pairs(r1)
        r0.near_sum()
        r1.far()
    with scope('b_own'):
        r1.near_own()
    ay.finish()

    def weight_down(i):
        cols = pl.ds(pl.multiple_of(i * 256, 256), 256)
        left = act[:, :, cols].reshape(n * t, 256)
        gwd[cols, :] = mm(left, dy[...].reshape(n * t, d), T0).astype(BF)

    def weight_up(i):
        cols = pl.ds(pl.multiple_of(i * 256, 256), 256)
        left = hg[:, :, cols].reshape(n * t, 256)
        gwu[cols, :] = mm(left, dpre[...].reshape(n * t, f), T0).astype(BF)

    with scope('b_weights'):
        loop(0, f // 256, weight_down)
        loop(0, d // 256, weight_up)
    zero_fill(small)

    def down(blk):
        dy[blk] = mm(act[blk], wd[...]).astype(BF)

    def leave(rows):
        dg = rs.total(rows).astype(BF).astype(F32)
        hat, rstd = norm_rows(x1[rows, :])
        small[2] = small[2] + fold8(dg * hat, jnp.add)
        small[3] = small[3] + fold8(dg, jnp.add)
        dz = norm_back(dg * g2[...], hat, rstd)
        dyf = dyo[rows, :].astype(F32)
        dm = dyf + dz
        small[4] = small[4] + fold8(dm, jnp.add)
        small[5] = small[5] + fold8(dyf, jnp.add)
        mid[rows, :] = dm
        xg[me, rows, :] = dm.astype(BF)

    with scope('b_sum'):
        r1.near_sum()
    with scope('b_final'):
        r0.wait_final()
    with scope('b_leave'):
        rows_loop(st, 64, leave)
        g0.finish()
        d0.start()
    with scope('b_down'):
        loop(0, n, down)
        pairs(rm)
    with scope('b_final1'):
        r1.wait_final()
    with scope('b_leave1'):
        rows_loop(st, 64, leave, base=st)
        g1s.finish()
        d1.start()
    with scope('b_finish'):
        for job in (r0, r1):
            job.finish()
    reload = fetch(0, h_hbm, hg)

    def share(buf, off, send_sem, recv_sem):
        return pltpu.make_async_remote_copy(
            src_ref=buf.at[me], dst_ref=buf.at[me], send_sem=send_sem, recv_sem=recv_sem,
            device_id={'tp': (me + off) % n}, device_id_type=MESH)

    def all_in(buf, send_sem, recv_sem):
        return pltpu.make_async_remote_copy(
            src_ref=buf.at[most], dst_ref=buf.at[most], send_sem=send_sem, recv_sem=recv_sem,
            device_id={'tp': me}, device_id_type=MESH)

    def early_out():
        for i in range(4):
            early[me, i:i + 1, :] = col_sum(small[2 + i])
        for off in range(1, n):
            share(early, off, e_send, e_recv).start()

    def add_up(buf):
        total = buf[0]
        for b in range(1, n):
            total = total + buf[b]
        return total
    zero_fill(dk, dv)

    def back_block(i):
        dc = mm(xg[i], wof[me], NT).astype(BF)
        zero = jnp.zeros((t, 128), BF)
        prod = (dc.astype(F32) * o[i].astype(F32)).T
        dlt = (col_sum(prod[:64]), col_sum(prod[64:]))
        for head in PAIR:
            dom[head] = jnp.where(lane_mask(t, head), dc, zero)
        zero_fill(dqt)

        def pair_block(blocks, diag):
            cases = [(j, head) for j in blocks for head in PAIR]
            ps, dss = [], []
            for j, head in cases:
                s = mm(k[j], q[head, i], NT) + bt[head]
                if diag:
                    s = jnp.where(key <= qry, s, MASK_VALUE)
                p = jnp.exp(s + (slopes[head] * (j * t).astype(F32) - lse[head, i]))
                dp = mm(v[j], dom[head], NT).astype(BF).astype(F32)
                dss.append((p * (dp - dlt[head])).astype(BF))
                ps.append(p.astype(BF))
            wide = list(zip(cases, ps, dss))
            for j in blocks:
                dv[j] = dv[j] + sum(mm(p, dom[head]) for (b, head), p, _ in wide if b is j)
                dk[j] = dk[j] + sum(mm(ds, q[head, i]) for (b, head), _, ds in wide if b is j)
            for head in PAIR:
                rows = pl.ds(head * 64, 64)
                dqt[rows, :] = dqt[rows, :] + sum(mm(kt[b, rows, :], ds) for (b, h), _, ds in wide if h == head)

        twos(i, lambda blocks: pair_block(blocks, False))
        pair_block((i,), True)
        d3[i, :, :128] = (dqt[...].T * scale).astype(BF)

    def both_in(which):
        for job in (d0, d1):
            job.side(which)

    with scope('c_attend'):
        hooked(n, lambda step: back_block(ring.order(step)), {
            1: [arrive(both_in, 0), d0.near1, d0.near2],
            2: [d1.near1, rm.far, rm.near_own, d1.near2],
            4: [arrive(both_in, 1)],
            5: [arrive(both_in, 2)],
            6: [d0.far, d1.far, rm.near_sum, early_out],
            7: [arrive(both_in, 3)]})
    zero_fill(gbq)

    def back_in(xp):
        for cc in PAIR:
            blk = xp * 2 + cc
            d3[blk, :, 128:256] = dk[blk].astype(BF)
            d3[blk, :, 256:] = dv[blk].astype(BF)
            part[blk] = mm(d3[blk], wp[...]).astype(BF)
        rs.send_pair(xp)

    with scope('c_far'):
        back_in(ring.xf)
        rs.far()
    with scope('c_own'):
        back_in(ring.xr)
        back_in(ring.xl)
        rs.near_own()
        back_in(ring.x)
    reload.wait()

    def weight_in(i):
        cols = pl.ds(pl.multiple_of(i * 128, 128), 128)
        left = d3[:, :, cols].reshape(n * t, 128)
        grad = mm(left, hg[...].reshape(n * t, d), T0).astype(BF)
        for head in PAIR:
            gwt[head, i] = grad[head * 64:head * 64 + 64]

    def bias_in(b):
        gbq[...] = gbq[...] + fold8(d3[b].astype(F32), jnp.add)

    with scope('c_weights'):
        loop(0, len(TRIPLE), weight_in)
        loop(0, n, bias_in)
    with scope('c_sum'):
        rs.near_sum()
    with scope('c_gwo'):
        gwo[...] = mm(o[...].reshape(n * t, 128), xg[...].reshape(n * t, d), T0).astype(BF)
    with scope('c_mfinal'):
        rm.wait_final()

    def finish_y(rows):
        m = rm.total(rows).astype(BF).astype(F32)
        y[rows, :] = (x1[rows, :] + m + bd[...]).astype(BF)
    rows_loop(t, 64, finish_y)
    with scope('c_final'):
        rs.wait_final()

    def sum_in(rows):
        dh = rs.total(rows).astype(BF).astype(F32)
        hat, _ = norm_rows(xo[rows, :].astype(F32))
        small[0] = small[0] + fold8(dh * hat, jnp.add)
        small[1] = small[1] + fold8(dh, jnp.add)

    def last(rows):
        dh = rs.total(rows).astype(BF).astype(F32)
        hat, rstd = norm_rows(xo[rows, :].astype(F32))
        gx[rows, :] = (mid[rows, :] + norm_back(dh * g1[...], hat, rstd)).astype(BF)

    with scope('c_sums'):
        rows_loop(t, 64, sum_in)
    for i in PAIR:
        late[me, i:i + 1, :] = col_sum(small[i])
    with scope('c_share'):
        for off in range(1, n):
            share(late, off, l_send, l_recv).start()
        rows_loop(t, 64, last)
        all_in(early, e_send, e_recv).wait_recv()
        sums[2:6, :] = add_up(early)
        all_in(late, l_send, l_recv).wait_recv()
        sums[0:2, :] = add_up(late)
        all_in(early, e_send, e_recv).wait_send()
        all_in(late, l_send, l_recv).wait_send()
        all_in(o, o_send, o_recv).wait_send()
    with scope('d_finish'):
        for job in (rs, rm, d0, d1):
            job.finish()


def kernel_out(n_big, *refs):
    count = n_big + 3
    srcs, refs = refs[:count], refs[count:]
    outs, refs = refs[:n_big + 8], refs[n_big + 8:]
    bufs, tail, sem_out = srcs, refs[:-1], refs[-1]
    gbq, gbu, sums = bufs[n_big:]
    o_bq, o_bu, o_sums = tail
    kept = list(bufs[:n_big]) + [o_bq, o_bu] + [o_sums.at[i:i + 1] for i in range(6)]
    backs = [pltpu.make_async_copy(b, a, sem_out.at[i]) for i, (a, b) in enumerate(zip(outs, kept))]
    for back in backs[:n_big]:
        back.start()
    o_bu[...] = col_sum(gbu[...])
    row = col_sum(gbq[...])
    e = o_bq.shape[2]
    for part_no in TRIPLE:
        for head in PAIR:
            at = (part_no * 2 + head) * e
            o_bq[part_no, head:head + 1, :] = row[:, at:at + e]
    o_sums[...] = sums[...]
    for back in backs[n_big:]:
        back.start()
    for back in backs:
        back.wait()


def inside():
    return pl.BlockSpec(memory_space=VMEM)


def anywhere():
    return pl.BlockSpec(memory_space=pl.ANY)


def smem():
    return pl.BlockSpec(memory_space=pltpu.SMEM)


def solution(mesh):
    n = mesh.shape['tp']

    def local_step(x, ln1_gamma, ln1_beta, w_qkv, b_qkv, w_out, b_out, ln2_gamma, ln2_beta, w_up, b_up, w_down, b_down, grad_y):
        t, d = x.shape[1], x.shape[2]
        heads, e = w_qkv.shape[1], w_qkv.shape[3]
        he = heads * e
        f = w_up.shape[1]
        scale = e ** -0.5
        slopes = jnp.asarray(alibi_slopes(heads * n))
        x2, dy2 = x[0], grad_y[0]
        row = lambda vec: vec.reshape(1, -1)
        wt = w_qkv.transpose(1, 2, 3, 0).reshape(heads * 3 * e, d)
        bq = b_qkv.transpose(1, 0, 2)
        sds = jax.ShapeDtypeStruct
        rows, full, half = (t, d), (n, t, d), (n, t, he)
        both, line = (len(PAIR),) + half, (len(PAIR), n, 1, t)
        packed = (len(TRIPLE) * he, d)
        params = lambda cid: pltpu.CompilerParams(collective_id=cid, has_side_effects=True, vmem_limit_bytes=VLIM)
        dma = pltpu.SemaphoreType.DMA

        vm = lambda dims, kind=BF: VMEM(dims, kind)
        stat, turned = (len(PAIR), 8, t), (n, he, t)
        vecs = (row(ln1_gamma), row(ln1_beta), bq, row(b_out), row(ln2_gamma), row(ln2_beta), row(b_up), row(b_down))
        results = [sds(rows, BF), sds(rows, BF), sds((8, d), F32), sds((heads, len(TRIPLE), e, d), BF),
                   sds((8, len(TRIPLE) * he), F32), sds((he, d), BF), sds((d, f), BF), sds((8, f), F32), sds((f, d), BF)]
        y, gx, sums, gwt, gbq, gwo, gwu, gbu, gwd, _ = pl.pallas_call(
            functools.partial(kernel_main, n, scale, len(vecs), len(results)),
            name='layer',
            out_shape=[vm(b.shape, b.dtype) for b in results] + [sds(full, BF)],
            in_specs=[anywhere()] * (6 + len(vecs)) + [smem()],
            out_specs=[inside()] * len(results) + [anywhere()],
            scratch_shapes=[vm(b.shape, b.dtype) for b in vecs] + [vm(full), vm(rows), vm(rows), vm(full), vm(full), vm(packed), vm(packed), vm((n, he, d)),
                            vm((d, f)), vm((f, d)), vm(both), vm(half), vm(half), vm(turned), vm(turned), vm(half),
                            vm(line, F32), vm(rows), vm((len(PAIR), n, t, t), F32), vm(stat, F32), vm(stat, F32),
                            vm((he, t), F32), vm((len(PAIR), t, t), F32), vm(rows, F32), vm((n, t, f)), vm((n, t, f)),
                            vm(rows, F32), vm((len(PAIR), t, he)), vm((he, t), F32), vm(half, F32), vm(half, F32),
                            vm((n, t, len(TRIPLE) * he)), vm((6, 8, d), F32), vm((n, 4, d), F32), vm((n, 2, d), F32), vm(full)]
            + scatter_buffers(n, t, d) * 2 + scatter_sems() * 3 + gather_sems() * 3 + [dma((n,))] * 2 + [dma((len(vecs),))],
            compiler_params=params(0),
        )(x2, dy2, wt, w_out, w_up, w_down, *vecs, slopes)

        big = (y, gx, gwt, gwo, gwu, gwd)
        little = (gbq, gbu, sums)
        bias_dims, up_dims = (len(TRIPLE), heads, e), (1, f)
        res = pl.pallas_call(
            functools.partial(kernel_out, len(big)),
            name='results',
            compiler_params=pltpu.CompilerParams(vmem_limit_bytes=8 * 1024 * 1024),
            out_shape=[sds(b.shape, b.dtype) for b in big] + [sds(bias_dims, F32), sds(up_dims, F32)] + [sds((1, d), F32)] * 6,
            in_specs=[inside()] * (len(big) + 3),
            out_specs=[anywhere()] * (len(big) + 8),
            scratch_shapes=[vm(bias_dims, F32), vm(up_dims, F32), vm((8, d), F32), dma((len(big) + 8,))],
        )(*big, *little)
        y, gx, gwt, gwo, gwu, gwd, gbq, gbu, s_g1, s_b1, s_g2, s_b2, s_bo, s_bd = res
        vec = lambda a: a.reshape(-1)
        return (y[None], gx[None], vec(s_g1), vec(s_b1), gwt.transpose(3, 0, 1, 2), gbq.transpose(1, 0, 2), gwo, vec(s_bo),
                vec(s_g2), vec(s_b2), gwu, vec(gbu), gwd, vec(s_bd))

    row_spec = P('dp', 'tp', None)
    in_specs = (row_spec, P(), P(), P(None, 'tp', None, None), P('tp', None, None), P('tp', None), P(), P(), P(),
                P(None, 'tp'), P('tp'), P('tp', None), P(), row_spec)
    out_specs = (row_spec, row_spec, P('dp'), P('dp'), P('dp', 'tp', None, None), P(('dp', 'tp'), None, None),
                 P(('dp', 'tp'), None), P('dp'), P('dp'), P('dp'), P('dp', 'tp'), P(('dp', 'tp')), P(('dp', 'tp'), None), P('dp'))
    return jax.shard_map(local_step, mesh=mesh, in_specs=in_specs, out_specs=out_specs, check_vma=False)
```

```python
import functools
import math
import jax
import jax.numpy as jnp
import numpy as np
from jax import lax
from jax.experimental import pallas as pl
from jax.experimental.pallas import tpu as pltpu
from jax.sharding import PartitionSpec as P

EPS = 1e-5
MASK_VALUE = -1e30
BF, F32 = jnp.bfloat16, jnp.float32
VMEM = pltpu.VMEM
MESH = pl.DeviceIdType.MESH
scope = jax.named_scope
VLIM = 58 * 1024 * 1024
GELU_C = math.sqrt(2.0 / math.pi)
PAIR = LOW, HIGH = (0, 1)
TRIPLE = (0, 1, 2)
NN = (((1,), (0,)), ((), ()))
T0 = (((0,), (0,)), ((), ()))
NT = (((1,), (1,)), ((), ()))


def alibi_slopes(n_heads):
    closest = 2 ** int(math.floor(math.log2(n_heads)))
    base_ratio = 2.0 ** (-8.0 / closest)
    extra_ratio = 2.0 ** (-4.0 / closest)
    remaining = min(closest, n_heads - closest)
    slopes = [base_ratio ** (i + 1) for i in range(closest)]
    slopes = slopes + [extra_ratio ** (2 * i + 1) for i in range(remaining)]
    return np.array(slopes, dtype=np.float32)


def mm(a, b, dims=NN):
    return lax.dot_general(a, b, dims, preferred_element_type=F32)


def loop(lo, hi, body, unroll=1):
    def step(i, carry):
        body(i)
        return carry
    lax.fori_loop(lo, hi, step, 0, unroll=unroll)


def twos(count, body):
    loop(0, count // 2, lambda i: body((2 * i, 2 * i + 1)))

    @pl.when(count % 2 == 1)
    def _():
        body((count - 1,))


def rows_loop(total, rows, body, base=0):
    loop(0, total // rows, lambda r: body(pl.ds(pl.multiple_of(base + r * rows, rows), rows)))


def row_mean(z):
    return jnp.mean(z, axis=-1, keepdims=True)


def col_sum(z):
    return jnp.sum(z, axis=0, keepdims=True)


def norm_back(grad, hat, rstd):
    return rstd * (grad - row_mean(grad) - hat * row_mean(grad * hat))


def zero_fill(*refs):
    for ref in refs:
        ref[...] = jnp.zeros(ref.shape, ref.dtype)


def sort_weight(wp, wt):
    e = wp.shape[0] // 6
    for part_no in TRIPLE:
        for head in PAIR:
            dst = (part_no * 2 + head) * e
            src = (head * 3 + part_no) * e
            wp[dst:dst + e, :] = wt[src:src + e, :]


def norm_rows(z):
    cen = z - row_mean(z)
    rstd = lax.rsqrt(row_mean(cen * cen) + EPS)
    return cen * rstd, rstd


def fold8(v, op):
    out = v[0:8]
    for k in range(1, v.shape[0] // 8):
        out = op(out, v[8 * k:8 * k + 8])
    return out


class Ring:
    def __init__(self, n):
        self.n = n
        nx = n // 2
        self.me = lax.axis_index('tp')
        self.x = self.me // 2
        self.c = self.me % 2
        self.nx = nx
        self.xr = (self.x + 1) % nx
        self.xl = (self.x + nx - 1) % nx
        self.xf = (self.x + 2) % nx
        self.right = self.xr * 2 + self.c
        self.left = self.xl * 2 + self.c
        self.far = self.xf * 2 + self.c
        other = 1 - self.c
        self.partner = self.x * 2 + other
        self.others = [xp * 2 + other for xp in (self.x, self.xl, self.xr, self.xf)]

    def order(self, s):
        odd = s % 2
        dx = jnp.where(s < 2, 0, jnp.where(s >= 6, 2, jnp.where(odd == 0, self.nx - 1, 1)))
        mid = jnp.where(s < 4, 0, 1)
        dc = jnp.where(s < 2, odd, jnp.where(s >= 6, odd, mid))
        return ((self.x + dx) % self.nx) * 2 + (self.c + dc) % 2

    def barrier(self):
        sem = pltpu.get_barrier_semaphore()
        peers = [self.right, self.left, self.partner]
        for peer in peers:
            pl.semaphore_signal(sem, inc=1, device_id={'tp': peer}, device_id_type=MESH)
        pl.semaphore_wait(sem, len(peers))


class Gather:
    LEFT, RIGHT, FAR, SIDE = 0, 2, 4, 6
    SLOTS = 10

    def __init__(self, ring, buf, ssem, rsem, base=0, size=None, cut=None):
        self.ring, self.buf, self.ssem, self.rsem = ring, buf, ssem, rsem
        self.base = base
        self.size = size or buf.shape[1]
        self.cut = cut or self.size // 2
        self.drained = False

    def rows(self, half):
        if half == LOW:
            return pl.ds(self.base, self.cut)
        return pl.ds(self.base + self.cut, self.size - self.cut)

    def copy(self, ref, dev, slot, onward):
        return pltpu.make_async_remote_copy(
            src_ref=ref, dst_ref=ref, send_sem=self.ssem.at[onward], recv_sem=self.rsem.at[slot],
            device_id={'tp': dev}, device_id_type=MESH)

    def send(self, blk, half, dev, slot, onward=LOW):
        self.copy(self.buf.at[blk, self.rows(half)], dev, slot, onward).start()

    def wait(self, blk, half, slot):
        self.copy(self.buf.at[blk, self.rows(half)], self.ring.me, slot, LOW).wait_recv()

    def side(self, which):
        ref = self.buf.at[self.ring.others[which], pl.ds(self.base, self.size)]
        self.copy(ref, self.ring.me, self.SIDE + which, LOW).wait_recv()

    def start(self):
        r = self.ring
        for half in PAIR:
            self.send(r.me, half, r.right, self.LEFT + half)
            self.send(r.me, HIGH - half, r.left, self.RIGHT + HIGH - half)
        for half in PAIR:
            self.send(r.me, half, r.partner, self.SIDE)

    def near1(self):
        r = self.ring
        self.wait(r.left, LOW, self.LEFT)
        self.send(r.left, LOW, r.right, self.FAR, HIGH)
        self.send(r.left, LOW, r.partner, self.SIDE + 1)
        self.wait(r.right, HIGH, self.RIGHT + HIGH)
        self.send(r.right, HIGH, r.left, self.FAR + HIGH, HIGH)
        self.send(r.right, HIGH, r.partner, self.SIDE + 2)

    def near2(self):
        r = self.ring
        self.wait(r.left, HIGH, self.LEFT + HIGH)
        self.send(r.left, HIGH, r.partner, self.SIDE + 1)
        self.wait(r.right, LOW, self.RIGHT)
        self.send(r.right, LOW, r.partner, self.SIDE + 2)

    def far(self):
        r = self.ring
        for half in PAIR:
            self.wait(r.far, half, self.FAR + half)
            self.send(r.far, half, r.partner, self.SIDE + 3)

    def gone(self, blocks, onward):
        ref = self.buf.at[pl.ds(0, blocks), pl.ds(self.base, self.size)]
        self.copy(ref, self.ring.right, LOW, onward).wait_send()

    def drain(self):
        self.gone(1, HIGH)
        self.drained = True

    def finish(self):
        self.gone(6, LOW)
        if not self.drained:
            self.gone(1, HIGH)


class Scatter:
    def __init__(self, ring, part, pair, stage, land, ssem, rsem, base=0, size=None):
        self.ring, self.part, self.pair, self.stage, self.land = ring, part, pair, stage, land
        self.ssem, self.rsem = ssem, rsem
        self.base = base
        self.size = size or part.shape[1]
        self.half = self.size // 2

    def cp_pair(self, xp):
        r = self.ring
        rows = pl.ds(self.base, self.size)
        return pltpu.make_async_remote_copy(
            src_ref=self.part.at[xp * 2 + (1 - r.c), rows], dst_ref=self.pair.at[xp, rows], send_sem=self.ssem.at[LOW],
            recv_sem=self.rsem.at[xp], device_id={'tp': r.partner}, device_id_type=MESH)

    def cp(self, slot, half, dst_slot, dev):
        rows = pl.ds(self.base + half * self.half, self.half)
        return pltpu.make_async_remote_copy(
            src_ref=self.stage.at[slot, rows], dst_ref=self.land.at[dst_slot, rows],
            send_sem=self.ssem.at[HIGH], recv_sem=self.rsem.at[4 + 2 * dst_slot + half],
            device_id={'tp': dev}, device_id_type=MESH)

    def wait_land(self, dst_slot, half):
        self.cp(0, half, dst_slot, self.ring.me).wait_recv()

    def wait_pair(self, xp):
        self.cp_pair(xp).wait_recv()

    def send_pair(self, xp):
        self.cp_pair(xp).start()

    def mix(self, slot, xp, half, with_far=False):
        blk = xp * 2 + self.ring.c
        step = 32

        def body(i):
            rows = pl.ds(pl.multiple_of(self.base + half * self.half + i * step, step), step)
            total = self.part[blk, rows, :].astype(F32) + self.pair[xp, rows, :].astype(F32)
            if with_far:
                total = total + self.land[0, rows, :].astype(F32)
            self.stage[slot, rows, :] = total.astype(BF)
        loop(0, self.half // step, body)

    def far(self):
        r = self.ring
        self.wait_pair(r.xf)
        self.mix(0, r.xf, 0)
        self.cp(0, 0, 0, r.right).start()
        self.mix(0, r.xf, 1)
        self.cp(0, 1, 0, r.left).start()

    def near_own(self):
        r = self.ring
        self.wait_pair(r.xr)
        self.mix(1, r.xr, 1)
        self.cp(1, 1, 1, r.right).start()
        self.wait_pair(r.xl)
        self.mix(2, r.xl, 0)
        self.cp(2, 0, 2, r.left).start()

    def near_sum(self):
        r = self.ring
        self.wait_land(0, 0)
        self.mix(1, r.xr, 0, with_far=True)
        self.cp(1, 0, 1, r.right).start()
        self.wait_land(0, 1)
        self.mix(2, r.xl, 1, with_far=True)
        self.cp(2, 1, 2, r.left).start()

    def wait_final(self):
        self.wait_pair(self.ring.x)
        for slot in (1, 2):
            for half in PAIR:
                self.wait_land(slot, half)

    def total(self, rows):
        r = self.ring
        return (self.part[r.me, rows, :].astype(F32) + self.pair[r.x, rows, :].astype(F32)
                + self.land[1, rows, :].astype(F32) + self.land[2, rows, :].astype(F32))

    def finish(self):
        r = self.ring
        rows = pl.ds(self.base, self.size)
        for ref, which in ((self.pair.at[:, rows], LOW), (self.stage.at[:, rows], HIGH)):
            pltpu.make_async_remote_copy(
                src_ref=ref, dst_ref=ref, send_sem=self.ssem.at[which], recv_sem=self.rsem.at[0],
                device_id={'tp': r.partner}, device_id_type=MESH).wait_send()


def scatter_buffers(n, rows, d):
    return [VMEM((n // 2, rows, d), BF), VMEM((3, rows, d), BF), VMEM((3, rows, d), BF)]


def scatter_sems():
    return [pltpu.SemaphoreType.DMA((2,)), pltpu.SemaphoreType.DMA((4 + 6,))]


def hooked(count, body, hooks):
    def step(i):
        for at, actions in hooks.items():
            @pl.when(i == at)
            def _():
                for act in actions:
                    act()
        body(i)
    loop(0, count, step)


def gather_sems():
    return [pltpu.SemaphoreType.DMA((2,)), pltpu.SemaphoreType.DMA((Gather.SLOTS,))]


def lane_mask(rows, h):
    lane = lax.broadcasted_iota(jnp.int32, (rows, 128), 1)
    return (lane < 64) if h == 0 else (lane >= 64)


def attend_block(i, q_ref, k_ref, vt_ref, o_ref, lse_ref, s_ref, m_ref, l_ref, acc_ref, bt_ref, slopes):
    t = q_ref.shape[2]
    e = acc_ref.shape[0] // 2
    key = lax.broadcasted_iota(jnp.int32, (t, t), 0)
    qry = lax.broadcasted_iota(jnp.int32, (t, t), 1)
    for h in PAIR:
        m_ref[h] = jnp.full((8, t), MASK_VALUE, F32)
        l_ref[h] = jnp.zeros((8, t), F32)
    zero_fill(acc_ref)

    def shift(h, j):
        return slopes[h] * (j * t).astype(F32)

    def score(blocks, diag):
        top = [m_ref[h] for h in PAIR]
        for j in blocks:
            for h in PAIR:
                s = mm(k_ref[j], q_ref[h, i], NT) + bt_ref[h]
                if diag:
                    s = jnp.where(key <= qry, s, MASK_VALUE)
                s_ref[h, j] = s
                top[h] = jnp.maximum(top[h], fold8(s, jnp.maximum) + shift(h, j))
        for h in PAIR:
            m_ref[h] = top[h]

    twos(i, lambda blocks: score(blocks, False))
    score((i,), True)
    top = [jnp.max(m_ref[h], axis=0, keepdims=True) for h in PAIR]

    def denom(j):
        for h in PAIR:
            l_ref[h] = l_ref[h] + fold8(jnp.exp(s_ref[h, j] + (shift(h, j) - top[h])), jnp.add)

    loop(0, i + 1, denom)
    for h in PAIR:
        lse_ref[h, i] = top[h] + jnp.log(col_sum(l_ref[h]))

    def values(blocks):
        for h in PAIR:
            rows = pl.ds(h * e, e)
            total = acc_ref[rows, :]
            for j in blocks:
                p = jnp.exp(s_ref[h, j] + (shift(h, j) - lse_ref[h, i])).astype(BF)
                total = total + mm(vt_ref[j, rows, :], p)
            acc_ref[rows, :] = total

    twos(i + 1, values)
    o_ref[i] = acc_ref[...].T.astype(BF)


def kernel_main(n, scale, n_vec, n_out, x_hbm, dy_hbm, wt_hbm, wo_hbm, wu_hbm, wd_hbm, *refs):
    vec_hbm, (slopes_ref,), refs = refs[:n_vec], refs[n_vec:n_vec + 1], refs[n_vec + 1:]
    results, (h_hbm,), refs = refs[:n_out], refs[n_out:n_out + 1], refs[n_out + 1:]
    vecs, refs = refs[:n_vec], refs[n_vec:]
    run_layer(n, scale, vec_hbm, vecs, results, x_hbm, dy_hbm, wt_hbm, wo_hbm, wu_hbm, wd_hbm, slopes_ref, h_hbm, *refs)


def run_layer(n, scale, vec_hbm, vecs, results, x_hbm, dy_hbm, wt_hbm, wo_hbm, wu_hbm, wd_hbm, slopes_ref, h_hbm,
                xg, xo, dyo, dy, hg, wt, wp, wof, wu, wd, q, k, v, kt, vt, o, lse, orow, s_ref, m_ref, l_ref, acc, bt,
                x1, act, dpre, mid, dom, dqt, dk, dv, d3, small, early, late, part,
                *rest):
    g1, b1, bqkv, bo, g2, b2, bu, bd = vecs
    y, gx, sums, gwt, gbq, gwo, gwu, gbu, gwd = results
    rest = list(rest)

    def take(count):
        head = rest[:count]
        del rest[:count]
        return head

    ring = Ring(n)
    me = ring.me
    t, d, f = xg.shape[1], xg.shape[2], wu.shape[1]
    rs_bufs, rm_bufs = take(3), take(3)
    st = t // 2
    streams = (0, st)
    r_sems = [take(2) for _ in PAIR]
    r0, r1 = [Scatter(ring, part, *rs_bufs, *sems, base=base, size=st) for base, sems in zip(streams, r_sems)]
    rs = Scatter(ring, part, *rs_bufs, *r_sems[0])
    rm = Scatter(ring, dy, *rm_bufs, *take(2))
    g_sems = [take(2) for _ in PAIR]
    ax, aw = [Gather(ring, buf, *sems) for buf, sems in zip((xg, wof), g_sems)]
    ay = Gather(ring, dy, *take(2), cut=t // 4)
    g0, g1s = [Gather(ring, hg, *sems, base=base, size=st) for base, sems in zip(streams, g_sems)]
    d0, d1 = [Gather(ring, xg, *sems, base=base, size=st) for base, sems in zip(streams, g_sems)]
    few, local, vec_sem = take(3)
    o_send, o_recv, e_send, e_recv, l_send, l_recv = [few.at[i] for i in range(6)]

    def fetch(i, src, dst):
        cp = pltpu.make_async_copy(src, dst, local.at[i])
        cp.start()
        return cp

    in_x, in_wo, in_dy, in_wt = (fetch(0, x_hbm, xg.at[me]), fetch(1, wo_hbm, wof.at[me]),
                                 fetch(2, dy_hbm, dy.at[me]), fetch(3, wt_hbm, wt))
    later = [fetch(4, wu_hbm, wu), fetch(5, wd_hbm, wd), fetch(6, x_hbm, xo), fetch(7, dy_hbm, dyo)]
    vec_in = [pltpu.make_async_copy(a, b, vec_sem.at[i]) for i, (a, b) in enumerate(zip(vec_hbm, vecs))]
    for cp in vec_in:
        cp.start()
    ring.barrier()
    in_x.wait()
    ax.start()
    for cp in vec_in:
        cp.wait()
    in_wt.wait()
    sort_weight(wp, wt)
    in_wo.wait()
    in_dy.wait()
    bias = jnp.concatenate([bqkv[kind, head:head + 1, :] for kind in TRIPLE for head in PAIR], axis=1)

    def project(blk):
        def norm(rows):
            hat, _ = norm_rows(xg[blk, rows, :].astype(F32))
            hg[blk, rows, :] = (hat * g1[...] + b1[...]).astype(BF)
        rows_loop(t, 64, norm)
        out = mm(hg[blk], wp[...], NT) + bias
        out = out.astype(BF)
        zero = jnp.zeros((t, 128), BF)
        qs = (out[:, :128].astype(F32) * scale).astype(BF)
        for head in PAIR:
            q[head, blk] = jnp.where(lane_mask(t, head), qs, zero)
        k[blk] = out[:, 128:256]
        v[blk] = out[:, 256:]
        kt[blk] = out[:, 128:256].T
        vt[blk] = out[:, 256:].T
        fetch(0, hg.at[blk], h_hbm.at[blk])

    arrive = functools.partial
    with scope('a_gather'):
        hooked(n, lambda step: project(ring.order(step)), {
            1: [arrive(ax.side, 0)],
            2: [ax.near1, ax.near2],
            4: [arrive(ax.side, 1)],
            5: [arrive(ax.side, 2)],
            6: [ax.drain, aw.start, ax.far, ay.start],
            7: [arrive(ax.side, 3)]})
    slopes = [slopes_ref[me * 2 + head] for head in PAIR]
    key = lax.broadcasted_iota(jnp.int32, (t, t), 0)
    qry = lax.broadcasted_iota(jnp.int32, (t, t), 1)
    for head in PAIR:
        bt[head] = slopes[head] * key.astype(F32)

    def send_o(i):
        cols = pl.ds(pl.multiple_of(me * 128, 128), 128)
        return pltpu.make_async_remote_copy(
            src_ref=o.at[i], dst_ref=orow.at[:, cols], send_sem=o_send, recv_sem=o_recv,
            device_id={'tp': i}, device_id_type=MESH)

    def one_block(step):
        i = ring.order(n - 1 - step)
        attend_block(i, q, k, vt, o, lse, s_ref, m_ref, l_ref, acc, bt, slopes)

        @pl.when(step < n - 1)
        def _():
            send_o(i).start()

    with scope('a_attend'):
        ax.finish()
        pltpu.make_async_copy(hg, h_hbm, local.at[0]).wait()
        hooked(n, one_block, {4: [aw.near1], 5: [aw.near2]})
    most = pl.ds(0, n - 1)
    with scope('a_wait'):
        aw.far()
        ay.near1()
        orow[:, pl.ds(pl.multiple_of(me * 128, 128), 128)] = o[me]
        wide = orow.at[:, pl.ds(0, (n - 1) * 128)]
        pltpu.make_async_remote_copy(
            src_ref=wide, dst_ref=wide, send_sem=o_send, recv_sem=o_recv,
            device_id={'tp': me}, device_id_type=MESH).wait_recv()
        for which in range(4):
            aw.side(which)
        aw.finish()
        later[2].wait()
    with scope('a_out'):
        x1[...] = mm(orow[...], wof[...].reshape(n * 128, d)).astype(BF).astype(F32)

        def enter(rows):
            row = xo[rows, :].astype(F32) + x1[rows, :] + bo[...]
            x1[rows, :] = row
            hat, _ = norm_rows(row)
            hg[me, rows, :] = (hat * g2[...] + b2[...]).astype(BF)
        rows_loop(st, 64, enter)
        g0.start()
        rows_loop(st, 64, enter, base=st)
    for cp in (later[0], later[1], later[3]):
        cp.wait()
    zero_fill(gbu)
    ay.side(0)

    def rest():
        ay.near2()
        ay.far()
        for which in range(1, 4):
            ay.side(which)

    def mlp(blk, stream):
        rows = pl.ds(pl.multiple_of(stream * st, st), st)
        pre = mm(hg[blk, rows, :], wu[...]) + bu[...]
        cot = mm(dy[blk, rows, :], wd[...], NT).astype(BF).astype(F32)
        sq = pre * pre
        th = jnp.tanh(GELU_C * (pre + 0.044715 * sq * pre))
        cdf = 0.5 * (1.0 + th)
        act[blk, rows, :] = (pre * cdf).astype(BF)
        slope = cdf + pre * (0.5 * (1.0 - th * th)) * (GELU_C * (1.0 + 3 * 0.044715 * sq))
        dp = cot * slope
        gbu[...] = gbu[...] + fold8(dp, jnp.add)
        dpb = dp.astype(BF)
        dpre[blk, rows, :] = dpb
        part[blk, rows, :] = mm(dpb, wu[...], NT).astype(BF)

    chips = (ring.xf, ring.xr, ring.xl, ring.x)
    def pairs(job):
        for xp in chips:
            job.send_pair(xp)

    def item(step):
        late = (step == 4) | (step == 5) | (step >= 10)
        pos = jnp.where(step < 4, step, jnp.where(step < 6, step - 4, jnp.where(step < 10, step - 2, step - 8)))
        mlp(ring.order(pos), jnp.where(late, 1, 0))

    with scope('b_gather'):
        hooked(2 * n, item, {
            1: [arrive(g0.side, 0)],
            2: [rest, g0.near1, g1s.start, g0.near2],
            5: [arrive(g1s.side, 0)],
            6: [arrive(g0.side, 1)],
            7: [arrive(g0.side, 2)],
            8: [g0.far],
            9: [arrive(g0.side, 3)],
            10: [arrive(pairs, r0), g1s.near1, r0.far, g1s.near2],
            12: [r0.near_own, arrive(g1s.side, 1)],
            13: [arrive(g1s.side, 2)],
            14: [g1s.far],
            15: [arrive(g1s.side, 3)]})
    with scope('b_far'):
        pairs(r1)
        r0.near_sum()
        r1.far()
    with scope('b_own'):
        r1.near_own()
    ay.finish()

    def weight_down(i):
        cols = pl.ds(pl.multiple_of(i * 256, 256), 256)
        left = act[:, :, cols].reshape(n * t, 256)
        gwd[cols, :] = mm(left, dy[...].reshape(n * t, d), T0).astype(BF)

    def weight_up(i):
        cols = pl.ds(pl.multiple_of(i * 256, 256), 256)
        left = hg[:, :, cols].reshape(n * t, 256)
        gwu[cols, :] = mm(left, dpre[...].reshape(n * t, f), T0).astype(BF)

    with scope('b_weights'):
        loop(0, f // 256, weight_down)
        loop(0, d // 256, weight_up)
    zero_fill(small)

    def down(blk):
        dy[blk] = mm(act[blk], wd[...]).astype(BF)

    def leave(rows):
        dg = rs.total(rows).astype(BF).astype(F32)
        hat, rstd = norm_rows(x1[rows, :])
        small[2] = small[2] + fold8(dg * hat, jnp.add)
        small[3] = small[3] + fold8(dg, jnp.add)
        dz = norm_back(dg * g2[...], hat, rstd)
        dyf = dyo[rows, :].astype(F32)
        dm = dyf + dz
        small[4] = small[4] + fold8(dm, jnp.add)
        small[5] = small[5] + fold8(dyf, jnp.add)
        mid[rows, :] = dm
        xg[me, rows, :] = dm.astype(BF)

    with scope('b_sum'):
        r1.near_sum()
    with scope('b_final'):
        r0.wait_final()
    with scope('b_leave'):
        rows_loop(st, 64, leave)
        g0.finish()
        d0.start()
    with scope('b_down'):
        loop(0, n, down)
        pairs(rm)
    with scope('b_final1'):
        r1.wait_final()
    with scope('b_leave1'):
        rows_loop(st, 64, leave, base=st)
        g1s.finish()
        d1.start()
    with scope('b_finish'):
        for job in (r0, r1):
            job.finish()
    reload = fetch(0, h_hbm, hg)

    def share(buf, off, send_sem, recv_sem):
        return pltpu.make_async_remote_copy(
            src_ref=buf.at[me], dst_ref=buf.at[me], send_sem=send_sem, recv_sem=recv_sem,
            device_id={'tp': (me + off) % n}, device_id_type=MESH)

    def all_in(buf, send_sem, recv_sem):
        return pltpu.make_async_remote_copy(
            src_ref=buf.at[most], dst_ref=buf.at[most], send_sem=send_sem, recv_sem=recv_sem,
            device_id={'tp': me}, device_id_type=MESH)

    def early_out():
        for i in range(4):
            early[me, i:i + 1, :] = col_sum(small[2 + i])
        for off in range(1, n):
            share(early, off, e_send, e_recv).start()

    def add_up(buf):
        total = buf[0]
        for b in range(1, n):
            total = total + buf[b]
        return total
    zero_fill(dk, dv)

    def back_block(i):
        dc = mm(xg[i], wof[me], NT).astype(BF)
        zero = jnp.zeros((t, 128), BF)
        prod = (dc.astype(F32) * o[i].astype(F32)).T
        dlt = (col_sum(prod[:64]), col_sum(prod[64:]))
        for head in PAIR:
            dom[head] = jnp.where(lane_mask(t, head), dc, zero)
        zero_fill(dqt)

        def pair_block(blocks, diag):
            cases = [(j, head) for j in blocks for head in PAIR]
            ps, dss = [], []
            for j, head in cases:
                s = mm(k[j], q[head, i], NT) + bt[head]
                if diag:
                    s = jnp.where(key <= qry, s, MASK_VALUE)
                p = jnp.exp(s + (slopes[head] * (j * t).astype(F32) - lse[head, i]))
                dp = mm(v[j], dom[head], NT).astype(BF).astype(F32)
                dss.append((p * (dp - dlt[head])).astype(BF))
                ps.append(p.astype(BF))
            wide = list(zip(cases, ps, dss))
            for j in blocks:
                dv[j] = dv[j] + sum(mm(p, dom[head]) for (b, head), p, _ in wide if b is j)
                dk[j] = dk[j] + sum(mm(ds, q[head, i]) for (b, head), _, ds in wide if b is j)
            for head in PAIR:
                rows = pl.ds(head * 64, 64)
                dqt[rows, :] = dqt[rows, :] + sum(mm(kt[b, rows, :], ds) for (b, h), _, ds in wide if h == head)

        twos(i, lambda blocks: pair_block(blocks, False))
        pair_block((i,), True)
        d3[i, :, :128] = (dqt[...].T * scale).astype(BF)

    def both_in(which):
        for job in (d0, d1):
            job.side(which)

    with scope('c_attend'):
        hooked(n, lambda step: back_block(ring.order(step)), {
            1: [arrive(both_in, 0), d0.near1, d0.near2],
            2: [d1.near1, rm.far, rm.near_own, d1.near2],
            4: [arrive(both_in, 1)],
            5: [arrive(both_in, 2)],
            6: [d0.far, d1.far, rm.near_sum],
            7: [arrive(both_in, 3)]})
    zero_fill(gbq)

    def back_in(xp):
        for cc in PAIR:
            blk = xp * 2 + cc
            d3[blk, :, 128:256] = dk[blk].astype(BF)
            d3[blk, :, 256:] = dv[blk].astype(BF)
            part[blk] = mm(d3[blk], wp[...]).astype(BF)
        rs.send_pair(xp)

    with scope('c_far'):
        back_in(ring.xf)
        rs.far()
    with scope('c_own'):
        back_in(ring.xr)
        back_in(ring.xl)
        rs.near_own()
        back_in(ring.x)
    reload.wait()

    def weight_in(i):
        cols = pl.ds(pl.multiple_of(i * 128, 128), 128)
        left = d3[:, :, cols].reshape(n * t, 128)
        grad = mm(left, hg[...].reshape(n * t, d), T0).astype(BF)
        for head in PAIR:
            gwt[head, i] = grad[head * 64:head * 64 + 64]

    def bias_in(b):
        gbq[...] = gbq[...] + fold8(d3[b].astype(F32), jnp.add)

    with scope('c_weights'):
        loop(0, len(TRIPLE), weight_in)
        loop(0, n, bias_in)
    with scope('c_sum'):
        rs.near_sum()
        early_out()
    with scope('c_gwo'):
        gwo[...] = mm(o[...].reshape(n * t, 128), xg[...].reshape(n * t, d), T0).astype(BF)
    with scope('c_mfinal'):
        rm.wait_final()

    def finish_y(rows):
        m = rm.total(rows).astype(BF).astype(F32)
        y[rows, :] = (x1[rows, :] + m + bd[...]).astype(BF)
    rows_loop(t, 64, finish_y)
    with scope('c_final'):
        rs.wait_final()

    def sum_in(rows):
        dh = rs.total(rows).astype(BF).astype(F32)
        hat, _ = norm_rows(xo[rows, :].astype(F32))
        small[0] = small[0] + fold8(dh * hat, jnp.add)
        small[1] = small[1] + fold8(dh, jnp.add)

    def last(rows):
        dh = rs.total(rows).astype(BF).astype(F32)
        hat, rstd = norm_rows(xo[rows, :].astype(F32))
        gx[rows, :] = (mid[rows, :] + norm_back(dh * g1[...], hat, rstd)).astype(BF)

    with scope('c_sums'):
        rows_loop(t, 64, sum_in)
    for i in PAIR:
        late[me, i:i + 1, :] = col_sum(small[i])
    with scope('c_share'):
        for off in range(1, n):
            share(late, off, l_send, l_recv).start()
        rows_loop(t, 64, last)
        all_in(early, e_send, e_recv).wait_recv()
        sums[2:6, :] = add_up(early)
        all_in(late, l_send, l_recv).wait_recv()
        sums[0:2, :] = add_up(late)
        all_in(early, e_send, e_recv).wait_send()
        all_in(late, l_send, l_recv).wait_send()
        all_in(o, o_send, o_recv).wait_send()
    with scope('d_finish'):
        for job in (rs, rm, d0, d1):
            job.finish()


def kernel_out(n_big, *refs):
    count = n_big + 3
    srcs, refs = refs[:count], refs[count:]
    outs, refs = refs[:n_big + 8], refs[n_big + 8:]
    bufs, tail, sem_out = srcs, refs[:-1], refs[-1]
    gbq, gbu, sums = bufs[n_big:]
    o_bq, o_bu, o_sums = tail
    kept = list(bufs[:n_big]) + [o_bq, o_bu] + [o_sums.at[i:i + 1] for i in range(6)]
    backs = [pltpu.make_async_copy(b, a, sem_out.at[i]) for i, (a, b) in enumerate(zip(outs, kept))]
    for back in backs[:n_big]:
        back.start()
    o_bu[...] = col_sum(gbu[...])
    row = col_sum(gbq[...])
    e = o_bq.shape[2]
    for part_no in TRIPLE:
        for head in PAIR:
            at = (part_no * 2 + head) * e
            o_bq[part_no, head:head + 1, :] = row[:, at:at + e]
    o_sums[...] = sums[...]
    for back in backs[n_big:]:
        back.start()
    for back in backs:
        back.wait()


def inside():
    return pl.BlockSpec(memory_space=VMEM)


def anywhere():
    return pl.BlockSpec(memory_space=pl.ANY)


def smem():
    return pl.BlockSpec(memory_space=pltpu.SMEM)


def solution(mesh):
    n = mesh.shape['tp']

    def local_step(x, ln1_gamma, ln1_beta, w_qkv, b_qkv, w_out, b_out, ln2_gamma, ln2_beta, w_up, b_up, w_down, b_down, grad_y):
        t, d = x.shape[1], x.shape[2]
        heads, e = w_qkv.shape[1], w_qkv.shape[3]
        he = heads * e
        f = w_up.shape[1]
        scale = e ** -0.5
        slopes = jnp.asarray(alibi_slopes(heads * n))
        x2, dy2 = x[0], grad_y[0]
        row = lambda vec: vec.reshape(1, -1)
        wt = w_qkv.transpose(1, 2, 3, 0).reshape(heads * 3 * e, d)
        bq = b_qkv.transpose(1, 0, 2)
        sds = jax.ShapeDtypeStruct
        rows, full, half = (t, d), (n, t, d), (n, t, he)
        both, line = (len(PAIR),) + half, (len(PAIR), n, 1, t)
        packed = (len(TRIPLE) * he, d)
        params = lambda cid: pltpu.CompilerParams(collective_id=cid, has_side_effects=True, vmem_limit_bytes=VLIM)
        dma = pltpu.SemaphoreType.DMA

        vm = lambda dims, kind=BF: VMEM(dims, kind)
        stat, turned = (len(PAIR), 8, t), (n, he, t)
        vecs = (row(ln1_gamma), row(ln1_beta), bq, row(b_out), row(ln2_gamma), row(ln2_beta), row(b_up), row(b_down))
        results = [sds(rows, BF), sds(rows, BF), sds((8, d), F32), sds((heads, len(TRIPLE), e, d), BF),
                   sds((8, len(TRIPLE) * he), F32), sds((he, d), BF), sds((d, f), BF), sds((8, f), F32), sds((f, d), BF)]
        y, gx, sums, gwt, gbq, gwo, gwu, gbu, gwd, _ = pl.pallas_call(
            functools.partial(kernel_main, n, scale, len(vecs), len(results)),
            name='layer',
            out_shape=[vm(b.shape, b.dtype) for b in results] + [sds(full, BF)],
            in_specs=[anywhere()] * (6 + len(vecs)) + [smem()],
            out_specs=[inside()] * len(results) + [anywhere()],
            scratch_shapes=[vm(b.shape, b.dtype) for b in vecs] + [vm(full), vm(rows), vm(rows), vm(full), vm(full), vm(packed), vm(packed), vm((n, he, d)),
                            vm((d, f)), vm((f, d)), vm(both), vm(half), vm(half), vm(turned), vm(turned), vm(half),
                            vm(line, F32), vm(rows), vm((len(PAIR), n, t, t), F32), vm(stat, F32), vm(stat, F32),
                            vm((he, t), F32), vm((len(PAIR), t, t), F32), vm(rows, F32), vm((n, t, f)), vm((n, t, f)),
                            vm(rows, F32), vm((len(PAIR), t, he)), vm((he, t), F32), vm(half, F32), vm(half, F32),
                            vm((n, t, len(TRIPLE) * he)), vm((6, 8, d), F32), vm((n, 4, d), F32), vm((n, 2, d), F32), vm(full)]
            + scatter_buffers(n, t, d) * 2 + scatter_sems() * 3 + gather_sems() * 3 + [dma((n,))] * 2 + [dma((len(vecs),))],
            compiler_params=params(0),
        )(x2, dy2, wt, w_out, w_up, w_down, *vecs, slopes)

        big = (y, gx, gwt, gwo, gwu, gwd)
        little = (gbq, gbu, sums)
        bias_dims, up_dims = (len(TRIPLE), heads, e), (1, f)
        res = pl.pallas_call(
            functools.partial(kernel_out, len(big)),
            name='results',
            compiler_params=pltpu.CompilerParams(vmem_limit_bytes=8 * 1024 * 1024),
            out_shape=[sds(b.shape, b.dtype) for b in big] + [sds(bias_dims, F32), sds(up_dims, F32)] + [sds((1, d), F32)] * 6,
            in_specs=[inside()] * (len(big) + 3),
            out_specs=[anywhere()] * (len(big) + 8),
            scratch_shapes=[vm(bias_dims, F32), vm(up_dims, F32), vm((8, d), F32), dma((len(big) + 8,))],
        )(*big, *little)
        y, gx, gwt, gwo, gwu, gwd, gbq, gbu, s_g1, s_b1, s_g2, s_b2, s_bo, s_bd = res
        vec = lambda a: a.reshape(-1)
        return (y[None], gx[None], vec(s_g1), vec(s_b1), gwt.transpose(3, 0, 1, 2), gbq.transpose(1, 0, 2), gwo, vec(s_bo),
                vec(s_g2), vec(s_b2), gwu, vec(gbu), gwd, vec(s_bd))

    row_spec = P('dp', 'tp', None)
    in_specs = (row_spec, P(), P(), P(None, 'tp', None, None), P('tp', None, None), P('tp', None), P(), P(), P(),
                P(None, 'tp'), P('tp'), P('tp', None), P(), row_spec)
    out_specs = (row_spec, row_spec, P('dp'), P('dp'), P('dp', 'tp', None, None), P(('dp', 'tp'), None, None),
                 P(('dp', 'tp'), None), P('dp'), P('dp'), P('dp'), P('dp', 'tp'), P(('dp', 'tp')), P(('dp', 'tp'), None), P('dp'))
    return jax.shard_map(local_step, mesh=mesh, in_specs=in_specs, out_specs=out_specs, check_vma=False)
```

```python
import functools
import math
import jax
import jax.numpy as jnp
import numpy as np
from jax import lax
from jax.experimental import pallas as pl
from jax.experimental.pallas import tpu as pltpu
from jax.sharding import PartitionSpec as P

EPS = 1e-5
MASK_VALUE = -1e30
BF, F32 = jnp.bfloat16, jnp.float32
VMEM = pltpu.VMEM
MESH = pl.DeviceIdType.MESH
scope = jax.named_scope
VLIM = 58 * 1024 * 1024
GELU_C = math.sqrt(2.0 / math.pi)
PAIR = LOW, HIGH = (0, 1)
TRIPLE = (0, 1, 2)
NN = (((1,), (0,)), ((), ()))
T0 = (((0,), (0,)), ((), ()))
NT = (((1,), (1,)), ((), ()))


def alibi_slopes(n_heads):
    closest = 2 ** int(math.floor(math.log2(n_heads)))
    base_ratio = 2.0 ** (-8.0 / closest)
    extra_ratio = 2.0 ** (-4.0 / closest)
    remaining = min(closest, n_heads - closest)
    slopes = [base_ratio ** (i + 1) for i in range(closest)]
    slopes = slopes + [extra_ratio ** (2 * i + 1) for i in range(remaining)]
    return np.array(slopes, dtype=np.float32)


def mm(a, b, dims=NN):
    return lax.dot_general(a, b, dims, preferred_element_type=F32)


def loop(lo, hi, body, unroll=1):
    def step(i, carry):
        body(i)
        return carry
    lax.fori_loop(lo, hi, step, 0, unroll=unroll)


def twos(count, body):
    loop(0, count // 2, lambda i: body((2 * i, 2 * i + 1)))

    @pl.when(count % 2 == 1)
    def _():
        body((count - 1,))


def rows_loop(total, rows, body, base=0):
    loop(0, total // rows, lambda r: body(pl.ds(pl.multiple_of(base + r * rows, rows), rows)))


def row_mean(z):
    return jnp.mean(z, axis=-1, keepdims=True)


def col_sum(z):
    return jnp.sum(z, axis=0, keepdims=True)


def norm_back(grad, hat, rstd):
    return rstd * (grad - row_mean(grad) - hat * row_mean(grad * hat))


def zero_fill(*refs):
    for ref in refs:
        ref[...] = jnp.zeros(ref.shape, ref.dtype)


def sort_weight(wp, wt):
    e = wp.shape[0] // 6
    for part_no in TRIPLE:
        for head in PAIR:
            dst = (part_no * 2 + head) * e
            src = (head * 3 + part_no) * e
            wp[dst:dst + e, :] = wt[src:src + e, :]


def norm_rows(z):
    cen = z - row_mean(z)
    rstd = lax.rsqrt(row_mean(cen * cen) + EPS)
    return cen * rstd, rstd


def fold8(v, op):
    out = v[0:8]
    for k in range(1, v.shape[0] // 8):
        out = op(out, v[8 * k:8 * k + 8])
    return out


class Ring:
    def __init__(self, n):
        self.n = n
        nx = n // 2
        self.me = lax.axis_index('tp')
        self.x = self.me // 2
        self.c = self.me % 2
        self.nx = nx
        self.xr = (self.x + 1) % nx
        self.xl = (self.x + nx - 1) % nx
        self.xf = (self.x + 2) % nx
        self.right = self.xr * 2 + self.c
        self.left = self.xl * 2 + self.c
        self.far = self.xf * 2 + self.c
        other = 1 - self.c
        self.partner = self.x * 2 + other
        self.others = [xp * 2 + other for xp in (self.x, self.xl, self.xr, self.xf)]

    def order(self, s):
        odd = s % 2
        dx = jnp.where(s < 2, 0, jnp.where(s >= 6, 2, jnp.where(odd == 0, self.nx - 1, 1)))
        mid = jnp.where(s < 4, 0, 1)
        dc = jnp.where(s < 2, odd, jnp.where(s >= 6, odd, mid))
        return ((self.x + dx) % self.nx) * 2 + (self.c + dc) % 2

    def barrier(self):
        sem = pltpu.get_barrier_semaphore()
        peers = [self.right, self.left, self.partner]
        for peer in peers:
            pl.semaphore_signal(sem, inc=1, device_id={'tp': peer}, device_id_type=MESH)
        pl.semaphore_wait(sem, len(peers))


class Gather:
    LEFT, RIGHT, FAR, SIDE = 0, 2, 4, 6
    SLOTS = 10

    def __init__(self, ring, buf, ssem, rsem, base=0, size=None, cut=None):
        self.ring, self.buf, self.ssem, self.rsem = ring, buf, ssem, rsem
        self.base = base
        self.size = size or buf.shape[1]
        self.cut = cut or self.size // 2
        self.drained = False

    def rows(self, half):
        if half == LOW:
            return pl.ds(self.base, self.cut)
        return pl.ds(self.base + self.cut, self.size - self.cut)

    def copy(self, ref, dev, slot, onward):
        return pltpu.make_async_remote_copy(
            src_ref=ref, dst_ref=ref, send_sem=self.ssem.at[onward], recv_sem=self.rsem.at[slot],
            device_id={'tp': dev}, device_id_type=MESH)

    def send(self, blk, half, dev, slot, onward=LOW):
        self.copy(self.buf.at[blk, self.rows(half)], dev, slot, onward).start()

    def wait(self, blk, half, slot):
        self.copy(self.buf.at[blk, self.rows(half)], self.ring.me, slot, LOW).wait_recv()

    def side(self, which):
        ref = self.buf.at[self.ring.others[which], pl.ds(self.base, self.size)]
        self.copy(ref, self.ring.me, self.SIDE + which, LOW).wait_recv()

    def start(self):
        r = self.ring
        for half in PAIR:
            self.send(r.me, half, r.right, self.LEFT + half)
            self.send(r.me, HIGH - half, r.left, self.RIGHT + HIGH - half)
        for half in PAIR:
            self.send(r.me, half, r.partner, self.SIDE)

    def near1(self):
        r = self.ring
        self.wait(r.left, LOW, self.LEFT)
        self.send(r.left, LOW, r.right, self.FAR, HIGH)
        self.send(r.left, LOW, r.partner, self.SIDE + 1)
        self.wait(r.right, HIGH, self.RIGHT + HIGH)
        self.send(r.right, HIGH, r.left, self.FAR + HIGH, HIGH)
        self.send(r.right, HIGH, r.partner, self.SIDE + 2)

    def near2(self):
        r = self.ring
        self.wait(r.left, HIGH, self.LEFT + HIGH)
        self.send(r.left, HIGH, r.partner, self.SIDE + 1)
        self.wait(r.right, LOW, self.RIGHT)
        self.send(r.right, LOW, r.partner, self.SIDE + 2)

    def far(self):
        r = self.ring
        for half in PAIR:
            self.wait(r.far, half, self.FAR + half)
            self.send(r.far, half, r.partner, self.SIDE + 3)

    def gone(self, blocks, onward):
        ref = self.buf.at[pl.ds(0, blocks), pl.ds(self.base, self.size)]
        self.copy(ref, self.ring.right, LOW, onward).wait_send()

    def drain(self):
        self.gone(1, HIGH)
        self.drained = True

    def finish(self):
        self.gone(6, LOW)
        if not self.drained:
            self.gone(1, HIGH)


class Scatter:
    def __init__(self, ring, part, pair, stage, land, ssem, rsem, base=0, size=None):
        self.ring, self.part, self.pair, self.stage, self.land = ring, part, pair, stage, land
        self.ssem, self.rsem = ssem, rsem
        self.base = base
        self.size = size or part.shape[1]
        self.half = self.size // 2

    def cp_pair(self, xp):
        r = self.ring
        rows = pl.ds(self.base, self.size)
        return pltpu.make_async_remote_copy(
            src_ref=self.part.at[xp * 2 + (1 - r.c), rows], dst_ref=self.pair.at[xp, rows], send_sem=self.ssem.at[LOW],
            recv_sem=self.rsem.at[xp], device_id={'tp': r.partner}, device_id_type=MESH)

    def cp(self, slot, half, dst_slot, dev):
        rows = pl.ds(self.base + half * self.half, self.half)
        return pltpu.make_async_remote_copy(
            src_ref=self.stage.at[slot, rows], dst_ref=self.land.at[dst_slot, rows],
            send_sem=self.ssem.at[HIGH], recv_sem=self.rsem.at[4 + 2 * dst_slot + half],
            device_id={'tp': dev}, device_id_type=MESH)

    def wait_land(self, dst_slot, half):
        self.cp(0, half, dst_slot, self.ring.me).wait_recv()

    def wait_pair(self, xp):
        self.cp_pair(xp).wait_recv()

    def send_pair(self, xp):
        self.cp_pair(xp).start()

    def mix(self, slot, xp, half, with_far=False):
        blk = xp * 2 + self.ring.c
        step = 32

        def body(i):
            rows = pl.ds(pl.multiple_of(self.base + half * self.half + i * step, step), step)
            total = self.part[blk, rows, :].astype(F32) + self.pair[xp, rows, :].astype(F32)
            if with_far:
                total = total + self.land[0, rows, :].astype(F32)
            self.stage[slot, rows, :] = total.astype(BF)
        loop(0, self.half // step, body)

    def far(self):
        r = self.ring
        self.wait_pair(r.xf)
        self.mix(0, r.xf, 0)
        self.cp(0, 0, 0, r.right).start()
        self.mix(0, r.xf, 1)
        self.cp(0, 1, 0, r.left).start()

    def near_own(self):
        r = self.ring
        self.wait_pair(r.xr)
        self.mix(1, r.xr, 1)
        self.cp(1, 1, 1, r.right).start()
        self.wait_pair(r.xl)
        self.mix(2, r.xl, 0)
        self.cp(2, 0, 2, r.left).start()

    def near_sum(self):
        r = self.ring
        self.wait_land(0, 0)
        self.mix(1, r.xr, 0, with_far=True)
        self.cp(1, 0, 1, r.right).start()
        self.wait_land(0, 1)
        self.mix(2, r.xl, 1, with_far=True)
        self.cp(2, 1, 2, r.left).start()

    def wait_final(self):
        self.wait_pair(self.ring.x)
        for slot in (1, 2):
            for half in PAIR:
                self.wait_land(slot, half)

    def total(self, rows):
        r = self.ring
        return (self.part[r.me, rows, :].astype(F32) + self.pair[r.x, rows, :].astype(F32)
                + self.land[1, rows, :].astype(F32) + self.land[2, rows, :].astype(F32))

    def finish(self):
        r = self.ring
        rows = pl.ds(self.base, self.size)
        for ref, which in ((self.pair.at[:, rows], LOW), (self.stage.at[:, rows], HIGH)):
            pltpu.make_async_remote_copy(
                src_ref=ref, dst_ref=ref, send_sem=self.ssem.at[which], recv_sem=self.rsem.at[0],
                device_id={'tp': r.partner}, device_id_type=MESH).wait_send()


def scatter_buffers(n, rows, d):
    return [VMEM((n // 2, rows, d), BF), VMEM((3, rows, d), BF), VMEM((3, rows, d), BF)]


def scatter_sems():
    return [pltpu.SemaphoreType.DMA((2,)), pltpu.SemaphoreType.DMA((4 + 6,))]


def hooked(count, body, hooks):
    def step(i):
        for at, actions in hooks.items():
            @pl.when(i == at)
            def _():
                for act in actions:
                    act()
        body(i)
    loop(0, count, step)


def gather_sems():
    return [pltpu.SemaphoreType.DMA((2,)), pltpu.SemaphoreType.DMA((Gather.SLOTS,))]


def lane_mask(rows, h):
    lane = lax.broadcasted_iota(jnp.int32, (rows, 128), 1)
    return (lane < 64) if h == 0 else (lane >= 64)


def attend_block(i, q_ref, k_ref, vt_ref, o_ref, lse_ref, s_ref, m_ref, l_ref, acc_ref, bt_ref, slopes):
    t = q_ref.shape[2]
    e = acc_ref.shape[0] // 2
    key = lax.broadcasted_iota(jnp.int32, (t, t), 0)
    qry = lax.broadcasted_iota(jnp.int32, (t, t), 1)
    for h in PAIR:
        m_ref[h] = jnp.full((8, t), MASK_VALUE, F32)
        l_ref[h] = jnp.zeros((8, t), F32)
    zero_fill(acc_ref)

    def shift(h, j):
        return slopes[h] * (j * t).astype(F32)

    def score(blocks, diag):
        top = [m_ref[h] for h in PAIR]
        for j in blocks:
            for h in PAIR:
                s = mm(k_ref[j], q_ref[h, i], NT) + bt_ref[h]
                if diag:
                    s = jnp.where(key <= qry, s, MASK_VALUE)
                s_ref[h, j] = s
                top[h] = jnp.maximum(top[h], fold8(s, jnp.maximum) + shift(h, j))
        for h in PAIR:
            m_ref[h] = top[h]

    twos(i, lambda blocks: score(blocks, False))
    score((i,), True)
    top = [jnp.max(m_ref[h], axis=0, keepdims=True) for h in PAIR]

    def denom(j):
        for h in PAIR:
            l_ref[h] = l_ref[h] + fold8(jnp.exp(s_ref[h, j] + (shift(h, j) - top[h])), jnp.add)

    loop(0, i + 1, denom)
    for h in PAIR:
        lse_ref[h, i] = top[h] + jnp.log(col_sum(l_ref[h]))

    def values(blocks):
        for h in PAIR:
            rows = pl.ds(h * e, e)
            total = acc_ref[rows, :]
            for j in blocks:
                p = jnp.exp(s_ref[h, j] + (shift(h, j) - lse_ref[h, i])).astype(BF)
                total = total + mm(vt_ref[j, rows, :], p)
            acc_ref[rows, :] = total

    twos(i + 1, values)
    o_ref[i] = acc_ref[...].T.astype(BF)


def kernel_main(n, scale, n_vec, n_out, x_hbm, dy_hbm, wt_hbm, wo_hbm, wu_hbm, wd_hbm, *refs):
    vec_hbm, (slopes_ref,), refs = refs[:n_vec], refs[n_vec:n_vec + 1], refs[n_vec + 1:]
    results, (h_hbm,), refs = refs[:n_out], refs[n_out:n_out + 1], refs[n_out + 1:]
    vecs, refs = refs[:n_vec], refs[n_vec:]
    run_layer(n, scale, vec_hbm, vecs, results, x_hbm, dy_hbm, wt_hbm, wo_hbm, wu_hbm, wd_hbm, slopes_ref, h_hbm, *refs)


def run_layer(n, scale, vec_hbm, vecs, results, x_hbm, dy_hbm, wt_hbm, wo_hbm, wu_hbm, wd_hbm, slopes_ref, h_hbm,
                xg, xo, dyo, dy, hg, wt, wp, wof, wu, wd, q, k, v, kt, vt, o, lse, orow, s_ref, m_ref, l_ref, acc, bt,
                x1, act, dpre, mid, dom, dqt, dk, dv, d3, small, early, late, part,
                *rest):
    g1, b1, bqkv, bo, g2, b2, bu, bd = vecs
    y, gx, sums, gwt, gbq, gwo, gwu, gbu, gwd = results
    rest = list(rest)

    def take(count):
        head = rest[:count]
        del rest[:count]
        return head

    ring = Ring(n)
    me = ring.me
    t, d, f = xg.shape[1], xg.shape[2], wu.shape[1]
    rs_bufs, rm_bufs = take(3), take(3)
    st = t // 2
    streams = (0, st)
    r_sems = [take(2) for _ in PAIR]
    r0, r1 = [Scatter(ring, part, *rs_bufs, *sems, base=base, size=st) for base, sems in zip(streams, r_sems)]
    rs = Scatter(ring, part, *rs_bufs, *r_sems[0])
    rm = Scatter(ring, dy, *rm_bufs, *take(2))
    g_sems = [take(2) for _ in PAIR]
    ax, aw = [Gather(ring, buf, *sems) for buf, sems in zip((xg, wof), g_sems)]
    ay = Gather(ring, dy, *take(2), cut=3 * t // 4)
    g0, g1s = [Gather(ring, hg, *sems, base=base, size=st) for base, sems in zip(streams, g_sems)]
    d0, d1 = [Gather(ring, xg, *sems, base=base, size=st) for base, sems in zip(streams, g_sems)]
    few, local, vec_sem = take(3)
    o_send, o_recv, e_send, e_recv, l_send, l_recv = [few.at[i] for i in range(6)]

    def fetch(i, src, dst):
        cp = pltpu.make_async_copy(src, dst, local.at[i])
        cp.start()
        return cp

    in_x, in_wo, in_dy, in_wt = (fetch(0, x_hbm, xg.at[me]), fetch(1, wo_hbm, wof.at[me]),
                                 fetch(2, dy_hbm, dy.at[me]), fetch(3, wt_hbm, wt))
    later = [fetch(4, wu_hbm, wu), fetch(5, wd_hbm, wd), fetch(6, x_hbm, xo), fetch(7, dy_hbm, dyo)]
    vec_in = [pltpu.make_async_copy(a, b, vec_sem.at[i]) for i, (a, b) in enumerate(zip(vec_hbm, vecs))]
    for cp in vec_in:
        cp.start()
    ring.barrier()
    in_x.wait()
    ax.start()
    for cp in vec_in:
        cp.wait()
    in_wt.wait()
    sort_weight(wp, wt)
    in_wo.wait()
    in_dy.wait()
    bias = jnp.concatenate([bqkv[kind, head:head + 1, :] for kind in TRIPLE for head in PAIR], axis=1)

    def project(blk):
        def norm(rows):
            hat, _ = norm_rows(xg[blk, rows, :].astype(F32))
            hg[blk, rows, :] = (hat * g1[...] + b1[...]).astype(BF)
        rows_loop(t, 64, norm)
        out = mm(hg[blk], wp[...], NT) + bias
        out = out.astype(BF)
        zero = jnp.zeros((t, 128), BF)
        qs = (out[:, :128].astype(F32) * scale).astype(BF)
        for head in PAIR:
            q[head, blk] = jnp.where(lane_mask(t, head), qs, zero)
        k[blk] = out[:, 128:256]
        v[blk] = out[:, 256:]
        kt[blk] = out[:, 128:256].T
        vt[blk] = out[:, 256:].T
        fetch(0, hg.at[blk], h_hbm.at[blk])

    arrive = functools.partial
    with scope('a_gather'):
        hooked(n, lambda step: project(ring.order(step)), {
            1: [arrive(ax.side, 0)],
            2: [ax.near1, ax.near2],
            4: [arrive(ax.side, 1)],
            5: [arrive(ax.side, 2)],
            6: [ax.drain, aw.start, ax.far, ay.start],
            7: [arrive(ax.side, 3)]})
    slopes = [slopes_ref[me * 2 + head] for head in PAIR]
    key = lax.broadcasted_iota(jnp.int32, (t, t), 0)
    qry = lax.broadcasted_iota(jnp.int32, (t, t), 1)
    for head in PAIR:
        bt[head] = slopes[head] * key.astype(F32)

    def send_o(i):
        cols = pl.ds(pl.multiple_of(me * 128, 128), 128)
        return pltpu.make_async_remote_copy(
            src_ref=o.at[i], dst_ref=orow.at[:, cols], send_sem=o_send, recv_sem=o_recv,
            device_id={'tp': i}, device_id_type=MESH)

    def one_block(step):
        i = ring.order(n - 1 - step)
        attend_block(i, q, k, vt, o, lse, s_ref, m_ref, l_ref, acc, bt, slopes)

        @pl.when(step < n - 1)
        def _():
            send_o(i).start()

    with scope('a_attend'):
        ax.finish()
        pltpu.make_async_copy(hg, h_hbm, local.at[0]).wait()
        hooked(n, one_block, {4: [aw.near1], 5: [aw.near2]})
    most = pl.ds(0, n - 1)
    with scope('a_wait'):
        aw.far()
        ay.near1()
        orow[:, pl.ds(pl.multiple_of(me * 128, 128), 128)] = o[me]
        wide = orow.at[:, pl.ds(0, (n - 1) * 128)]
        pltpu.make_async_remote_copy(
            src_ref=wide, dst_ref=wide, send_sem=o_send, recv_sem=o_recv,
            device_id={'tp': me}, device_id_type=MESH).wait_recv()
        for which in range(4):
            aw.side(which)
        aw.finish()
        later[2].wait()
    with scope('a_out'):
        x1[...] = mm(orow[...], wof[...].reshape(n * 128, d)).astype(BF).astype(F32)

        def enter(rows):
            row = xo[rows, :].astype(F32) + x1[rows, :] + bo[...]
            x1[rows, :] = row
            hat, _ = norm_rows(row)
            hg[me, rows, :] = (hat * g2[...] + b2[...]).astype(BF)
        rows_loop(st, 64, enter)
        g0.start()
        rows_loop(st, 64, enter, base=st)
    for cp in (later[0], later[1], later[3]):
        cp.wait()
    zero_fill(gbu)
    ay.side(0)

    def rest():
        ay.near2()
        ay.far()
        for which in range(1, 4):
            ay.side(which)

    def mlp(blk, stream):
        rows = pl.ds(pl.multiple_of(stream * st, st), st)
        pre = mm(hg[blk, rows, :], wu[...]) + bu[...]
        cot = mm(dy[blk, rows, :], wd[...], NT).astype(BF).astype(F32)
        sq = pre * pre
        th = jnp.tanh(GELU_C * (pre + 0.044715 * sq * pre))
        cdf = 0.5 * (1.0 + th)
        act[blk, rows, :] = (pre * cdf).astype(BF)
        slope = cdf + pre * (0.5 * (1.0 - th * th)) * (GELU_C * (1.0 + 3 * 0.044715 * sq))
        dp = cot * slope
        gbu[...] = gbu[...] + fold8(dp, jnp.add)
        dpb = dp.astype(BF)
        dpre[blk, rows, :] = dpb
        part[blk, rows, :] = mm(dpb, wu[...], NT).astype(BF)

    chips = (ring.xf, ring.xr, ring.xl, ring.x)
    def pairs(job):
        for xp in chips:
            job.send_pair(xp)

    def item(step):
        late = (step == 4) | (step == 5) | (step >= 10)
        pos = jnp.where(step < 4, step, jnp.where(step < 6, step - 4, jnp.where(step < 10, step - 2, step - 8)))
        mlp(ring.order(pos), jnp.where(late, 1, 0))

    with scope('b_gather'):
        hooked(2 * n, item, {
            1: [arrive(g0.side, 0)],
            2: [rest, g0.near1, g1s.start, g0.near2],
            5: [arrive(g1s.side, 0)],
            6: [arrive(g0.side, 1)],
            7: [arrive(g0.side, 2)],
            8: [g0.far],
            9: [arrive(g0.side, 3)],
            10: [arrive(pairs, r0), g1s.near1, r0.far, g1s.near2],
            12: [r0.near_own, arrive(g1s.side, 1)],
            13: [arrive(g1s.side, 2)],
            14: [g1s.far],
            15: [arrive(g1s.side, 3)]})
    with scope('b_far'):
        pairs(r1)
        r0.near_sum()
        r1.far()
    with scope('b_own'):
        r1.near_own()
    ay.finish()

    def weight_down(i):
        cols = pl.ds(pl.multiple_of(i * 256, 256), 256)
        left = act[:, :, cols].reshape(n * t, 256)
        gwd[cols, :] = mm(left, dy[...].reshape(n * t, d), T0).astype(BF)

    def weight_up(i):
        cols = pl.ds(pl.multiple_of(i * 256, 256), 256)
        left = hg[:, :, cols].reshape(n * t, 256)
        gwu[cols, :] = mm(left, dpre[...].reshape(n * t, f), T0).astype(BF)

    with scope('b_weights'):
        loop(0, f // 256, weight_down)
        loop(0, d // 256, weight_up)
    zero_fill(small)

    def down(blk):
        dy[blk] = mm(act[blk], wd[...]).astype(BF)

    def leave(rows):
        dg = rs.total(rows).astype(BF).astype(F32)
        hat, rstd = norm_rows(x1[rows, :])
        small[2] = small[2] + fold8(dg * hat, jnp.add)
        small[3] = small[3] + fold8(dg, jnp.add)
        dz = norm_back(dg * g2[...], hat, rstd)
        dyf = dyo[rows, :].astype(F32)
        dm = dyf + dz
        small[4] = small[4] + fold8(dm, jnp.add)
        small[5] = small[5] + fold8(dyf, jnp.add)
        mid[rows, :] = dm
        xg[me, rows, :] = dm.astype(BF)

    with scope('b_sum'):
        r1.near_sum()
    with scope('b_final'):
        r0.wait_final()
    with scope('b_leave'):
        rows_loop(st, 64, leave)
        g0.finish()
        d0.start()
    with scope('b_down'):
        loop(0, n, down)
        pairs(rm)
    with scope('b_final1'):
        r1.wait_final()
    with scope('b_leave1'):
        rows_loop(st, 64, leave, base=st)
        g1s.finish()
        d1.start()
    with scope('b_finish'):
        for job in (r0, r1):
            job.finish()
    reload = fetch(0, h_hbm, hg)

    def share(buf, off, send_sem, recv_sem):
        return pltpu.make_async_remote_copy(
            src_ref=buf.at[me], dst_ref=buf.at[me], send_sem=send_sem, recv_sem=recv_sem,
            device_id={'tp': (me + off) % n}, device_id_type=MESH)

    def all_in(buf, send_sem, recv_sem):
        return pltpu.make_async_remote_copy(
            src_ref=buf.at[most], dst_ref=buf.at[most], send_sem=send_sem, recv_sem=recv_sem,
            device_id={'tp': me}, device_id_type=MESH)

    def early_out():
        for i in range(4):
            early[me, i:i + 1, :] = col_sum(small[2 + i])
        for off in range(1, n):
            share(early, off, e_send, e_recv).start()

    def add_up(buf):
        total = buf[0]
        for b in range(1, n):
            total = total + buf[b]
        return total
    zero_fill(dk, dv)

    def back_block(i):
        dc = mm(xg[i], wof[me], NT).astype(BF)
        zero = jnp.zeros((t, 128), BF)
        prod = (dc.astype(F32) * o[i].astype(F32)).T
        dlt = (col_sum(prod[:64]), col_sum(prod[64:]))
        for head in PAIR:
            dom[head] = jnp.where(lane_mask(t, head), dc, zero)
        zero_fill(dqt)

        def pair_block(blocks, diag):
            cases = [(j, head) for j in blocks for head in PAIR]
            ps, dss = [], []
            for j, head in cases:
                s = mm(k[j], q[head, i], NT) + bt[head]
                if diag:
                    s = jnp.where(key <= qry, s, MASK_VALUE)
                p = jnp.exp(s + (slopes[head] * (j * t).astype(F32) - lse[head, i]))
                dp = mm(v[j], dom[head], NT).astype(BF).astype(F32)
                dss.append((p * (dp - dlt[head])).astype(BF))
                ps.append(p.astype(BF))
            wide = list(zip(cases, ps, dss))
            for j in blocks:
                dv[j] = dv[j] + sum(mm(p, dom[head]) for (b, head), p, _ in wide if b is j)
                dk[j] = dk[j] + sum(mm(ds, q[head, i]) for (b, head), _, ds in wide if b is j)
            for head in PAIR:
                rows = pl.ds(head * 64, 64)
                dqt[rows, :] = dqt[rows, :] + sum(mm(kt[b, rows, :], ds) for (b, h), _, ds in wide if h == head)

        twos(i, lambda blocks: pair_block(blocks, False))
        pair_block((i,), True)
        d3[i, :, :128] = (dqt[...].T * scale).astype(BF)

    def both_in(which):
        for job in (d0, d1):
            job.side(which)

    with scope('c_attend'):
        hooked(n, lambda step: back_block(ring.order(step)), {
            1: [arrive(both_in, 0), d0.near1, d0.near2],
            2: [d1.near1, rm.far, rm.near_own, d1.near2],
            4: [arrive(both_in, 1)],
            5: [arrive(both_in, 2)],
            6: [d0.far, d1.far, rm.near_sum],
            7: [arrive(both_in, 3)]})
    zero_fill(gbq)

    def back_in(xp):
        for off in (1, 0):
            blk = xp * 2 + (ring.c + off) % 2
            d3[blk, :, 128:256] = dk[blk].astype(BF)
            d3[blk, :, 256:] = dv[blk].astype(BF)
            part[blk] = mm(d3[blk], wp[...]).astype(BF)
            if off:
                rs.send_pair(xp)

    with scope('c_far'):
        back_in(ring.xf)
        rs.far()
    with scope('c_own'):
        back_in(ring.xr)
        back_in(ring.xl)
        rs.near_own()
        back_in(ring.x)
    reload.wait()

    def weight_in(i):
        cols = pl.ds(pl.multiple_of(i * 128, 128), 128)
        left = d3[:, :, cols].reshape(n * t, 128)
        grad = mm(left, hg[...].reshape(n * t, d), T0).astype(BF)
        for head in PAIR:
            gwt[head, i] = grad[head * 64:head * 64 + 64]

    def bias_in(b):
        gbq[...] = gbq[...] + fold8(d3[b].astype(F32), jnp.add)

    with scope('c_weights'):
        loop(0, len(TRIPLE), weight_in)
        loop(0, n, bias_in)
    with scope('c_sum'):
        rs.near_sum()
        early_out()
    with scope('c_gwo'):
        gwo[...] = mm(o[...].reshape(n * t, 128), xg[...].reshape(n * t, d), T0).astype(BF)
    with scope('c_mfinal'):
        rm.wait_final()

    def finish_y(rows):
        m = rm.total(rows).astype(BF).astype(F32)
        y[rows, :] = (x1[rows, :] + m + bd[...]).astype(BF)
    rows_loop(t, 64, finish_y)
    with scope('c_final'):
        rs.wait_final()

    def sum_in(rows):
        dh = rs.total(rows).astype(BF).astype(F32)
        hat, _ = norm_rows(xo[rows, :].astype(F32))
        small[0] = small[0] + fold8(dh * hat, jnp.add)
        small[1] = small[1] + fold8(dh, jnp.add)

    def last(rows):
        dh = rs.total(rows).astype(BF).astype(F32)
        hat, rstd = norm_rows(xo[rows, :].astype(F32))
        gx[rows, :] = (mid[rows, :] + norm_back(dh * g1[...], hat, rstd)).astype(BF)

    with scope('c_sums'):
        rows_loop(t, 64, sum_in)
    for i in PAIR:
        late[me, i:i + 1, :] = col_sum(small[i])
    with scope('c_share'):
        for off in range(1, n):
            share(late, off, l_send, l_recv).start()
        rows_loop(t, 64, last)
        all_in(early, e_send, e_recv).wait_recv()
        sums[2:6, :] = add_up(early)
        all_in(late, l_send, l_recv).wait_recv()
        sums[0:2, :] = add_up(late)
        all_in(early, e_send, e_recv).wait_send()
        all_in(late, l_send, l_recv).wait_send()
        all_in(o, o_send, o_recv).wait_send()
    with scope('d_finish'):
        for job in (rs, rm, d0, d1):
            job.finish()


def kernel_out(n_big, *refs):
    count = n_big + 3
    srcs, refs = refs[:count], refs[count:]
    outs, refs = refs[:n_big + 8], refs[n_big + 8:]
    bufs, tail, sem_out = srcs, refs[:-1], refs[-1]
    gbq, gbu, sums = bufs[n_big:]
    o_bq, o_bu, o_sums = tail
    kept = list(bufs[:n_big]) + [o_bq, o_bu] + [o_sums.at[i:i + 1] for i in range(6)]
    backs = [pltpu.make_async_copy(b, a, sem_out.at[i]) for i, (a, b) in enumerate(zip(outs, kept))]
    for back in backs[:n_big]:
        back.start()
    o_bu[...] = col_sum(gbu[...])
    row = col_sum(gbq[...])
    e = o_bq.shape[2]
    for part_no in TRIPLE:
        for head in PAIR:
            at = (part_no * 2 + head) * e
            o_bq[part_no, head:head + 1, :] = row[:, at:at + e]
    o_sums[...] = sums[...]
    for back in backs[n_big:]:
        back.start()
    for back in backs:
        back.wait()


def inside():
    return pl.BlockSpec(memory_space=VMEM)


def anywhere():
    return pl.BlockSpec(memory_space=pl.ANY)


def smem():
    return pl.BlockSpec(memory_space=pltpu.SMEM)


def solution(mesh):
    n = mesh.shape['tp']

    def local_step(x, ln1_gamma, ln1_beta, w_qkv, b_qkv, w_out, b_out, ln2_gamma, ln2_beta, w_up, b_up, w_down, b_down, grad_y):
        t, d = x.shape[1], x.shape[2]
        heads, e = w_qkv.shape[1], w_qkv.shape[3]
        he = heads * e
        f = w_up.shape[1]
        scale = e ** -0.5
        slopes = jnp.asarray(alibi_slopes(heads * n))
        x2, dy2 = x[0], grad_y[0]
        row = lambda vec: vec.reshape(1, -1)
        wt = w_qkv.transpose(1, 2, 3, 0).reshape(heads * 3 * e, d)
        bq = b_qkv.transpose(1, 0, 2)
        sds = jax.ShapeDtypeStruct
        rows, full, half = (t, d), (n, t, d), (n, t, he)
        both, line = (len(PAIR),) + half, (len(PAIR), n, 1, t)
        packed = (len(TRIPLE) * he, d)
        params = lambda cid: pltpu.CompilerParams(collective_id=cid, has_side_effects=True, vmem_limit_bytes=VLIM)
        dma = pltpu.SemaphoreType.DMA

        vm = lambda dims, kind=BF: VMEM(dims, kind)
        stat, turned = (len(PAIR), 8, t), (n, he, t)
        vecs = (row(ln1_gamma), row(ln1_beta), bq, row(b_out), row(ln2_gamma), row(ln2_beta), row(b_up), row(b_down))
        results = [sds(rows, BF), sds(rows, BF), sds((8, d), F32), sds((heads, len(TRIPLE), e, d), BF),
                   sds((8, len(TRIPLE) * he), F32), sds((he, d), BF), sds((d, f), BF), sds((8, f), F32), sds((f, d), BF)]
        y, gx, sums, gwt, gbq, gwo, gwu, gbu, gwd, _ = pl.pallas_call(
            functools.partial(kernel_main, n, scale, len(vecs), len(results)),
            name='layer',
            out_shape=[vm(b.shape, b.dtype) for b in results] + [sds(full, BF)],
            in_specs=[anywhere()] * (6 + len(vecs)) + [smem()],
            out_specs=[inside()] * len(results) + [anywhere()],
            scratch_shapes=[vm(b.shape, b.dtype) for b in vecs] + [vm(full), vm(rows), vm(rows), vm(full), vm(full), vm(packed), vm(packed), vm((n, he, d)),
                            vm((d, f)), vm((f, d)), vm(both), vm(half), vm(half), vm(turned), vm(turned), vm(half),
                            vm(line, F32), vm(rows), vm((len(PAIR), n, t, t), F32), vm(stat, F32), vm(stat, F32),
                            vm((he, t), F32), vm((len(PAIR), t, t), F32), vm(rows, F32), vm((n, t, f)), vm((n, t, f)),
                            vm(rows, F32), vm((len(PAIR), t, he)), vm((he, t), F32), vm(half, F32), vm(half, F32),
                            vm((n, t, len(TRIPLE) * he)), vm((6, 8, d), F32), vm((n, 4, d), F32), vm((n, 2, d), F32), vm(full)]
            + scatter_buffers(n, t, d) * 2 + scatter_sems() * 3 + gather_sems() * 3 + [dma((n,))] * 2 + [dma((len(vecs),))],
            compiler_params=params(0),
        )(x2, dy2, wt, w_out, w_up, w_down, *vecs, slopes)

        big = (y, gx, gwt, gwo, gwu, gwd)
        little = (gbq, gbu, sums)
        bias_dims, up_dims = (len(TRIPLE), heads, e), (1, f)
        res = pl.pallas_call(
            functools.partial(kernel_out, len(big)),
            name='results',
            compiler_params=pltpu.CompilerParams(vmem_limit_bytes=8 * 1024 * 1024),
            out_shape=[sds(b.shape, b.dtype) for b in big] + [sds(bias_dims, F32), sds(up_dims, F32)] + [sds((1, d), F32)] * 6,
            in_specs=[inside()] * (len(big) + 3),
            out_specs=[anywhere()] * (len(big) + 8),
            scratch_shapes=[vm(bias_dims, F32), vm(up_dims, F32), vm((8, d), F32), dma((len(big) + 8,))],
        )(*big, *little)
        y, gx, gwt, gwo, gwu, gwd, gbq, gbu, s_g1, s_b1, s_g2, s_b2, s_bo, s_bd = res
        vec = lambda a: a.reshape(-1)
        return (y[None], gx[None], vec(s_g1), vec(s_b1), gwt.transpose(3, 0, 1, 2), gbq.transpose(1, 0, 2), gwo, vec(s_bo),
                vec(s_g2), vec(s_b2), gwu, vec(gbu), gwd, vec(s_bd))

    row_spec = P('dp', 'tp', None)
    in_specs = (row_spec, P(), P(), P(None, 'tp', None, None), P('tp', None, None), P('tp', None), P(), P(), P(),
                P(None, 'tp'), P('tp'), P('tp', None), P(), row_spec)
    out_specs = (row_spec, row_spec, P('dp'), P('dp'), P('dp', 'tp', None, None), P(('dp', 'tp'), None, None),
                 P(('dp', 'tp'), None), P('dp'), P('dp'), P('dp'), P('dp', 'tp'), P(('dp', 'tp')), P(('dp', 'tp'), None), P('dp'))
    return jax.shard_map(local_step, mesh=mesh, in_specs=in_specs, out_specs=out_specs, check_vma=False)
```

```python
import functools
import math
import jax
import jax.numpy as jnp
import numpy as np
from jax import lax
from jax.experimental import pallas as pl
from jax.experimental.pallas import tpu as pltpu
from jax.sharding import PartitionSpec as P

EPS = 1e-5
MASK_VALUE = -1e30
BF, F32 = jnp.bfloat16, jnp.float32
VMEM = pltpu.VMEM
MESH = pl.DeviceIdType.MESH
scope = jax.named_scope
VLIM = 58 * 1024 * 1024
GELU_C = math.sqrt(2.0 / math.pi)
PAIR = LOW, HIGH = (0, 1)
TRIPLE = (0, 1, 2)
NN = (((1,), (0,)), ((), ()))
T0 = (((0,), (0,)), ((), ()))
NT = (((1,), (1,)), ((), ()))


def alibi_slopes(n_heads):
    closest = 2 ** int(math.floor(math.log2(n_heads)))
    base_ratio = 2.0 ** (-8.0 / closest)
    extra_ratio = 2.0 ** (-4.0 / closest)
    remaining = min(closest, n_heads - closest)
    slopes = [base_ratio ** (i + 1) for i in range(closest)]
    slopes = slopes + [extra_ratio ** (2 * i + 1) for i in range(remaining)]
    return np.array(slopes, dtype=np.float32)


def mm(a, b, dims=NN):
    return lax.dot_general(a, b, dims, preferred_element_type=F32)


def loop(lo, hi, body, unroll=1):
    def step(i, carry):
        body(i)
        return carry
    lax.fori_loop(lo, hi, step, 0, unroll=unroll)


def twos(count, body):
    loop(0, count // 2, lambda i: body((2 * i, 2 * i + 1)))

    @pl.when(count % 2 == 1)
    def _():
        body((count - 1,))


def rows_loop(total, rows, body, base=0):
    loop(0, total // rows, lambda r: body(pl.ds(pl.multiple_of(base + r * rows, rows), rows)))


def row_mean(z):
    return jnp.mean(z, axis=-1, keepdims=True)


def col_sum(z):
    return jnp.sum(z, axis=0, keepdims=True)


def norm_back(grad, hat, rstd):
    return rstd * (grad - row_mean(grad) - hat * row_mean(grad * hat))


def zero_fill(*refs):
    for ref in refs:
        ref[...] = jnp.zeros(ref.shape, ref.dtype)


def sort_weight(wp, wt):
    e = wp.shape[0] // 6
    for part_no in TRIPLE:
        for head in PAIR:
            dst = (part_no * 2 + head) * e
            src = (head * 3 + part_no) * e
            wp[dst:dst + e, :] = wt[src:src + e, :]


def norm_rows(z):
    cen = z - row_mean(z)
    rstd = lax.rsqrt(row_mean(cen * cen) + EPS)
    return cen * rstd, rstd


def fold8(v, op):
    out = v[0:8]
    for k in range(1, v.shape[0] // 8):
        out = op(out, v[8 * k:8 * k + 8])
    return out


class Ring:
    def __init__(self, n):
        self.n = n
        nx = n // 2
        self.me = lax.axis_index('tp')
        self.x = self.me // 2
        self.c = self.me % 2
        self.nx = nx
        self.xr = (self.x + 1) % nx
        self.xl = (self.x + nx - 1) % nx
        self.xf = (self.x + 2) % nx
        self.right = self.xr * 2 + self.c
        self.left = self.xl * 2 + self.c
        self.far = self.xf * 2 + self.c
        other = 1 - self.c
        self.partner = self.x * 2 + other
        self.others = [xp * 2 + other for xp in (self.x, self.xl, self.xr, self.xf)]

    def order(self, s):
        odd = s % 2
        dx = jnp.where(s < 2, 0, jnp.where(s >= 6, 2, jnp.where(odd == 0, self.nx - 1, 1)))
        mid = jnp.where(s < 4, 0, 1)
        dc = jnp.where(s < 2, odd, jnp.where(s >= 6, odd, mid))
        return ((self.x + dx) % self.nx) * 2 + (self.c + dc) % 2

    def barrier(self):
        sem = pltpu.get_barrier_semaphore()
        peers = [self.right, self.left, self.partner]
        for peer in peers:
            pl.semaphore_signal(sem, inc=1, device_id={'tp': peer}, device_id_type=MESH)
        pl.semaphore_wait(sem, len(peers))


class Gather:
    LEFT, RIGHT, FAR, SIDE = 0, 2, 4, 6
    SLOTS = 10

    def __init__(self, ring, buf, ssem, rsem, base=0, size=None, cut=None):
        self.ring, self.buf, self.ssem, self.rsem = ring, buf, ssem, rsem
        self.base = base
        self.size = size or buf.shape[1]
        self.cut = cut or self.size // 2
        self.drained = False

    def rows(self, half):
        if half == LOW:
            return pl.ds(self.base, self.cut)
        return pl.ds(self.base + self.cut, self.size - self.cut)

    def copy(self, ref, dev, slot, onward):
        return pltpu.make_async_remote_copy(
            src_ref=ref, dst_ref=ref, send_sem=self.ssem.at[onward], recv_sem=self.rsem.at[slot],
            device_id={'tp': dev}, device_id_type=MESH)

    def send(self, blk, half, dev, slot, onward=LOW):
        self.copy(self.buf.at[blk, self.rows(half)], dev, slot, onward).start()

    def wait(self, blk, half, slot):
        self.copy(self.buf.at[blk, self.rows(half)], self.ring.me, slot, LOW).wait_recv()

    def side(self, which):
        ref = self.buf.at[self.ring.others[which], pl.ds(self.base, self.size)]
        self.copy(ref, self.ring.me, self.SIDE + which, LOW).wait_recv()

    def start(self):
        r = self.ring
        for half in PAIR:
            self.send(r.me, half, r.right, self.LEFT + half)
            self.send(r.me, HIGH - half, r.left, self.RIGHT + HIGH - half)
        for half in PAIR:
            self.send(r.me, half, r.partner, self.SIDE)

    def near1(self):
        r = self.ring
        self.wait(r.left, LOW, self.LEFT)
        self.send(r.left, LOW, r.right, self.FAR, HIGH)
        self.send(r.left, LOW, r.partner, self.SIDE + 1)
        self.wait(r.right, HIGH, self.RIGHT + HIGH)
        self.send(r.right, HIGH, r.left, self.FAR + HIGH, HIGH)
        self.send(r.right, HIGH, r.partner, self.SIDE + 2)

    def near2(self):
        r = self.ring
        self.wait(r.left, HIGH, self.LEFT + HIGH)
        self.send(r.left, HIGH, r.partner, self.SIDE + 1)
        self.wait(r.right, LOW, self.RIGHT)
        self.send(r.right, LOW, r.partner, self.SIDE + 2)

    def far(self):
        r = self.ring
        for half in PAIR:
            self.wait(r.far, half, self.FAR + half)
            self.send(r.far, half, r.partner, self.SIDE + 3)

    def gone(self, blocks, onward):
        ref = self.buf.at[pl.ds(0, blocks), pl.ds(self.base, self.size)]
        self.copy(ref, self.ring.right, LOW, onward).wait_send()

    def drain(self):
        self.gone(1, HIGH)
        self.drained = True

    def finish(self):
        self.gone(6, LOW)
        if not self.drained:
            self.gone(1, HIGH)


class Scatter:
    def __init__(self, ring, part, pair, stage, land, ssem, rsem, base=0, size=None):
        self.ring, self.part, self.pair, self.stage, self.land = ring, part, pair, stage, land
        self.ssem, self.rsem = ssem, rsem
        self.base = base
        self.size = size or part.shape[1]
        self.half = self.size // 2

    def cp_pair(self, xp):
        r = self.ring
        rows = pl.ds(self.base, self.size)
        return pltpu.make_async_remote_copy(
            src_ref=self.part.at[xp * 2 + (1 - r.c), rows], dst_ref=self.pair.at[xp, rows], send_sem=self.ssem.at[LOW],
            recv_sem=self.rsem.at[xp], device_id={'tp': r.partner}, device_id_type=MESH)

    def cp(self, slot, half, dst_slot, dev):
        rows = pl.ds(self.base + half * self.half, self.half)
        return pltpu.make_async_remote_copy(
            src_ref=self.stage.at[slot, rows], dst_ref=self.land.at[dst_slot, rows],
            send_sem=self.ssem.at[HIGH], recv_sem=self.rsem.at[4 + 2 * dst_slot + half],
            device_id={'tp': dev}, device_id_type=MESH)

    def wait_land(self, dst_slot, half):
        self.cp(0, half, dst_slot, self.ring.me).wait_recv()

    def wait_pair(self, xp):
        self.cp_pair(xp).wait_recv()

    def send_pair(self, xp):
        self.cp_pair(xp).start()

    def mix(self, slot, xp, half, with_far=False):
        blk = xp * 2 + self.ring.c
        step = 32

        def body(i):
            rows = pl.ds(pl.multiple_of(self.base + half * self.half + i * step, step), step)
            total = self.part[blk, rows, :].astype(F32) + self.pair[xp, rows, :].astype(F32)
            if with_far:
                total = total + self.land[0, rows, :].astype(F32)
            self.stage[slot, rows, :] = total.astype(BF)
        loop(0, self.half // step, body)

    def far(self):
        r = self.ring
        self.wait_pair(r.xf)
        self.mix(0, r.xf, 0)
        self.cp(0, 0, 0, r.right).start()
        self.mix(0, r.xf, 1)
        self.cp(0, 1, 0, r.left).start()

    def near_own(self):
        r = self.ring
        self.wait_pair(r.xr)
        self.mix(1, r.xr, 1)
        self.cp(1, 1, 1, r.right).start()
        self.wait_pair(r.xl)
        self.mix(2, r.xl, 0)
        self.cp(2, 0, 2, r.left).start()

    def near_sum(self):
        r = self.ring
        self.wait_land(0, 0)
        self.mix(1, r.xr, 0, with_far=True)
        self.cp(1, 0, 1, r.right).start()
        self.wait_land(0, 1)
        self.mix(2, r.xl, 1, with_far=True)
        self.cp(2, 1, 2, r.left).start()

    def wait_final(self):
        self.wait_pair(self.ring.x)
        for slot in (1, 2):
            for half in PAIR:
                self.wait_land(slot, half)

    def total(self, rows):
        r = self.ring
        return (self.part[r.me, rows, :].astype(F32) + self.pair[r.x, rows, :].astype(F32)
                + self.land[1, rows, :].astype(F32) + self.land[2, rows, :].astype(F32))

    def finish(self):
        r = self.ring
        rows = pl.ds(self.base, self.size)
        for ref, which in ((self.pair.at[:, rows], LOW), (self.stage.at[:, rows], HIGH)):
            pltpu.make_async_remote_copy(
                src_ref=ref, dst_ref=ref, send_sem=self.ssem.at[which], recv_sem=self.rsem.at[0],
                device_id={'tp': r.partner}, device_id_type=MESH).wait_send()


def scatter_buffers(n, rows, d):
    return [VMEM((n // 2, rows, d), BF), VMEM((3, rows, d), BF), VMEM((3, rows, d), BF)]


def scatter_sems():
    return [pltpu.SemaphoreType.DMA((2,)), pltpu.SemaphoreType.DMA((4 + 6,))]


def hooked(count, body, hooks):
    def step(i):
        for at, actions in hooks.items():
            @pl.when(i == at)
            def _():
                for act in actions:
                    act()
        body(i)
    loop(0, count, step)


def gather_sems():
    return [pltpu.SemaphoreType.DMA((2,)), pltpu.SemaphoreType.DMA((Gather.SLOTS,))]


def lane_mask(rows, h):
    lane = lax.broadcasted_iota(jnp.int32, (rows, 128), 1)
    return (lane < 64) if h == 0 else (lane >= 64)


def attend_block(i, q_ref, k_ref, vt_ref, o_ref, lse_ref, s_ref, m_ref, l_ref, acc_ref, bt_ref, slopes):
    t = q_ref.shape[2]
    e = acc_ref.shape[0] // 2
    key = lax.broadcasted_iota(jnp.int32, (t, t), 0)
    qry = lax.broadcasted_iota(jnp.int32, (t, t), 1)
    for h in PAIR:
        m_ref[h] = jnp.full((8, t), MASK_VALUE, F32)
        l_ref[h] = jnp.zeros((8, t), F32)
    zero_fill(acc_ref)

    def shift(h, j):
        return slopes[h] * (j * t).astype(F32)

    def score(blocks, diag):
        top = [m_ref[h] for h in PAIR]
        for j in blocks:
            for h in PAIR:
                s = mm(k_ref[j], q_ref[h, i], NT) + bt_ref[h]
                if diag:
                    s = jnp.where(key <= qry, s, MASK_VALUE)
                s_ref[h, j] = s
                top[h] = jnp.maximum(top[h], fold8(s, jnp.maximum) + shift(h, j))
        for h in PAIR:
            m_ref[h] = top[h]

    twos(i, lambda blocks: score(blocks, False))
    score((i,), True)
    top = [jnp.max(m_ref[h], axis=0, keepdims=True) for h in PAIR]

    def denom(j):
        for h in PAIR:
            l_ref[h] = l_ref[h] + fold8(jnp.exp(s_ref[h, j] + (shift(h, j) - top[h])), jnp.add)

    loop(0, i + 1, denom)
    for h in PAIR:
        lse_ref[h, i] = top[h] + jnp.log(col_sum(l_ref[h]))

    def values(blocks):
        for h in PAIR:
            rows = pl.ds(h * e, e)
            total = acc_ref[rows, :]
            for j in blocks:
                p = jnp.exp(s_ref[h, j] + (shift(h, j) - lse_ref[h, i])).astype(BF)
                total = total + mm(vt_ref[j, rows, :], p)
            acc_ref[rows, :] = total

    twos(i + 1, values)
    o_ref[i] = acc_ref[...].T.astype(BF)


def kernel_main(n, scale, n_vec, n_out, x_hbm, dy_hbm, wt_hbm, wo_hbm, wu_hbm, wd_hbm, *refs):
    vec_hbm, (slopes_ref,), refs = refs[:n_vec], refs[n_vec:n_vec + 1], refs[n_vec + 1:]
    results, (h_hbm,), refs = refs[:n_out], refs[n_out:n_out + 1], refs[n_out + 1:]
    vecs, refs = refs[:n_vec], refs[n_vec:]
    run_layer(n, scale, vec_hbm, vecs, results, x_hbm, dy_hbm, wt_hbm, wo_hbm, wu_hbm, wd_hbm, slopes_ref, h_hbm, *refs)


def run_layer(n, scale, vec_hbm, vecs, results, x_hbm, dy_hbm, wt_hbm, wo_hbm, wu_hbm, wd_hbm, slopes_ref, h_hbm,
                xg, xo, dyo, dy, hg, wt, wp, wof, wu, wd, q, k, v, kt, vt, o, lse, orow, s_ref, m_ref, l_ref, acc, bt,
                x1, act, dpre, mid, dom, dqt, dk, dv, d3, small, early, late, part,
                *rest):
    g1, b1, bqkv, bo, g2, b2, bu, bd = vecs
    y, gx, sums, gwt, gbq, gwo, gwu, gbu, gwd = results
    rest = list(rest)

    def take(count):
        head = rest[:count]
        del rest[:count]
        return head

    ring = Ring(n)
    me = ring.me
    t, d, f = xg.shape[1], xg.shape[2], wu.shape[1]
    rs_bufs, rm_bufs = take(3), take(3)
    st = t // 2
    streams = (0, st)
    r_sems = [take(2) for _ in PAIR]
    r0, r1 = [Scatter(ring, part, *rs_bufs, *sems, base=base, size=st) for base, sems in zip(streams, r_sems)]
    rs = Scatter(ring, part, *rs_bufs, *r_sems[0])
    rm = Scatter(ring, dy, *rm_bufs, *take(2))
    g_sems = [take(2) for _ in PAIR]
    ax, aw = [Gather(ring, buf, *sems) for buf, sems in zip((xg, wof), g_sems)]
    ay = Gather(ring, dy, *take(2))
    g0, g1s = [Gather(ring, hg, *sems, base=base, size=st) for base, sems in zip(streams, g_sems)]
    d0, d1 = [Gather(ring, xg, *sems, base=base, size=st) for base, sems in zip(streams, g_sems)]
    few, local, vec_sem = take(3)
    o_send, o_recv, e_send, e_recv, l_send, l_recv = [few.at[i] for i in range(6)]

    def fetch(i, src, dst):
        cp = pltpu.make_async_copy(src, dst, local.at[i])
        cp.start()
        return cp

    in_x, in_wo, in_dy, in_wt = (fetch(0, x_hbm, xg.at[me]), fetch(1, wo_hbm, wof.at[me]),
                                 fetch(2, dy_hbm, dy.at[me]), fetch(3, wt_hbm, wt))
    later = [fetch(4, wu_hbm, wu), fetch(5, wd_hbm, wd), fetch(6, x_hbm, xo), fetch(7, dy_hbm, dyo)]
    vec_in = [pltpu.make_async_copy(a, b, vec_sem.at[i]) for i, (a, b) in enumerate(zip(vec_hbm, vecs))]
    for cp in vec_in:
        cp.start()
    ring.barrier()
    in_x.wait()
    ax.start()
    for cp in vec_in:
        cp.wait()
    in_wt.wait()
    sort_weight(wp, wt)
    in_wo.wait()
    in_dy.wait()
    bias = jnp.concatenate([bqkv[kind, head:head + 1, :] for kind in TRIPLE for head in PAIR], axis=1)

    def project(blk):
        def norm(rows):
            hat, _ = norm_rows(xg[blk, rows, :].astype(F32))
            hg[blk, rows, :] = (hat * g1[...] + b1[...]).astype(BF)
        rows_loop(t, 64, norm)
        out = mm(hg[blk], wp[...], NT) + bias
        out = out.astype(BF)
        zero = jnp.zeros((t, 128), BF)
        qs = (out[:, :128].astype(F32) * scale).astype(BF)
        for head in PAIR:
            q[head, blk] = jnp.where(lane_mask(t, head), qs, zero)
        k[blk] = out[:, 128:256]
        v[blk] = out[:, 256:]
        kt[blk] = out[:, 128:256].T
        vt[blk] = out[:, 256:].T
        fetch(0, hg.at[blk], h_hbm.at[blk])

    arrive = functools.partial
    with scope('a_gather'):
        hooked(n, lambda step: project(ring.order(step)), {
            1: [arrive(ax.side, 0)],
            2: [ax.near1, ax.near2],
            4: [arrive(ax.side, 1)],
            5: [arrive(ax.side, 2)],
            6: [ax.drain, aw.start, ax.far, ay.start],
            7: [arrive(ax.side, 3)]})
    slopes = [slopes_ref[me * 2 + head] for head in PAIR]
    key = lax.broadcasted_iota(jnp.int32, (t, t), 0)
    qry = lax.broadcasted_iota(jnp.int32, (t, t), 1)
    for head in PAIR:
        bt[head] = slopes[head] * key.astype(F32)

    def send_o(i):
        cols = pl.ds(pl.multiple_of(me * 128, 128), 128)
        return pltpu.make_async_remote_copy(
            src_ref=o.at[i], dst_ref=orow.at[:, cols], send_sem=o_send, recv_sem=o_recv,
            device_id={'tp': i}, device_id_type=MESH)

    def one_block(step):
        i = ring.order(n - 1 - step)
        attend_block(i, q, k, vt, o, lse, s_ref, m_ref, l_ref, acc, bt, slopes)

        @pl.when(step < n - 1)
        def _():
            send_o(i).start()

    with scope('a_attend'):
        ax.finish()
        pltpu.make_async_copy(hg, h_hbm, local.at[0]).wait()
        hooked(n, one_block, {4: [aw.near1], 5: [aw.near2]})
    most = pl.ds(0, n - 1)
    with scope('a_wait'):
        aw.far()
        ay.near1()
        orow[:, pl.ds(pl.multiple_of(me * 128, 128), 128)] = o[me]
        wide = orow.at[:, pl.ds(0, (n - 1) * 128)]
        pltpu.make_async_remote_copy(
            src_ref=wide, dst_ref=wide, send_sem=o_send, recv_sem=o_recv,
            device_id={'tp': me}, device_id_type=MESH).wait_recv()
        for which in range(4):
            aw.side(which)
        aw.finish()
        later[2].wait()
    with scope('a_out'):
        x1[...] = mm(orow[...], wof[...].reshape(n * 128, d)).astype(BF).astype(F32)

        def enter(rows):
            row = xo[rows, :].astype(F32) + x1[rows, :] + bo[...]
            x1[rows, :] = row
            hat, _ = norm_rows(row)
            hg[me, rows, :] = (hat * g2[...] + b2[...]).astype(BF)
        rows_loop(st, 64, enter)
        g0.start()
        rows_loop(st, 64, enter, base=st)
    for cp in (later[0], later[1], later[3]):
        cp.wait()
    zero_fill(gbu)
    ay.side(0)

    def rest():
        ay.near2()
        ay.far()
        for which in range(1, 4):
            ay.side(which)

    def mlp(blk, stream):
        rows = pl.ds(pl.multiple_of(stream * st, st), st)
        pre = mm(hg[blk, rows, :], wu[...]) + bu[...]
        cot = mm(dy[blk, rows, :], wd[...], NT).astype(BF).astype(F32)
        sq = pre * pre
        th = jnp.tanh(GELU_C * (pre + 0.044715 * sq * pre))
        cdf = 0.5 * (1.0 + th)
        act[blk, rows, :] = (pre * cdf).astype(BF)
        slope = cdf + pre * (0.5 * (1.0 - th * th)) * (GELU_C * (1.0 + 3 * 0.044715 * sq))
        dp = cot * slope
        gbu[...] = gbu[...] + fold8(dp, jnp.add)
        dpb = dp.astype(BF)
        dpre[blk, rows, :] = dpb
        part[blk, rows, :] = mm(dpb, wu[...], NT).astype(BF)

    chips = (ring.xf, ring.xr, ring.xl, ring.x)
    def pairs(job):
        for xp in chips:
            job.send_pair(xp)

    def item(step):
        late = (step == 4) | (step == 5) | (step >= 10)
        pos = jnp.where(step < 4, step, jnp.where(step < 6, step - 4, jnp.where(step < 10, step - 2, step - 8)))
        mlp(ring.order(pos), jnp.where(late, 1, 0))

    with scope('b_gather'):
        hooked(2 * n, item, {
            1: [arrive(g0.side, 0)],
            2: [rest, g0.near1, g1s.start, g0.near2],
            5: [arrive(g1s.side, 0)],
            6: [arrive(g0.side, 1)],
            7: [arrive(g0.side, 2)],
            8: [g0.far],
            9: [arrive(g0.side, 3)],
            10: [arrive(pairs, r0), g1s.near1, r0.far, g1s.near2],
            12: [r0.near_own, arrive(g1s.side, 1)],
            13: [arrive(g1s.side, 2)],
            14: [g1s.far],
            15: [arrive(g1s.side, 3)]})
    with scope('b_far'):
        pairs(r1)
        r0.near_sum()
        r1.far()
    with scope('b_own'):
        r1.near_own()
    ay.finish()

    def weight_down(i):
        cols = pl.ds(pl.multiple_of(i * 256, 256), 256)
        left = act[:, :, cols].reshape(n * t, 256)
        gwd[cols, :] = mm(left, dy[...].reshape(n * t, d), T0).astype(BF)

    def weight_up(i):
        cols = pl.ds(pl.multiple_of(i * 256, 256), 256)
        left = hg[:, :, cols].reshape(n * t, 256)
        gwu[cols, :] = mm(left, dpre[...].reshape(n * t, f), T0).astype(BF)

    with scope('b_weights'):
        loop(0, f // 256, weight_down)
        loop(0, d // 256, weight_up)
    zero_fill(small)

    def down(blk):
        dy[blk] = mm(act[blk], wd[...]).astype(BF)

    def leave(rows):
        dg = rs.total(rows).astype(BF).astype(F32)
        hat, rstd = norm_rows(x1[rows, :])
        small[2] = small[2] + fold8(dg * hat, jnp.add)
        small[3] = small[3] + fold8(dg, jnp.add)
        dz = norm_back(dg * g2[...], hat, rstd)
        dyf = dyo[rows, :].astype(F32)
        dm = dyf + dz
        small[4] = small[4] + fold8(dm, jnp.add)
        small[5] = small[5] + fold8(dyf, jnp.add)
        mid[rows, :] = dm
        xg[me, rows, :] = dm.astype(BF)

    with scope('b_sum'):
        r1.near_sum()
    with scope('b_final'):
        r0.wait_final()
    with scope('b_leave'):
        rows_loop(st, 64, leave)
        g0.finish()
        d0.start()
    with scope('b_down'):
        loop(0, n, down)
        pairs(rm)
    with scope('b_final1'):
        r1.wait_final()
    with scope('b_leave1'):
        rows_loop(st, 64, leave, base=st)
        g1s.finish()
        d1.start()
    with scope('b_finish'):
        for job in (r0, r1):
            job.finish()
    reload = fetch(0, h_hbm, hg)

    def share(buf, off, send_sem, recv_sem):
        return pltpu.make_async_remote_copy(
            src_ref=buf.at[me], dst_ref=buf.at[me], send_sem=send_sem, recv_sem=recv_sem,
            device_id={'tp': (me + off) % n}, device_id_type=MESH)

    def all_in(buf, send_sem, recv_sem):
        return pltpu.make_async_remote_copy(
            src_ref=buf.at[most], dst_ref=buf.at[most], send_sem=send_sem, recv_sem=recv_sem,
            device_id={'tp': me}, device_id_type=MESH)

    def early_out():
        for i in range(4):
            early[me, i:i + 1, :] = col_sum(small[2 + i])
        for off in range(1, n):
            share(early, off, e_send, e_recv).start()

    def add_up(buf):
        total = buf[0]
        for b in range(1, n):
            total = total + buf[b]
        return total
    zero_fill(dk, dv)

    def back_block(i):
        dc = mm(xg[i], wof[me], NT).astype(BF)
        zero = jnp.zeros((t, 128), BF)
        prod = (dc.astype(F32) * o[i].astype(F32)).T
        dlt = (col_sum(prod[:64]), col_sum(prod[64:]))
        for head in PAIR:
            dom[head] = jnp.where(lane_mask(t, head), dc, zero)
        zero_fill(dqt)

        def pair_block(blocks, diag):
            cases = [(j, head) for j in blocks for head in PAIR]
            ps, dss = [], []
            for j, head in cases:
                s = mm(k[j], q[head, i], NT) + bt[head]
                if diag:
                    s = jnp.where(key <= qry, s, MASK_VALUE)
                p = jnp.exp(s + (slopes[head] * (j * t).astype(F32) - lse[head, i]))
                dp = mm(v[j], dom[head], NT).astype(BF).astype(F32)
                dss.append((p * (dp - dlt[head])).astype(BF))
                ps.append(p.astype(BF))
            wide = list(zip(cases, ps, dss))
            for j in blocks:
                dv[j] = dv[j] + sum(mm(p, dom[head]) for (b, head), p, _ in wide if b is j)
                dk[j] = dk[j] + sum(mm(ds, q[head, i]) for (b, head), _, ds in wide if b is j)
            for head in PAIR:
                rows = pl.ds(head * 64, 64)
                dqt[rows, :] = dqt[rows, :] + sum(mm(kt[b, rows, :], ds) for (b, h), _, ds in wide if h == head)

        twos(i, lambda blocks: pair_block(blocks, False))
        pair_block((i,), True)
        d3[i, :, :128] = (dqt[...].T * scale).astype(BF)

    def both_in(which):
        for job in (d0, d1):
            job.side(which)

    with scope('c_attend'):
        hooked(n, lambda step: back_block(ring.order(step)), {
            1: [arrive(both_in, 0), d0.near1, d0.near2],
            2: [d1.near1, rm.far, rm.near_own, d1.near2],
            4: [arrive(both_in, 1)],
            5: [arrive(both_in, 2)],
            6: [d0.far, d1.far, rm.near_sum],
            7: [arrive(both_in, 3)]})
    zero_fill(gbq)

    def back_in(xp):
        for off in (1, 0):
            blk = xp * 2 + (ring.c + off) % 2
            d3[blk, :, 128:256] = dk[blk].astype(BF)
            d3[blk, :, 256:] = dv[blk].astype(BF)
            part[blk] = mm(d3[blk], wp[...]).astype(BF)
            if off:
                rs.send_pair(xp)

    with scope('c_far'):
        back_in(ring.xf)
        rs.far()
    with scope('c_own'):
        back_in(ring.xr)
        back_in(ring.xl)
        rs.near_own()
        back_in(ring.x)
    reload.wait()

    def weight_in(i):
        cols = pl.ds(pl.multiple_of(i * 128, 128), 128)
        left = d3[:, :, cols].reshape(n * t, 128)
        grad = mm(left, hg[...].reshape(n * t, d), T0).astype(BF)
        for head in PAIR:
            gwt[head, i] = grad[head * 64:head * 64 + 64]

    def bias_in(b):
        gbq[...] = gbq[...] + fold8(d3[b].astype(F32), jnp.add)

    with scope('c_weights'):
        loop(0, len(TRIPLE), weight_in)
        loop(0, n, bias_in)
    with scope('c_sum'):
        rs.near_sum()
    with scope('c_gwo'):
        gwo[...] = mm(o[...].reshape(n * t, 128), xg[...].reshape(n * t, d), T0).astype(BF)
    with scope('c_mfinal'):
        rm.wait_final()

    def finish_y(rows):
        m = rm.total(rows).astype(BF).astype(F32)
        y[rows, :] = (x1[rows, :] + m + bd[...]).astype(BF)
    rows_loop(t, 64, finish_y)
    with scope('c_final'):
        rs.wait_final()
        early_out()

    def sum_in(rows):
        dh = rs.total(rows).astype(BF).astype(F32)
        hat, _ = norm_rows(xo[rows, :].astype(F32))
        small[0] = small[0] + fold8(dh * hat, jnp.add)
        small[1] = small[1] + fold8(dh, jnp.add)

    def last(rows):
        dh = rs.total(rows).astype(BF).astype(F32)
        hat, rstd = norm_rows(xo[rows, :].astype(F32))
        gx[rows, :] = (mid[rows, :] + norm_back(dh * g1[...], hat, rstd)).astype(BF)

    with scope('c_sums'):
        rows_loop(t, 64, sum_in)
    for i in PAIR:
        late[me, i:i + 1, :] = col_sum(small[i])
    with scope('c_share'):
        for off in range(1, n):
            share(late, off, l_send, l_recv).start()
        rows_loop(t, 64, last)
        all_in(early, e_send, e_recv).wait_recv()
        sums[2:6, :] = add_up(early)
        all_in(late, l_send, l_recv).wait_recv()
        sums[0:2, :] = add_up(late)
        all_in(early, e_send, e_recv).wait_send()
        all_in(late, l_send, l_recv).wait_send()
        all_in(o, o_send, o_recv).wait_send()
    with scope('d_finish'):
        for job in (rs, rm, d0, d1):
            job.finish()


def kernel_out(n_big, *refs):
    count = n_big + 3
    srcs, refs = refs[:count], refs[count:]
    outs, refs = refs[:n_big + 8], refs[n_big + 8:]
    bufs, tail, sem_out = srcs, refs[:-1], refs[-1]
    gbq, gbu, sums = bufs[n_big:]
    o_bq, o_bu, o_sums = tail
    kept = list(bufs[:n_big]) + [o_bq, o_bu] + [o_sums.at[i:i + 1] for i in range(6)]
    backs = [pltpu.make_async_copy(b, a, sem_out.at[i]) for i, (a, b) in enumerate(zip(outs, kept))]
    for back in backs[:n_big]:
        back.start()
    o_bu[...] = col_sum(gbu[...])
    row = col_sum(gbq[...])
    e = o_bq.shape[2]
    for part_no in TRIPLE:
        for head in PAIR:
            at = (part_no * 2 + head) * e
            o_bq[part_no, head:head + 1, :] = row[:, at:at + e]
    o_sums[...] = sums[...]
    for back in backs[n_big:]:
        back.start()
    for back in backs:
        back.wait()


def inside():
    return pl.BlockSpec(memory_space=VMEM)


def anywhere():
    return pl.BlockSpec(memory_space=pl.ANY)


def smem():
    return pl.BlockSpec(memory_space=pltpu.SMEM)


def solution(mesh):
    n = mesh.shape['tp']

    def local_step(x, ln1_gamma, ln1_beta, w_qkv, b_qkv, w_out, b_out, ln2_gamma, ln2_beta, w_up, b_up, w_down, b_down, grad_y):
        t, d = x.shape[1], x.shape[2]
        heads, e = w_qkv.shape[1], w_qkv.shape[3]
        he = heads * e
        f = w_up.shape[1]
        scale = e ** -0.5
        slopes = jnp.asarray(alibi_slopes(heads * n))
        x2, dy2 = x[0], grad_y[0]
        row = lambda vec: vec.reshape(1, -1)
        wt = w_qkv.transpose(1, 2, 3, 0).reshape(heads * 3 * e, d)
        bq = b_qkv.transpose(1, 0, 2)
        sds = jax.ShapeDtypeStruct
        rows, full, half = (t, d), (n, t, d), (n, t, he)
        both, line = (len(PAIR),) + half, (len(PAIR), n, 1, t)
        packed = (len(TRIPLE) * he, d)
        params = lambda cid: pltpu.CompilerParams(collective_id=cid, has_side_effects=True, vmem_limit_bytes=VLIM)
        dma = pltpu.SemaphoreType.DMA

        vm = lambda dims, kind=BF: VMEM(dims, kind)
        stat, turned = (len(PAIR), 8, t), (n, he, t)
        vecs = (row(ln1_gamma), row(ln1_beta), bq, row(b_out), row(ln2_gamma), row(ln2_beta), row(b_up), row(b_down))
        results = [sds(rows, BF), sds(rows, BF), sds((8, d), F32), sds((heads, len(TRIPLE), e, d), BF),
                   sds((8, len(TRIPLE) * he), F32), sds((he, d), BF), sds((d, f), BF), sds((8, f), F32), sds((f, d), BF)]
        y, gx, sums, gwt, gbq, gwo, gwu, gbu, gwd, _ = pl.pallas_call(
            functools.partial(kernel_main, n, scale, len(vecs), len(results)),
            name='layer',
            out_shape=[vm(b.shape, b.dtype) for b in results] + [sds(full, BF)],
            in_specs=[anywhere()] * (6 + len(vecs)) + [smem()],
            out_specs=[inside()] * len(results) + [anywhere()],
            scratch_shapes=[vm(b.shape, b.dtype) for b in vecs] + [vm(full), vm(rows), vm(rows), vm(full), vm(full), vm(packed), vm(packed), vm((n, he, d)),
                            vm((d, f)), vm((f, d)), vm(both), vm(half), vm(half), vm(turned), vm(turned), vm(half),
                            vm(line, F32), vm(rows), vm((len(PAIR), n, t, t), F32), vm(stat, F32), vm(stat, F32),
                            vm((he, t), F32), vm((len(PAIR), t, t), F32), vm(rows, F32), vm((n, t, f)), vm((n, t, f)),
                            vm(rows, F32), vm((len(PAIR), t, he)), vm((he, t), F32), vm(half, F32), vm(half, F32),
                            vm((n, t, len(TRIPLE) * he)), vm((6, 8, d), F32), vm((n, 4, d), F32), vm((n, 2, d), F32), vm(full)]
            + scatter_buffers(n, t, d) * 2 + scatter_sems() * 3 + gather_sems() * 3 + [dma((n,))] * 2 + [dma((len(vecs),))],
            compiler_params=params(0),
        )(x2, dy2, wt, w_out, w_up, w_down, *vecs, slopes)

        big = (y, gx, gwt, gwo, gwu, gwd)
        little = (gbq, gbu, sums)
        bias_dims, up_dims = (len(TRIPLE), heads, e), (1, f)
        res = pl.pallas_call(
            functools.partial(kernel_out, len(big)),
            name='results',
            compiler_params=pltpu.CompilerParams(vmem_limit_bytes=8 * 1024 * 1024),
            out_shape=[sds(b.shape, b.dtype) for b in big] + [sds(bias_dims, F32), sds(up_dims, F32)] + [sds((1, d), F32)] * 6,
            in_specs=[inside()] * (len(big) + 3),
            out_specs=[anywhere()] * (len(big) + 8),
            scratch_shapes=[vm(bias_dims, F32), vm(up_dims, F32), vm((8, d), F32), dma((len(big) + 8,))],
        )(*big, *little)
        y, gx, gwt, gwo, gwu, gwd, gbq, gbu, s_g1, s_b1, s_g2, s_b2, s_bo, s_bd = res
        vec = lambda a: a.reshape(-1)
        return (y[None], gx[None], vec(s_g1), vec(s_b1), gwt.transpose(3, 0, 1, 2), gbq.transpose(1, 0, 2), gwo, vec(s_bo),
                vec(s_g2), vec(s_b2), gwu, vec(gbu), gwd, vec(s_bd))

    row_spec = P('dp', 'tp', None)
    in_specs = (row_spec, P(), P(), P(None, 'tp', None, None), P('tp', None, None), P('tp', None), P(), P(), P(),
                P(None, 'tp'), P('tp'), P('tp', None), P(), row_spec)
    out_specs = (row_spec, row_spec, P('dp'), P('dp'), P('dp', 'tp', None, None), P(('dp', 'tp'), None, None),
                 P(('dp', 'tp'), None), P('dp'), P('dp'), P('dp'), P('dp', 'tp'), P(('dp', 'tp')), P(('dp', 'tp'), None), P('dp'))
    return jax.shard_map(local_step, mesh=mesh, in_specs=in_specs, out_specs=out_specs, check_vma=False)
```

```python
import functools
import math
import jax
import jax.numpy as jnp
import numpy as np
from jax import lax
from jax.experimental import pallas as pl
from jax.experimental.pallas import tpu as pltpu
from jax.sharding import PartitionSpec as P

EPS = 1e-5
MASK_VALUE = -1e30
BF, F32 = jnp.bfloat16, jnp.float32
VMEM = pltpu.VMEM
MESH = pl.DeviceIdType.MESH
scope = jax.named_scope
VLIM = 58 * 1024 * 1024
GELU_C = math.sqrt(2.0 / math.pi)
PAIR = LOW, HIGH = (0, 1)
TRIPLE = (0, 1, 2)
NN = (((1,), (0,)), ((), ()))
T0 = (((0,), (0,)), ((), ()))
NT = (((1,), (1,)), ((), ()))


def alibi_slopes(n_heads):
    closest = 2 ** int(math.floor(math.log2(n_heads)))
    base_ratio = 2.0 ** (-8.0 / closest)
    extra_ratio = 2.0 ** (-4.0 / closest)
    remaining = min(closest, n_heads - closest)
    slopes = [base_ratio ** (i + 1) for i in range(closest)]
    slopes = slopes + [extra_ratio ** (2 * i + 1) for i in range(remaining)]
    return np.array(slopes, dtype=np.float32)


def mm(a, b, dims=NN):
    return lax.dot_general(a, b, dims, preferred_element_type=F32)


def loop(lo, hi, body, unroll=1):
    def step(i, carry):
        body(i)
        return carry
    lax.fori_loop(lo, hi, step, 0, unroll=unroll)


def twos(count, body):
    loop(0, count // 2, lambda i: body((2 * i, 2 * i + 1)))

    @pl.when(count % 2 == 1)
    def _():
        body((count - 1,))


def rows_loop(total, rows, body, base=0):
    loop(0, total // rows, lambda r: body(pl.ds(pl.multiple_of(base + r * rows, rows), rows)))


def row_mean(z):
    return jnp.mean(z, axis=-1, keepdims=True)


def col_sum(z):
    return jnp.sum(z, axis=0, keepdims=True)


def norm_back(grad, hat, rstd):
    return rstd * (grad - row_mean(grad) - hat * row_mean(grad * hat))


def zero_fill(*refs):
    for ref in refs:
        ref[...] = jnp.zeros(ref.shape, ref.dtype)


def sort_weight(wp, wt):
    e = wp.shape[0] // 6
    for part_no in TRIPLE:
        for head in PAIR:
            dst = (part_no * 2 + head) * e
            src = (head * 3 + part_no) * e
            wp[dst:dst + e, :] = wt[src:src + e, :]


def norm_rows(z):
    cen = z - row_mean(z)
    rstd = lax.rsqrt(row_mean(cen * cen) + EPS)
    return cen * rstd, rstd


def fold8(v, op):
    out = v[0:8]
    for k in range(1, v.shape[0] // 8):
        out = op(out, v[8 * k:8 * k + 8])
    return out


class Ring:
    def __init__(self, n):
        self.n = n
        nx = n // 2
        self.me = lax.axis_index('tp')
        self.x = self.me // 2
        self.c = self.me % 2
        self.nx = nx
        self.xr = (self.x + 1) % nx
        self.xl = (self.x + nx - 1) % nx
        self.xf = (self.x + 2) % nx
        self.right = self.xr * 2 + self.c
        self.left = self.xl * 2 + self.c
        self.far = self.xf * 2 + self.c
        other = 1 - self.c
        self.partner = self.x * 2 + other
        self.others = [xp * 2 + other for xp in (self.x, self.xl, self.xr, self.xf)]

    def order(self, s):
        odd = s % 2
        dx = jnp.where(s < 2, 0, jnp.where(s >= 6, 2, jnp.where(odd == 0, self.nx - 1, 1)))
        mid = jnp.where(s < 4, 0, 1)
        dc = jnp.where(s < 2, odd, jnp.where(s >= 6, odd, mid))
        return ((self.x + dx) % self.nx) * 2 + (self.c + dc) % 2

    def barrier(self):
        sem = pltpu.get_barrier_semaphore()
        peers = [self.right, self.left, self.partner]
        for peer in peers:
            pl.semaphore_signal(sem, inc=1, device_id={'tp': peer}, device_id_type=MESH)
        pl.semaphore_wait(sem, len(peers))


class Gather:
    LEFT, RIGHT, FAR, SIDE = 0, 2, 4, 6
    SLOTS = 10

    def __init__(self, ring, buf, ssem, rsem, base=0, size=None, cut=None):
        self.ring, self.buf, self.ssem, self.rsem = ring, buf, ssem, rsem
        self.base = base
        self.size = size or buf.shape[1]
        self.cut = cut or self.size // 2
        self.drained = False

    def rows(self, half):
        if half == LOW:
            return pl.ds(self.base, self.cut)
        return pl.ds(self.base + self.cut, self.size - self.cut)

    def copy(self, ref, dev, slot, onward):
        return pltpu.make_async_remote_copy(
            src_ref=ref, dst_ref=ref, send_sem=self.ssem.at[onward], recv_sem=self.rsem.at[slot],
            device_id={'tp': dev}, device_id_type=MESH)

    def send(self, blk, half, dev, slot, onward=LOW):
        self.copy(self.buf.at[blk, self.rows(half)], dev, slot, onward).start()

    def wait(self, blk, half, slot):
        self.copy(self.buf.at[blk, self.rows(half)], self.ring.me, slot, LOW).wait_recv()

    def side(self, which):
        ref = self.buf.at[self.ring.others[which], pl.ds(self.base, self.size)]
        self.copy(ref, self.ring.me, self.SIDE + which, LOW).wait_recv()

    def start(self):
        r = self.ring
        for half in PAIR:
            self.send(r.me, half, r.right, self.LEFT + half)
            self.send(r.me, HIGH - half, r.left, self.RIGHT + HIGH - half)
        for half in PAIR:
            self.send(r.me, half, r.partner, self.SIDE)

    def near1(self):
        r = self.ring
        self.wait(r.left, LOW, self.LEFT)
        self.send(r.left, LOW, r.right, self.FAR, HIGH)
        self.send(r.left, LOW, r.partner, self.SIDE + 1)
        self.wait(r.right, HIGH, self.RIGHT + HIGH)
        self.send(r.right, HIGH, r.left, self.FAR + HIGH, HIGH)
        self.send(r.right, HIGH, r.partner, self.SIDE + 2)

    def near2(self):
        r = self.ring
        self.wait(r.left, HIGH, self.LEFT + HIGH)
        self.send(r.left, HIGH, r.partner, self.SIDE + 1)
        self.wait(r.right, LOW, self.RIGHT)
        self.send(r.right, LOW, r.partner, self.SIDE + 2)

    def far(self):
        r = self.ring
        for half in PAIR:
            self.wait(r.far, half, self.FAR + half)
            self.send(r.far, half, r.partner, self.SIDE + 3)

    def gone(self, blocks, onward):
        ref = self.buf.at[pl.ds(0, blocks), pl.ds(self.base, self.size)]
        self.copy(ref, self.ring.right, LOW, onward).wait_send()

    def drain(self):
        self.gone(1, HIGH)
        self.drained = True

    def finish(self):
        self.gone(6, LOW)
        if not self.drained:
            self.gone(1, HIGH)


class Scatter:
    def __init__(self, ring, part, pair, stage, land, ssem, rsem, base=0, size=None):
        self.ring, self.part, self.pair, self.stage, self.land = ring, part, pair, stage, land
        self.ssem, self.rsem = ssem, rsem
        self.base = base
        self.size = size or part.shape[1]
        self.half = self.size // 2

    def cp_pair(self, xp):
        r = self.ring
        rows = pl.ds(self.base, self.size)
        return pltpu.make_async_remote_copy(
            src_ref=self.part.at[xp * 2 + (1 - r.c), rows], dst_ref=self.pair.at[xp, rows], send_sem=self.ssem.at[LOW],
            recv_sem=self.rsem.at[xp], device_id={'tp': r.partner}, device_id_type=MESH)

    def cp(self, slot, half, dst_slot, dev):
        rows = pl.ds(self.base + half * self.half, self.half)
        return pltpu.make_async_remote_copy(
            src_ref=self.stage.at[slot, rows], dst_ref=self.land.at[dst_slot, rows],
            send_sem=self.ssem.at[HIGH], recv_sem=self.rsem.at[4 + 2 * dst_slot + half],
            device_id={'tp': dev}, device_id_type=MESH)

    def wait_land(self, dst_slot, half):
        self.cp(0, half, dst_slot, self.ring.me).wait_recv()

    def wait_pair(self, xp):
        self.cp_pair(xp).wait_recv()

    def send_pair(self, xp):
        self.cp_pair(xp).start()

    def mix(self, slot, xp, half, with_far=False):
        blk = xp * 2 + self.ring.c
        step = 32

        def body(i):
            rows = pl.ds(pl.multiple_of(self.base + half * self.half + i * step, step), step)
            total = self.part[blk, rows, :].astype(F32) + self.pair[xp, rows, :].astype(F32)
            if with_far:
                total = total + self.land[0, rows, :].astype(F32)
            self.stage[slot, rows, :] = total.astype(BF)
        loop(0, self.half // step, body)

    def far(self):
        r = self.ring
        self.wait_pair(r.xf)
        self.mix(0, r.xf, 0)
        self.cp(0, 0, 0, r.right).start()
        self.mix(0, r.xf, 1)
        self.cp(0, 1, 0, r.left).start()

    def near_own(self):
        r = self.ring
        self.wait_pair(r.xr)
        self.mix(1, r.xr, 1)
        self.cp(1, 1, 1, r.right).start()
        self.wait_pair(r.xl)
        self.mix(2, r.xl, 0)
        self.cp(2, 0, 2, r.left).start()

    def near_sum(self):
        r = self.ring
        self.wait_land(0, 0)
        self.mix(1, r.xr, 0, with_far=True)
        self.cp(1, 0, 1, r.right).start()
        self.wait_land(0, 1)
        self.mix(2, r.xl, 1, with_far=True)
        self.cp(2, 1, 2, r.left).start()

    def wait_final(self):
        self.wait_pair(self.ring.x)
        for slot in (1, 2):
            for half in PAIR:
                self.wait_land(slot, half)

    def total(self, rows):
        r = self.ring
        return (self.part[r.me, rows, :].astype(F32) + self.pair[r.x, rows, :].astype(F32)
                + self.land[1, rows, :].astype(F32) + self.land[2, rows, :].astype(F32))

    def finish(self):
        r = self.ring
        rows = pl.ds(self.base, self.size)
        for ref, which in ((self.pair.at[:, rows], LOW), (self.stage.at[:, rows], HIGH)):
            pltpu.make_async_remote_copy(
                src_ref=ref, dst_ref=ref, send_sem=self.ssem.at[which], recv_sem=self.rsem.at[0],
                device_id={'tp': r.partner}, device_id_type=MESH).wait_send()


def scatter_buffers(n, rows, d):
    return [VMEM((n // 2, rows, d), BF), VMEM((3, rows, d), BF), VMEM((3, rows, d), BF)]


def scatter_sems():
    return [pltpu.SemaphoreType.DMA((2,)), pltpu.SemaphoreType.DMA((4 + 6,))]


def hooked(count, body, hooks):
    def step(i):
        for at, actions in hooks.items():
            @pl.when(i == at)
            def _():
                for act in actions:
                    act()
        body(i)
    loop(0, count, step)


def gather_sems():
    return [pltpu.SemaphoreType.DMA((2,)), pltpu.SemaphoreType.DMA((Gather.SLOTS,))]


def lane_mask(rows, h):
    lane = lax.broadcasted_iota(jnp.int32, (rows, 128), 1)
    return (lane < 64) if h == 0 else (lane >= 64)


def attend_block(i, q_ref, k_ref, vt_ref, o_ref, lse_ref, s_ref, m_ref, l_ref, acc_ref, bt_ref, slopes):
    t = q_ref.shape[2]
    e = acc_ref.shape[0] // 2
    key = lax.broadcasted_iota(jnp.int32, (t, t), 0)
    qry = lax.broadcasted_iota(jnp.int32, (t, t), 1)
    for h in PAIR:
        m_ref[h] = jnp.full((8, t), MASK_VALUE, F32)
        l_ref[h] = jnp.zeros((8, t), F32)
    zero_fill(acc_ref)

    def shift(h, j):
        return slopes[h] * (j * t).astype(F32)

    def score(blocks, diag):
        top = [m_ref[h] for h in PAIR]
        for j in blocks:
            for h in PAIR:
                s = mm(k_ref[j], q_ref[h, i], NT) + bt_ref[h]
                if diag:
                    s = jnp.where(key <= qry, s, MASK_VALUE)
                s_ref[h, j] = s
                top[h] = jnp.maximum(top[h], fold8(s, jnp.maximum) + shift(h, j))
        for h in PAIR:
            m_ref[h] = top[h]

    twos(i, lambda blocks: score(blocks, False))
    score((i,), True)
    top = [jnp.max(m_ref[h], axis=0, keepdims=True) for h in PAIR]

    def denom(j):
        for h in PAIR:
            l_ref[h] = l_ref[h] + fold8(jnp.exp(s_ref[h, j] + (shift(h, j) - top[h])), jnp.add)

    loop(0, i + 1, denom)
    for h in PAIR:
        lse_ref[h, i] = top[h] + jnp.log(col_sum(l_ref[h]))

    def values(blocks):
        for h in PAIR:
            rows = pl.ds(h * e, e)
            total = acc_ref[rows, :]
            for j in blocks:
                p = jnp.exp(s_ref[h, j] + (shift(h, j) - lse_ref[h, i])).astype(BF)
                total = total + mm(vt_ref[j, rows, :], p)
            acc_ref[rows, :] = total

    twos(i + 1, values)
    o_ref[i] = acc_ref[...].T.astype(BF)


def kernel_main(n, scale, n_vec, n_out, x_hbm, dy_hbm, wt_hbm, wo_hbm, wu_hbm, wd_hbm, *refs):
    vec_hbm, (slopes_ref,), refs = refs[:n_vec], refs[n_vec:n_vec + 1], refs[n_vec + 1:]
    results, (h_hbm,), refs = refs[:n_out], refs[n_out:n_out + 1], refs[n_out + 1:]
    vecs, refs = refs[:n_vec], refs[n_vec:]
    run_layer(n, scale, vec_hbm, vecs, results, x_hbm, dy_hbm, wt_hbm, wo_hbm, wu_hbm, wd_hbm, slopes_ref, h_hbm, *refs)


def run_layer(n, scale, vec_hbm, vecs, results, x_hbm, dy_hbm, wt_hbm, wo_hbm, wu_hbm, wd_hbm, slopes_ref, h_hbm,
                xg, xo, dyo, dy, hg, wt, wp, wof, wu, wd, q, k, v, kt, vt, o, lse, orow, s_ref, m_ref, l_ref, acc, bt,
                x1, act, dpre, mid, dom, dqt, dk, dv, d3, small, early, late, part,
                *rest):
    g1, b1, bqkv, bo, g2, b2, bu, bd = vecs
    y, gx, sums, gwt, gbq, gwo, gwu, gbu, gwd = results
    rest = list(rest)

    def take(count):
        head = rest[:count]
        del rest[:count]
        return head

    ring = Ring(n)
    me = ring.me
    t, d, f = xg.shape[1], xg.shape[2], wu.shape[1]
    rs_bufs, rm_bufs = take(3), take(3)
    st = t // 2
    streams = (0, st)
    r_sems = [take(2) for _ in PAIR]
    r0, r1 = [Scatter(ring, part, *rs_bufs, *sems, base=base, size=st) for base, sems in zip(streams, r_sems)]
    rs = Scatter(ring, part, *rs_bufs, *r_sems[0])
    rm = Scatter(ring, dy, *rm_bufs, *take(2))
    g_sems = [take(2) for _ in PAIR]
    ax, aw = [Gather(ring, buf, *sems) for buf, sems in zip((xg, wof), g_sems)]
    ay = Gather(ring, dy, *take(2))
    g0, g1s = [Gather(ring, hg, *sems, base=base, size=st) for base, sems in zip(streams, g_sems)]
    d0, d1 = [Gather(ring, xg, *sems, base=base, size=st) for base, sems in zip(streams, g_sems)]
    few, local, vec_sem = take(3)
    o_send, o_recv, e_send, e_recv, l_send, l_recv = [few.at[i] for i in range(6)]

    def fetch(i, src, dst):
        cp = pltpu.make_async_copy(src, dst, local.at[i])
        cp.start()
        return cp

    in_x, in_wo, in_dy, in_wt = (fetch(0, x_hbm, xg.at[me]), fetch(1, wo_hbm, wof.at[me]),
                                 fetch(2, dy_hbm, dy.at[me]), fetch(3, wt_hbm, wt))
    later = [fetch(4, wu_hbm, wu), fetch(5, wd_hbm, wd), fetch(6, x_hbm, xo), fetch(7, dy_hbm, dyo)]
    vec_in = [pltpu.make_async_copy(a, b, vec_sem.at[i]) for i, (a, b) in enumerate(zip(vec_hbm, vecs))]
    for cp in vec_in:
        cp.start()
    ring.barrier()
    in_x.wait()
    ax.start()
    for cp in vec_in:
        cp.wait()
    in_wt.wait()
    sort_weight(wp, wt)
    in_wo.wait()
    in_dy.wait()
    bias = jnp.concatenate([bqkv[kind, head:head + 1, :] for kind in TRIPLE for head in PAIR], axis=1)

    def project(blk):
        def norm(rows):
            hat, _ = norm_rows(xg[blk, rows, :].astype(F32))
            hg[blk, rows, :] = (hat * g1[...] + b1[...]).astype(BF)
        rows_loop(t, 64, norm)
        out = mm(hg[blk], wp[...], NT) + bias
        out = out.astype(BF)
        zero = jnp.zeros((t, 128), BF)
        qs = (out[:, :128].astype(F32) * scale).astype(BF)
        for head in PAIR:
            q[head, blk] = jnp.where(lane_mask(t, head), qs, zero)
        k[blk] = out[:, 128:256]
        v[blk] = out[:, 256:]
        kt[blk] = out[:, 128:256].T
        vt[blk] = out[:, 256:].T
        fetch(0, hg.at[blk], h_hbm.at[blk])

    arrive = functools.partial
    with scope('a_gather'):
        hooked(n, lambda step: project(ring.order(step)), {
            1: [arrive(ax.side, 0)],
            2: [ax.near1, ax.near2],
            4: [arrive(ax.side, 1)],
            5: [arrive(ax.side, 2)],
            6: [ax.drain, aw.start, ax.far, ay.start],
            7: [arrive(ax.side, 3)]})
    slopes = [slopes_ref[me * 2 + head] for head in PAIR]
    key = lax.broadcasted_iota(jnp.int32, (t, t), 0)
    qry = lax.broadcasted_iota(jnp.int32, (t, t), 1)
    for head in PAIR:
        bt[head] = slopes[head] * key.astype(F32)

    def send_o(i):
        cols = pl.ds(pl.multiple_of(me * 128, 128), 128)
        return pltpu.make_async_remote_copy(
            src_ref=o.at[i], dst_ref=orow.at[:, cols], send_sem=o_send, recv_sem=o_recv,
            device_id={'tp': i}, device_id_type=MESH)

    def one_block(step):
        i = ring.order(n - 1 - step)
        attend_block(i, q, k, vt, o, lse, s_ref, m_ref, l_ref, acc, bt, slopes)

        @pl.when(step < n - 1)
        def _():
            send_o(i).start()

    with scope('a_attend'):
        ax.finish()
        pltpu.make_async_copy(hg, h_hbm, local.at[0]).wait()
        hooked(n, one_block, {4: [aw.near1], 5: [aw.near2]})
    most = pl.ds(0, n - 1)
    with scope('a_wait'):
        aw.far()
        ay.near1()
        orow[:, pl.ds(pl.multiple_of(me * 128, 128), 128)] = o[me]
        wide = orow.at[:, pl.ds(0, (n - 1) * 128)]
        pltpu.make_async_remote_copy(
            src_ref=wide, dst_ref=wide, send_sem=o_send, recv_sem=o_recv,
            device_id={'tp': me}, device_id_type=MESH).wait_recv()
        for which in range(4):
            aw.side(which)
        aw.finish()
        later[2].wait()
    with scope('a_out'):
        x1[...] = mm(orow[...], wof[...].reshape(n * 128, d)).astype(BF).astype(F32)

        def enter(rows):
            row = xo[rows, :].astype(F32) + x1[rows, :] + bo[...]
            x1[rows, :] = row
            hat, _ = norm_rows(row)
            hg[me, rows, :] = (hat * g2[...] + b2[...]).astype(BF)
        rows_loop(st, 64, enter)
        g0.start()
        rows_loop(st, 64, enter, base=st)
    for cp in (later[0], later[1], later[3]):
        cp.wait()
    zero_fill(gbu)
    ay.side(0)

    def rest():
        ay.near2()
        ay.far()
        for which in range(1, 4):
            ay.side(which)

    def mlp(blk, stream):
        rows = pl.ds(pl.multiple_of(stream * st, st), st)
        pre = mm(hg[blk, rows, :], wu[...]) + bu[...]
        cot = mm(dy[blk, rows, :], wd[...], NT).astype(BF).astype(F32)
        sq = pre * pre
        th = jnp.tanh(GELU_C * (pre + 0.044715 * sq * pre))
        cdf = 0.5 * (1.0 + th)
        act[blk, rows, :] = (pre * cdf).astype(BF)
        slope = cdf + pre * (0.5 * (1.0 - th * th)) * (GELU_C * (1.0 + 3 * 0.044715 * sq))
        dp = cot * slope
        gbu[...] = gbu[...] + fold8(dp, jnp.add)
        dpb = dp.astype(BF)
        dpre[blk, rows, :] = dpb
        part[blk, rows, :] = mm(dpb, wu[...], NT).astype(BF)

    chips = (ring.xf, ring.xr, ring.xl, ring.x)
    def pairs(job):
        for xp in chips:
            job.send_pair(xp)

    def item(step):
        late = (step == 4) | (step == 5) | (step >= 10)
        pos = jnp.where(step < 4, step, jnp.where(step < 6, step - 4, jnp.where(step < 10, step - 2, step - 8)))
        mlp(ring.order(pos), jnp.where(late, 1, 0))

    with scope('b_gather'):
        hooked(2 * n, item, {
            1: [arrive(g0.side, 0)],
            2: [rest, g0.near1, g1s.start, g0.near2],
            5: [arrive(g1s.side, 0)],
            6: [arrive(g0.side, 1)],
            7: [arrive(g0.side, 2)],
            8: [g0.far],
            9: [arrive(g0.side, 3)],
            10: [arrive(pairs, r0), g1s.near1, r0.far, g1s.near2],
            12: [r0.near_own, arrive(g1s.side, 1)],
            13: [arrive(g1s.side, 2)],
            14: [g1s.far],
            15: [arrive(g1s.side, 3), r0.near_sum]})
    with scope('b_far'):
        pairs(r1)
        r1.far()
    with scope('b_own'):
        r1.near_own()
    ay.finish()

    def weight_down(i):
        cols = pl.ds(pl.multiple_of(i * 256, 256), 256)
        left = act[:, :, cols].reshape(n * t, 256)
        gwd[cols, :] = mm(left, dy[...].reshape(n * t, d), T0).astype(BF)

    def weight_up(i):
        cols = pl.ds(pl.multiple_of(i * 256, 256), 256)
        left = hg[:, :, cols].reshape(n * t, 256)
        gwu[cols, :] = mm(left, dpre[...].reshape(n * t, f), T0).astype(BF)

    with scope('b_weights'):
        loop(0, f // 256, weight_down)
        loop(0, d // 256, weight_up)
    zero_fill(small)

    def down(blk):
        dy[blk] = mm(act[blk], wd[...]).astype(BF)

    def leave(rows):
        dg = rs.total(rows).astype(BF).astype(F32)
        hat, rstd = norm_rows(x1[rows, :])
        small[2] = small[2] + fold8(dg * hat, jnp.add)
        small[3] = small[3] + fold8(dg, jnp.add)
        dz = norm_back(dg * g2[...], hat, rstd)
        dyf = dyo[rows, :].astype(F32)
        dm = dyf + dz
        small[4] = small[4] + fold8(dm, jnp.add)
        small[5] = small[5] + fold8(dyf, jnp.add)
        mid[rows, :] = dm
        xg[me, rows, :] = dm.astype(BF)

    with scope('b_sum'):
        r1.near_sum()
    with scope('b_final'):
        r0.wait_final()
    with scope('b_leave'):
        rows_loop(st, 64, leave)
        g0.finish()
        d0.start()
    with scope('b_down'):
        loop(0, n, down)
        pairs(rm)
    with scope('b_final1'):
        r1.wait_final()
    with scope('b_leave1'):
        rows_loop(st, 64, leave, base=st)
        g1s.finish()
        d1.start()
    with scope('b_finish'):
        for job in (r0, r1):
            job.finish()
    reload = fetch(0, h_hbm, hg)

    def share(buf, off, send_sem, recv_sem):
        return pltpu.make_async_remote_copy(
            src_ref=buf.at[me], dst_ref=buf.at[me], send_sem=send_sem, recv_sem=recv_sem,
            device_id={'tp': (me + off) % n}, device_id_type=MESH)

    def all_in(buf, send_sem, recv_sem):
        return pltpu.make_async_remote_copy(
            src_ref=buf.at[most], dst_ref=buf.at[most], send_sem=send_sem, recv_sem=recv_sem,
            device_id={'tp': me}, device_id_type=MESH)

    def early_out():
        for i in range(4):
            early[me, i:i + 1, :] = col_sum(small[2 + i])
        for off in range(1, n):
            share(early, off, e_send, e_recv).start()

    def add_up(buf):
        total = buf[0]
        for b in range(1, n):
            total = total + buf[b]
        return total
    zero_fill(dk, dv)

    def back_block(i):
        dc = mm(xg[i], wof[me], NT).astype(BF)
        zero = jnp.zeros((t, 128), BF)
        prod = (dc.astype(F32) * o[i].astype(F32)).T
        dlt = (col_sum(prod[:64]), col_sum(prod[64:]))
        for head in PAIR:
            dom[head] = jnp.where(lane_mask(t, head), dc, zero)
        zero_fill(dqt)

        def pair_block(blocks, diag):
            cases = [(j, head) for j in blocks for head in PAIR]
            ps, dss = [], []
            for j, head in cases:
                s = mm(k[j], q[head, i], NT) + bt[head]
                if diag:
                    s = jnp.where(key <= qry, s, MASK_VALUE)
                p = jnp.exp(s + (slopes[head] * (j * t).astype(F32) - lse[head, i]))
                dp = mm(v[j], dom[head], NT).astype(BF).astype(F32)
                dss.append((p * (dp - dlt[head])).astype(BF))
                ps.append(p.astype(BF))
            wide = list(zip(cases, ps, dss))
            for j in blocks:
                dv[j] = dv[j] + sum(mm(p, dom[head]) for (b, head), p, _ in wide if b is j)
                dk[j] = dk[j] + sum(mm(ds, q[head, i]) for (b, head), _, ds in wide if b is j)
            for head in PAIR:
                rows = pl.ds(head * 64, 64)
                dqt[rows, :] = dqt[rows, :] + sum(mm(kt[b, rows, :], ds) for (b, h), _, ds in wide if h == head)

        twos(i, lambda blocks: pair_block(blocks, False))
        pair_block((i,), True)
        d3[i, :, :128] = (dqt[...].T * scale).astype(BF)

    def both_in(which):
        for job in (d0, d1):
            job.side(which)

    with scope('c_attend'):
        hooked(n, lambda step: back_block(ring.order(step)), {
            1: [arrive(both_in, 0), d0.near1, d0.near2],
            2: [d1.near1, rm.far, rm.near_own, d1.near2],
            4: [arrive(both_in, 1)],
            5: [arrive(both_in, 2)],
            6: [d0.far, d1.far, rm.near_sum],
            7: [arrive(both_in, 3)]})
    zero_fill(gbq)

    def back_in(xp):
        for off in (1, 0):
            blk = xp * 2 + (ring.c + off) % 2
            d3[blk, :, 128:256] = dk[blk].astype(BF)
            d3[blk, :, 256:] = dv[blk].astype(BF)
            part[blk] = mm(d3[blk], wp[...]).astype(BF)
            if off:
                rs.send_pair(xp)

    with scope('c_far'):
        back_in(ring.xf)
        rs.far()
    with scope('c_own'):
        back_in(ring.xr)
        back_in(ring.xl)
        rs.near_own()
        back_in(ring.x)
    reload.wait()

    def weight_in(i):
        cols = pl.ds(pl.multiple_of(i * 128, 128), 128)
        left = d3[:, :, cols].reshape(n * t, 128)
        grad = mm(left, hg[...].reshape(n * t, d), T0).astype(BF)
        for head in PAIR:
            gwt[head, i] = grad[head * 64:head * 64 + 64]

    def bias_in(b):
        gbq[...] = gbq[...] + fold8(d3[b].astype(F32), jnp.add)

    with scope('c_weights'):
        loop(0, len(TRIPLE), weight_in)
        loop(0, n, bias_in)
    with scope('c_sum'):
        rs.near_sum()
    with scope('c_gwo'):
        gwo[...] = mm(o[...].reshape(n * t, 128), xg[...].reshape(n * t, d), T0).astype(BF)
    with scope('c_mfinal'):
        rm.wait_final()

    def finish_y(rows):
        m = rm.total(rows).astype(BF).astype(F32)
        y[rows, :] = (x1[rows, :] + m + bd[...]).astype(BF)
    rows_loop(t, 64, finish_y)
    with scope('c_final'):
        rs.wait_final()
        early_out()

    def sum_in(rows):
        dh = rs.total(rows).astype(BF).astype(F32)
        hat, _ = norm_rows(xo[rows, :].astype(F32))
        small[0] = small[0] + fold8(dh * hat, jnp.add)
        small[1] = small[1] + fold8(dh, jnp.add)

    def last(rows):
        dh = rs.total(rows).astype(BF).astype(F32)
        hat, rstd = norm_rows(xo[rows, :].astype(F32))
        gx[rows, :] = (mid[rows, :] + norm_back(dh * g1[...], hat, rstd)).astype(BF)

    with scope('c_sums'):
        rows_loop(t, 64, sum_in)
    for i in PAIR:
        late[me, i:i + 1, :] = col_sum(small[i])
    with scope('c_share'):
        for off in range(1, n):
            share(late, off, l_send, l_recv).start()
        rows_loop(t, 64, last)
        all_in(early, e_send, e_recv).wait_recv()
        sums[2:6, :] = add_up(early)
        all_in(late, l_send, l_recv).wait_recv()
        sums[0:2, :] = add_up(late)
        all_in(early, e_send, e_recv).wait_send()
        all_in(late, l_send, l_recv).wait_send()
        all_in(o, o_send, o_recv).wait_send()
    with scope('d_finish'):
        for job in (rs, rm, d0, d1):
            job.finish()


def kernel_out(n_big, *refs):
    count = n_big + 3
    srcs, refs = refs[:count], refs[count:]
    outs, refs = refs[:n_big + 8], refs[n_big + 8:]
    bufs, tail, sem_out = srcs, refs[:-1], refs[-1]
    gbq, gbu, sums = bufs[n_big:]
    o_bq, o_bu, o_sums = tail
    kept = list(bufs[:n_big]) + [o_bq, o_bu] + [o_sums.at[i:i + 1] for i in range(6)]
    backs = [pltpu.make_async_copy(b, a, sem_out.at[i]) for i, (a, b) in enumerate(zip(outs, kept))]
    for back in backs[:n_big]:
        back.start()
    o_bu[...] = col_sum(gbu[...])
    row = col_sum(gbq[...])
    e = o_bq.shape[2]
    for part_no in TRIPLE:
        for head in PAIR:
            at = (part_no * 2 + head) * e
            o_bq[part_no, head:head + 1, :] = row[:, at:at + e]
    o_sums[...] = sums[...]
    for back in backs[n_big:]:
        back.start()
    for back in backs:
        back.wait()


def inside():
    return pl.BlockSpec(memory_space=VMEM)


def anywhere():
    return pl.BlockSpec(memory_space=pl.ANY)


def smem():
    return pl.BlockSpec(memory_space=pltpu.SMEM)


def solution(mesh):
    n = mesh.shape['tp']

    def local_step(x, ln1_gamma, ln1_beta, w_qkv, b_qkv, w_out, b_out, ln2_gamma, ln2_beta, w_up, b_up, w_down, b_down, grad_y):
        t, d = x.shape[1], x.shape[2]
        heads, e = w_qkv.shape[1], w_qkv.shape[3]
        he = heads * e
        f = w_up.shape[1]
        scale = e ** -0.5
        slopes = jnp.asarray(alibi_slopes(heads * n))
        x2, dy2 = x[0], grad_y[0]
        row = lambda vec: vec.reshape(1, -1)
        wt = w_qkv.transpose(1, 2, 3, 0).reshape(heads * 3 * e, d)
        bq = b_qkv.transpose(1, 0, 2)
        sds = jax.ShapeDtypeStruct
        rows, full, half = (t, d), (n, t, d), (n, t, he)
        both, line = (len(PAIR),) + half, (len(PAIR), n, 1, t)
        packed = (len(TRIPLE) * he, d)
        params = lambda cid: pltpu.CompilerParams(collective_id=cid, has_side_effects=True, vmem_limit_bytes=VLIM)
        dma = pltpu.SemaphoreType.DMA

        vm = lambda dims, kind=BF: VMEM(dims, kind)
        stat, turned = (len(PAIR), 8, t), (n, he, t)
        vecs = (row(ln1_gamma), row(ln1_beta), bq, row(b_out), row(ln2_gamma), row(ln2_beta), row(b_up), row(b_down))
        results = [sds(rows, BF), sds(rows, BF), sds((8, d), F32), sds((heads, len(TRIPLE), e, d), BF),
                   sds((8, len(TRIPLE) * he), F32), sds((he, d), BF), sds((d, f), BF), sds((8, f), F32), sds((f, d), BF)]
        y, gx, sums, gwt, gbq, gwo, gwu, gbu, gwd, _ = pl.pallas_call(
            functools.partial(kernel_main, n, scale, len(vecs), len(results)),
            name='layer',
            out_shape=[vm(b.shape, b.dtype) for b in results] + [sds(full, BF)],
            in_specs=[anywhere()] * (6 + len(vecs)) + [smem()],
            out_specs=[inside()] * len(results) + [anywhere()],
            scratch_shapes=[vm(b.shape, b.dtype) for b in vecs] + [vm(full), vm(rows), vm(rows), vm(full), vm(full), vm(packed), vm(packed), vm((n, he, d)),
                            vm((d, f)), vm((f, d)), vm(both), vm(half), vm(half), vm(turned), vm(turned), vm(half),
                            vm(line, F32), vm(rows), vm((len(PAIR), n, t, t), F32), vm(stat, F32), vm(stat, F32),
                            vm((he, t), F32), vm((len(PAIR), t, t), F32), vm(rows, F32), vm((n, t, f)), vm((n, t, f)),
                            vm(rows, F32), vm((len(PAIR), t, he)), vm((he, t), F32), vm(half, F32), vm(half, F32),
                            vm((n, t, len(TRIPLE) * he)), vm((6, 8, d), F32), vm((n, 4, d), F32), vm((n, 2, d), F32), vm(full)]
            + scatter_buffers(n, t, d) * 2 + scatter_sems() * 3 + gather_sems() * 3 + [dma((n,))] * 2 + [dma((len(vecs),))],
            compiler_params=params(0),
        )(x2, dy2, wt, w_out, w_up, w_down, *vecs, slopes)

        big = (y, gx, gwt, gwo, gwu, gwd)
        little = (gbq, gbu, sums)
        bias_dims, up_dims = (len(TRIPLE), heads, e), (1, f)
        res = pl.pallas_call(
            functools.partial(kernel_out, len(big)),
            name='results',
            compiler_params=pltpu.CompilerParams(vmem_limit_bytes=8 * 1024 * 1024),
            out_shape=[sds(b.shape, b.dtype) for b in big] + [sds(bias_dims, F32), sds(up_dims, F32)] + [sds((1, d), F32)] * 6,
            in_specs=[inside()] * (len(big) + 3),
            out_specs=[anywhere()] * (len(big) + 8),
            scratch_shapes=[vm(bias_dims, F32), vm(up_dims, F32), vm((8, d), F32), dma((len(big) + 8,))],
        )(*big, *little)
        y, gx, gwt, gwo, gwu, gwd, gbq, gbu, s_g1, s_b1, s_g2, s_b2, s_bo, s_bd = res
        vec = lambda a: a.reshape(-1)
        return (y[None], gx[None], vec(s_g1), vec(s_b1), gwt.transpose(3, 0, 1, 2), gbq.transpose(1, 0, 2), gwo, vec(s_bo),
                vec(s_g2), vec(s_b2), gwu, vec(gbu), gwd, vec(s_bd))

    row_spec = P('dp', 'tp', None)
    in_specs = (row_spec, P(), P(), P(None, 'tp', None, None), P('tp', None, None), P('tp', None), P(), P(), P(),
                P(None, 'tp'), P('tp'), P('tp', None), P(), row_spec)
    out_specs = (row_spec, row_spec, P('dp'), P('dp'), P('dp', 'tp', None, None), P(('dp', 'tp'), None, None),
                 P(('dp', 'tp'), None), P('dp'), P('dp'), P('dp'), P('dp', 'tp'), P(('dp', 'tp')), P(('dp', 'tp'), None), P('dp'))
    return jax.shard_map(local_step, mesh=mesh, in_specs=in_specs, out_specs=out_specs, check_vma=False)
```
